32 devices in a mesh: dp: 8 (over y, x, core), mp: 4 (over z).
Axes of the slice: x: 2, y: 2, z: 4, core: 2. Of those that a mesh axis runs over, the one named last changes fastest.
Arguments:
- layer_input: float32 [12288, 1024], P(('dp', 'mp')), may hold values from -6 to 6
- norm_gains: bfloat16 [2, 1024], replicated, may hold values from 0.5 to 1.5
- query_weight: bfloat16 [1024, 1024], P(None, 'mp'), may hold values from -0.03125 to 0.03125
- key_value_weight: bfloat16 [1024, 2, 1024], P(None, None, 'mp'), may hold values from -0.1875 to 0.1875
- output_weight: bfloat16 [1024, 1024], P('mp'), may hold values from -1 to 1
- gate_up_weight: bfloat16 [1024, 2, 2816], P(None, None, 'mp'), may hold values from -0.1875 to 0.1875
- down_weight: bfloat16 [2816, 1024], P('mp'), may hold values from -0.15625 to 0.15625
- bias_tables: bfloat16 [3, 32, 16], P(None, None, 'mp'), may hold values from -3 to 3
- doc_lengths: int32 [16], P('dp'), may hold values from 522 to 768, as said below
- box_bins: int32 [2, 12288], P(None, 'dp'), may hold values from 0 to 63
- cotangent: float32 [12288, 1024], P(('dp', 'mp')), may hold values from -6 to 6
Outputs:
- layer_output: float32 [12288, 1024], P(('dp', 'mp'))
- input_grad: float32 [12288, 1024], P(('dp', 'mp'))
- gain_grad: float32 [2, 1024], P(None, ('dp', 'mp'))
- query_grad: float32 [1024, 1024], P('dp', 'mp')
- key_value_grad: float32 [1024, 2, 1024], P('dp', None, 'mp')
- output_grad: float32 [1024, 1024], P('mp', 'dp')
- gate_up_grad: float32 [1024, 2, 2816], P('dp', None, 'mp')
- down_grad: float32 [2816, 1024], P('mp', 'dp')
- table_grad: float32 [3, 32, 16], P(None, 'dp', 'mp')
The draws below stay inside these ranges and needn't reach their ends.
Inputs may be any that keep to these rules, and one draw needn't show every extreme that they name: `doc_lengths`: each aligned block of 8 slots holds exactly one table slot of 768 tokens; the others are forms of 522 to 706 tokens; positions at or beyond a slot's length are padding.
All inputs are finite; a program needn't handle non-finite values.
Results may differ from the reference program's by a relative error of at most 0.02.
Values may be sent and summed in bfloat16 or wider, within the bound.
A program may use at most 256 MiB of HBM per device.

```python
import jax
import jax.numpy as jnp
from jax import lax

D = 1024
HEADS = 16
HEAD_DIM = 64
FF = 2816
NBUCK = 32
NBIN = 64
SLOT_LEN = 768
INNER = 1024
SLOTS = 16
TOKENS = 12288


def draw_doc_lengths(key, part):
    pick_key, form_key = jax.random.split(key)
    block_count = SLOTS // 8
    table_place = jax.random.randint(pick_key, (block_count,), 0, 8)
    slot_index = jnp.arange(SLOTS, dtype=jnp.int32)
    is_table = slot_index % 8 == jnp.repeat(table_place, 8)
    form_lengths = jax.random.randint(form_key, (SLOTS,), SLOT_LEN * 17 // 25, SLOT_LEN * 23 // 25 + 1)
    return jnp.where(is_table, SLOT_LEN, form_lengths).astype(jnp.int32)


def with_ends(array, own_key, low, top_value):
    longest = array.shape.index(max(array.shape))
    spots = []
    for shift in (0, 1):
        where = [jax.random.randint(jax.random.fold_in(own_key, axis), (), 0, length) for axis, length in enumerate(array.shape)]
        where[longest] = (where[longest] + shift) % array.shape[longest]
        spots.append(tuple(where))
    return array.at[spots[0]].set(low).at[spots[1]].set(top_value)


def level_of(own_key, dims, cuts, least, high):
    def one(dim, blocks):
        steps = jax.random.uniform(jax.random.fold_in(jax.random.fold_in(own_key, 6), dim), (blocks,), jnp.float32, least / len(cuts), high / len(cuts))
        return jnp.repeat(jnp.exp(steps), dims[dim] // blocks).reshape((-1,) + (1,) * (len(dims) - dim - 1))

    factor_of = one(*cuts[0])
    for cut in cuts[1:]:
        factor_of = factor_of * one(*cut)
    return factor_of


def centred(rng, shape, width, most, pieces=(), held_as=jnp.bfloat16):
    entries = width * jax.random.normal(rng, shape, jnp.float32)
    if pieces:
        entries = entries * level_of(rng, shape, pieces, -0.22, 0.18)
    return jnp.clip(entries, -most, most).astype(held_as)


def setup_inputs(seed: int = 0) -> dict:
    arg_keys = jax.random.split(jax.random.key(seed), 12)
    layer_input = centred(arg_keys[0], (TOKENS, D), 1.0, 6.0, ((0, 32),), jnp.float32)
    norm_gains = jnp.clip(1.0 + 0.1 * jax.random.normal(arg_keys[1], (2, D), jnp.float32), 0.5, 1.5).astype(jnp.bfloat16)
    query_weight = centred(arg_keys[2], (D, INNER), (D * 28) ** -0.5, 0.03125, ((1, 4),))
    key_value_weight = centred(arg_keys[3], (D, 2, INNER), D ** -0.5, 0.1875, ((2, 4),))
    output_weight = centred(arg_keys[4], (INNER, D), (INNER // 32) ** -0.5, 1.0, ((0, 4),))
    gate_up_weight = centred(arg_keys[5], (D, 2, FF), D ** -0.5, 0.1875, ((2, 4),))
    down_weight = centred(arg_keys[6], (FF, D), (FF // 2) ** -0.5, 0.15625, ((0, 4),))
    bias_tables = centred(arg_keys[7], (3, NBUCK, HEADS), 0.5, 3.0, ((2, 4),))
    doc_lengths = draw_doc_lengths(jax.random.fold_in(arg_keys[11], 71), 0)
    box_bins = with_ends(jax.random.randint(arg_keys[9], (2, TOKENS), 0, NBIN), jax.random.fold_in(arg_keys[9], 1), 0, NBIN - 1).astype(jnp.int32)
    cotangent = centred(arg_keys[10], (TOKENS, D), 1.0, 6.0, ((0, 32),), jnp.float32)
    return {"layer_input": layer_input, "norm_gains": norm_gains, "query_weight": query_weight, "key_value_weight": key_value_weight, "output_weight": output_weight, "gate_up_weight": gate_up_weight, "down_weight": down_weight, "bias_tables": bias_tables, "doc_lengths": doc_lengths, "box_bins": box_bins, "cotangent": cotangent}


@jax.custom_vjp
def low(v):
    return lax.optimization_barrier(v.astype(jnp.bfloat16)).astype(jnp.float32)

@jax.custom_vjp
def low_back(v):
    return v

def low_keep(v):
    return (low(v), None)

def low_pass(kept, grad):
    return (grad,)

def back_keep(v):
    return (v, None)

def back_low(kept, grad):
    return (low(grad),)
low.defvjp(low_keep, low_pass)
low_back.defvjp(back_keep, back_low)
EPSILON = 1e-06
THRESHOLDS = (8, 12, 16, 23, 32, 46, 64, 91)
NEG_FILL = -1e+30

def bucket_of(relative):
    distance = jnp.abs(relative)
    bucket = jnp.minimum(distance, 7)
    for threshold in THRESHOLDS:
        bucket = bucket + (distance >= threshold).astype(jnp.int32)
    return bucket + 16 * (relative > 0).astype(jnp.int32)

def rms_scale(values, gain_vector):
    return values * lax.rsqrt(lax.optimization_barrier(jnp.mean(values * values, axis=-1, keepdims=True)) + EPSILON) * gain_vector

def forward(layer_input, norm_gains, query_weight, key_value_weight, output_weight, gate_up_weight, down_weight, bias_tables, doc_lengths, box_bins):
    highest = lax.Precision.HIGHEST
    positions = jnp.arange(SLOT_LEN, dtype=jnp.int32)
    line_buckets = bucket_of(positions[None, :] - positions[:, None])
    line_bias = jnp.transpose(jnp.take(bias_tables[0], line_buckets, axis=0), (2, 0, 1))
    normed = low(rms_scale(layer_input, norm_gains[0]))
    queries = low_back(low(jnp.dot(normed, query_weight, precision=highest)))
    key_values = low_back(low(jnp.einsum('td,dkc->tkc', normed, key_value_weight, precision=highest)))
    head_shape = (SLOTS, SLOT_LEN, HEADS, HEAD_DIM)
    query_slots = queries.reshape(head_shape)
    key_slots = key_values[:, 0].reshape(head_shape)
    value_slots = key_values[:, 1].reshape(head_shape)
    box_slots = jnp.transpose(box_bins.reshape(2, SLOTS, SLOT_LEN), (1, 0, 2))

    def attend(slot_items):
        query_part, key_part, value_part, box_part, length_part = slot_items
        layout_x = jnp.take(bias_tables[1], bucket_of(box_part[0][None, :] - box_part[0][:, None]), axis=0)
        layout_y = jnp.take(bias_tables[2], bucket_of(box_part[1][None, :] - box_part[1][:, None]), axis=0)
        layout_bias = jnp.transpose(layout_x + layout_y, (2, 0, 1))
        scores = jnp.einsum('ihd,jhd->hij', query_part, key_part, precision=highest) + line_bias + layout_bias
        scores = low_back(scores)
        key_valid = positions < length_part
        scores = jnp.where(key_valid[None, None, :], scores, NEG_FILL)
        attn_probs = jax.nn.softmax(scores, axis=-1)
        mixed_heads = jnp.einsum('hij,jhd->ihd', low(attn_probs), value_part, precision=highest)
        return mixed_heads.reshape(SLOT_LEN, HEADS * HEAD_DIM)
    attended = lax.map(jax.checkpoint(attend), (query_slots, key_slots, value_slots, box_slots, doc_lengths))
    heads_out = low_back(low(attended.reshape(TOKENS, HEADS * HEAD_DIM)))
    branch = low_back(jnp.dot(heads_out, output_weight, precision=highest))
    residual = layer_input + branch
    normed_second = low(rms_scale(residual, norm_gains[1]))
    gate_up = low_back(jnp.einsum('td,dkf->tkf', normed_second, gate_up_weight, precision=highest))
    activated = low(jax.nn.gelu(gate_up[:, 0], approximate=True) * gate_up[:, 1])
    return residual + low_back(jnp.dot(activated, down_weight, precision=highest))

def reference(layer_input, norm_gains, query_weight, key_value_weight, output_weight, gate_up_weight, down_weight, bias_tables, doc_lengths, box_bins, cotangent):

    def closed(input_value, gains_value, query_value, key_value_value, output_value, gate_up_value, down_value, tables_value):
        return forward(input_value, gains_value, query_value, key_value_value, output_value, gate_up_value, down_value, tables_value, doc_lengths, box_bins)
    layer_output, pullback = jax.vjp(closed, layer_input.astype(jnp.float32), norm_gains.astype(jnp.float32), query_weight.astype(jnp.float32), key_value_weight.astype(jnp.float32), output_weight.astype(jnp.float32), gate_up_weight.astype(jnp.float32), down_weight.astype(jnp.float32), bias_tables.astype(jnp.float32))
    gradients = pullback(cotangent.astype(jnp.float32))
    return (layer_output, gradients[0], gradients[1], gradients[2], gradients[3], gradients[4], gradients[5], gradients[6], gradients[7])
```

```python
from functools import partial

import jax
import jax.numpy as jnp
import numpy as np
from jax import lax
from jax.experimental import pallas as pl
from jax.experimental.pallas import tpu as pltpu
from jax.sharding import PartitionSpec as P

NBIN = 64
EPSILON = 1e-06
THRESHOLDS = (8, 12, 16, 23, 32, 46, 64, 91)
NEG_FILL = -1e30
LANES = 128
MESH = pl.DeviceIdType.MESH
HBM = pltpu.MemorySpace.HBM
BF16 = jnp.bfloat16
F32 = jnp.float32


def bucket_of(relative):
    distance = jnp.abs(relative)
    bucket = jnp.minimum(distance, 7)
    for threshold in THRESHOLDS:
        bucket = bucket + (distance >= threshold).astype(jnp.int32)
    return bucket + 16 * (relative > 0).astype(jnp.int32)


def inverse_rms(values):
    return lax.rsqrt(jnp.mean(values * values, axis=-1, keepdims=True) + EPSILON)


def dot_f32(left, right, left_dim, right_dim):
    return lax.dot_general(
        left, right, (((left_dim,), (right_dim,)), ((), ())), preferred_element_type=F32
    )


def three_parts(values):
    high = values.astype(BF16)
    rest = values - high.astype(F32)
    middle = rest.astype(BF16)
    low = (rest - middle.astype(F32)).astype(BF16)
    return high, middle, low


def lane_ids(shape):
    return lax.broadcasted_iota(jnp.int32, shape, 1)


def row_ids(shape):
    return lax.broadcasted_iota(jnp.int32, shape, 0)


def attend_kernel(
    q_ref, k_ref, v_ref, layout_ref, line_ref, key_extra_ref, query_bins_ref,
    out_ref, lse_ref,
    key_aug, query_aug, strip, scores, probs,
):
    head_size, rows = q_ref.shape
    keys = k_ref.shape[1]
    blocks = keys // LANES
    width = strip.shape[1]

    @pl.when(pl.program_id(0) == 0)
    def _():
        key_aug[...] = key_extra_ref[...]
        tail = row_ids((64, rows))
        query_aug[pl.ds(192, 64), :] = jnp.where(tail == 0, 1.0, 0.0).astype(BF16)

    both = jnp.concatenate([k_ref[...], v_ref[...]], axis=0).T
    low_lanes = lane_ids((keys, LANES)) < head_size
    key_aug[:, 0:LANES] = jnp.where(low_lanes, both, key_extra_ref[:, 0:LANES])
    query_aug[pl.ds(0, 64), :] = q_ref[...]
    query_aug[pl.ds(64, 128), :] = jnp.dot(
        layout_ref[0], query_bins_ref[...], preferred_element_type=F32
    ).astype(BF16)
    strip[...] = pltpu.roll(
        jnp.broadcast_to(line_ref[0], (LANES, width)), 0, 1, stride=1, stride_axis=0
    )
    query_all = query_aug[...]
    top = jnp.full((1, rows), -jnp.inf, F32)
    for block in range(blocks):
        here = pl.ds(block * LANES, LANES)
        part = jnp.dot(key_aug[here, :], query_all, preferred_element_type=F32)
        part = part + strip[:, pl.ds((blocks - 1 - block) * LANES, rows)]
        scores[here, :] = part
        top = jnp.maximum(top, jnp.max(part, axis=0, keepdims=True))
    total = jnp.zeros((1, rows), F32)
    for block in range(blocks):
        here = pl.ds(block * LANES, LANES)
        part = jnp.exp(scores[here, :] - top)
        total = total + jnp.sum(part, axis=0, keepdims=True)
        probs[here, :] = part.astype(BF16)
    mixed = jnp.dot(v_ref[...], probs[...], preferred_element_type=F32)
    out_ref[...] = (mixed / total).astype(BF16)
    lse_ref[0] = top + jnp.log(total)


def attend_back_kernel(
    q_ref, k_ref, v_ref, out_ref, out_grad_ref, lse_ref, layout_ref, line_ref,
    key_extra_ref, key_extra_t_ref, query_bins_ref, query_bins_t_ref,
    dq_ref, dk_ref, dv_ref, line_grad_ref, layout_grad_ref,
    key_aug, key_aug_t, query_aug, value_aug, grad_aug, strip, strip_grad, probs_grad,
):
    head_size, rows = q_ref.shape
    keys = k_ref.shape[1]
    blocks = keys // LANES
    width = strip.shape[1]

    @pl.when(pl.program_id(0) == 0)
    def _():
        key_aug[...] = key_extra_ref[...]
        key_aug_t[pl.ds(64, 128), :] = key_extra_t_ref[...]
        tail = row_ids((64, rows))
        query_aug[pl.ds(192, 64), :] = jnp.where(tail == 0, 1.0, 0.0).astype(BF16)

    both = jnp.concatenate([k_ref[...], v_ref[...]], axis=0).T
    lanes = lane_ids((keys, LANES))
    key_aug[:, 0:LANES] = jnp.where(lanes < head_size, both, key_extra_ref[:, 0:LANES])
    ones = jnp.where(lanes < 3, 1.0, 0.0).astype(BF16)
    value_aug[...] = jnp.where(lanes < head_size, ones, both)
    key_aug_t[pl.ds(0, 64), :] = k_ref[...]
    query_aug[pl.ds(0, 64), :] = q_ref[...]
    query_aug[pl.ds(64, 128), :] = jnp.dot(
        layout_ref[0], query_bins_ref[...], preferred_element_type=F32
    ).astype(BF16)
    high, middle, low = three_parts(-lse_ref[0])
    tail = row_ids((64, rows))
    rows_of = lambda part: jnp.broadcast_to(part.astype(F32), (64, rows))
    query_aug[pl.ds(192, 64), :] = jnp.where(
        tail == 0, 1.0,
        jnp.where(
            tail == 1, rows_of(high),
            jnp.where(tail == 2, rows_of(middle), jnp.where(tail == 3, rows_of(low), 0.0)),
        ),
    ).astype(BF16)
    row_dot = jnp.sum(
        out_grad_ref[...].astype(F32) * out_ref[...].astype(F32), axis=0, keepdims=True
    )
    high, middle, low = three_parts(-row_dot)
    grad_aug[pl.ds(0, 64), :] = jnp.where(
        tail == 0, rows_of(high),
        jnp.where(tail == 1, rows_of(middle), jnp.where(tail == 2, rows_of(low), 0.0)),
    ).astype(BF16)
    grad_aug[pl.ds(64, 64), :] = out_grad_ref[...]
    strip[...] = pltpu.roll(
        jnp.broadcast_to(line_ref[0], (LANES, width)), 0, 1, stride=1, stride_axis=0
    )
    strip_grad[...] = jnp.zeros_like(strip_grad)
    query_and_grad = jnp.concatenate([q_ref[...], out_grad_ref[...]], axis=0).T
    query_all = query_aug[...]
    grad_all = grad_aug[...]
    half = lane_ids((LANES, LANES)) < head_size
    for block in range(blocks):
        here = pl.ds(block * LANES, LANES)
        band = pl.ds((blocks - 1 - block) * LANES, rows)
        part = jnp.dot(key_aug[here, :], query_all, preferred_element_type=F32)
        part = jnp.exp(part + strip[:, band])
        slope = part * jnp.dot(value_aug[here, :], grad_all, preferred_element_type=F32)
        strip_grad[:, band] = strip_grad[:, band] + slope
        slope = slope.astype(BF16)
        probs_grad[here, :] = slope
        key_part = jnp.dot(slope, query_and_grad, preferred_element_type=F32)
        value_part = jnp.dot(part.astype(BF16), query_and_grad, preferred_element_type=F32)
        turned = jnp.where(half, key_part, value_part).T.astype(BF16)
        dk_ref[:, here] = turned[0:64]
        dv_ref[:, here] = turned[64:128]
    query_part = jnp.dot(key_aug_t[...], probs_grad[...], preferred_element_type=F32)
    dq_ref[...] = query_part[0:64].astype(BF16)
    layout_grad_ref[0] = jnp.dot(
        query_part[64:192].astype(BF16), query_bins_t_ref[...], preferred_element_type=F32
    )
    folded = strip_grad[pl.ds(0, 8), :]
    for group in range(1, LANES // 8):
        folded = folded + pltpu.roll(strip_grad[pl.ds(group * 8, 8), :], width - group * 8, 1)
    line = folded[0:1]
    for row in range(1, 8):
        line = line + pltpu.roll(folded[row : row + 1], width - row, 1)
    line_grad_ref[0] = line


class Place:
    def __init__(self, mp_size):
        self.dp = lax.axis_index("dp")
        self.mp = lax.axis_index("mp")
        self.mp_size = mp_size
        self.core = lax.rem(self.dp, 2)
        self.x = lax.rem(lax.div(self.dp, 2), 2)
        self.y = lax.div(self.dp, 4)
        self.to_core = (self.dp + 1 - 2 * self.core, self.mp)
        self.to_x = (self.dp + 2 - 4 * self.x, self.mp)
        self.to_y = (self.dp + 4 - 8 * self.y, self.mp)

    def to_mp(self, step):
        return (self.dp, lax.rem(self.mp + step, self.mp_size))

    def from_mp(self, step):
        return lax.rem(self.mp + self.mp_size - step, self.mp_size)

    def partners(self):
        others = [self.to_mp(step) for step in range(1, self.mp_size)]
        return [self.to_core, self.to_x, self.to_y] + others


def meet(place):
    barrier = pltpu.get_barrier_semaphore()
    partners = place.partners()
    for partner in partners:
        pl.semaphore_signal(barrier, inc=1, device_id=partner, device_id_type=MESH)
    pl.semaphore_wait(barrier, len(partners))


class Copy:
    def __init__(self, source, target, send, receive=None, partner=None):
        self.parts = (source, target, send, receive, partner)

    def made(self):
        source, target, send, receive, partner = self.parts
        if partner is None:
            return pltpu.make_async_copy(source, target, send)
        return pltpu.make_async_remote_copy(
            src_ref=source, dst_ref=target, send_sem=send, recv_sem=receive,
            device_id=partner, device_id_type=MESH,
        )

    def start(self):
        self.made().start()

    def wait(self):
        self.made().wait()

    def wait_send(self):
        self.made().wait_send()

    def wait_recv(self):
        self.made().wait_recv()


def remote(source, target, send, receive, partner):
    return Copy(source, target, send, receive, partner)


def lanes_at(block, count):
    return pl.ds(pl.multiple_of(block * LANES, LANES), count * LANES)


class Gather:
    LAGS = 4

    def __init__(self, place, pieces, outs, sems):
        self.place, self.pieces, self.outs = place, pieces, outs
        self.z_send, self.z_recv, self.own_sem, self.send, self.recv = sems
        self.items = [(c, k) for c in range(len(pieces)) for k in range(place.mp_size)]
        self.steps = len(self.items) + self.LAGS

    @staticmethod
    def semaphores(count, mp_size):
        dma = pltpu.SemaphoreType.DMA
        items = count * mp_size
        return [
            dma((count, mp_size)), dma((count, mp_size)), dma((count,)), dma((items, 6)), dma((items, 6))
        ]

    def rows(self, c, source, half):
        n = self.pieces[c].shape[1]
        if half is None:
            return pl.ds(pl.multiple_of(source * n, 16), n)
        return pl.ds(pl.multiple_of(source * n + half * (n // 2), 16), n // 2)

    def window(self, c, source, half, block, count):
        return self.outs[c].at[:, self.rows(c, source, half), lanes_at(block, count)]

    def own(self, c):
        place = self.place
        block = place.core * 4 + place.y * 2 + place.x
        return Copy(
            self.pieces[c], self.window(c, place.mp, None, block, 1), self.own_sem.at[c]
        )

    def along_mp(self, c, step):
        place = self.place
        block = place.core * 4 + place.y * 2 + place.x
        return remote(
            self.pieces[c], self.window(c, place.mp, None, block, 1),
            self.z_send.at[c, step], self.z_recv.at[c, step], place.to_mp(step),
        )

    def start_chunk(self, c):
        self.own(c).start()
        for step in range(1, self.place.mp_size):
            self.along_mp(c, step).start()

    def copies(self, t):
        c, k = self.items[t]
        place = self.place
        source = place.from_mp(k)
        base = place.core * 4
        mine = base + place.y * 2 + place.x
        turned = base + (1 - place.y) * 2 + place.x

        def copy(i, half, block, count, partner):
            here = self.window(c, source, half, block, count)
            return remote(here, here, self.send.at[t, i], self.recv.at[t, i], partner)

        first = [copy(0, 0, mine, 1, place.to_x), copy(1, 1, mine, 1, place.to_y)]
        second = [
            copy(2, 0, base + place.y * 2, 2, place.to_y),
            copy(3, 1, mine, 1, place.to_x),
            copy(4, 1, turned, 1, place.to_x),
        ]
        third = [copy(5, None, base, 4, place.to_core)]
        return first, second, third

    def step(self, s):
        count = len(self.items)
        if s == 0:
            self.start_chunk(0)
            if len(self.pieces) > 1:
                self.start_chunk(1)
        if s < count:
            c, k = self.items[s]
            if k == 0:
                self.own(c).wait()
                if s > 0 and c + 1 < len(self.pieces):
                    self.start_chunk(c + 1)
            else:
                self.along_mp(c, k).wait_recv()
            for copy in self.copies(s)[0]:
                copy.start()
        if 0 <= s - 1 < count:
            first, second, _ = self.copies(s - 1)
            for copy in first:
                copy.wait_recv()
            for copy in second:
                copy.start()
        if 0 <= s - 2 < count:
            _, second, third = self.copies(s - 2)
            for copy in second:
                copy.wait_recv()
            third[0].start()
        if 0 <= s - 4 < count:
            first, second, third = self.copies(s - 4)
            third[0].wait_recv()
            for copy in first + second + third:
                copy.wait_send()
            c, k = self.items[s - 4]
            if k > 0:
                self.along_mp(c, k).wait_send()


def add_rows(target, target_index, source, source_index):
    lead, rows, lanes = target_index
    source_rows, source_lanes = source_index
    row_start, count = rows
    source_start = source_rows
    size = 32
    while count % size:
        size //= 2

    def body(i, carry):
        here = pl.ds(pl.multiple_of(row_start + i * size, size), size)
        there = pl.ds(pl.multiple_of(source_start + i * size, size), size)
        for part in range(lead):
            target[part, here, lanes] = target[part, here, lanes] + source[part, there, source_lanes]
        return carry

    lax.fori_loop(0, count // size, body, 0)


class Scatter:
    LAGS = 4

    def __init__(self, place, fulls, outs, buffers, sems):
        self.place, self.fulls, self.outs = place, fulls, outs
        self.sums, self.from_core, self.from_first, self.from_second, self.from_mp = buffers
        self.own_sem, self.send, self.recv = sems
        self.items = [
            (c, k) for c in range(len(fulls)) for k in list(range(1, place.mp_size)) + [0]
        ]
        self.steps = len(self.items) + self.LAGS + 1

    @staticmethod
    def semaphores(count, mp_size):
        dma = pltpu.SemaphoreType.DMA
        items = count * mp_size
        return [dma((items,)), dma((items, 7)), dma((items, 7))]

    @staticmethod
    def buffers(shapes, mp_size):
        out = []
        for blocks in (4, 4, 2, 1, 1):
            for lead, n in shapes:
                out.append(pltpu.VMEM((mp_size, lead, n, blocks * LANES), BF16))
        return out

    @staticmethod
    def group(refs, count):
        return [refs[i * count : (i + 1) * count] for i in range(5)]

    def size(self, c):
        return self.fulls[c].shape[0], self.fulls[c].shape[1] // self.place.mp_size

    def copies(self, t):
        c, k = self.items[t]
        place = self.place
        lead, n = self.size(c)
        target = lax.rem(place.mp + k, place.mp_size)
        rows = pl.ds(pl.multiple_of(target * n, 16), n)
        top, bottom = pl.ds(0, n // 2), pl.ds(n // 2, n // 2)
        every = pl.ds(0, lead)
        sums = self.sums[c].at[k]
        full = self.fulls[c]

        def copy(i, source, landing, partner):
            return remote(source, landing, self.send.at[t, i], self.recv.at[t, i], partner)

        own = Copy(
            full.at[:, rows, lanes_at(place.core * 4, 4)], sums, self.own_sem.at[t]
        )
        core = copy(
            0, full.at[:, rows, lanes_at((1 - place.core) * 4, 4)], self.from_core[c].at[k], place.to_core
        )
        landing = self.from_first[c].at[k]
        first = [
            copy(
                1, sums.at[every, top, lanes_at((1 - place.y) * 2, 2)],
                landing.at[every, top, pl.ds(0, 256)], place.to_y,
            ),
            copy(
                2, sums.at[every, bottom, lanes_at(1 - place.x, 1)],
                landing.at[every, bottom, pl.ds(0, 128)], place.to_x,
            ),
            copy(
                3, sums.at[every, bottom, lanes_at(3 - place.x, 1)],
                landing.at[every, bottom, pl.ds(128, 128)], place.to_x,
            ),
        ]
        landing = self.from_second[c].at[k]
        second = [
            copy(
                4, sums.at[every, top, lanes_at(place.y * 2 + 1 - place.x, 1)],
                landing.at[every, top, pl.ds(0, 128)], place.to_x,
            ),
            copy(
                5, sums.at[every, bottom, lanes_at((1 - place.y) * 2 + place.x, 1)],
                landing.at[every, bottom, pl.ds(0, 128)], place.to_y,
            ),
        ]
        third = None
        if k > 0:
            third = copy(
                6, sums.at[:, :, lanes_at(place.y * 2 + place.x, 1)], self.from_mp[c].at[k],
                place.to_mp(k),
            )
        return own, core, first, second, third

    def step(self, s):
        count = len(self.items)
        place = self.place
        if s < count:
            own, core, *_ = self.copies(s)
            core.start()
            own.start()
        if 0 <= s - 1 < count:
            t = s - 1
            c, k = self.items[t]
            lead, n = self.size(c)
            own, core, first, *_ = self.copies(t)
            own.wait()
            core.wait_recv()
            add_rows(
                self.sums[c].at[k], (lead, (0, n), pl.ds(0, 512)), self.from_core[c].at[k], (0, pl.ds(0, 512))
            )
            for copy in first:
                copy.start()
        if 0 <= s - 2 < count:
            t = s - 2
            c, k = self.items[t]
            lead, n = self.size(c)
            _, _, first, second, _ = self.copies(t)
            for copy in first:
                copy.wait_recv()
            sums, landing = self.sums[c].at[k], self.from_first[c].at[k]
            half = n // 2
            add_rows(sums, (lead, (0, half), lanes_at(place.y * 2, 2)), landing, (0, pl.ds(0, 256)))
            add_rows(sums, (lead, (half, half), lanes_at(place.x, 1)), landing, (half, pl.ds(0, 128)))
            add_rows(
                sums, (lead, (half, half), lanes_at(2 + place.x, 1)), landing, (half, pl.ds(128, 128))
            )
            for copy in second:
                copy.start()
        if 0 <= s - 3 < count:
            t = s - 3
            c, k = self.items[t]
            lead, n = self.size(c)
            _, _, _, second, third = self.copies(t)
            for copy in second:
                copy.wait_recv()
            sums, landing = self.sums[c].at[k], self.from_second[c].at[k]
            mine = lanes_at(place.y * 2 + place.x, 1)
            add_rows(sums, (lead, (0, n), mine), landing, (0, pl.ds(0, 128)))
            if third is not None:
                third.start()
        if 0 <= s - 5 < count:
            t = s - 5
            c, k = self.items[t]
            _, core, first, second, third = self.copies(t)
            for copy in [core] + first + second:
                copy.wait_send()
            if third is not None:
                third.wait_send()
                third.wait_recv()
            else:
                self.finish(c)

    def finish(self, c):
        place = self.place
        lead, n = self.size(c)
        mine = lanes_at(place.y * 2 + place.x, 1)
        sums, landing, out = self.sums[c], self.from_mp[c], self.outs[c]
        size = 32
        while n % size:
            size //= 2

        def body(i, carry):
            here = pl.ds(pl.multiple_of(i * size, size), size)
            for part in range(lead):
                total = sums[0, part, here, mine].astype(F32)
                for k in range(1, place.mp_size):
                    total = total + landing[k, part, here, :].astype(F32)
                out[part, here, :] = total
            return carry

        lax.fori_loop(0, n // size, body, 0)


def attention_shapes(head_count, head_size, rows, keys, width):
    whole = lambda shape: pl.BlockSpec(shape, lambda head: (0,) * len(shape))
    column = lambda size: pl.BlockSpec((head_size, size), lambda head: (head, 0))
    page = lambda a, b: pl.BlockSpec((1, a, b), lambda head: (head, 0, 0))
    return whole, column, page


def attend(mp_size, pieces, queries, keys_t, values_t, layout, line, key_extra, query_bins):
    inner, rows = queries.shape
    keys = keys_t.shape[1]
    head_count, _, width = line.shape
    head_size = inner // head_count
    whole, column, page = attention_shapes(head_count, head_size, rows, keys, width)
    hbm = pl.BlockSpec(memory_space=HBM)
    return pl.pallas_call(
        partial(attend_gather_kernel, mp_size, head_count, len(pieces)) if pieces else attend_kernel,
        grid=(head_count,),
        out_shape=(
            jax.ShapeDtypeStruct((inner, rows), BF16),
            jax.ShapeDtypeStruct((head_count, 1, rows), F32),
        )
        + tuple(
            jax.ShapeDtypeStruct((p.shape[0], p.shape[1] * mp_size, 8 * LANES), BF16) for p in pieces
        ),
        in_specs=[
            column(rows), column(keys), column(keys), page(128, 128), page(1, width),
            whole((keys, 256)), whole((128, rows)),
        ]
        + [hbm] * len(pieces),
        out_specs=(column(rows), page(1, rows)) + (hbm,) * len(pieces),
        scratch_shapes=[
            pltpu.VMEM((keys, 256), BF16),
            pltpu.VMEM((256, rows), BF16),
            pltpu.VMEM((LANES, width), F32),
            pltpu.VMEM((keys, rows), F32),
            pltpu.VMEM((keys, rows), BF16),
        ]
        + (Gather.semaphores(len(pieces), mp_size) if pieces else []),
        compiler_params=pltpu.CompilerParams(
            dimension_semantics=("arbitrary",), vmem_limit_bytes=32 << 20,
            **(dict(collective_id=1, has_side_effects=True) if pieces else {}),
        ),
        name="attend",
    )(queries, keys_t, values_t, layout, line, key_extra, query_bins, *pieces)


def attend_back(
    mp_size, fulls, queries, keys_t, values_t, heads_out, heads_grad, lse, layout, line,
    key_extra, key_extra_t, query_bins, query_bins_t,
):
    inner, rows = queries.shape
    keys = keys_t.shape[1]
    head_count, _, width = line.shape
    head_size = inner // head_count
    whole, column, page = attention_shapes(head_count, head_size, rows, keys, width)
    hbm = pl.BlockSpec(memory_space=HBM)
    sizes = [(full.shape[0], full.shape[1] // mp_size) for full in fulls]
    return pl.pallas_call(
        partial(attend_back_scatter_kernel, mp_size, head_count, len(fulls))
        if fulls
        else attend_back_kernel,
        grid=(head_count,),
        out_shape=(
            jax.ShapeDtypeStruct((inner, rows), BF16),
            jax.ShapeDtypeStruct((inner, keys), BF16),
            jax.ShapeDtypeStruct((inner, keys), BF16),
            jax.ShapeDtypeStruct((head_count, 1, width), F32),
            jax.ShapeDtypeStruct((head_count, 128, 128), F32),
        )
        + tuple(jax.ShapeDtypeStruct((lead, n, LANES), F32) for lead, n in sizes),
        in_specs=[
            column(rows), column(keys), column(keys), column(rows), column(rows),
            page(1, rows), page(128, 128), page(1, width),
            whole((keys, 256)), whole((128, keys)), whole((128, rows)), whole((rows, 128)),
        ]
        + [hbm] * len(fulls),
        out_specs=(column(rows), column(keys), column(keys), page(1, width), page(128, 128))
        + tuple(whole((lead, n, LANES)) for lead, n in sizes),
        scratch_shapes=[
            pltpu.VMEM((keys, 256), BF16),
            pltpu.VMEM((192, keys), BF16),
            pltpu.VMEM((256, rows), BF16),
            pltpu.VMEM((keys, 128), BF16),
            pltpu.VMEM((128, rows), BF16),
            pltpu.VMEM((LANES, width), F32),
            pltpu.VMEM((LANES, width), F32),
            pltpu.VMEM((keys, rows), BF16),
        ]
        + (Scatter.buffers(sizes, mp_size) + Scatter.semaphores(len(fulls), mp_size) if fulls else []),
        compiler_params=pltpu.CompilerParams(
            dimension_semantics=("arbitrary",), vmem_limit_bytes=56 << 20,
            **(dict(collective_id=2, has_side_effects=True) if fulls else {}),
        ),
        name="attend_back",
    )(
        queries, keys_t, values_t, heads_out, heads_grad, lse, layout, line,
        key_extra, key_extra_t, query_bins, query_bins_t, *fulls,
    )


def spread(step_count, heads):
    if step_count <= heads:
        return [[s] if s < step_count else [] for s in range(heads)]
    return [[s for s in range(step_count) if s * heads // step_count == h] for h in range(heads)]


def run_steps(task, heads):
    head = pl.program_id(0)
    for h, steps in enumerate(spread(task.steps, heads)):
        if steps:

            @pl.when(head == h)
            def _(steps=steps):
                for s in steps:
                    task.step(s)


def attend_gather_kernel(mp_size, heads, count, *refs):
    ins, refs = refs[:7], refs[7:]
    pieces, refs = refs[:count], refs[count:]
    outs, refs = refs[:2], refs[2:]
    fulls, refs = refs[:count], refs[count:]
    scratch, sems = refs[:5], refs[5:]
    place = Place(mp_size)

    @pl.when(pl.program_id(0) == 0)
    def _():
        meet(place)

    run_steps(Gather(place, pieces, fulls, sems), heads)
    attend_kernel(*ins, *outs, *scratch)


def attend_back_scatter_kernel(mp_size, heads, count, *refs):
    ins, refs = refs[:12], refs[12:]
    fulls, refs = refs[:count], refs[count:]
    outs, refs = refs[:5], refs[5:]
    sums, refs = refs[:count], refs[count:]
    scratch, refs = refs[:8], refs[8:]
    buffers, sems = Scatter.group(refs[: 5 * count], count), refs[5 * count :]
    place = Place(mp_size)

    @pl.when(pl.program_id(0) == 0)
    def _():
        meet(place)

    run_steps(Scatter(place, fulls, sums, buffers, sems), heads)
    attend_back_kernel(*ins, *outs, *scratch)


def gather_first_kernel(mp_size, group, *refs):
    weights, normed, table, full, slot_rows, tables, *sems = refs
    row_sems, table_sems, sems = sems[:3], sems[3:6], sems[6:]
    place = Place(mp_size)
    rows = normed.shape[0]
    first = lax.div(place.mp, group) * group
    member = lax.rem(place.mp, group)
    window = slot_rows.at[pl.ds(pl.multiple_of(member * rows, 16), rows), :]
    copies = []
    for k in range(1, group):
        peer = (place.dp, first + lax.rem(member + k, group))
        copies.append(remote(normed, window, row_sems[0].at[k], row_sems[1].at[k], peer))
    for k in range(1, mp_size):
        copies.append(
            remote(table, tables.at[place.mp], table_sems[0].at[k], table_sems[1].at[k], place.to_mp(k))
        )
    own = [
        Copy(normed, window, row_sems[2].at[0]),
        Copy(table, tables.at[place.mp], table_sems[2].at[0]),
    ]
    gather = Gather(place, [weights], [full], sems)
    for copy in own:
        copy.start()
    meet(place)
    gather.step(0)
    for copy in copies:
        copy.start()
    for s in range(1, gather.steps):
        gather.step(s)
    for copy in own:
        copy.wait()
    for copy in copies:
        copy.wait_send()
        copy.wait_recv()


def gather_first(mp_size, group, weights, normed, table):
    lead, n, _ = weights.shape
    rows, model_width = normed.shape
    dma = pltpu.SemaphoreType.DMA
    hbm = pl.BlockSpec(memory_space=HBM)
    return pl.pallas_call(
        partial(gather_first_kernel, mp_size, group),
        out_shape=(
            jax.ShapeDtypeStruct((lead, mp_size * n, model_width), BF16),
            jax.ShapeDtypeStruct((group * rows, model_width), BF16),
            jax.ShapeDtypeStruct((mp_size, 8, LANES), F32),
        ),
        in_specs=[hbm] * 3,
        out_specs=(hbm,) * 3,
        scratch_shapes=[dma((group,)), dma((group,)), dma((1,)), dma((mp_size,)), dma((mp_size,)), dma((1,))]
        + Gather.semaphores(1, mp_size),
        compiler_params=pltpu.CompilerParams(collective_id=0, has_side_effects=True),
        name="gather_first",
    )(weights, normed, table)


def last_kernel(mp_size, group, *refs):
    (full, slot_grad, own_grad, layer_input, residual_grad, gains, small,
     out, input_grad, small_out, *refs) = refs
    buffers, refs = Scatter.group(refs[:5], 1), refs[5:]
    peers, stage, stage_in, row_sems, stage_sems = refs[:3] + [refs[3:5], refs[5:7]]
    sems = refs[7:]
    place = Place(mp_size)
    rows, model_width = own_grad.shape
    first = lax.div(place.mp, group) * group
    member = lax.rem(place.mp, group)
    rows_out = []
    for k in range(1, group):
        other = lax.rem(member + k, group)
        rows_out.append(
            remote(
                slot_grad.at[pl.ds(pl.multiple_of(other * rows, 16), rows), :], peers.at[k - 1],
                row_sems[0].at[k], row_sems[1].at[k], (place.dp, first + other),
            )
        )
    partners = [place.to_core, place.to_x, place.to_y]
    bit = 1
    while bit < mp_size:
        flipped = place.mp + bit - 2 * bit * lax.rem(lax.div(place.mp, bit), 2)
        partners.append((place.dp, flipped))
        bit *= 2
    stages = [
        remote(stage.at[i], stage_in.at[i], stage_sems[0].at[i], stage_sems[1].at[i], partner)
        for i, partner in enumerate(partners)
    ]
    scatter = Scatter(place, [full], [out], buffers, sems)
    meet(place)
    for copy in rows_out:
        copy.start()
    for s in range(5):
        scatter.step(s)
    for copy in rows_out:
        copy.wait_recv()
    size = 16

    def body(i, total):
        here = pl.ds(pl.multiple_of(i * size, size), size)
        grad = own_grad[here, :]
        for k in range(group - 1):
            grad = grad + peers[k, here, :].astype(F32)
        values = layer_input[here, :]
        scale = lax.rsqrt(jnp.mean(values * values, axis=1, keepdims=True) + EPSILON)
        scaled = gains[0:1, :] * grad
        mean = jnp.mean(scaled * values, axis=1, keepdims=True)
        input_grad[here, :] = (
            residual_grad[here, :] + scale * scaled - values * (scale * scale * scale * mean)
        )
        product = grad * values * scale
        return total + product[0:8] + product[8:16]

    total = lax.fori_loop(0, rows // size, body, jnp.zeros((8, model_width), F32))
    gain = jnp.sum(total, axis=0, keepdims=True)
    for i in range(model_width // LANES):
        stage[0, i : i + 1, :] = gain[:, i * LANES : (i + 1) * LANES]
    gain_rows = model_width // LANES
    stage[0, gain_rows : small.shape[0] + gain_rows, :] = small[...]
    stages[0].start()
    at = 5
    for i, copy in enumerate(stages):
        if at < scatter.steps:
            scatter.step(at)
            at += 1
        copy.wait_recv()
        if i + 1 < len(stages):
            stage[i + 1] = stage[i] + stage_in[i]
            stages[i + 1].start()
        else:
            small_out[...] = stage[i] + stage_in[i]
    for s in range(at, scatter.steps):
        scatter.step(s)
    for copy in rows_out + stages:
        copy.wait_send()


def last_step(mp_size, group, full, slot_grad, own_grad, layer_input, residual_grad, gains, small):
    lead, total_rows, model_width = full.shape
    n = total_rows // mp_size
    rows = own_grad.shape[0]
    small_rows = small.shape[0] + model_width // LANES
    count = 3 + (mp_size - 1).bit_length()
    dma = pltpu.SemaphoreType.DMA
    hbm = pl.BlockSpec(memory_space=HBM)
    vmem = pl.BlockSpec(memory_space=pltpu.VMEM)
    return pl.pallas_call(
        partial(last_kernel, mp_size, group),
        out_shape=(
            jax.ShapeDtypeStruct((lead, n, LANES), F32),
            jax.ShapeDtypeStruct((rows, model_width), F32),
            jax.ShapeDtypeStruct((small_rows, LANES), F32),
        ),
        in_specs=[hbm, hbm] + [vmem] * 5,
        out_specs=(vmem,) * 3,
        scratch_shapes=Scatter.buffers([(lead, n)], mp_size)
        + [
            pltpu.VMEM((max(group - 1, 1), rows, model_width), BF16),
            pltpu.VMEM((count, small_rows, LANES), F32),
            pltpu.VMEM((count, small_rows, LANES), F32),
            dma((group,)), dma((group,)), dma((count,)), dma((count,)),
        ]
        + Scatter.semaphores(1, mp_size),
        compiler_params=pltpu.CompilerParams(
            collective_id=3, has_side_effects=True, vmem_limit_bytes=48 << 20
        ),
        name="last_step",
    )(full, slot_grad, own_grad, layer_input, residual_grad, gains, small)


def line_onehot(first_row, width, key_blocks):
    place = jnp.arange(width, dtype=jnp.int32)
    place = jnp.where(place >= width - LANES, place - width, place)
    offset = LANES * (key_blocks - 1) - place - first_row
    return (bucket_of(offset)[:, None] == jnp.arange(32, dtype=jnp.int32)[None, :]).astype(F32)


def bin_onehot():
    bins = np.arange(NBIN)
    offset = bins[:, None] - bins[None, :]
    distance = np.abs(offset)
    bucket = np.minimum(distance, 7) + sum((distance >= t).astype(np.int64) for t in THRESHOLDS)
    bucket = bucket + 16 * (offset > 0)
    return jnp.asarray(bucket[:, :, None] == np.arange(32), F32)


def gather_rows(local, axis_name):
    return lax.all_gather(local, axis_name, axis=0, tiled=True)


def scatter_grad(full):
    summed = lax.psum_scatter(full, "dp", scatter_dimension=1, tiled=True)
    return lax.psum_scatter(summed, "mp", scatter_dimension=0, tiled=True)


def per_device(
    dp_size, mp_size,
    layer_input, norm_gains, query_weight, key_value_weight, output_weight,
    gate_up_weight, down_weight, bias_tables, doc_lengths, box_bins, cotangent,
):
    rows, model_width = layer_input.shape
    doc_count = doc_lengths.shape[0]
    slot_span = box_bins.shape[1] // doc_count
    group = mp_size // doc_count
    mp_index = lax.axis_index("mp")
    doc = mp_index // group
    first_row = (mp_index % group) * rows
    key_blocks = slot_span // LANES
    width = LANES * (key_blocks + (rows + LANES - 1) // LANES)
    groups = [[d * group + i for i in range(group)] for d in range(doc_count)]
    gain_first = norm_gains[0].astype(F32)
    gain_second = norm_gains[1].astype(F32)

    scale_first = inverse_rms(layer_input)
    normed = (layer_input * scale_first * gain_first).astype(BF16)
    heads_here = bias_tables.shape[2]
    head_count = heads_here * mp_size
    custom = dp_size == 8 and model_width == 8 * LANES and mp_size & (mp_size - 1) == 0
    custom = custom and 3 * 32 * heads_here <= 8 * LANES

    if custom:
        dp_index = lax.axis_index("dp")
        column = ((dp_index % 2) * 4 + dp_index // 2) * LANES
        piece = lambda weight, axis: lax.dynamic_slice_in_dim(weight, column, LANES, axis)
        key_value_piece = jnp.transpose(piece(key_value_weight, 0), (1, 2, 0))
        first_pieces = jnp.stack(
            [
                piece(query_weight, 0).T, key_value_piece[0], key_value_piece[1], piece(output_weight, 1)
            ]
        )
        pieces = [
            jnp.transpose(piece(gate_up_weight, 0), (1, 2, 0)), piece(down_weight, 1)[None]
        ]
        table_piece = bias_tables.astype(F32).reshape(-1)
        table_piece = jnp.pad(table_piece, (0, 8 * LANES - table_piece.shape[0])).reshape(8, LANES)
        w_first, slot_normed, tables = gather_first(
            mp_size, group, first_pieces, normed, table_piece
        )
        w_query, w_key, w_value, w_output = w_first
        tables = tables.reshape(mp_size, -1)[:, : bias_tables.size]
        tables = jnp.moveaxis(tables.reshape(mp_size, 3, 32, heads_here), 0, 2)
        tables = tables.reshape(3, 32, head_count)
    else:
        pieces = []
        w_query = gather_rows(query_weight.T, "mp")
        w_key = gather_rows(key_value_weight[:, 0].T, "mp")
        w_value = gather_rows(key_value_weight[:, 1].T, "mp")
        w_output = gather_rows(output_weight, "mp")
        w_gate = gather_rows(gate_up_weight[:, 0].T, "mp")
        w_up = gather_rows(gate_up_weight[:, 1].T, "mp")
        w_down = gather_rows(down_weight, "mp")
        tables = lax.all_gather(bias_tables, "mp", axis=2, tiled=True).astype(F32)
        slot_normed = lax.all_gather(normed, "mp", axis=0, tiled=True, axis_index_groups=groups)

    onehot_line = line_onehot(first_row, width, key_blocks)
    line = jnp.dot(onehot_line, tables[0], precision=lax.Precision.HIGHEST)
    line = line.T.reshape(head_count, 1, width)
    onehot_bin = bin_onehot()
    x_part = jnp.einsum("ban,nh->hba", onehot_bin, tables[1], precision=lax.Precision.HIGHEST)
    y_part = jnp.einsum("ban,nh->hba", onehot_bin, tables[2], precision=lax.Precision.HIGHEST)
    empty = jnp.zeros_like(x_part)
    layout = jnp.concatenate(
        [jnp.concatenate([x_part, empty], axis=2), jnp.concatenate([empty, y_part], axis=2)], axis=1
    ).astype(BF16)
    key_bins = lax.dynamic_slice(box_bins, (0, doc * slot_span), (2, slot_span))
    own_bins = lax.dynamic_slice(key_bins, (0, first_row), (2, rows))
    bin_ids = jnp.arange(NBIN, dtype=jnp.int32)

    def placed_rows(bins):
        return jnp.concatenate(
            [bins[0][:, None] == bin_ids, bins[1][:, None] == bin_ids], axis=1
        ).astype(BF16)

    def placed_lanes(bins):
        return jnp.concatenate(
            [bin_ids[:, None] == bins[0][None], bin_ids[:, None] == bins[1][None]], axis=0
        ).astype(BF16)

    length = lax.dynamic_index_in_dim(doc_lengths, doc, keepdims=False)
    masked = jnp.arange(slot_span, dtype=jnp.int32)[:, None] >= length
    key_placed = placed_rows(key_bins)
    key_extra = jnp.concatenate(
        [
            jnp.zeros((slot_span, 64), BF16),
            key_placed,
            jnp.where(masked, NEG_FILL, 0.0).astype(BF16),
            jnp.ones((slot_span, 3), BF16),
            jnp.zeros((slot_span, 60), BF16),
        ],
        axis=1,
    )
    key_extra_t = placed_lanes(key_bins)
    query_bins_t = placed_rows(own_bins)
    query_bins = placed_lanes(own_bins)

    queries = dot_f32(w_query, normed, 1, 1).astype(BF16)
    keys_t = dot_f32(w_key, slot_normed, 1, 1).astype(BF16)
    values_t = dot_f32(w_value, slot_normed, 1, 1).astype(BF16)
    heads_out, lse, *gathered = attend(
        mp_size, pieces, queries, keys_t, values_t, layout, line, key_extra, query_bins
    )
    if custom:
        (w_gate, w_up), (w_down,) = gathered
    residual = layer_input + dot_f32(heads_out, w_output, 0, 0)
    scale_second = inverse_rms(residual)
    normed_second = (residual * scale_second * gain_second).astype(BF16)
    gate = dot_f32(normed_second, w_gate, 1, 1)
    up = dot_f32(normed_second, w_up, 1, 1)
    gelu_value, gelu_pull = jax.vjp(lambda v: jax.nn.gelu(v, approximate=True), gate)
    activated = (gelu_value * up).astype(BF16)
    layer_output = residual + dot_f32(activated, w_down, 1, 0)

    def by_owner(values):
        if not custom:
            return values
        parts = values.reshape(-1, 4, 2, LANES)
        return jnp.swapaxes(parts, 1, 2).reshape(values.shape)

    out_low = cotangent.astype(BF16)
    down_full = dot_f32(activated, by_owner(out_low), 0, 0).astype(BF16)
    act_grad = dot_f32(out_low, w_down, 1, 1)
    gate_low = gelu_pull(act_grad * up)[0].astype(BF16)
    up_low = (act_grad * gelu_value).astype(BF16)
    second_by_owner = by_owner(normed_second)
    gate_full = dot_f32(gate_low, second_by_owner, 0, 0).astype(BF16)
    up_full = dot_f32(up_low, second_by_owner, 0, 0).astype(BF16)
    second_grad = dot_f32(gate_low, w_gate, 1, 0) + dot_f32(up_low, w_up, 1, 0)
    gain_second_grad = jnp.sum(second_grad * residual * scale_second, axis=0)
    scaled = gain_second * second_grad
    residual_grad = (
        cotangent
        + scale_second * scaled
        - residual * scale_second**3 * jnp.mean(scaled * residual, axis=-1, keepdims=True)
    )

    branch_low = residual_grad.astype(BF16)
    output_full = dot_f32(heads_out, by_owner(branch_low), 1, 0).astype(BF16)
    heads_grad = dot_f32(w_output, branch_low, 1, 1).astype(BF16)
    fulls = [jnp.stack([gate_full, up_full]), down_full[None]] if custom else []
    dq, dk, dv, line_grad, layout_grad, *scattered = attend_back(
        mp_size, fulls, queries, keys_t, values_t, heads_out, heads_grad, lse, layout, line,
        key_extra, key_extra_t, query_bins, query_bins_t,
    )
    slot_by_owner = by_owner(slot_normed)
    query_full = dot_f32(dq, by_owner(normed), 1, 0).astype(BF16)
    key_full = dot_f32(dk, slot_by_owner, 1, 0).astype(BF16)
    value_full = dot_f32(dv, slot_by_owner, 1, 0).astype(BF16)
    slot_grad = dot_f32(dk, w_key, 0, 0) + dot_f32(dv, w_value, 0, 0)
    query_part = dot_f32(dq, w_query, 0, 0)

    line_part = jnp.dot(onehot_line.T, line_grad[:, 0].T, precision=lax.Precision.HIGHEST)
    x_part = jnp.einsum(
        "ban,hba->nh", onehot_bin, layout_grad[:, :64, :64], precision=lax.Precision.HIGHEST
    )
    y_part = jnp.einsum(
        "ban,hba->nh", onehot_bin, layout_grad[:, 64:, 64:], precision=lax.Precision.HIGHEST
    )
    table_full = jnp.stack([line_part, x_part, y_part])

    if custom:
        own_grad = query_part + lax.dynamic_slice_in_dim(slot_grad, first_row, rows, 0)
        first_full = jnp.stack([query_full, key_full, value_full, output_full])
        small = jnp.concatenate([gain_second_grad, table_full.reshape(-1)])
        small_rows = small.shape[0] // LANES
        small = jnp.pad(small.reshape(small_rows, LANES), ((0, -small_rows % 8), (0, 0)))
        summed, input_grad, small = last_step(
            mp_size, group, first_full, slot_grad.astype(BF16), own_grad, layer_input,
            residual_grad, norm_gains.astype(F32), small,
        )
        small = small.reshape(-1)
        gains = small[: 2 * model_width].reshape(2, model_width)
        share = model_width // (dp_size * mp_size)
        at = (dp_index * mp_size + mp_index) * share
        gain_grad = lax.dynamic_slice(gains, (0, at), (2, share))
        table = small[2 * model_width : 2 * model_width + 3 * 32 * head_count]
        table_grad = lax.dynamic_slice(
            table.reshape(3, 32, head_count),
            (0, dp_index * (32 // dp_size), mp_index * heads_here),
            (3, 32 // dp_size, heads_here),
        )
        (gate_up_sum, (down_grad,)) = scattered
        query_grad = summed[0].T
        key_value_grad = jnp.transpose(summed[1:3], (2, 0, 1))
        output_grad = summed[3]
        gate_up_grad = jnp.transpose(gate_up_sum, (2, 0, 1))
    else:
        first_grad = query_part + lax.psum_scatter(
            slot_grad.astype(BF16), "mp", scatter_dimension=0, tiled=True, axis_index_groups=groups
        ).astype(F32)
        gain_first_grad = jnp.sum(first_grad * layer_input * scale_first, axis=0)
        scaled = gain_first * first_grad
        input_grad = (
            residual_grad
            + scale_first * scaled
            - layer_input * scale_first**3 * jnp.mean(scaled * layer_input, axis=-1, keepdims=True)
        )
        gain_grad = lax.psum_scatter(
            jnp.stack([gain_first_grad, gain_second_grad]), ("dp", "mp"), scatter_dimension=1,
            tiled=True,
        )
        table_grad = lax.psum_scatter(
            lax.psum_scatter(table_full, "mp", scatter_dimension=2, tiled=True),
            "dp", scatter_dimension=1, tiled=True,
        )
        query_grad = scatter_grad(query_full).T.astype(F32)
        key_value_grad = jnp.stack(
            [scatter_grad(key_full).T, scatter_grad(value_full).T], axis=1
        ).astype(F32)
        output_grad = scatter_grad(output_full).astype(F32)
        gate_up_grad = jnp.stack(
            [scatter_grad(gate_full).T, scatter_grad(up_full).T], axis=1
        ).astype(F32)
        down_grad = scatter_grad(down_full).astype(F32)
    return (
        layer_output, input_grad, gain_grad, query_grad, key_value_grad,
        output_grad, gate_up_grad, down_grad, table_grad,
    )


def solution(mesh):
    return jax.shard_map(
        partial(per_device, mesh.shape["dp"], mesh.shape["mp"]),
        mesh=mesh,
        in_specs=(
            P(("dp", "mp"), None),
            P(),
            P(None, "mp"),
            P(None, None, "mp"),
            P("mp", None),
            P(None, None, "mp"),
            P("mp", None),
            P(None, None, "mp"),
            P("dp"),
            P(None, "dp"),
            P(("dp", "mp"), None),
        ),
        out_specs=(
            P(("dp", "mp"), None),
            P(("dp", "mp"), None),
            P(None, ("dp", "mp")),
            P("dp", "mp"),
            P("dp", None, "mp"),
            P("mp", "dp"),
            P("dp", None, "mp"),
            P("mp", "dp"),
            P(None, "dp", "mp"),
        ),
        check_vma=False,
    )
```

```python
from functools import partial

import jax
import jax.numpy as jnp
import numpy as np
from jax import lax
from jax.experimental import pallas as pl
from jax.experimental.pallas import tpu as pltpu
from jax.sharding import PartitionSpec as P

NBIN = 64
EPSILON = 1e-06
THRESHOLDS = (8, 12, 16, 23, 32, 46, 64, 91)
NEG_FILL = -1e30
LANES = 128
MESH = pl.DeviceIdType.MESH
HBM = pltpu.MemorySpace.HBM
BF16 = jnp.bfloat16
F32 = jnp.float32


def bucket_of(relative):
    distance = jnp.abs(relative)
    bucket = jnp.minimum(distance, 7)
    for threshold in THRESHOLDS:
        bucket = bucket + (distance >= threshold).astype(jnp.int32)
    return bucket + 16 * (relative > 0).astype(jnp.int32)


def inverse_rms(values):
    return lax.rsqrt(jnp.mean(values * values, axis=-1, keepdims=True) + EPSILON)


def dot_f32(left, right, left_dim, right_dim):
    return lax.dot_general(
        left, right, (((left_dim,), (right_dim,)), ((), ())), preferred_element_type=F32
    )


def three_parts(values):
    high = values.astype(BF16)
    rest = values - high.astype(F32)
    middle = rest.astype(BF16)
    low = (rest - middle.astype(F32)).astype(BF16)
    return high, middle, low


def lane_ids(shape):
    return lax.broadcasted_iota(jnp.int32, shape, 1)


def row_ids(shape):
    return lax.broadcasted_iota(jnp.int32, shape, 0)


def attend_kernel(
    q_ref, k_ref, v_ref, layout_ref, line_ref, key_extra_ref, query_bins_ref,
    out_ref, lse_ref,
    key_aug, query_aug, strip, scores, probs,
):
    head_size, rows = q_ref.shape
    keys = k_ref.shape[1]
    blocks = keys // LANES
    width = strip.shape[1]

    @pl.when(pl.program_id(0) == 0)
    def _():
        key_aug[...] = key_extra_ref[...]
        tail = row_ids((64, rows))
        query_aug[pl.ds(192, 64), :] = jnp.where(tail == 0, 1.0, 0.0).astype(BF16)

    both = jnp.concatenate([k_ref[...], v_ref[...]], axis=0).T
    low_lanes = lane_ids((keys, LANES)) < head_size
    key_aug[:, 0:LANES] = jnp.where(low_lanes, both, key_extra_ref[:, 0:LANES])
    query_aug[pl.ds(0, 64), :] = q_ref[...]
    query_aug[pl.ds(64, 128), :] = jnp.dot(
        layout_ref[0], query_bins_ref[...], preferred_element_type=F32
    ).astype(BF16)
    strip[...] = pltpu.roll(
        jnp.broadcast_to(line_ref[0], (LANES, width)), 0, 1, stride=1, stride_axis=0
    )
    query_all = query_aug[...]
    top = jnp.full((1, rows), -jnp.inf, F32)
    for block in range(blocks):
        here = pl.ds(block * LANES, LANES)
        part = jnp.dot(key_aug[here, :], query_all, preferred_element_type=F32)
        part = part + strip[:, pl.ds((blocks - 1 - block) * LANES, rows)]
        scores[here, :] = part
        top = jnp.maximum(top, jnp.max(part, axis=0, keepdims=True))
    total = jnp.zeros((1, rows), F32)
    for block in range(blocks):
        here = pl.ds(block * LANES, LANES)
        part = jnp.exp(scores[here, :] - top)
        total = total + jnp.sum(part, axis=0, keepdims=True)
        probs[here, :] = part.astype(BF16)
    mixed = jnp.dot(v_ref[...], probs[...], preferred_element_type=F32)
    out_ref[...] = (mixed / total).astype(BF16)
    lse_ref[0] = top + jnp.log(total)


def attend_back_kernel(
    q_ref, k_ref, v_ref, out_ref, out_grad_ref, lse_ref, layout_ref, line_ref,
    key_extra_ref, key_extra_t_ref, query_bins_ref, query_bins_t_ref,
    dq_ref, dk_ref, dv_ref, line_grad_ref, layout_grad_ref,
    key_aug, key_aug_t, query_aug, value_aug, grad_aug, strip, strip_grad, probs_grad,
):
    head_size, rows = q_ref.shape
    keys = k_ref.shape[1]
    blocks = keys // LANES
    width = strip.shape[1]

    @pl.when(pl.program_id(0) == 0)
    def _():
        key_aug[...] = key_extra_ref[...]
        key_aug_t[pl.ds(64, 128), :] = key_extra_t_ref[...]
        tail = row_ids((64, rows))
        query_aug[pl.ds(192, 64), :] = jnp.where(tail == 0, 1.0, 0.0).astype(BF16)

    both = jnp.concatenate([k_ref[...], v_ref[...]], axis=0).T
    lanes = lane_ids((keys, LANES))
    key_aug[:, 0:LANES] = jnp.where(lanes < head_size, both, key_extra_ref[:, 0:LANES])
    ones = jnp.where(lanes < 3, 1.0, 0.0).astype(BF16)
    value_aug[...] = jnp.where(lanes < head_size, ones, both)
    key_aug_t[pl.ds(0, 64), :] = k_ref[...]
    query_aug[pl.ds(0, 64), :] = q_ref[...]
    query_aug[pl.ds(64, 128), :] = jnp.dot(
        layout_ref[0], query_bins_ref[...], preferred_element_type=F32
    ).astype(BF16)
    high, middle, low = three_parts(-lse_ref[0])
    tail = row_ids((64, rows))
    rows_of = lambda part: jnp.broadcast_to(part.astype(F32), (64, rows))
    query_aug[pl.ds(192, 64), :] = jnp.where(
        tail == 0, 1.0,
        jnp.where(
            tail == 1, rows_of(high),
            jnp.where(tail == 2, rows_of(middle), jnp.where(tail == 3, rows_of(low), 0.0)),
        ),
    ).astype(BF16)
    row_dot = jnp.sum(
        out_grad_ref[...].astype(F32) * out_ref[...].astype(F32), axis=0, keepdims=True
    )
    high, middle, low = three_parts(-row_dot)
    grad_aug[pl.ds(0, 64), :] = jnp.where(
        tail == 0, rows_of(high),
        jnp.where(tail == 1, rows_of(middle), jnp.where(tail == 2, rows_of(low), 0.0)),
    ).astype(BF16)
    grad_aug[pl.ds(64, 64), :] = out_grad_ref[...]
    strip[...] = pltpu.roll(
        jnp.broadcast_to(line_ref[0], (LANES, width)), 0, 1, stride=1, stride_axis=0
    )
    strip_grad[...] = jnp.zeros_like(strip_grad)
    query_and_grad = jnp.concatenate([q_ref[...], out_grad_ref[...]], axis=0).T
    query_all = query_aug[...]
    grad_all = grad_aug[...]
    half = lane_ids((LANES, LANES)) < head_size
    for block in range(blocks):
        here = pl.ds(block * LANES, LANES)
        band = pl.ds((blocks - 1 - block) * LANES, rows)
        part = jnp.dot(key_aug[here, :], query_all, preferred_element_type=F32)
        part = jnp.exp(part + strip[:, band])
        slope = part * jnp.dot(value_aug[here, :], grad_all, preferred_element_type=F32)
        strip_grad[:, band] = strip_grad[:, band] + slope
        slope = slope.astype(BF16)
        probs_grad[here, :] = slope
        key_part = jnp.dot(slope, query_and_grad, preferred_element_type=F32)
        value_part = jnp.dot(part.astype(BF16), query_and_grad, preferred_element_type=F32)
        turned = jnp.where(half, key_part, value_part).T.astype(BF16)
        dk_ref[:, here] = turned[0:64]
        dv_ref[:, here] = turned[64:128]
    query_part = jnp.dot(key_aug_t[...], probs_grad[...], preferred_element_type=F32)
    dq_ref[...] = query_part[0:64].astype(BF16)
    layout_grad_ref[0] = jnp.dot(
        query_part[64:192].astype(BF16), query_bins_t_ref[...], preferred_element_type=F32
    )
    folded = strip_grad[pl.ds(0, 8), :]
    for group in range(1, LANES // 8):
        folded = folded + pltpu.roll(strip_grad[pl.ds(group * 8, 8), :], width - group * 8, 1)
    line = folded[0:1]
    for row in range(1, 8):
        line = line + pltpu.roll(folded[row : row + 1], width - row, 1)
    line_grad_ref[0] = line


class Place:
    def __init__(self, mp_size):
        self.dp = lax.axis_index("dp")
        self.mp = lax.axis_index("mp")
        self.mp_size = mp_size
        self.core = lax.rem(self.dp, 2)
        self.x = lax.rem(lax.div(self.dp, 2), 2)
        self.y = lax.div(self.dp, 4)
        self.to_core = (self.dp + 1 - 2 * self.core, self.mp)
        self.to_x = (self.dp + 2 - 4 * self.x, self.mp)
        self.to_y = (self.dp + 4 - 8 * self.y, self.mp)

    def to_mp(self, step):
        return (self.dp, lax.rem(self.mp + step, self.mp_size))

    def from_mp(self, step):
        return lax.rem(self.mp + self.mp_size - step, self.mp_size)

    def partners(self):
        others = [self.to_mp(step) for step in range(1, self.mp_size)]
        return [self.to_core, self.to_x, self.to_y] + others


def meet(place):
    barrier = pltpu.get_barrier_semaphore()
    partners = place.partners()
    for partner in partners:
        pl.semaphore_signal(barrier, inc=1, device_id=partner, device_id_type=MESH)
    pl.semaphore_wait(barrier, len(partners))


class Copy:
    def __init__(self, source, target, send, receive=None, partner=None):
        self.parts = (source, target, send, receive, partner)

    def made(self):
        source, target, send, receive, partner = self.parts
        if partner is None:
            return pltpu.make_async_copy(source, target, send)
        return pltpu.make_async_remote_copy(
            src_ref=source, dst_ref=target, send_sem=send, recv_sem=receive,
            device_id=partner, device_id_type=MESH,
        )

    def start(self):
        self.made().start()

    def wait(self):
        self.made().wait()

    def wait_send(self):
        self.made().wait_send()

    def wait_recv(self):
        self.made().wait_recv()


def remote(source, target, send, receive, partner):
    return Copy(source, target, send, receive, partner)


def lanes_at(block, count):
    return pl.ds(pl.multiple_of(block * LANES, LANES), count * LANES)


class Gather:
    LAGS = 2

    def __init__(self, place, pieces, outs, sems, items=None):
        self.place, self.pieces, self.outs = place, pieces, outs
        self.z_send, self.z_recv, self.own_sem, self.send, self.recv = sems
        self.items = items or [(c, k) for c in range(len(pieces)) for k in range(place.mp_size)]
        self.steps = len(self.items) + self.LAGS

    @staticmethod
    def semaphores(count, mp_size):
        dma = pltpu.SemaphoreType.DMA
        items = count * mp_size
        return [
            dma((count, mp_size)), dma((count, mp_size)), dma((count,)), dma((items, 6)), dma((items, 6))
        ]

    def rows(self, c, source, half):
        n = self.pieces[c].shape[1]
        if half is None:
            return pl.ds(pl.multiple_of(source * n, 16), n)
        return pl.ds(pl.multiple_of(source * n + half * (n // 2), 16), n // 2)

    def window(self, c, source, half, block, count):
        return self.outs[c].at[:, self.rows(c, source, half), lanes_at(block, count)]

    def own(self, c):
        place = self.place
        block = place.core * 4 + place.y * 2 + place.x
        return Copy(
            self.pieces[c], self.window(c, place.mp, None, block, 1), self.own_sem.at[c]
        )

    def along_mp(self, c, step):
        place = self.place
        block = place.core * 4 + place.y * 2 + place.x
        return remote(
            self.pieces[c], self.window(c, place.mp, None, block, 1),
            self.z_send.at[c, step], self.z_recv.at[c, step], place.to_mp(step),
        )

    def start_chunk(self, c):
        self.own(c).start()
        for step in range(1, self.place.mp_size):
            self.along_mp(c, step).start()

    def copies(self, t):
        c, k = self.items[t]
        place = self.place
        source = place.from_mp(k)
        base = place.core * 4
        mine = base + place.y * 2 + place.x
        turned = base + (1 - place.y) * 2 + place.x

        def copy(i, half, block, count, partner):
            here = self.window(c, source, half, block, count)
            return remote(here, here, self.send.at[t, i], self.recv.at[t, i], partner)

        first = [copy(0, 0, mine, 1, place.to_x), copy(1, 1, mine, 1, place.to_y)]
        second = [
            copy(2, 0, base + place.y * 2, 2, place.to_y),
            copy(3, 1, mine, 1, place.to_x),
            copy(4, 1, turned, 1, place.to_x),
        ]
        third = [copy(5, None, base, 4, place.to_core)]
        return first, second, third

    def step(self, s):
        count = len(self.items)
        if 0 <= s - 2 < count:
            _, second, third = self.copies(s - 2)
            for copy in second:
                copy.wait_recv()
            third[0].start()
        if 0 <= s - 1 < count:
            first, second, _ = self.copies(s - 1)
            for copy in first:
                copy.wait_recv()
            for copy in second:
                copy.start()
        if s < count:
            c, k = self.items[s]
            if k == 0:
                self.own(c).wait()
            else:
                self.along_mp(c, k).wait_recv()
            for copy in self.copies(s)[0]:
                copy.start()

    def done(self, t):
        self.copies(t)[2][0].wait_recv()

    def close(self):
        for t, (c, k) in enumerate(self.items):
            first, second, third = self.copies(t)
            for copy in first + second + third:
                copy.wait_send()
            if k > 0:
                self.along_mp(c, k).wait_send()


def add_rows(target, target_index, source, source_index):
    lead, rows, lanes = target_index
    source_rows, source_lanes = source_index
    row_start, count = rows
    source_start = source_rows
    size = 32
    while count % size:
        size //= 2

    def body(i, carry):
        here = pl.ds(pl.multiple_of(row_start + i * size, size), size)
        there = pl.ds(pl.multiple_of(source_start + i * size, size), size)
        for part in range(lead):
            target[part, here, lanes] = target[part, here, lanes] + source[part, there, source_lanes]
        return carry

    lax.fori_loop(0, count // size, body, 0)


class Scatter:
    def __init__(self, place, fulls, outs, scratch, items):
        self.place, self.fulls, self.outs, self.items = place, fulls, outs, items
        count = len(fulls)
        self.whole = [len(full.shape) == 3 for full in fulls]
        buffers = [scratch[i * count : (i + 1) * count] for i in range(5)]
        self.sums, self.from_first, self.from_second, self.from_mp, self.staged = buffers
        self.own_sem, self.send, self.recv = scratch[5 * count :]
        self.steps = len(items) + 5

    @staticmethod
    def scratch(shapes, whole, mp_size):
        out = []
        for blocks in (4, 2, 1, 1):
            for lead, n in shapes:
                out.append(pltpu.VMEM((mp_size, lead, n, blocks * LANES), BF16))
        for (lead, n), is_whole in zip(shapes, whole):
            out.append(pltpu.VMEM((lead, n, 4 * LANES) if is_whole else (1, 8, LANES), BF16))
        dma = pltpu.SemaphoreType.DMA
        count = len(shapes) * mp_size
        return out + [dma((count,)), dma((count, 7)), dma((count, 7))]

    def size(self, c):
        return self.sums[c].shape[1], self.sums[c].shape[2]

    def source(self, t):
        c, k = self.items[t]
        if not self.whole[c]:
            return self.fulls[c].at[(k + self.place.mp_size - 1) % self.place.mp_size % 2]
        lead, n = self.size(c)
        target = lax.rem(self.place.mp + k, self.place.mp_size)
        return self.fulls[c].at[:, pl.ds(pl.multiple_of(target * n, 16), n), :]

    def from_core(self, t):
        c, k = self.items[t]
        place = self.place
        return remote(
            self.source(t).at[:, :, lanes_at((1 - place.core) * 4, 4)], self.sums[c].at[k],
            self.send.at[t, 0], self.recv.at[t, 0], place.to_core,
        )

    def own(self, t):
        c, _ = self.items[t]
        return Copy(
            self.source(t).at[:, :, lanes_at(self.place.core * 4, 4)], self.staged[c], self.own_sem.at[t]
        )

    def copies(self, t):
        c, k = self.items[t]
        place = self.place
        lead, n = self.size(c)
        top, bottom = pl.ds(0, n // 2), pl.ds(n // 2, n // 2)
        every = pl.ds(0, lead)
        sums = self.sums[c].at[k]

        def copy(i, source, landing, partner):
            return remote(source, landing, self.send.at[t, i], self.recv.at[t, i], partner)

        landing = self.from_first[c].at[k]
        first = [
            copy(
                1, sums.at[every, top, lanes_at((1 - place.y) * 2, 2)],
                landing.at[every, top, pl.ds(0, 256)], place.to_y,
            ),
            copy(
                2, sums.at[every, bottom, lanes_at(1 - place.x, 1)],
                landing.at[every, bottom, pl.ds(0, 128)], place.to_x,
            ),
            copy(
                3, sums.at[every, bottom, lanes_at(3 - place.x, 1)],
                landing.at[every, bottom, pl.ds(128, 128)], place.to_x,
            ),
        ]
        landing = self.from_second[c].at[k]
        second = [
            copy(
                4, sums.at[every, top, lanes_at(place.y * 2 + 1 - place.x, 1)],
                landing.at[every, top, pl.ds(0, 128)], place.to_x,
            ),
            copy(
                5, sums.at[every, bottom, lanes_at((1 - place.y) * 2 + place.x, 1)],
                landing.at[every, bottom, pl.ds(0, 128)], place.to_y,
            ),
        ]
        third = None
        if k > 0:
            third = copy(
                6, sums.at[:, :, lanes_at(place.y * 2 + place.x, 1)], self.from_mp[c].at[k],
                place.to_mp(k),
            )
        return first, second, third

    def step(self, s):
        count = len(self.items)
        place = self.place
        if s < count:
            self.from_core(s).start()
        if 0 <= s - 1 < count:
            t = s - 1
            c, k = self.items[t]
            lead, n = self.size(c)
            first, *_ = self.copies(t)
            self.from_core(t).wait_recv()
            if self.whole[c]:
                self.own(t).wait()
                add_rows(self.sums[c].at[k], (lead, (0, n), pl.ds(0, 512)), self.staged[c], (0, pl.ds(0, 512)))
            else:
                add_rows(
                    self.sums[c].at[k], (lead, (0, n), pl.ds(0, 512)),
                    self.source(t), (0, lanes_at(place.core * 4, 4)),
                )
            for copy in first:
                copy.start()
        if s < count and self.whole[self.items[s][0]]:
            self.own(s).start()
        if 0 <= s - 2 < count:
            t = s - 2
            c, k = self.items[t]
            lead, n = self.size(c)
            first, second, _ = self.copies(t)
            for copy in first:
                copy.wait_recv()
            sums, landing = self.sums[c].at[k], self.from_first[c].at[k]
            half = n // 2
            add_rows(sums, (lead, (0, half), lanes_at(place.y * 2, 2)), landing, (0, pl.ds(0, 256)))
            add_rows(sums, (lead, (half, half), lanes_at(place.x, 1)), landing, (half, pl.ds(0, 128)))
            add_rows(
                sums, (lead, (half, half), lanes_at(2 + place.x, 1)), landing, (half, pl.ds(128, 128))
            )
            for copy in second:
                copy.start()
        if 0 <= s - 3 < count:
            t = s - 3
            c, k = self.items[t]
            lead, n = self.size(c)
            _, second, third = self.copies(t)
            for copy in second:
                copy.wait_recv()
            sums, landing = self.sums[c].at[k], self.from_second[c].at[k]
            mine = lanes_at(place.y * 2 + place.x, 1)
            add_rows(sums, (lead, (0, n), mine), landing, (0, pl.ds(0, 128)))
            if third is not None:
                third.start()
        if 0 <= s - 5 < count:
            t = s - 5
            c, k = self.items[t]
            third = self.copies(t)[2]
            if third is not None:
                third.wait_recv()
            else:
                self.finish(c)

    def left(self, t):
        self.from_core(t).wait_send()

    def close(self):
        for t, (c, k) in enumerate(self.items):
            first, second, third = self.copies(t)
            if self.whole[c] or k in (0, self.place.mp_size - 1):
                self.from_core(t).wait_send()
            for copy in first + second:
                copy.wait_send()
            if third is not None:
                third.wait_send()

    def finish(self, c):
        place = self.place
        lead, n = self.size(c)
        mine = lanes_at(place.y * 2 + place.x, 1)
        sums, landing, out = self.sums[c], self.from_mp[c], self.outs[c]
        size = 32
        while n % size:
            size //= 2

        def body(i, carry):
            here = pl.ds(pl.multiple_of(i * size, size), size)
            for part in range(lead):
                total = sums[0, part, here, mine].astype(F32)
                for k in range(1, place.mp_size):
                    total = total + landing[k, part, here, :].astype(F32)
                out[part, here, :] = total
            return carry

        lax.fori_loop(0, n // size, body, 0)


def attention_shapes(head_count, head_size, rows, keys, width):
    whole = lambda shape: pl.BlockSpec(shape, lambda head: (0,) * len(shape))
    column = lambda size: pl.BlockSpec((head_size, size), lambda head: (head, 0))
    page = lambda a, b: pl.BlockSpec((1, a, b), lambda head: (head, 0, 0))
    return whole, column, page


def attend(queries, keys_t, values_t, layout, line, key_extra, query_bins):
    inner, rows = queries.shape
    keys = keys_t.shape[1]
    head_count, _, width = line.shape
    head_size = inner // head_count
    whole, column, page = attention_shapes(head_count, head_size, rows, keys, width)
    return pl.pallas_call(
        attend_kernel,
        grid=(head_count,),
        out_shape=(
            jax.ShapeDtypeStruct((inner, rows), BF16),
            jax.ShapeDtypeStruct((head_count, 1, rows), F32),
        ),
        in_specs=[
            column(rows), column(keys), column(keys), page(128, 128), page(1, width),
            whole((keys, 256)), whole((128, rows)),
        ],
        out_specs=(column(rows), page(1, rows)),
        scratch_shapes=[
            pltpu.VMEM((keys, 256), BF16),
            pltpu.VMEM((256, rows), BF16),
            pltpu.VMEM((LANES, width), F32),
            pltpu.VMEM((keys, rows), F32),
            pltpu.VMEM((keys, rows), BF16),
        ],
        compiler_params=pltpu.CompilerParams(
            dimension_semantics=("arbitrary",), vmem_limit_bytes=32 << 20
        ),
        name="attend",
    )(queries, keys_t, values_t, layout, line, key_extra, query_bins)


def attend_back(
    queries, keys_t, values_t, heads_out, heads_grad, lse, layout, line,
    key_extra, key_extra_t, query_bins, query_bins_t,
):
    inner, rows = queries.shape
    keys = keys_t.shape[1]
    head_count, _, width = line.shape
    head_size = inner // head_count
    whole, column, page = attention_shapes(head_count, head_size, rows, keys, width)
    return pl.pallas_call(
        attend_back_kernel,
        grid=(head_count,),
        out_shape=(
            jax.ShapeDtypeStruct((inner, rows), BF16),
            jax.ShapeDtypeStruct((inner, keys), BF16),
            jax.ShapeDtypeStruct((inner, keys), BF16),
            jax.ShapeDtypeStruct((head_count, 1, width), F32),
            jax.ShapeDtypeStruct((head_count, 128, 128), F32),
        ),
        in_specs=[
            column(rows), column(keys), column(keys), column(rows), column(rows),
            page(1, rows), page(128, 128), page(1, width),
            whole((keys, 256)), whole((128, keys)), whole((128, rows)), whole((rows, 128)),
        ],
        out_specs=(column(rows), column(keys), column(keys), page(1, width), page(128, 128)),
        scratch_shapes=[
            pltpu.VMEM((keys, 256), BF16),
            pltpu.VMEM((192, keys), BF16),
            pltpu.VMEM((256, rows), BF16),
            pltpu.VMEM((keys, 128), BF16),
            pltpu.VMEM((128, rows), BF16),
            pltpu.VMEM((LANES, width), F32),
            pltpu.VMEM((LANES, width), F32),
            pltpu.VMEM((keys, rows), BF16),
        ],
        compiler_params=pltpu.CompilerParams(
            dimension_semantics=("arbitrary",), vmem_limit_bytes=32 << 20
        ),
        name="attend_back",
    )(
        queries, keys_t, values_t, heads_out, heads_grad, lse, layout, line,
        key_extra, key_extra_t, query_bins, query_bins_t,
    )


def forward_items(mp_size):
    items = [(0, 0), (1, 0), (2, 0)] + [(0, k) for k in range(1, mp_size)]
    for k in range(1, mp_size):
        items += [(1, k), (2, k)]
    return items


def forward_kernel(
    mp_size, group,
    first_ref, gate_up_ref, down_ref, normed_t_ref, table_ref, key_info_ref, line_hot_ref,
    bin_hot_ref, input_ref, gain_ref, cotangent_ref,
    w_first, queries, keys_t, values_t, heads_out, lse, layout, line, key_extra, key_extra_t,
    slot_owner, residual, layer_output, second_grad, gate_up_full, down_full, tables,
    slot_t, w_gate_up, w_down, first_here, key_aug, query_aug, strip, scores, probs,
    second_t, second_owner, out_owner, out_t,
    hidden_a, hidden_b, hidden_c, act_t, low_t, stage_gate_up, stage_down,
    row_send, row_recv, row_own, table_send, table_recv, table_own, load_sem, store_sem, *sems,
):
    place = Place(mp_size)
    rows, model_width = input_ref.shape
    keys = keys_t.shape[1]
    blocks = keys // LANES
    width = strip.shape[1]
    inner_here = first_ref.shape[1]
    heads_here = inner_here // 64
    hidden = gate_up_ref.shape[1]
    member = lax.rem(place.mp, group)
    first_peer = place.mp - member
    own_lanes = pl.ds(pl.multiple_of(member * rows, LANES), rows)

    items = forward_items(mp_size)
    gather = Gather(
        place, [first_ref, gate_up_ref, down_ref], [w_first, w_gate_up, w_down], sems, items
    )
    at = {item: t for t, item in enumerate(items)}

    row_copies = [
        remote(
            normed_t_ref, slot_t.at[:, own_lanes], row_send.at[k], row_recv.at[k],
            (place.dp, first_peer + lax.rem(member + k, group)),
        )
        for k in range(1, group)
    ]
    table_copies = [
        remote(table_ref, tables.at[place.mp], table_send.at[k], table_recv.at[k], place.to_mp(k))
        for k in range(1, mp_size)
    ]
    row_here = Copy(normed_t_ref, slot_t.at[:, own_lanes], row_own.at[0])
    table_here = Copy(table_ref, tables.at[place.mp], table_own.at[0])

    row_here.start()
    table_here.start()
    meet(place)
    gather.start_chunk(0)
    for copy in table_copies + row_copies:
        copy.start()
    gather.start_chunk(1)
    gather.start_chunk(2)
    gather.step(0)

    key_rows = row_ids((64, keys)).astype(F32)
    x_place = jnp.where(key_rows == key_info_ref[0:1, :], 1.0, 0.0).astype(BF16)
    y_place = jnp.where(key_rows == key_info_ref[1:2, :], 1.0, 0.0).astype(BF16)
    key_extra_t[0:64, :] = x_place
    key_extra_t[64:128, :] = y_place
    tail = jnp.where(
        key_rows == 0.0, key_info_ref[2:3, :], jnp.where(key_rows < 4.0, 1.0, 0.0)
    ).astype(BF16)
    turned = jnp.concatenate([jnp.zeros((64, keys), BF16), x_place, y_place, tail], axis=0).T
    key_extra[...] = turned
    key_aug[...] = turned
    query_aug[pl.ds(192, 64), :] = jnp.where(row_ids((64, rows)) == 0, 1.0, 0.0).astype(BF16)
    gather.step(1)
    for block in range(model_width // LANES):
        owner = block_owner(block)
        out_owner[:, owner * LANES : (owner + 1) * LANES] = cotangent_ref[
            :, block * LANES : (block + 1) * LANES
        ].astype(BF16)
    out_t[...] = cotangent_ref[...].astype(BF16).T
    residual[...] = input_ref[...]
    layer_output[...] = jnp.zeros_like(layer_output)
    second_grad[...] = jnp.zeros_like(second_grad)
    row_here.wait()
    table_here.wait()
    gather.step(2)

    head_units = mp_size * heads_here
    plan = {}
    total = gather.steps
    for k in range(1, mp_size):
        need = at[(0, k)] + 2
        plan.setdefault((k * heads_here, 0), []).append(need)
    for k in range(mp_size):
        need = at[(2, k)] + 2
        plan.setdefault((head_units + k, 0), []).append(need)
    table = {}
    done = 2
    order = sorted(plan.items())
    for (unit, point), needs in order:
        need = max(needs)
        if need <= done:
            continue
        missing = list(range(done + 1, need + 1))
        spots = [(unit, 0)]
        if unit >= head_units:
            before = [(unit - 1, p) for p in (3, 2, 1)] if unit > head_units else []
            if unit == head_units:
                before = [(unit - 1, 0), (unit - 2, 0), (unit - 3, 0)]
        else:
            before = [(unit - 1, 0), (unit - 2, 0), (unit - 3, 0)]
        spots = spots + before
        for i, s in enumerate(reversed(missing)):
            table.setdefault(spots[min(i, len(spots) - 1)], []).append(s)
        done = need
    for spot in table:
        table[spot].sort()
    rest = list(range(done + 1, total))

    def communicate(unit, point):
        for (at_unit, at_point), steps in table.items():
            if at_point == point:

                @pl.when(unit == at_unit)
                def _(steps=steps):
                    for s in steps:
                        gather.step(s)

    def head_unit(unit, carry):
        communicate(unit, 0)
        step = lax.div(unit, heads_here)
        inside = lax.rem(unit, heads_here)
        source = place.from_mp(step)
        base = pl.multiple_of(source * inner_here, 16)
        head = source * heads_here + inside

        @pl.when(inside == 0)
        def _():
            for k in range(mp_size):

                @pl.when(step == k)
                def _(k=k):
                    gather.done(at[(0, k)])
                    if k == 0:
                        for copy in row_copies:
                            copy.wait_recv()
                    else:
                        table_copies[k - 1].wait_recv()

            load = Copy(w_first.at[:, pl.ds(base, inner_here), :], first_here, load_sem.at[0])
            load.start()
            hot = tables[source].astype(BF16)
            line[source] = jnp.dot(hot[0:8], line_hot_ref[...], preferred_element_type=F32)
            bins = jnp.dot(hot[8:24], bin_hot_ref[...], preferred_element_type=F32)
            for i in range(heads_here):
                x_line = jnp.broadcast_to(bins[i : i + 1], (64, LANES))
                y_line = jnp.broadcast_to(bins[8 + i : 9 + i], (64, LANES))
                left = lane_ids((64, LANES)) < 64
                x_part = pltpu.roll(x_line, 0, 1, stride=1, stride_axis=0)
                y_part = pltpu.roll(y_line, 64, 1, stride=1, stride_axis=0)
                layout[source * heads_here + i] = jnp.concatenate(
                    [jnp.where(left, x_part, 0.0), jnp.where(left, 0.0, y_part)], axis=0
                ).astype(BF16)
            load.wait()
            here = pl.ds(base, inner_here)
            queries[here, :] = jnp.dot(
                first_here[0], normed_t_ref[...], preferred_element_type=F32
            ).astype(BF16)
            keys_t[here, :] = jnp.dot(
                first_here[1], slot_t[...], preferred_element_type=F32
            ).astype(BF16)
            values_t[here, :] = jnp.dot(
                first_here[2], slot_t[...], preferred_element_type=F32
            ).astype(BF16)

        here = pl.ds(pl.multiple_of(head * 64, 16), 64)
        both = jnp.concatenate([keys_t[here, :], values_t[here, :]], axis=0).T
        low_lanes = lane_ids((keys, LANES)) < 64
        key_aug[:, 0:LANES] = jnp.where(low_lanes, both, key_extra[:, 0:LANES])
        query_aug[pl.ds(0, 64), :] = queries[here, :]
        query_aug[pl.ds(64, 128), :] = jnp.dot(
            layout[head], key_extra_t[:, own_lanes], preferred_element_type=F32
        ).astype(BF16)
        strip[...] = pltpu.roll(
            jnp.broadcast_to(line[source, pl.ds(inside, 1), :], (LANES, width)), 0, 1,
            stride=1, stride_axis=0,
        )
        query_all = query_aug[...]
        top = jnp.full((1, rows), -jnp.inf, F32)
        for block in range(blocks):
            some = pl.ds(block * LANES, LANES)
            part = jnp.dot(key_aug[some, :], query_all, preferred_element_type=F32)
            part = part + strip[:, pl.ds((blocks - 1 - block) * LANES, rows)]
            scores[some, :] = part
            top = jnp.maximum(top, jnp.max(part, axis=0, keepdims=True))
        sums = jnp.zeros((1, rows), F32)
        for block in range(blocks):
            some = pl.ds(block * LANES, LANES)
            part = jnp.exp(scores[some, :] - top)
            sums = sums + jnp.sum(part, axis=0, keepdims=True)
            probs[some, :] = part.astype(BF16)
        mixed = jnp.dot(values_t[here, :], probs[...], preferred_element_type=F32)
        heads_out[here, :] = (mixed / sums).astype(BF16)
        lse[head] = top + jnp.log(sums)

        @pl.when(inside == heads_here - 1)
        def _():
            part = heads_out[pl.ds(base, inner_here), :].T
            residual[...] = residual[...] + jnp.dot(
                part, first_here[3], preferred_element_type=F32
            )

        return carry

    lax.fori_loop(0, head_units, head_unit, 0)
    for block in range(model_width // LANES):
        owner = block_owner(block)
        slot_owner[:, owner * LANES : (owner + 1) * LANES] = slot_t[
            block * LANES : (block + 1) * LANES, :
        ].T

    def norm_rows(i, carry):
        here = pl.ds(pl.multiple_of(i * 16, 16), 16)
        values = residual[here, :]
        scale = lax.rsqrt(jnp.mean(values * values, axis=1, keepdims=True) + EPSILON)
        normed = (values * scale * gain_ref[...]).astype(BF16)
        second_owner[here, :] = normed
        return carry

    lax.fori_loop(0, rows // 16, norm_rows, 0)
    second_t[...] = second_owner[...].T
    turned_blocks = [second_owner[:, b * LANES : (b + 1) * LANES] for b in range(model_width // LANES)]
    for block, values in enumerate(turned_blocks):
        owner = block_owner(block)
        second_owner[:, owner * LANES : (owner + 1) * LANES] = values

    def store(step):
        source = place.from_mp(step)
        here = pl.ds(pl.multiple_of(source * hidden, 16), hidden)
        return [
            Copy(stage_gate_up, gate_up_full.at[:, here, :], store_sem.at[0]),
            Copy(stage_down, down_full.at[:, here, :], store_sem.at[1]),
        ]

    def hidden_unit(step, carry):
        unit = step + head_units
        communicate(unit, 0)
        source = place.from_mp(step)
        here = pl.ds(pl.multiple_of(source * hidden, 16), hidden)
        for k in range(mp_size):

            @pl.when(step == k)
            def _(k=k):
                gather.done(at[(1, k)])
                gather.done(at[(2, k)])

        hidden_a[...] = jnp.dot(w_gate_up[0, here, :], second_t[...], preferred_element_type=F32)
        hidden_b[...] = jnp.dot(w_gate_up[1, here, :], second_t[...], preferred_element_type=F32)
        communicate(unit, 1)
        hidden_c[...] = jnp.dot(w_down[0, here, :], out_t[...], preferred_element_type=F32)

        def activate(i, inner_carry):
            some = pl.ds(pl.multiple_of(i * 16, 16), 16)
            gate, up, slope = hidden_a[some, :], hidden_b[some, :], hidden_c[some, :]
            square = gate * gate
            factor = 0.7978845608028654
            bent = jnp.tanh(factor * gate * (1.0 + 0.044715 * square))
            half = 0.5 * (1.0 + bent)
            value = gate * half
            change = half + 0.5 * gate * (1.0 - bent * bent) * (
                factor * (1.0 + 3.0 * 0.044715 * square)
            )
            act_t[some, :] = (value * up).astype(BF16)
            low_t[some, :] = (slope * up * change).astype(BF16)
            low_t[pl.ds(pl.multiple_of(hidden + i * 16, 16), 16), :] = (slope * value).astype(BF16)
            return inner_carry

        lax.fori_loop(0, hidden // 16, activate, 0)
        communicate(unit, 2)

        @pl.when(step > 0)
        def _():
            for copy in store(step):
                copy.wait()

        stage_down[0] = jnp.dot(act_t[...], out_owner[...], preferred_element_type=F32).astype(BF16)
        stage_gate_up[0] = jnp.dot(
            low_t[0:hidden], second_owner[...], preferred_element_type=F32
        ).astype(BF16)
        stage_gate_up[1] = jnp.dot(
            low_t[hidden:], second_owner[...], preferred_element_type=F32
        ).astype(BF16)
        for copy in store(step):
            copy.start()
        communicate(unit, 3)
        layer_output[...] = layer_output[...] + dot_f32(act_t[...].T, w_down[0, here, :], 1, 0)
        second_grad[...] = (
            second_grad[...]
            + dot_f32(low_t[0:hidden].T, w_gate_up[0, here, :], 1, 0)
            + dot_f32(low_t[hidden:].T, w_gate_up[1, here, :], 1, 0)
        )
        return carry

    lax.fori_loop(0, mp_size, hidden_unit, 0)
    layer_output[...] = layer_output[...] + residual[...]
    for s in rest:
        gather.step(s)
    for copy in store(mp_size - 1):
        copy.wait()
    gather.close()
    for copy in row_copies + table_copies:
        copy.wait_send()


def block_owner(block):
    return (block % 2) * 4 + block // 2


def forward(mp_size, group, pieces, normed_t, table, key_info, line_hot, bin_hot, layer_input, gain, cotangent):
    first, gate_up, down = pieces
    rows, model_width = layer_input.shape
    keys = key_info.shape[1]
    width = line_hot.shape[1]
    inner_here, hidden = first.shape[1], gate_up.shape[1]
    inner, total_hidden = inner_here * mp_size, hidden * mp_size
    head_count = inner // 64
    dma = pltpu.SemaphoreType.DMA
    hbm = pl.BlockSpec(memory_space=HBM)
    vmem = pl.BlockSpec(memory_space=pltpu.VMEM)
    shape = jax.ShapeDtypeStruct
    out = [
        (shape((4, inner, model_width), BF16), hbm),
        (shape((inner, rows), BF16), vmem),
        (shape((inner, keys), BF16), vmem),
        (shape((inner, keys), BF16), vmem),
        (shape((inner, rows), BF16), vmem),
        (shape((head_count, 1, rows), F32), vmem),
        (shape((head_count, 128, 128), BF16), vmem),
        (shape((mp_size, 8, width), F32), vmem),
        (shape((keys, 256), BF16), vmem),
        (shape((128, keys), BF16), vmem),
        (shape((keys, model_width), BF16), vmem),
        (shape((rows, model_width), F32), vmem),
        (shape((rows, model_width), F32), vmem),
        (shape((rows, model_width), F32), vmem),
        (shape((2, total_hidden, model_width), BF16), hbm),
        (shape((1, total_hidden, model_width), BF16), hbm),
        (shape((mp_size, 24, LANES), F32), vmem),
    ]
    return pl.pallas_call(
        partial(forward_kernel, mp_size, group),
        out_shape=tuple(o[0] for o in out),
        in_specs=[hbm] * 3 + [vmem] * 8,
        out_specs=tuple(o[1] for o in out),
        scratch_shapes=[
            pltpu.VMEM((model_width, keys), BF16),
            pltpu.VMEM((2, total_hidden, model_width), BF16),
            pltpu.VMEM((1, total_hidden, model_width), BF16),
            pltpu.VMEM((4, inner_here, model_width), BF16),
            pltpu.VMEM((keys, 256), BF16),
            pltpu.VMEM((256, rows), BF16),
            pltpu.VMEM((LANES, width), F32),
            pltpu.VMEM((keys, rows), F32),
            pltpu.VMEM((keys, rows), BF16),
            pltpu.VMEM((model_width, rows), BF16),
            pltpu.VMEM((rows, model_width), BF16),
            pltpu.VMEM((rows, model_width), BF16),
            pltpu.VMEM((model_width, rows), BF16),
            pltpu.VMEM((hidden, rows), F32),
            pltpu.VMEM((hidden, rows), F32),
            pltpu.VMEM((hidden, rows), F32),
            pltpu.VMEM((hidden, rows), BF16),
            pltpu.VMEM((2 * hidden, rows), BF16),
            pltpu.VMEM((2, hidden, model_width), BF16),
            pltpu.VMEM((1, hidden, model_width), BF16),
            dma((group,)), dma((group,)), dma((1,)),
            dma((mp_size,)), dma((mp_size,)), dma((1,)), dma((1,)), dma((2,)),
        ]
        + Gather.semaphores(3, mp_size),
        compiler_params=pltpu.CompilerParams(
            collective_id=0, has_side_effects=True, vmem_limit_bytes=62 << 20
        ),
        name="forward",
    )(first, gate_up, down, normed_t, table, key_info, line_hot, bin_hot, layer_input, gain, cotangent)


def backward_items(mp_size):
    order = list(range(1, mp_size)) + [0]
    items = [(c, order[0]) for c in (0, 1)]
    for last, k in zip(order, order[1:]):
        items += [(0, k), (1, k), (2, last)]
    return items + [(2, order[-1])]


def unskewed(values, first, count, shift):
    width = values.shape[1]
    folded = None
    for group in range(count // 8):
        part = values[pl.ds(first + group * 8, 8), :]
        back = (-(group * 8 + shift)) % width
        part = pltpu.roll(part, back, 1) if back else part
        folded = part if folded is None else folded + part
    total = folded[0:1]
    for row in range(1, 8):
        total = total + pltpu.roll(folded[row : row + 1], width - row, 1)
    return total


def exact_dot(left, right):
    parts = three_parts(left)
    return sum(dot_f32(part, right, 1, 1) for part in parts)


def backward_kernel(mp_size, group, *refs):
    (
        gate_up_full, down_full, w_first, queries, keys_t, values_t, heads_out,
        residual_in, second_in, cotangent_in,
        lse, layout, line, key_extra, key_extra_t, slot_owner, layer_input, gains, line_hot, bin_hot,
        input_grad, small_out, gate_up_sum, down_sum, first_sum,
        *refs,
    ) = refs
    (
        slot_grad, own_grad, residual_grad, branch_owner, branch_t, w_query, w_output, w_kv,
        q_here, k_here, v_here, out_here, grad_here, dq_here, dk_here, dv_here, kv_here,
        key_aug, key_aug_t, query_aug, value_aug, grad_aug, strip, strip_grad, probs_grad,
        layout_grad, line_sums, bin_sums, gain_part, rows_out, peers, stage, stage_in, full_here,
        load_sem, value_sem, row_send, row_recv, stage_send, stage_recv,
        *refs,
    ) = refs
    place = Place(mp_size)
    rows, model_width = layer_input.shape
    keys = slot_owner.shape[0]
    blocks = keys // LANES
    inner_here = q_here.shape[0]
    heads_here = inner_here // 64
    member = lax.rem(place.mp, group)
    first_peer = place.mp - member
    own_start = pl.multiple_of(member * rows, LANES)
    own_lanes = pl.ds(own_start, rows)

    items = backward_items(mp_size)
    fulls = [gate_up_full, down_full, full_here]
    scatter = Scatter(place, fulls, [gate_up_sum, down_sum, first_sum], refs, items)

    loads = [
        Copy(second_in, slot_grad.at[pl.ds(0, rows), :], value_sem.at[0]),
        Copy(residual_in, slot_grad.at[pl.ds(rows, rows), :], value_sem.at[1]),
        Copy(cotangent_in, input_grad, value_sem.at[2]),
    ]
    for copy in loads:
        copy.start()
    meet(place)
    scatter.step(0)
    key_aug[...] = key_extra[...]
    key_aug_t[pl.ds(64, 128), :] = key_extra_t[...]
    for copy in loads:
        copy.wait()

    def norm_back(i, total):
        here = pl.ds(pl.multiple_of(i * 16, 16), 16)
        grad = slot_grad[here, :]
        values = slot_grad[pl.ds(pl.multiple_of(rows + i * 16, 16), 16), :]
        scale = lax.rsqrt(jnp.mean(values * values, axis=1, keepdims=True) + EPSILON)
        scaled = gains[1:2, :] * grad
        mean = jnp.mean(scaled * values, axis=1, keepdims=True)
        result = input_grad[here, :] + scale * scaled - values * (scale * scale * scale * mean)
        residual_grad[here, :] = result
        branch_owner[here, :] = result.astype(BF16)
        product = grad * values * scale
        return total + product[0:8] + product[8:16]

    total = lax.fori_loop(0, rows // 16, norm_back, jnp.zeros((8, model_width), F32))
    gain_part[1:2, :] = jnp.sum(total, axis=0, keepdims=True)
    scatter.step(1)
    branch_t[...] = branch_owner[...].T
    parts = [branch_owner[:, b * LANES : (b + 1) * LANES] for b in range(model_width // LANES)]
    for block, values in enumerate(parts):
        owner = block_owner(block)
        branch_owner[:, owner * LANES : (owner + 1) * LANES] = values
    slot_grad[...] = jnp.zeros_like(slot_grad)
    own_grad[...] = jnp.zeros_like(own_grad)
    scatter.step(2)

    plan = {}
    for block in range(mp_size - 1):
        plan[(block, 1)] = [3 * block + 3]
        plan[(block, 2)] = [3 * block + 4]
        if block + 2 < mp_size:
            plan[(block + 1, 0)] = [3 * block + 5]
    done = 3 * mp_size - 1
    plan[(mp_size - 1, 2)] = [done]

    def communicate(block, point):
        for (at_block, at_point), steps in plan.items():
            if at_point == point:

                @pl.when(block == at_block)
                def _(steps=steps):
                    for s in steps:
                        scatter.step(s)

    def block_unit(block, carry):
        communicate(block, 0)
        step = lax.rem(block + 1, mp_size)
        target = lax.rem(place.mp + step, mp_size)
        base = pl.multiple_of(target * inner_here, 16)
        here = pl.ds(base, inner_here)
        slot = lax.rem(block, 2)
        copies = [
            Copy(w_first.at[0, here, :], w_query, load_sem.at[0]),
            Copy(w_first.at[3, here, :], w_output, load_sem.at[1]),
            Copy(queries.at[here, :], q_here, load_sem.at[2]),
            Copy(keys_t.at[here, :], k_here, load_sem.at[3]),
            Copy(values_t.at[here, :], v_here, load_sem.at[4]),
            Copy(heads_out.at[here, :], out_here, load_sem.at[5]),
        ]
        for i in range(heads_here):
            for part in range(2):
                copies.append(
                    Copy(
                        w_first.at[1 + part, pl.ds(pl.multiple_of(base + i * 64, 16), 64), :],
                        w_kv.at[pl.ds(i * 128 + part * 64, 64), :],
                        load_sem.at[6 + 2 * i + part],
                    )
                )
        for copy in copies:
            copy.start()
        for copy in copies:
            copy.wait()

        for b in range(2, mp_size):

            @pl.when(block == b)
            def _(b=b):
                scatter.left(items.index((2, (b - 1) % mp_size)))

        grad_here[...] = jnp.dot(w_output[...], branch_t[...], preferred_element_type=F32).astype(BF16)
        full_here[slot, 3] = jnp.dot(
            out_here[...], branch_owner[...], preferred_element_type=F32
        ).astype(BF16)

        def head_unit(inside, inner_carry):
            head = target * heads_here + inside
            some = pl.ds(pl.multiple_of(inside * 64, 16), 64)
            q_head, k_head, v_head = q_here[some, :], k_here[some, :], v_here[some, :]
            grad_head = grad_here[some, :]
            both = jnp.concatenate([k_head, v_head], axis=0).T
            lanes = lane_ids((keys, LANES))
            key_aug[:, 0:LANES] = jnp.where(lanes < 64, both, key_extra[:, 0:LANES])
            ones = jnp.where(lanes < 3, 1.0, 0.0).astype(BF16)
            value_aug[...] = jnp.where(lanes < 64, ones, both)
            key_aug_t[pl.ds(0, 64), :] = k_head
            query_aug[pl.ds(0, 64), :] = q_head
            query_aug[pl.ds(64, 128), :] = jnp.dot(
                layout[head], key_extra_t[:, own_lanes], preferred_element_type=F32
            ).astype(BF16)
            high, middle, low = three_parts(-lse[head])
            tail = row_ids((64, rows))
            rows_of = lambda part: jnp.broadcast_to(part.astype(F32), (64, rows))
            query_aug[pl.ds(192, 64), :] = jnp.where(
                tail == 0, 1.0,
                jnp.where(
                    tail == 1, rows_of(high),
                    jnp.where(tail == 2, rows_of(middle), jnp.where(tail == 3, rows_of(low), 0.0)),
                ),
            ).astype(BF16)
            row_dot = jnp.sum(
                grad_head.astype(F32) * out_here[some, :].astype(F32), axis=0, keepdims=True
            )
            high, middle, low = three_parts(-row_dot)
            grad_aug[pl.ds(0, 64), :] = jnp.where(
                tail == 0, rows_of(high),
                jnp.where(tail == 1, rows_of(middle), jnp.where(tail == 2, rows_of(low), 0.0)),
            ).astype(BF16)
            grad_aug[pl.ds(64, 64), :] = grad_head
            width = strip.shape[1]
            strip[...] = pltpu.roll(
                jnp.broadcast_to(line[target, pl.ds(inside, 1), :], (LANES, width)), 0, 1,
                stride=1, stride_axis=0,
            )
            strip_grad[...] = jnp.zeros_like(strip_grad)
            query_and_grad = jnp.concatenate([q_head, grad_head], axis=0).T
            query_all = query_aug[...]
            grad_all = grad_aug[...]
            half = lane_ids((LANES, LANES)) < 64
            kv_lanes = pl.ds(pl.multiple_of(inside * LANES, LANES), LANES)
            for part_index in range(blocks):
                these = pl.ds(part_index * LANES, LANES)
                band = pl.ds((blocks - 1 - part_index) * LANES, rows)
                part = jnp.dot(key_aug[these, :], query_all, preferred_element_type=F32)
                part = jnp.exp(part + strip[:, band])
                slope = part * jnp.dot(value_aug[these, :], grad_all, preferred_element_type=F32)
                strip_grad[:, band] = strip_grad[:, band] + slope
                slope = slope.astype(BF16)
                probs_grad[these, :] = slope
                key_part = jnp.dot(slope, query_and_grad, preferred_element_type=F32)
                value_part = jnp.dot(part.astype(BF16), query_and_grad, preferred_element_type=F32)
                joined = jnp.where(half, key_part, value_part)
                kv_here[these, kv_lanes] = joined.astype(BF16)
                turned = joined.T.astype(BF16)
                dk_here[some, these] = turned[0:64]
                dv_here[some, these] = turned[64:128]
            query_part = jnp.dot(key_aug_t[...], probs_grad[...], preferred_element_type=F32)
            dq_here[some, :] = query_part[0:64].astype(BF16)
            bins = dot_f32(query_part[64:192].astype(BF16), key_extra_t[:, own_lanes], 1, 1)
            left = lane_ids((LANES, LANES)) < 64
            upper = row_ids((LANES, LANES)) < 64
            layout_grad[...] = jnp.where(left == upper, bins, 0.0)
            bin_sums[0, pl.ds(head, 1), :] = unskewed(layout_grad, 0, 64, 0)
            bin_sums[1, pl.ds(head, 1), :] = unskewed(layout_grad, 64, 64, 64)
            line_sums[pl.ds(head, 1), :] = unskewed(strip_grad, 0, LANES, 0)
            return inner_carry

        half_heads = heads_here // 2
        lax.fori_loop(0, half_heads, head_unit, 0)
        communicate(block, 1)
        lax.fori_loop(half_heads, heads_here, head_unit, 0)
        full_here[slot, 0] = jnp.dot(
            dq_here[...], slot_owner[pl.ds(own_start, rows), :], preferred_element_type=F32
        ).astype(BF16)
        full_here[slot, 1] = jnp.dot(
            dk_here[...], slot_owner[...], preferred_element_type=F32
        ).astype(BF16)
        full_here[slot, 2] = jnp.dot(
            dv_here[...], slot_owner[...], preferred_element_type=F32
        ).astype(BF16)
        slot_grad[...] = slot_grad[...] + jnp.dot(
            kv_here[...], w_kv[...], preferred_element_type=F32
        )
        own_grad[...] = own_grad[...] + jnp.dot(
            dq_here[...].T, w_query[...], preferred_element_type=F32
        )
        communicate(block, 2)
        return carry

    lax.fori_loop(0, mp_size, block_unit, 0)

    copies = []
    for k in range(1, group):
        other = lax.rem(member + k, group)
        rows_out[k - 1] = slot_grad[pl.ds(pl.multiple_of(other * rows, 16), rows), :].astype(BF16)
        copies.append(
            remote(
                rows_out.at[k - 1], peers.at[k - 1], row_send.at[k], row_recv.at[k],
                (place.dp, first_peer + other),
            )
        )
    for copy in copies:
        copy.start()
    steps = list(range(done + 1, scatter.steps))
    for s in steps[:1]:
        scatter.step(s)

    gain_rows = model_width // LANES
    head_count = bin_sums.shape[1]
    stage[0, 2 * gain_rows : 2 * gain_rows + head_count, :] = exact_dot(line_sums[...], line_hot[...])
    for i in range(2):
        start = 2 * gain_rows + (1 + i) * head_count
        stage[0, start : start + head_count, :] = exact_dot(bin_sums[i], bin_hot[...])
    for s in steps[1:2]:
        scatter.step(s)
    for copy in copies:
        copy.wait_recv()

    def input_back(i, total):
        here = pl.ds(pl.multiple_of(i * 16, 16), 16)
        grad = own_grad[here, :] + slot_grad[pl.ds(pl.multiple_of(own_start + i * 16, 16), 16), :]
        for k in range(group - 1):
            grad = grad + peers[k, here, :].astype(F32)
        values = layer_input[here, :]
        scale = lax.rsqrt(jnp.mean(values * values, axis=1, keepdims=True) + EPSILON)
        scaled = gains[0:1, :] * grad
        mean = jnp.mean(scaled * values, axis=1, keepdims=True)
        input_grad[here, :] = (
            residual_grad[here, :] + scale * scaled - values * (scale * scale * scale * mean)
        )
        product = grad * values * scale
        return total + product[0:8] + product[8:16]

    total = lax.fori_loop(0, rows // 16, input_back, jnp.zeros((8, model_width), F32))
    gain_part[0:1, :] = jnp.sum(total, axis=0, keepdims=True)
    for which in range(2):
        for i in range(gain_rows):
            row = which * gain_rows + i
            stage[0, row : row + 1, :] = gain_part[which : which + 1, i * LANES : (i + 1) * LANES]

    partners = [place.to_core, place.to_x, place.to_y]
    bit = 1
    while bit < mp_size:
        flipped = place.mp + bit - 2 * bit * lax.rem(lax.div(place.mp, bit), 2)
        partners.append((place.dp, flipped))
        bit *= 2
    sums = [
        remote(stage.at[i], stage_in.at[i], stage_send.at[i], stage_recv.at[i], partner)
        for i, partner in enumerate(partners)
    ]
    sums[0].start()
    steps = steps[2:]
    for i, copy in enumerate(sums):
        for s in steps[:1]:
            scatter.step(s)
        steps = steps[1:]
        copy.wait_recv()
        if i + 1 < len(sums):
            stage[i + 1] = stage[i] + stage_in[i]
            sums[i + 1].start()
        else:
            small_out[...] = stage[i] + stage_in[i]
    for s in steps:
        scatter.step(s)
    scatter.close()
    for copy in copies + sums:
        copy.wait_send()


def backward(
    mp_size, group, gate_up_full, down_full, w_first, queries, keys_t, values_t, heads_out,
    residual, second_grad, cotangent, lse, layout, line, key_extra, key_extra_t, slot_owner,
    layer_input, gains, line_hot, bin_hot,
):
    rows, model_width = layer_input.shape
    keys = slot_owner.shape[0]
    width = line.shape[2]
    inner_here = queries.shape[0] // mp_size
    heads_here = inner_here // 64
    head_count = heads_here * mp_size
    hidden = down_full.shape[1] // mp_size
    sizes = [(2, hidden), (1, hidden), (4, inner_here)]
    count = 3 + (mp_size - 1).bit_length()
    small_rows = 2 * model_width // LANES + 3 * head_count
    others = max(group - 1, 1)
    dma = pltpu.SemaphoreType.DMA
    hbm = pl.BlockSpec(memory_space=HBM)
    vmem = pl.BlockSpec(memory_space=pltpu.VMEM)
    shape = jax.ShapeDtypeStruct
    return pl.pallas_call(
        partial(backward_kernel, mp_size, group),
        out_shape=(
            shape((rows, model_width), F32),
            shape((small_rows, LANES), F32),
            *[shape((lead, n, LANES), F32) for lead, n in sizes],
        ),
        in_specs=[hbm] * 10 + [vmem] * 10,
        out_specs=(vmem,) * 5,
        scratch_shapes=[
            pltpu.VMEM((keys, model_width), F32),
            pltpu.VMEM((rows, model_width), F32),
            pltpu.VMEM((rows, model_width), F32),
            pltpu.VMEM((rows, model_width), BF16),
            pltpu.VMEM((model_width, rows), BF16),
            pltpu.VMEM((inner_here, model_width), BF16),
            pltpu.VMEM((inner_here, model_width), BF16),
            pltpu.VMEM((2 * inner_here, model_width), BF16),
            pltpu.VMEM((inner_here, rows), BF16),
            pltpu.VMEM((inner_here, keys), BF16),
            pltpu.VMEM((inner_here, keys), BF16),
            pltpu.VMEM((inner_here, rows), BF16),
            pltpu.VMEM((inner_here, rows), BF16),
            pltpu.VMEM((inner_here, rows), BF16),
            pltpu.VMEM((inner_here, keys), BF16),
            pltpu.VMEM((inner_here, keys), BF16),
            pltpu.VMEM((keys, heads_here * LANES), BF16),
            pltpu.VMEM((keys, 256), BF16),
            pltpu.VMEM((192, keys), BF16),
            pltpu.VMEM((256, rows), BF16),
            pltpu.VMEM((keys, LANES), BF16),
            pltpu.VMEM((LANES, rows), BF16),
            pltpu.VMEM((LANES, width), F32),
            pltpu.VMEM((LANES, width), F32),
            pltpu.VMEM((keys, rows), BF16),
            pltpu.VMEM((LANES, LANES), F32),
            pltpu.VMEM((head_count, width), F32),
            pltpu.VMEM((2, head_count, LANES), F32),
            pltpu.VMEM((2, model_width), F32),
            pltpu.VMEM((others, rows, model_width), BF16),
            pltpu.VMEM((others, rows, model_width), BF16),
            pltpu.VMEM((count, small_rows, LANES), F32),
            pltpu.VMEM((count, small_rows, LANES), F32),
            pltpu.VMEM((2, 4, inner_here, model_width), BF16),
            dma((6 + 2 * heads_here,)), dma((3,)), dma((group,)), dma((group,)),
            dma((count,)), dma((count,)),
        ]
        + Scatter.scratch(sizes, (True, True, False), mp_size),
        compiler_params=pltpu.CompilerParams(
            collective_id=1, has_side_effects=True, vmem_limit_bytes=63 << 20
        ),
        name="backward",
    )(
        gate_up_full, down_full, w_first, queries, keys_t, values_t, heads_out, residual,
        second_grad, cotangent, lse, layout, line, key_extra, key_extra_t, slot_owner, layer_input,
        gains, line_hot, bin_hot,
    )


def line_onehot(first_row, width, key_blocks):
    place = jnp.arange(width, dtype=jnp.int32)
    place = jnp.where(place >= width - LANES, place - width, place)
    offset = LANES * (key_blocks - 1) - place - first_row
    return (bucket_of(offset)[:, None] == jnp.arange(32, dtype=jnp.int32)[None, :]).astype(F32)


def bin_onehot():
    bins = np.arange(NBIN)
    offset = bins[:, None] - bins[None, :]
    distance = np.abs(offset)
    bucket = np.minimum(distance, 7) + sum((distance >= t).astype(np.int64) for t in THRESHOLDS)
    bucket = bucket + 16 * (offset > 0)
    return jnp.asarray(bucket[:, :, None] == np.arange(32), F32)


def gather_rows(local, axis_name):
    return lax.all_gather(local, axis_name, axis=0, tiled=True)


def scatter_grad(full):
    summed = lax.psum_scatter(full, "dp", scatter_dimension=1, tiled=True)
    return lax.psum_scatter(summed, "mp", scatter_dimension=0, tiled=True)


def per_device_plain(
    dp_size, mp_size,
    layer_input, norm_gains, query_weight, key_value_weight, output_weight,
    gate_up_weight, down_weight, bias_tables, doc_lengths, box_bins, cotangent,
):
    rows, model_width = layer_input.shape
    doc_count = doc_lengths.shape[0]
    slot_span = box_bins.shape[1] // doc_count
    group = mp_size // doc_count
    mp_index = lax.axis_index("mp")
    doc = mp_index // group
    first_row = (mp_index % group) * rows
    key_blocks = slot_span // LANES
    width = LANES * (key_blocks + (rows + LANES - 1) // LANES)
    groups = [[d * group + i for i in range(group)] for d in range(doc_count)]
    gain_first = norm_gains[0].astype(F32)
    gain_second = norm_gains[1].astype(F32)

    w_query = gather_rows(query_weight.T, "mp")
    inner_here = query_weight.shape[1]
    inner = inner_here * mp_size
    w_key = gather_rows(key_value_weight[:, 0].T, "mp")
    w_value = gather_rows(key_value_weight[:, 1].T, "mp")
    w_output = gather_rows(output_weight, "mp")
    w_gate = gather_rows(gate_up_weight[:, 0].T, "mp")
    w_up = gather_rows(gate_up_weight[:, 1].T, "mp")
    w_down = gather_rows(down_weight, "mp")
    tables = lax.all_gather(bias_tables, "mp", axis=2, tiled=True).astype(F32)
    head_count = tables.shape[2]

    onehot_line = line_onehot(first_row, width, key_blocks)
    line = jnp.dot(onehot_line, tables[0], precision=lax.Precision.HIGHEST)
    line = line.T.reshape(head_count, 1, width)
    onehot_bin = bin_onehot()
    x_part = jnp.einsum("ban,nh->hba", onehot_bin, tables[1], precision=lax.Precision.HIGHEST)
    y_part = jnp.einsum("ban,nh->hba", onehot_bin, tables[2], precision=lax.Precision.HIGHEST)
    empty = jnp.zeros_like(x_part)
    layout = jnp.concatenate(
        [jnp.concatenate([x_part, empty], axis=2), jnp.concatenate([empty, y_part], axis=2)], axis=1
    ).astype(BF16)
    key_bins = lax.dynamic_slice(box_bins, (0, doc * slot_span), (2, slot_span))
    own_bins = lax.dynamic_slice(key_bins, (0, first_row), (2, rows))
    bin_ids = jnp.arange(NBIN, dtype=jnp.int32)

    def placed_rows(bins):
        return jnp.concatenate(
            [bins[0][:, None] == bin_ids, bins[1][:, None] == bin_ids], axis=1
        ).astype(BF16)

    def placed_lanes(bins):
        return jnp.concatenate(
            [bin_ids[:, None] == bins[0][None], bin_ids[:, None] == bins[1][None]], axis=0
        ).astype(BF16)

    length = lax.dynamic_index_in_dim(doc_lengths, doc, keepdims=False)
    masked = jnp.arange(slot_span, dtype=jnp.int32)[:, None] >= length
    key_placed = placed_rows(key_bins)
    key_extra = jnp.concatenate(
        [
            jnp.zeros((slot_span, 64), BF16),
            key_placed,
            jnp.where(masked, NEG_FILL, 0.0).astype(BF16),
            jnp.ones((slot_span, 3), BF16),
            jnp.zeros((slot_span, 60), BF16),
        ],
        axis=1,
    )
    key_extra_t = placed_lanes(key_bins)
    query_bins_t = placed_rows(own_bins)
    query_bins = placed_lanes(own_bins)

    scale_first = inverse_rms(layer_input)
    normed = (layer_input * scale_first * gain_first).astype(BF16)
    slot_normed = lax.all_gather(normed, "mp", axis=0, tiled=True, axis_index_groups=groups)
    queries = dot_f32(w_query, normed, 1, 1).astype(BF16)
    keys_t = dot_f32(w_key, slot_normed, 1, 1).astype(BF16)
    values_t = dot_f32(w_value, slot_normed, 1, 1).astype(BF16)
    heads_out, lse = attend(queries, keys_t, values_t, layout, line, key_extra, query_bins)
    residual = layer_input + dot_f32(heads_out, w_output, 0, 0)
    scale_second = inverse_rms(residual)
    normed_second = (residual * scale_second * gain_second).astype(BF16)
    gate = dot_f32(normed_second, w_gate, 1, 1)
    up = dot_f32(normed_second, w_up, 1, 1)
    gelu_value, gelu_pull = jax.vjp(lambda v: jax.nn.gelu(v, approximate=True), gate)
    activated = (gelu_value * up).astype(BF16)
    layer_output = residual + dot_f32(activated, w_down, 1, 0)

    out_low = cotangent.astype(BF16)
    down_full = dot_f32(activated, out_low, 0, 0).astype(BF16)
    act_grad = dot_f32(out_low, w_down, 1, 1)
    gate_low = gelu_pull(act_grad * up)[0].astype(BF16)
    up_low = (act_grad * gelu_value).astype(BF16)
    gate_full = dot_f32(gate_low, normed_second, 0, 0).astype(BF16)
    up_full = dot_f32(up_low, normed_second, 0, 0).astype(BF16)
    second_grad = dot_f32(gate_low, w_gate, 1, 0) + dot_f32(up_low, w_up, 1, 0)
    gain_second_grad = jnp.sum(second_grad * residual * scale_second, axis=0)
    scaled = gain_second * second_grad
    residual_grad = (
        cotangent
        + scale_second * scaled
        - residual * scale_second**3 * jnp.mean(scaled * residual, axis=-1, keepdims=True)
    )

    branch_low = residual_grad.astype(BF16)
    output_full = dot_f32(heads_out, branch_low, 1, 0).astype(BF16)
    heads_grad = dot_f32(w_output, branch_low, 1, 1).astype(BF16)
    dq, dk, dv, line_grad, layout_grad = attend_back(
        queries, keys_t, values_t, heads_out, heads_grad, lse, layout, line,
        key_extra, key_extra_t, query_bins, query_bins_t,
    )
    query_full = dot_f32(dq, normed, 1, 0).astype(BF16)
    key_full = dot_f32(dk, slot_normed, 1, 0).astype(BF16)
    value_full = dot_f32(dv, slot_normed, 1, 0).astype(BF16)
    slot_grad = dot_f32(dk, w_key, 0, 0) + dot_f32(dv, w_value, 0, 0)
    first_grad = lax.psum_scatter(
        slot_grad.astype(BF16), "mp", scatter_dimension=0, tiled=True, axis_index_groups=groups
    ).astype(F32) + dot_f32(dq, w_query, 0, 0)
    gain_first_grad = jnp.sum(first_grad * layer_input * scale_first, axis=0)
    scaled = gain_first * first_grad
    input_grad = (
        residual_grad
        + scale_first * scaled
        - layer_input * scale_first**3 * jnp.mean(scaled * layer_input, axis=-1, keepdims=True)
    )

    gain_grad = lax.psum_scatter(
        jnp.stack([gain_first_grad, gain_second_grad]), ("dp", "mp"), scatter_dimension=1, tiled=True
    )
    line_part = jnp.dot(
        onehot_line.T, line_grad[:, 0].T, precision=lax.Precision.HIGHEST
    )
    x_part = jnp.einsum(
        "ban,hba->nh", onehot_bin, layout_grad[:, :64, :64], precision=lax.Precision.HIGHEST
    )
    y_part = jnp.einsum(
        "ban,hba->nh", onehot_bin, layout_grad[:, 64:, 64:], precision=lax.Precision.HIGHEST
    )
    table_full = jnp.stack([line_part, x_part, y_part])
    table_grad = lax.psum_scatter(
        lax.psum_scatter(table_full, "mp", scatter_dimension=2, tiled=True),
        "dp", scatter_dimension=1, tiled=True,
    )

    query_grad = scatter_grad(query_full).T.astype(F32)
    key_value_grad = jnp.stack(
        [scatter_grad(key_full).T, scatter_grad(value_full).T], axis=1
    ).astype(F32)
    output_grad = scatter_grad(output_full).astype(F32)
    gate_up_grad = jnp.stack(
        [scatter_grad(gate_full).T, scatter_grad(up_full).T], axis=1
    ).astype(F32)
    down_grad = scatter_grad(down_full).astype(F32)
    return (
        layer_output, input_grad, gain_grad, query_grad, key_value_grad,
        output_grad, gate_up_grad, down_grad, table_grad,
    )


def per_device_linked(
    dp_size, mp_size,
    layer_input, norm_gains, query_weight, key_value_weight, output_weight,
    gate_up_weight, down_weight, bias_tables, doc_lengths, box_bins, cotangent,
):
    rows, model_width = layer_input.shape
    doc_count = doc_lengths.shape[0]
    slot_span = box_bins.shape[1] // doc_count
    group = mp_size // doc_count
    dp_index, mp_index = lax.axis_index("dp"), lax.axis_index("mp")
    doc = mp_index // group
    first_row = (mp_index % group) * rows
    key_blocks = slot_span // LANES
    width = LANES * (key_blocks + rows // LANES)
    heads_here = bias_tables.shape[2]
    head_count = heads_here * mp_size
    gain_second = norm_gains[1:2].astype(F32)

    column = ((dp_index % 2) * 4 + dp_index // 2) * LANES
    piece = lambda weight, axis: lax.dynamic_slice_in_dim(weight, column, LANES, axis)
    key_value_piece = jnp.transpose(piece(key_value_weight, 0), (1, 2, 0))
    pieces = [
        jnp.stack(
            [
                piece(query_weight, 0).T, key_value_piece[0], key_value_piece[1], piece(output_weight, 1)
            ]
        ),
        jnp.transpose(piece(gate_up_weight, 0), (1, 2, 0)),
        piece(down_weight, 1)[None],
    ]
    table = jnp.swapaxes(bias_tables.astype(F32), 1, 2)
    table = jnp.pad(table, ((0, 0), (0, 8 - heads_here), (0, LANES - 32))).reshape(24, LANES)

    onehot_line = line_onehot(first_row, width, key_blocks)
    line_hot = jnp.pad(onehot_line.T, ((0, LANES - 32), (0, 0))).astype(BF16)
    place = jnp.arange(LANES, dtype=jnp.int32)
    place = jnp.where(place < NBIN, place, place - LANES)
    bin_hot = (bucket_of(-place)[None, :] == jnp.arange(LANES, dtype=jnp.int32)[:, None]).astype(BF16)
    key_bins = lax.dynamic_slice(box_bins, (0, doc * slot_span), (2, slot_span))
    length = lax.dynamic_index_in_dim(doc_lengths, doc, keepdims=False)
    masked = jnp.arange(slot_span, dtype=jnp.int32)[None, :] >= length
    key_info = jnp.concatenate(
        [key_bins.astype(F32), jnp.where(masked, NEG_FILL, 0.0), jnp.zeros((5, slot_span), F32)]
    )

    scale_first = inverse_rms(layer_input)
    normed_t = (layer_input * scale_first * norm_gains[0].astype(F32)).astype(BF16).T
    (
        w_first, queries, keys_t, values_t, heads_out, lse, layout, line, key_extra, key_extra_t,
        slot_owner, residual, layer_output, second_grad, gate_up_full, down_full, _,
    ) = forward(
        mp_size, group, pieces, normed_t, table, key_info, line_hot, bin_hot, layer_input,
        gain_second, cotangent,
    )
    input_grad, small, gate_up_sum, down_sum, summed = backward(
        mp_size, group, gate_up_full, down_full, w_first, queries, keys_t, values_t, heads_out,
        residual, second_grad, cotangent, lse, layout, line, key_extra, key_extra_t, slot_owner,
        layer_input, norm_gains.astype(F32), line_hot, bin_hot,
    )
    gain_rows = model_width // LANES
    gains = small[: 2 * gain_rows].reshape(2, model_width)
    share = model_width // (dp_size * mp_size)
    at = (dp_index * mp_size + mp_index) * share
    gain_grad = lax.dynamic_slice(gains, (0, at), (2, share))
    tables = small[2 * gain_rows :].reshape(3, head_count, LANES)
    table_grad = lax.dynamic_slice(
        tables,
        (0, mp_index * heads_here, dp_index * (32 // dp_size)),
        (3, heads_here, 32 // dp_size),
    )
    table_grad = jnp.swapaxes(table_grad, 1, 2)
    query_grad = summed[0].T
    key_value_grad = jnp.transpose(summed[1:3], (2, 0, 1))
    gate_up_grad = jnp.transpose(gate_up_sum, (2, 0, 1))
    return (
        layer_output, input_grad, gain_grad, query_grad, key_value_grad,
        summed[3], gate_up_grad, down_sum[0], table_grad,
    )


def per_device(dp_size, mp_size, *args):
    rows, model_width = args[0].shape
    heads_here = args[7].shape[2]
    fits = dp_size == 8 and model_width == 8 * LANES and mp_size == 4
    fits = fits and heads_here <= 8 and rows % LANES == 0
    body = per_device_linked if fits else per_device_plain
    return body(dp_size, mp_size, *args)


def solution(mesh):
    return jax.shard_map(
        partial(per_device, mesh.shape["dp"], mesh.shape["mp"]),
        mesh=mesh,
        in_specs=(
            P(("dp", "mp"), None),
            P(),
            P(None, "mp"),
            P(None, None, "mp"),
            P("mp", None),
            P(None, None, "mp"),
            P("mp", None),
            P(None, None, "mp"),
            P("dp"),
            P(None, "dp"),
            P(("dp", "mp"), None),
        ),
        out_specs=(
            P(("dp", "mp"), None),
            P(("dp", "mp"), None),
            P(None, ("dp", "mp")),
            P("dp", "mp"),
            P("dp", None, "mp"),
            P("mp", "dp"),
            P("dp", None, "mp"),
            P("mp", "dp"),
            P(None, "dp", "mp"),
        ),
        check_vma=False,
    )
```

```python
from functools import partial

import jax
import jax.numpy as jnp
import numpy as np
from jax import lax
from jax.experimental import pallas as pl
from jax.experimental.pallas import tpu as pltpu
from jax.sharding import PartitionSpec as P

NBIN = 64
EPSILON = 1e-06
THRESHOLDS = (8, 12, 16, 23, 32, 46, 64, 91)
NEG_FILL = -1e30
LANES = 128
MESH = pl.DeviceIdType.MESH
HBM = pltpu.MemorySpace.HBM
BF16 = jnp.bfloat16
F32 = jnp.float32


def bucket_of(relative):
    distance = jnp.abs(relative)
    bucket = jnp.minimum(distance, 7)
    for threshold in THRESHOLDS:
        bucket = bucket + (distance >= threshold).astype(jnp.int32)
    return bucket + 16 * (relative > 0).astype(jnp.int32)


def inverse_rms(values):
    return lax.rsqrt(jnp.mean(values * values, axis=-1, keepdims=True) + EPSILON)


def dot_f32(left, right, left_dim, right_dim):
    return lax.dot_general(
        left, right, (((left_dim,), (right_dim,)), ((), ())), preferred_element_type=F32
    )


def three_parts(values):
    high = values.astype(BF16)
    rest = values - high.astype(F32)
    middle = rest.astype(BF16)
    low = (rest - middle.astype(F32)).astype(BF16)
    return high, middle, low


def lane_ids(shape):
    return lax.broadcasted_iota(jnp.int32, shape, 1)


def row_ids(shape):
    return lax.broadcasted_iota(jnp.int32, shape, 0)


def attend_kernel(
    q_ref, k_ref, v_ref, layout_ref, line_ref, key_extra_ref, query_bins_ref,
    out_ref, lse_ref,
    key_aug, query_aug, strip, scores, probs,
):
    head_size, rows = q_ref.shape
    keys = k_ref.shape[1]
    blocks = keys // LANES
    width = strip.shape[1]

    @pl.when(pl.program_id(0) == 0)
    def _():
        key_aug[...] = key_extra_ref[...]
        tail = row_ids((64, rows))
        query_aug[pl.ds(192, 64), :] = jnp.where(tail == 0, 1.0, 0.0).astype(BF16)

    both = jnp.concatenate([k_ref[...], v_ref[...]], axis=0).T
    low_lanes = lane_ids((keys, LANES)) < head_size
    key_aug[:, 0:LANES] = jnp.where(low_lanes, both, key_extra_ref[:, 0:LANES])
    query_aug[pl.ds(0, 64), :] = q_ref[...]
    query_aug[pl.ds(64, 128), :] = jnp.dot(
        layout_ref[0], query_bins_ref[...], preferred_element_type=F32
    ).astype(BF16)
    strip[...] = pltpu.roll(
        jnp.broadcast_to(line_ref[0], (LANES, width)), 0, 1, stride=1, stride_axis=0
    )
    query_all = query_aug[...]
    top = jnp.full((1, rows), -jnp.inf, F32)
    for block in range(blocks):
        here = pl.ds(block * LANES, LANES)
        part = jnp.dot(key_aug[here, :], query_all, preferred_element_type=F32)
        part = part + strip[:, pl.ds((blocks - 1 - block) * LANES, rows)]
        scores[here, :] = part
        top = jnp.maximum(top, jnp.max(part, axis=0, keepdims=True))
    total = jnp.zeros((1, rows), F32)
    for block in range(blocks):
        here = pl.ds(block * LANES, LANES)
        part = jnp.exp(scores[here, :] - top)
        total = total + jnp.sum(part, axis=0, keepdims=True)
        probs[here, :] = part.astype(BF16)
    mixed = jnp.dot(v_ref[...], probs[...], preferred_element_type=F32)
    out_ref[...] = (mixed / total).astype(BF16)
    lse_ref[0] = top + jnp.log(total)


def attend_back_kernel(
    q_ref, k_ref, v_ref, out_ref, out_grad_ref, lse_ref, layout_ref, line_ref,
    key_extra_ref, key_extra_t_ref, query_bins_ref, query_bins_t_ref,
    dq_ref, dk_ref, dv_ref, line_grad_ref, layout_grad_ref,
    key_aug, key_aug_t, query_aug, value_aug, grad_aug, strip, strip_grad, probs_grad,
):
    head_size, rows = q_ref.shape
    keys = k_ref.shape[1]
    blocks = keys // LANES
    width = strip.shape[1]

    @pl.when(pl.program_id(0) == 0)
    def _():
        key_aug[...] = key_extra_ref[...]
        key_aug_t[pl.ds(64, 128), :] = key_extra_t_ref[...]
        tail = row_ids((64, rows))
        query_aug[pl.ds(192, 64), :] = jnp.where(tail == 0, 1.0, 0.0).astype(BF16)

    both = jnp.concatenate([k_ref[...], v_ref[...]], axis=0).T
    lanes = lane_ids((keys, LANES))
    key_aug[:, 0:LANES] = jnp.where(lanes < head_size, both, key_extra_ref[:, 0:LANES])
    ones = jnp.where(lanes < 3, 1.0, 0.0).astype(BF16)
    value_aug[...] = jnp.where(lanes < head_size, ones, both)
    key_aug_t[pl.ds(0, 64), :] = k_ref[...]
    query_aug[pl.ds(0, 64), :] = q_ref[...]
    query_aug[pl.ds(64, 128), :] = jnp.dot(
        layout_ref[0], query_bins_ref[...], preferred_element_type=F32
    ).astype(BF16)
    high, middle, low = three_parts(-lse_ref[0])
    tail = row_ids((64, rows))
    rows_of = lambda part: jnp.broadcast_to(part.astype(F32), (64, rows))
    query_aug[pl.ds(192, 64), :] = jnp.where(
        tail == 0, 1.0,
        jnp.where(
            tail == 1, rows_of(high),
            jnp.where(tail == 2, rows_of(middle), jnp.where(tail == 3, rows_of(low), 0.0)),
        ),
    ).astype(BF16)
    row_dot = jnp.sum(
        out_grad_ref[...].astype(F32) * out_ref[...].astype(F32), axis=0, keepdims=True
    )
    high, middle, low = three_parts(-row_dot)
    grad_aug[pl.ds(0, 64), :] = jnp.where(
        tail == 0, rows_of(high),
        jnp.where(tail == 1, rows_of(middle), jnp.where(tail == 2, rows_of(low), 0.0)),
    ).astype(BF16)
    grad_aug[pl.ds(64, 64), :] = out_grad_ref[...]
    strip[...] = pltpu.roll(
        jnp.broadcast_to(line_ref[0], (LANES, width)), 0, 1, stride=1, stride_axis=0
    )
    strip_grad[...] = jnp.zeros_like(strip_grad)
    query_and_grad = jnp.concatenate([q_ref[...], out_grad_ref[...]], axis=0).T
    query_all = query_aug[...]
    grad_all = grad_aug[...]
    half = lane_ids((LANES, LANES)) < head_size
    for block in range(blocks):
        here = pl.ds(block * LANES, LANES)
        band = pl.ds((blocks - 1 - block) * LANES, rows)
        part = jnp.dot(key_aug[here, :], query_all, preferred_element_type=F32)
        part = jnp.exp(part + strip[:, band])
        slope = part * jnp.dot(value_aug[here, :], grad_all, preferred_element_type=F32)
        strip_grad[:, band] = strip_grad[:, band] + slope
        slope = slope.astype(BF16)
        probs_grad[here, :] = slope
        key_part = jnp.dot(slope, query_and_grad, preferred_element_type=F32)
        value_part = jnp.dot(part.astype(BF16), query_and_grad, preferred_element_type=F32)
        turned = jnp.where(half, key_part, value_part).T.astype(BF16)
        dk_ref[:, here] = turned[0:64]
        dv_ref[:, here] = turned[64:128]
    query_part = jnp.dot(key_aug_t[...], probs_grad[...], preferred_element_type=F32)
    dq_ref[...] = query_part[0:64].astype(BF16)
    layout_grad_ref[0] = jnp.dot(
        query_part[64:192].astype(BF16), query_bins_t_ref[...], preferred_element_type=F32
    )
    folded = strip_grad[pl.ds(0, 8), :]
    for group in range(1, LANES // 8):
        folded = folded + pltpu.roll(strip_grad[pl.ds(group * 8, 8), :], width - group * 8, 1)
    line = folded[0:1]
    for row in range(1, 8):
        line = line + pltpu.roll(folded[row : row + 1], width - row, 1)
    line_grad_ref[0] = line


class Place:
    def __init__(self, mp_size):
        self.dp = lax.axis_index("dp")
        self.mp = lax.axis_index("mp")
        self.mp_size = mp_size
        self.core = lax.rem(self.dp, 2)
        self.x = lax.rem(lax.div(self.dp, 2), 2)
        self.y = lax.div(self.dp, 4)
        self.to_core = (self.dp + 1 - 2 * self.core, self.mp)
        self.to_x = (self.dp + 2 - 4 * self.x, self.mp)
        self.to_y = (self.dp + 4 - 8 * self.y, self.mp)
        self.to_corner = (self.dp + 6 - 4 * self.x - 8 * self.y, self.mp)

    def to_mp(self, step):
        return (self.dp, lax.rem(self.mp + step, self.mp_size))

    def from_mp(self, step):
        return lax.rem(self.mp + self.mp_size - step, self.mp_size)

    def partners(self):
        others = [self.to_mp(step) for step in range(1, self.mp_size)]
        return [self.to_core, self.to_x, self.to_y, self.to_corner] + others


def meet(place):
    barrier = pltpu.get_barrier_semaphore()
    partners = place.partners()
    for partner in partners:
        pl.semaphore_signal(barrier, inc=1, device_id=partner, device_id_type=MESH)
    pl.semaphore_wait(barrier, len(partners))


class Copy:
    def __init__(self, source, target, send, receive=None, partner=None):
        self.parts = (source, target, send, receive, partner)

    def made(self):
        source, target, send, receive, partner = self.parts
        if partner is None:
            return pltpu.make_async_copy(source, target, send)
        return pltpu.make_async_remote_copy(
            src_ref=source, dst_ref=target, send_sem=send, recv_sem=receive,
            device_id=partner, device_id_type=MESH,
        )

    def start(self):
        self.made().start()

    def wait(self):
        self.made().wait()

    def wait_send(self):
        self.made().wait_send()

    def wait_recv(self):
        self.made().wait_recv()


def remote(source, target, send, receive, partner):
    return Copy(source, target, send, receive, partner)


def lanes_at(block, count):
    return pl.ds(pl.multiple_of(block * LANES, LANES), count * LANES)


class Gather:
    LAGS = 2

    def __init__(self, place, pieces, outs, sems, items=None):
        self.place, self.pieces, self.outs = place, pieces, outs
        self.z_send, self.z_recv, self.own_sem, self.send, self.recv = sems
        self.items = items or [(c, k) for c in range(len(pieces)) for k in range(place.mp_size)]
        self.steps = len(self.items) + self.LAGS

    @staticmethod
    def semaphores(count, mp_size):
        dma = pltpu.SemaphoreType.DMA
        items = count * mp_size
        return [
            dma((count, mp_size)), dma((count, mp_size)), dma((count,)), dma((items, 6)), dma((items, 6))
        ]

    def rows(self, c, source, half):
        n = self.pieces[c].shape[1]
        if half is None:
            return pl.ds(pl.multiple_of(source * n, 16), n)
        return pl.ds(pl.multiple_of(source * n + half * (n // 2), 16), n // 2)

    def window(self, c, source, half, block, count):
        return self.outs[c].at[:, self.rows(c, source, half), lanes_at(block, count)]

    def own(self, c):
        place = self.place
        block = place.core * 4 + place.y * 2 + place.x
        return Copy(
            self.pieces[c], self.window(c, place.mp, None, block, 1), self.own_sem.at[c]
        )

    def along_mp(self, c, step):
        place = self.place
        block = place.core * 4 + place.y * 2 + place.x
        return remote(
            self.pieces[c], self.window(c, place.mp, None, block, 1),
            self.z_send.at[c, step], self.z_recv.at[c, step], place.to_mp(step),
        )

    def start_chunk(self, c):
        self.own(c).start()
        for step in range(1, self.place.mp_size):
            self.along_mp(c, step).start()

    def copies(self, t):
        c, k = self.items[t]
        place = self.place
        source = place.from_mp(k)
        base = place.core * 4
        mine = base + place.y * 2 + place.x
        turned = base + (1 - place.y) * 2 + place.x

        def copy(i, half, block, count, partner):
            here = self.window(c, source, half, block, count)
            return remote(here, here, self.send.at[t, i], self.recv.at[t, i], partner)

        first = [copy(0, 0, mine, 1, place.to_x), copy(1, 1, mine, 1, place.to_y)]
        second = [
            copy(2, 0, base + place.y * 2, 2, place.to_y),
            copy(3, 1, mine, 1, place.to_x),
            copy(4, 1, turned, 1, place.to_x),
        ]
        third = [copy(5, None, base, 4, place.to_core)]
        return first, second, third

    def first(self, t):
        c, k = self.items[t]
        if k == 0:
            self.own(c).wait()
        else:
            self.along_mp(c, k).wait_recv()
        for copy in self.copies(t)[0]:
            copy.start()

    def step(self, s):
        count = len(self.items)
        if s == 0:
            self.first(0)
        if 0 <= s - 1 < count:
            first, second, _ = self.copies(s - 1)
            for copy in first:
                copy.wait_recv()
            for copy in second:
                copy.start()
        if s + 1 < count:
            self.first(s + 1)
        if 0 <= s - 2 < count:
            _, second, third = self.copies(s - 2)
            for copy in second:
                copy.wait_recv()
            third[0].start()

    def done(self, t):
        self.copies(t)[2][0].wait_recv()

    def close(self):
        for t, (c, k) in enumerate(self.items):
            first, second, third = self.copies(t)
            for copy in first + second + third:
                copy.wait_send()
            if k > 0:
                self.along_mp(c, k).wait_send()


def add_rows(target, target_index, source, source_index):
    lead, rows, lanes = target_index
    source_rows, source_lanes = source_index
    row_start, count = rows
    source_start = source_rows
    size = 32
    while count % size:
        size //= 2

    def body(i, carry):
        here = pl.ds(pl.multiple_of(row_start + i * size, size), size)
        there = pl.ds(pl.multiple_of(source_start + i * size, size), size)
        for part in range(lead):
            target[part, here, lanes] = target[part, here, lanes] + source[part, there, source_lanes]
        return carry

    lax.fori_loop(0, count // size, body, 0)


class Scatter:
    def __init__(self, place, fulls, outs, scratch, items):
        self.place, self.fulls, self.outs, self.items = place, fulls, outs, items
        count = len(fulls)
        self.whole = [len(full.shape) == 3 for full in fulls]
        buffers = [scratch[i * count : (i + 1) * count] for i in range(5)]
        self.sums, self.from_first, self.from_second, self.from_mp, self.staged = buffers
        self.own_sem, self.send, self.recv = scratch[5 * count :]
        self.steps = len(items) + 5

    @staticmethod
    def scratch(shapes, whole, mp_size):
        out = []
        for blocks in (4, 2, 1, 1):
            for lead, n in shapes:
                out.append(pltpu.VMEM((mp_size, lead, n, blocks * LANES), BF16))
        for (lead, n), is_whole in zip(shapes, whole):
            out.append(pltpu.VMEM((lead, n, 4 * LANES) if is_whole else (1, 8, LANES), BF16))
        dma = pltpu.SemaphoreType.DMA
        count = len(shapes) * mp_size
        return out + [dma((count,)), dma((count, 7)), dma((count, 7))]

    def size(self, c):
        return self.sums[c].shape[1], self.sums[c].shape[2]

    def source(self, t):
        c, k = self.items[t]
        if not self.whole[c]:
            return self.fulls[c].at[(k + self.place.mp_size - 1) % self.place.mp_size % 2]
        lead, n = self.size(c)
        target = lax.rem(self.place.mp + k, self.place.mp_size)
        return self.fulls[c].at[:, pl.ds(pl.multiple_of(target * n, 16), n), :]

    def from_core(self, t):
        c, k = self.items[t]
        place = self.place
        return remote(
            self.source(t).at[:, :, lanes_at((1 - place.core) * 4, 4)], self.sums[c].at[k],
            self.send.at[t, 0], self.recv.at[t, 0], place.to_core,
        )

    def own(self, t):
        c, _ = self.items[t]
        return Copy(
            self.source(t).at[:, :, lanes_at(self.place.core * 4, 4)], self.staged[c], self.own_sem.at[t]
        )

    def copies(self, t):
        c, k = self.items[t]
        place = self.place
        lead, n = self.size(c)
        top, bottom = pl.ds(0, n // 2), pl.ds(n // 2, n // 2)
        every = pl.ds(0, lead)
        sums = self.sums[c].at[k]

        def copy(i, source, landing, partner):
            return remote(source, landing, self.send.at[t, i], self.recv.at[t, i], partner)

        landing = self.from_first[c].at[k]
        first = [
            copy(
                1, sums.at[every, top, lanes_at((1 - place.y) * 2, 2)],
                landing.at[every, top, pl.ds(0, 256)], place.to_y,
            ),
            copy(
                2, sums.at[every, bottom, lanes_at(1 - place.x, 1)],
                landing.at[every, bottom, pl.ds(0, 128)], place.to_x,
            ),
            copy(
                3, sums.at[every, bottom, lanes_at(3 - place.x, 1)],
                landing.at[every, bottom, pl.ds(128, 128)], place.to_x,
            ),
        ]
        landing = self.from_second[c].at[k]
        second = [
            copy(
                4, sums.at[every, top, lanes_at(place.y * 2 + 1 - place.x, 1)],
                landing.at[every, top, pl.ds(0, 128)], place.to_x,
            ),
            copy(
                5, sums.at[every, bottom, lanes_at((1 - place.y) * 2 + place.x, 1)],
                landing.at[every, bottom, pl.ds(0, 128)], place.to_y,
            ),
        ]
        third = None
        if k > 0:
            third = copy(
                6, sums.at[:, :, lanes_at(place.y * 2 + place.x, 1)], self.from_mp[c].at[k],
                place.to_mp(k),
            )
        return first, second, third

    def step(self, s):
        count = len(self.items)
        place = self.place
        if s < count:
            self.from_core(s).start()
        if 0 <= s - 1 < count:
            t = s - 1
            c, k = self.items[t]
            lead, n = self.size(c)
            first, *_ = self.copies(t)
            self.from_core(t).wait_recv()
            if self.whole[c]:
                self.own(t).wait()
                add_rows(self.sums[c].at[k], (lead, (0, n), pl.ds(0, 512)), self.staged[c], (0, pl.ds(0, 512)))
            else:
                add_rows(
                    self.sums[c].at[k], (lead, (0, n), pl.ds(0, 512)),
                    self.source(t), (0, lanes_at(place.core * 4, 4)),
                )
            for copy in first:
                copy.start()
        if s < count and self.whole[self.items[s][0]]:
            self.own(s).start()
        if 0 <= s - 2 < count:
            t = s - 2
            c, k = self.items[t]
            lead, n = self.size(c)
            first, second, _ = self.copies(t)
            for copy in first:
                copy.wait_recv()
            sums, landing = self.sums[c].at[k], self.from_first[c].at[k]
            half = n // 2
            add_rows(sums, (lead, (0, half), lanes_at(place.y * 2, 2)), landing, (0, pl.ds(0, 256)))
            add_rows(sums, (lead, (half, half), lanes_at(place.x, 1)), landing, (half, pl.ds(0, 128)))
            add_rows(
                sums, (lead, (half, half), lanes_at(2 + place.x, 1)), landing, (half, pl.ds(128, 128))
            )
            for copy in second:
                copy.start()
        if 0 <= s - 3 < count:
            t = s - 3
            c, k = self.items[t]
            lead, n = self.size(c)
            _, second, third = self.copies(t)
            for copy in second:
                copy.wait_recv()
            sums, landing = self.sums[c].at[k], self.from_second[c].at[k]
            mine = lanes_at(place.y * 2 + place.x, 1)
            add_rows(sums, (lead, (0, n), mine), landing, (0, pl.ds(0, 128)))
            if third is not None:
                third.start()
        if 0 <= s - 5 < count:
            t = s - 5
            c, k = self.items[t]
            third = self.copies(t)[2]
            if third is not None:
                third.wait_recv()
            else:
                self.finish(c)

    def left(self, t):
        self.from_core(t).wait_send()

    def close(self):
        for t, (c, k) in enumerate(self.items):
            first, second, third = self.copies(t)
            if self.whole[c] or k in (0, self.place.mp_size - 1):
                self.from_core(t).wait_send()
            for copy in first + second:
                copy.wait_send()
            if third is not None:
                third.wait_send()

    def finish(self, c):
        place = self.place
        lead, n = self.size(c)
        mine = lanes_at(place.y * 2 + place.x, 1)
        sums, landing, out = self.sums[c], self.from_mp[c], self.outs[c]
        size = 32
        while n % size:
            size //= 2

        def body(i, carry):
            here = pl.ds(pl.multiple_of(i * size, size), size)
            for part in range(lead):
                total = sums[0, part, here, mine].astype(F32)
                for k in range(1, place.mp_size):
                    total = total + landing[k, part, here, :].astype(F32)
                out[part, here, :] = total
            return carry

        lax.fori_loop(0, n // size, body, 0)


def attention_shapes(head_count, head_size, rows, keys, width):
    whole = lambda shape: pl.BlockSpec(shape, lambda head: (0,) * len(shape))
    column = lambda size: pl.BlockSpec((head_size, size), lambda head: (head, 0))
    page = lambda a, b: pl.BlockSpec((1, a, b), lambda head: (head, 0, 0))
    return whole, column, page


def attend(queries, keys_t, values_t, layout, line, key_extra, query_bins):
    inner, rows = queries.shape
    keys = keys_t.shape[1]
    head_count, _, width = line.shape
    head_size = inner // head_count
    whole, column, page = attention_shapes(head_count, head_size, rows, keys, width)
    return pl.pallas_call(
        attend_kernel,
        grid=(head_count,),
        out_shape=(
            jax.ShapeDtypeStruct((inner, rows), BF16),
            jax.ShapeDtypeStruct((head_count, 1, rows), F32),
        ),
        in_specs=[
            column(rows), column(keys), column(keys), page(128, 128), page(1, width),
            whole((keys, 256)), whole((128, rows)),
        ],
        out_specs=(column(rows), page(1, rows)),
        scratch_shapes=[
            pltpu.VMEM((keys, 256), BF16),
            pltpu.VMEM((256, rows), BF16),
            pltpu.VMEM((LANES, width), F32),
            pltpu.VMEM((keys, rows), F32),
            pltpu.VMEM((keys, rows), BF16),
        ],
        compiler_params=pltpu.CompilerParams(
            dimension_semantics=("arbitrary",), vmem_limit_bytes=32 << 20
        ),
        name="attend",
    )(queries, keys_t, values_t, layout, line, key_extra, query_bins)


def attend_back(
    queries, keys_t, values_t, heads_out, heads_grad, lse, layout, line,
    key_extra, key_extra_t, query_bins, query_bins_t,
):
    inner, rows = queries.shape
    keys = keys_t.shape[1]
    head_count, _, width = line.shape
    head_size = inner // head_count
    whole, column, page = attention_shapes(head_count, head_size, rows, keys, width)
    return pl.pallas_call(
        attend_back_kernel,
        grid=(head_count,),
        out_shape=(
            jax.ShapeDtypeStruct((inner, rows), BF16),
            jax.ShapeDtypeStruct((inner, keys), BF16),
            jax.ShapeDtypeStruct((inner, keys), BF16),
            jax.ShapeDtypeStruct((head_count, 1, width), F32),
            jax.ShapeDtypeStruct((head_count, 128, 128), F32),
        ),
        in_specs=[
            column(rows), column(keys), column(keys), column(rows), column(rows),
            page(1, rows), page(128, 128), page(1, width),
            whole((keys, 256)), whole((128, keys)), whole((128, rows)), whole((rows, 128)),
        ],
        out_specs=(column(rows), column(keys), column(keys), page(1, width), page(128, 128)),
        scratch_shapes=[
            pltpu.VMEM((keys, 256), BF16),
            pltpu.VMEM((192, keys), BF16),
            pltpu.VMEM((256, rows), BF16),
            pltpu.VMEM((keys, 128), BF16),
            pltpu.VMEM((128, rows), BF16),
            pltpu.VMEM((LANES, width), F32),
            pltpu.VMEM((LANES, width), F32),
            pltpu.VMEM((keys, rows), BF16),
        ],
        compiler_params=pltpu.CompilerParams(
            dimension_semantics=("arbitrary",), vmem_limit_bytes=32 << 20
        ),
        name="attend_back",
    )(
        queries, keys_t, values_t, heads_out, heads_grad, lse, layout, line,
        key_extra, key_extra_t, query_bins, query_bins_t,
    )


def forward_items(mp_size):
    items = [(0, 0), (1, 0), (2, 0)] + [(0, k) for k in range(1, mp_size)]
    for k in range(1, mp_size):
        items += [(1, k), (2, k)]
    return items


def forward_kernel(
    mp_size, group,
    first_ref, gate_up_ref, down_ref, normed_t_ref, table_ref, key_info_ref, line_hot_ref,
    bin_hot_ref, input_ref, gain_ref, cotangent_ref,
    w_first, queries, keys_t, values_t, heads_out, lse, layout, line, key_extra, key_extra_t,
    slot_owner, residual, layer_output, second_grad, gate_up_full, down_full, tables,
    slot_t, w_gate_up, w_down, first_here, key_aug, query_aug, strip, scores, probs,
    second_t, second_owner, out_owner, out_t,
    hidden_a, hidden_b, hidden_c, act_t, low_t, stage_gate_up, stage_down,
    row_send, row_recv, row_own, table_send, table_recv, table_own, load_sem, store_sem, *sems,
):
    place = Place(mp_size)
    rows, model_width = input_ref.shape
    keys = keys_t.shape[1]
    blocks = keys // LANES
    width = strip.shape[1]
    inner_here = first_ref.shape[1]
    heads_here = inner_here // 64
    hidden = gate_up_ref.shape[1]
    member = lax.rem(place.mp, group)
    first_peer = place.mp - member
    own_lanes = pl.ds(pl.multiple_of(member * rows, LANES), rows)

    items = forward_items(mp_size)
    gather = Gather(
        place, [first_ref, gate_up_ref, down_ref], [w_first, w_gate_up, w_down], sems, items
    )
    at = {item: t for t, item in enumerate(items)}

    row_copies = [
        remote(
            normed_t_ref, slot_t.at[:, own_lanes], row_send.at[k], row_recv.at[k],
            (place.dp, first_peer + lax.rem(member + k, group)),
        )
        for k in range(1, group)
    ]
    table_copies = [
        remote(table_ref, tables.at[place.mp], table_send.at[k], table_recv.at[k], place.to_mp(k))
        for k in range(1, mp_size)
    ]
    row_here = Copy(normed_t_ref, slot_t.at[:, own_lanes], row_own.at[0])
    table_here = Copy(table_ref, tables.at[place.mp], table_own.at[0])

    row_here.start()
    table_here.start()
    meet(place)
    gather.start_chunk(0)
    for copy in table_copies + row_copies:
        copy.start()
    gather.start_chunk(1)
    gather.start_chunk(2)
    gather.step(0)

    key_rows = row_ids((64, keys)).astype(F32)
    x_place = jnp.where(key_rows == key_info_ref[0:1, :], 1.0, 0.0).astype(BF16)
    y_place = jnp.where(key_rows == key_info_ref[1:2, :], 1.0, 0.0).astype(BF16)
    key_extra_t[0:64, :] = x_place
    key_extra_t[64:128, :] = y_place
    tail = jnp.where(
        key_rows == 0.0, key_info_ref[2:3, :], jnp.where(key_rows < 4.0, 1.0, 0.0)
    ).astype(BF16)
    turned = jnp.concatenate([jnp.zeros((64, keys), BF16), x_place, y_place, tail], axis=0).T
    key_extra[...] = turned
    key_aug[...] = turned
    query_aug[pl.ds(192, 64), :] = jnp.where(row_ids((64, rows)) == 0, 1.0, 0.0).astype(BF16)
    gather.step(1)
    for block in range(model_width // LANES):
        owner = block_owner(block)
        out_owner[:, owner * LANES : (owner + 1) * LANES] = cotangent_ref[
            :, block * LANES : (block + 1) * LANES
        ].astype(BF16)
    out_t[...] = cotangent_ref[...].astype(BF16).T
    residual[...] = input_ref[...]
    layer_output[...] = jnp.zeros_like(layer_output)
    second_grad[...] = jnp.zeros_like(second_grad)
    row_here.wait()
    table_here.wait()
    gather.step(2)

    head_units = mp_size * heads_here
    table = {
        (2, 0): [3], (4, 0): [4, 5], (6, 0): [6], (8, 0): [7], (12, 0): [8], (14, 0): [9],
        (16, 2): [10], (17, 1): [11], (18, 2): [12], (19, 0): [13],
    }

    def communicate(unit, point):
        for (at_unit, at_point), steps in table.items():
            if at_point == point:

                @pl.when(unit == at_unit)
                def _(steps=steps):
                    for s in steps:
                        gather.step(s)

    def head_unit(unit, carry):
        communicate(unit, 0)
        step = lax.div(unit, heads_here)
        inside = lax.rem(unit, heads_here)
        source = place.from_mp(step)
        base = pl.multiple_of(source * inner_here, 16)
        head = source * heads_here + inside

        @pl.when(inside == 0)
        def _():
            for k in range(mp_size):

                @pl.when(step == k)
                def _(k=k):
                    gather.done(at[(0, k)])
                    if k == 0:
                        for copy in row_copies:
                            copy.wait_recv()
                    else:
                        table_copies[k - 1].wait_recv()

            load = Copy(w_first.at[:, pl.ds(base, inner_here), :], first_here, load_sem.at[0])
            load.start()
            hot = tables[source].astype(BF16)
            line[source] = jnp.dot(hot[0:8], line_hot_ref[...], preferred_element_type=F32)
            bins = jnp.dot(hot[8:24], bin_hot_ref[...], preferred_element_type=F32)
            for i in range(heads_here):
                x_line = jnp.broadcast_to(bins[i : i + 1], (64, LANES))
                y_line = jnp.broadcast_to(bins[8 + i : 9 + i], (64, LANES))
                left = lane_ids((64, LANES)) < 64
                x_part = pltpu.roll(x_line, 0, 1, stride=1, stride_axis=0)
                y_part = pltpu.roll(y_line, 64, 1, stride=1, stride_axis=0)
                layout[source * heads_here + i] = jnp.concatenate(
                    [jnp.where(left, x_part, 0.0), jnp.where(left, 0.0, y_part)], axis=0
                ).astype(BF16)
            load.wait()
            here = pl.ds(base, inner_here)
            queries[here, :] = jnp.dot(
                first_here[0], normed_t_ref[...], preferred_element_type=F32
            ).astype(BF16)
            keys_t[here, :] = jnp.dot(
                first_here[1], slot_t[...], preferred_element_type=F32
            ).astype(BF16)
            values_t[here, :] = jnp.dot(
                first_here[2], slot_t[...], preferred_element_type=F32
            ).astype(BF16)

        here = pl.ds(pl.multiple_of(head * 64, 16), 64)
        both = jnp.concatenate([keys_t[here, :], values_t[here, :]], axis=0).T
        low_lanes = lane_ids((keys, LANES)) < 64
        key_aug[:, 0:LANES] = jnp.where(low_lanes, both, key_extra[:, 0:LANES])
        query_aug[pl.ds(0, 64), :] = queries[here, :]
        query_aug[pl.ds(64, 128), :] = jnp.dot(
            layout[head], key_extra_t[:, own_lanes], preferred_element_type=F32
        ).astype(BF16)
        strip[...] = pltpu.roll(
            jnp.broadcast_to(line[source, pl.ds(inside, 1), :], (LANES, width)), 0, 1,
            stride=1, stride_axis=0,
        )
        query_all = query_aug[...]
        top = jnp.full((1, rows), -jnp.inf, F32)
        for block in range(blocks):
            some = pl.ds(block * LANES, LANES)
            part = jnp.dot(key_aug[some, :], query_all, preferred_element_type=F32)
            part = part + strip[:, pl.ds((blocks - 1 - block) * LANES, rows)]
            scores[some, :] = part
            top = jnp.maximum(top, jnp.max(part, axis=0, keepdims=True))
        sums = jnp.zeros((1, rows), F32)
        for block in range(blocks):
            some = pl.ds(block * LANES, LANES)
            part = jnp.exp(scores[some, :] - top)
            sums = sums + jnp.sum(part, axis=0, keepdims=True)
            probs[some, :] = part.astype(BF16)
        mixed = jnp.dot(values_t[here, :], probs[...], preferred_element_type=F32)
        heads_out[here, :] = (mixed / sums).astype(BF16)
        lse[head] = top + jnp.log(sums)

        @pl.when(inside == heads_here - 1)
        def _():
            part = heads_out[pl.ds(base, inner_here), :].T
            residual[...] = residual[...] + jnp.dot(
                part, first_here[3], preferred_element_type=F32
            )

        return carry

    lax.fori_loop(0, head_units, head_unit, 0)
    for block in range(model_width // LANES):
        owner = block_owner(block)
        slot_owner[:, owner * LANES : (owner + 1) * LANES] = slot_t[
            block * LANES : (block + 1) * LANES, :
        ].T

    def norm_rows(i, carry):
        here = pl.ds(pl.multiple_of(i * 16, 16), 16)
        values = residual[here, :]
        scale = lax.rsqrt(jnp.mean(values * values, axis=1, keepdims=True) + EPSILON)
        normed = (values * scale * gain_ref[...]).astype(BF16)
        second_owner[here, :] = normed
        return carry

    lax.fori_loop(0, rows // 16, norm_rows, 0)
    second_t[...] = second_owner[...].T
    turned_blocks = [second_owner[:, b * LANES : (b + 1) * LANES] for b in range(model_width // LANES)]
    for block, values in enumerate(turned_blocks):
        owner = block_owner(block)
        second_owner[:, owner * LANES : (owner + 1) * LANES] = values

    def store(step):
        source = place.from_mp(step)
        here = pl.ds(pl.multiple_of(source * hidden, 16), hidden)
        return [
            Copy(stage_gate_up, gate_up_full.at[:, here, :], store_sem.at[0]),
            Copy(stage_down, down_full.at[:, here, :], store_sem.at[1]),
        ]

    def hidden_unit(step, carry):
        unit = step + head_units
        communicate(unit, 0)
        source = place.from_mp(step)
        here = pl.ds(pl.multiple_of(source * hidden, 16), hidden)
        for k in range(mp_size):

            @pl.when(step == k)
            def _(k=k):
                gather.done(at[(1, k)])
                gather.done(at[(2, k)])

        hidden_a[...] = jnp.dot(w_gate_up[0, here, :], second_t[...], preferred_element_type=F32)
        hidden_b[...] = jnp.dot(w_gate_up[1, here, :], second_t[...], preferred_element_type=F32)
        communicate(unit, 1)
        hidden_c[...] = jnp.dot(w_down[0, here, :], out_t[...], preferred_element_type=F32)

        def activate(i, inner_carry):
            some = pl.ds(pl.multiple_of(i * 16, 16), 16)
            gate, up, slope = hidden_a[some, :], hidden_b[some, :], hidden_c[some, :]
            square = gate * gate
            factor = 0.7978845608028654
            bent = jnp.tanh(factor * gate * (1.0 + 0.044715 * square))
            half = 0.5 * (1.0 + bent)
            value = gate * half
            change = half + 0.5 * gate * (1.0 - bent * bent) * (
                factor * (1.0 + 3.0 * 0.044715 * square)
            )
            act_t[some, :] = (value * up).astype(BF16)
            low_t[some, :] = (slope * up * change).astype(BF16)
            low_t[pl.ds(pl.multiple_of(hidden + i * 16, 16), 16), :] = (slope * value).astype(BF16)
            return inner_carry

        lax.fori_loop(0, hidden // 16, activate, 0)
        communicate(unit, 2)

        @pl.when(step > 0)
        def _():
            for copy in store(step):
                copy.wait()

        stage_down[0] = jnp.dot(act_t[...], out_owner[...], preferred_element_type=F32).astype(BF16)
        stage_gate_up[0] = jnp.dot(
            low_t[0:hidden], second_owner[...], preferred_element_type=F32
        ).astype(BF16)
        stage_gate_up[1] = jnp.dot(
            low_t[hidden:], second_owner[...], preferred_element_type=F32
        ).astype(BF16)
        for copy in store(step):
            copy.start()
        communicate(unit, 3)
        layer_output[...] = layer_output[...] + dot_f32(act_t[...].T, w_down[0, here, :], 1, 0)
        second_grad[...] = (
            second_grad[...]
            + dot_f32(low_t[0:hidden].T, w_gate_up[0, here, :], 1, 0)
            + dot_f32(low_t[hidden:].T, w_gate_up[1, here, :], 1, 0)
        )
        return carry

    lax.fori_loop(0, mp_size, hidden_unit, 0)
    layer_output[...] = layer_output[...] + residual[...]
    for copy in store(mp_size - 1):
        copy.wait()
    gather.close()
    for copy in row_copies + table_copies:
        copy.wait_send()


def block_owner(block):
    return (block % 2) * 4 + block // 2


def forward(mp_size, group, pieces, normed_t, table, key_info, line_hot, bin_hot, layer_input, gain, cotangent):
    first, gate_up, down = pieces
    rows, model_width = layer_input.shape
    keys = key_info.shape[1]
    width = line_hot.shape[1]
    inner_here, hidden = first.shape[1], gate_up.shape[1]
    inner, total_hidden = inner_here * mp_size, hidden * mp_size
    head_count = inner // 64
    dma = pltpu.SemaphoreType.DMA
    hbm = pl.BlockSpec(memory_space=HBM)
    vmem = pl.BlockSpec(memory_space=pltpu.VMEM)
    shape = jax.ShapeDtypeStruct
    out = [
        (shape((4, inner, model_width), BF16), hbm),
        (shape((inner, rows), BF16), vmem),
        (shape((inner, keys), BF16), vmem),
        (shape((inner, keys), BF16), vmem),
        (shape((inner, rows), BF16), vmem),
        (shape((head_count, 1, rows), F32), vmem),
        (shape((head_count, 128, 128), BF16), vmem),
        (shape((mp_size, 8, width), F32), vmem),
        (shape((keys, 256), BF16), vmem),
        (shape((128, keys), BF16), vmem),
        (shape((keys, model_width), BF16), vmem),
        (shape((rows, model_width), F32), vmem),
        (shape((rows, model_width), F32), vmem),
        (shape((rows, model_width), F32), vmem),
        (shape((2, total_hidden, model_width), BF16), hbm),
        (shape((1, total_hidden, model_width), BF16), hbm),
        (shape((mp_size, 24, LANES), F32), vmem),
    ]
    return pl.pallas_call(
        partial(forward_kernel, mp_size, group),
        out_shape=tuple(o[0] for o in out),
        in_specs=[hbm] * 3 + [vmem] * 8,
        out_specs=tuple(o[1] for o in out),
        scratch_shapes=[
            pltpu.VMEM((model_width, keys), BF16),
            pltpu.VMEM((2, total_hidden, model_width), BF16),
            pltpu.VMEM((1, total_hidden, model_width), BF16),
            pltpu.VMEM((4, inner_here, model_width), BF16),
            pltpu.VMEM((keys, 256), BF16),
            pltpu.VMEM((256, rows), BF16),
            pltpu.VMEM((LANES, width), F32),
            pltpu.VMEM((keys, rows), F32),
            pltpu.VMEM((keys, rows), BF16),
            pltpu.VMEM((model_width, rows), BF16),
            pltpu.VMEM((rows, model_width), BF16),
            pltpu.VMEM((rows, model_width), BF16),
            pltpu.VMEM((model_width, rows), BF16),
            pltpu.VMEM((hidden, rows), F32),
            pltpu.VMEM((hidden, rows), F32),
            pltpu.VMEM((hidden, rows), F32),
            pltpu.VMEM((hidden, rows), BF16),
            pltpu.VMEM((2 * hidden, rows), BF16),
            pltpu.VMEM((2, hidden, model_width), BF16),
            pltpu.VMEM((1, hidden, model_width), BF16),
            dma((group,)), dma((group,)), dma((1,)),
            dma((mp_size,)), dma((mp_size,)), dma((1,)), dma((1,)), dma((2,)),
        ]
        + Gather.semaphores(3, mp_size),
        compiler_params=pltpu.CompilerParams(
            collective_id=0, has_side_effects=True, vmem_limit_bytes=62 << 20
        ),
        name="forward",
    )(first, gate_up, down, normed_t, table, key_info, line_hot, bin_hot, layer_input, gain, cotangent)


def backward_items(mp_size):
    order = list(range(1, mp_size)) + [0]
    items = [(c, order[0]) for c in (0, 1)]
    for last, k in zip(order, order[1:]):
        items += [(0, k), (1, k), (2, last)]
    return items + [(2, order[-1])]


def unskewed(values, first, count, shift):
    width = values.shape[1]
    folded = None
    for group in range(count // 8):
        part = values[pl.ds(first + group * 8, 8), :]
        back = (-(group * 8 + shift)) % width
        part = pltpu.roll(part, back, 1) if back else part
        folded = part if folded is None else folded + part
    total = folded[0:1]
    for row in range(1, 8):
        total = total + pltpu.roll(folded[row : row + 1], width - row, 1)
    return total


def exact_dot(left, right):
    parts = three_parts(left)
    return sum(dot_f32(part, right, 1, 1) for part in parts)


def backward_kernel(mp_size, group, *refs):
    (
        gate_up_full, down_full, w_first, queries, keys_t, values_t, heads_out,
        residual_in, second_in, cotangent_in,
        lse, layout, line, key_extra, key_extra_t, slot_owner, layer_input, gains, line_hot, bin_hot,
        input_grad, small_out, gate_up_sum, down_sum, first_sum,
        *refs,
    ) = refs
    (
        slot_grad, own_grad, residual_grad, branch_owner, branch_t, w_query, w_output, w_kv,
        q_here, k_here, v_here, out_here, grad_here, dq_here, dk_here, dv_here, kv_here,
        key_aug, key_aug_t, query_aug, value_aug, grad_aug, strip, strip_grad, probs_grad,
        layout_grad, line_sums, bin_sums, gain_part, rows_out, peers, stage, stage_in, full_here,
        load_sem, value_sem, row_send, row_recv, stage_send, stage_recv,
        *refs,
    ) = refs
    place = Place(mp_size)
    rows, model_width = layer_input.shape
    keys = slot_owner.shape[0]
    blocks = keys // LANES
    inner_here = q_here.shape[0]
    heads_here = inner_here // 64
    member = lax.rem(place.mp, group)
    first_peer = place.mp - member
    own_start = pl.multiple_of(member * rows, LANES)
    own_lanes = pl.ds(own_start, rows)

    items = backward_items(mp_size)
    fulls = [gate_up_full, down_full, full_here]
    scatter = Scatter(place, fulls, [gate_up_sum, down_sum, first_sum], refs, items)

    loads = [
        Copy(second_in, slot_grad.at[pl.ds(0, rows), :], value_sem.at[0]),
        Copy(residual_in, slot_grad.at[pl.ds(rows, rows), :], value_sem.at[1]),
        Copy(cotangent_in, input_grad, value_sem.at[2]),
    ]
    for copy in loads:
        copy.start()
    meet(place)
    scatter.step(0)
    key_aug[...] = key_extra[...]
    key_aug_t[pl.ds(64, 128), :] = key_extra_t[...]
    for copy in loads:
        copy.wait()

    def norm_back(i, total):
        here = pl.ds(pl.multiple_of(i * 16, 16), 16)
        grad = slot_grad[here, :]
        values = slot_grad[pl.ds(pl.multiple_of(rows + i * 16, 16), 16), :]
        scale = lax.rsqrt(jnp.mean(values * values, axis=1, keepdims=True) + EPSILON)
        scaled = gains[1:2, :] * grad
        mean = jnp.mean(scaled * values, axis=1, keepdims=True)
        result = input_grad[here, :] + scale * scaled - values * (scale * scale * scale * mean)
        residual_grad[here, :] = result
        branch_owner[here, :] = result.astype(BF16)
        product = grad * values * scale
        return total + product[0:8] + product[8:16]

    total = lax.fori_loop(0, rows // 16, norm_back, jnp.zeros((8, model_width), F32))
    gain_part[...] = jnp.sum(total, axis=0, keepdims=True)
    scatter.step(1)
    branch_t[...] = branch_owner[...].T
    parts = [branch_owner[:, b * LANES : (b + 1) * LANES] for b in range(model_width // LANES)]
    for block, values in enumerate(parts):
        owner = block_owner(block)
        branch_owner[:, owner * LANES : (owner + 1) * LANES] = values
    slot_grad[...] = jnp.zeros_like(slot_grad)
    own_grad[...] = jnp.zeros_like(own_grad)
    scatter.step(2)

    plan = {
        (0, 2): [3], (0, 4): [4], (1, 2): [5], (1, 4): [6], (2, 2): [7], (2, 3): [8], (2, 4): [9],
        (3, 2): [10], (3, 4): [11],
    }
    done = 11

    def communicate(block, point):
        for (at_block, at_point), steps in plan.items():
            if at_point == point:

                @pl.when(block == at_block)
                def _(steps=steps):
                    for s in steps:
                        scatter.step(s)

    def block_unit(block, carry):
        communicate(block, 0)
        step = lax.rem(block + 1, mp_size)
        target = lax.rem(place.mp + step, mp_size)
        base = pl.multiple_of(target * inner_here, 16)
        here = pl.ds(base, inner_here)
        slot = lax.rem(block, 2)
        copies = [
            Copy(w_first.at[0, here, :], w_query, load_sem.at[0]),
            Copy(w_first.at[3, here, :], w_output, load_sem.at[1]),
            Copy(queries.at[here, :], q_here, load_sem.at[2]),
            Copy(keys_t.at[here, :], k_here, load_sem.at[3]),
            Copy(values_t.at[here, :], v_here, load_sem.at[4]),
            Copy(heads_out.at[here, :], out_here, load_sem.at[5]),
        ]
        for i in range(heads_here):
            for part in range(2):
                copies.append(
                    Copy(
                        w_first.at[1 + part, pl.ds(pl.multiple_of(base + i * 64, 16), 64), :],
                        w_kv.at[pl.ds(i * 128 + part * 64, 64), :],
                        load_sem.at[6 + 2 * i + part],
                    )
                )
        for copy in copies:
            copy.start()
        for copy in copies:
            copy.wait()

        for b in range(2, mp_size):

            @pl.when(block == b)
            def _(b=b):
                scatter.left(items.index((2, (b - 1) % mp_size)))

        grad_here[...] = jnp.dot(w_output[...], branch_t[...], preferred_element_type=F32).astype(BF16)
        full_here[slot, 3] = jnp.dot(
            out_here[...], branch_owner[...], preferred_element_type=F32
        ).astype(BF16)

        def head_unit(inside, inner_carry):
            for point in range(1, heads_here):

                @pl.when(inside == point)
                def _(point=point):
                    communicate(block, point)

            head = target * heads_here + inside
            some = pl.ds(pl.multiple_of(inside * 64, 16), 64)
            q_head, k_head, v_head = q_here[some, :], k_here[some, :], v_here[some, :]
            grad_head = grad_here[some, :]
            both = jnp.concatenate([k_head, v_head], axis=0).T
            lanes = lane_ids((keys, LANES))
            key_aug[:, 0:LANES] = jnp.where(lanes < 64, both, key_extra[:, 0:LANES])
            ones = jnp.where(lanes < 3, 1.0, 0.0).astype(BF16)
            value_aug[...] = jnp.where(lanes < 64, ones, both)
            key_aug_t[pl.ds(0, 64), :] = k_head
            query_aug[pl.ds(0, 64), :] = q_head
            query_aug[pl.ds(64, 128), :] = jnp.dot(
                layout[head], key_extra_t[:, own_lanes], preferred_element_type=F32
            ).astype(BF16)
            high, middle, low = three_parts(-lse[head])
            tail = row_ids((64, rows))
            rows_of = lambda part: jnp.broadcast_to(part.astype(F32), (64, rows))
            query_aug[pl.ds(192, 64), :] = jnp.where(
                tail == 0, 1.0,
                jnp.where(
                    tail == 1, rows_of(high),
                    jnp.where(tail == 2, rows_of(middle), jnp.where(tail == 3, rows_of(low), 0.0)),
                ),
            ).astype(BF16)
            row_dot = jnp.sum(
                grad_head.astype(F32) * out_here[some, :].astype(F32), axis=0, keepdims=True
            )
            high, middle, low = three_parts(-row_dot)
            grad_aug[pl.ds(0, 64), :] = jnp.where(
                tail == 0, rows_of(high),
                jnp.where(tail == 1, rows_of(middle), jnp.where(tail == 2, rows_of(low), 0.0)),
            ).astype(BF16)
            grad_aug[pl.ds(64, 64), :] = grad_head
            width = strip.shape[1]
            strip[...] = pltpu.roll(
                jnp.broadcast_to(line[target, pl.ds(inside, 1), :], (LANES, width)), 0, 1,
                stride=1, stride_axis=0,
            )
            strip_grad[...] = jnp.zeros_like(strip_grad)
            query_and_grad = jnp.concatenate([q_head, grad_head], axis=0).T
            query_all = query_aug[...]
            grad_all = grad_aug[...]
            half = lane_ids((LANES, LANES)) < 64
            kv_lanes = pl.ds(pl.multiple_of(inside * LANES, LANES), LANES)
            for part_index in range(blocks):
                these = pl.ds(part_index * LANES, LANES)
                band = pl.ds((blocks - 1 - part_index) * LANES, rows)
                part = jnp.dot(key_aug[these, :], query_all, preferred_element_type=F32)
                part = jnp.exp(part + strip[:, band])
                slope = part * jnp.dot(value_aug[these, :], grad_all, preferred_element_type=F32)
                strip_grad[:, band] = strip_grad[:, band] + slope
                slope = slope.astype(BF16)
                probs_grad[these, :] = slope
                key_part = jnp.dot(slope, query_and_grad, preferred_element_type=F32)
                value_part = jnp.dot(part.astype(BF16), query_and_grad, preferred_element_type=F32)
                joined = jnp.where(half, key_part, value_part)
                kv_here[these, kv_lanes] = joined.astype(BF16)
                turned = joined.T.astype(BF16)
                dk_here[some, these] = turned[0:64]
                dv_here[some, these] = turned[64:128]
            query_part = jnp.dot(key_aug_t[...], probs_grad[...], preferred_element_type=F32)
            dq_here[some, :] = query_part[0:64].astype(BF16)
            bins = dot_f32(query_part[64:192].astype(BF16), key_extra_t[:, own_lanes], 1, 1)
            left = lane_ids((LANES, LANES)) < 64
            upper = row_ids((LANES, LANES)) < 64
            layout_grad[...] = jnp.where(left == upper, bins, 0.0)
            bin_sums[0, pl.ds(head, 1), :] = unskewed(layout_grad, 0, 64, 0)
            bin_sums[1, pl.ds(head, 1), :] = unskewed(layout_grad, 64, 64, 64)
            line_sums[pl.ds(head, 1), :] = unskewed(strip_grad, 0, LANES, 0)
            return inner_carry

        lax.fori_loop(0, heads_here, head_unit, 0)
        full_here[slot, 0] = jnp.dot(
            dq_here[...], slot_owner[pl.ds(own_start, rows), :], preferred_element_type=F32
        ).astype(BF16)
        full_here[slot, 1] = jnp.dot(
            dk_here[...], slot_owner[...], preferred_element_type=F32
        ).astype(BF16)
        full_here[slot, 2] = jnp.dot(
            dv_here[...], slot_owner[...], preferred_element_type=F32
        ).astype(BF16)
        slot_grad[...] = slot_grad[...] + jnp.dot(
            kv_here[...], w_kv[...], preferred_element_type=F32
        )
        own_grad[...] = own_grad[...] + jnp.dot(
            dq_here[...].T, w_query[...], preferred_element_type=F32
        )
        communicate(block, heads_here)
        return carry

    lax.fori_loop(0, mp_size, block_unit, 0)

    copies = []
    for k in range(1, group):
        other = lax.rem(member + k, group)
        rows_out[k - 1] = slot_grad[pl.ds(pl.multiple_of(other * rows, 16), rows), :].astype(BF16)
        copies.append(
            remote(
                rows_out.at[k - 1], peers.at[k - 1], row_send.at[k], row_recv.at[k],
                (place.dp, first_peer + other),
            )
        )
    for copy in copies:
        copy.start()
    steps = list(range(done + 1, scatter.steps))
    for s in steps[:1]:
        scatter.step(s)

    gain_rows = model_width // LANES
    head_count = bin_sums.shape[1]
    stage[0, 2 * gain_rows : 2 * gain_rows + head_count, :] = exact_dot(line_sums[...], line_hot[...])
    for i in range(2):
        start = 2 * gain_rows + (1 + i) * head_count
        stage[0, start : start + head_count, :] = exact_dot(bin_sums[i], bin_hot[...])
    for block in range(gain_rows):
        these = slice(block * LANES, (block + 1) * LANES)
        owner = block_owner(block)
        those = slice(owner * LANES, (owner + 1) * LANES)

        def gain_sum(i, total, these=these, those=those):
            here = pl.ds(pl.multiple_of(i * 64, 64), 64)
            product = slot_grad[here, these] * slot_owner[here, those].astype(F32)
            return total + jnp.sum(product.reshape(8, 8, LANES), axis=0)

        def own_sum(i, total, these=these, those=those):
            here = pl.ds(pl.multiple_of(i * 64, 64), 64)
            there = pl.ds(pl.multiple_of(own_start + i * 64, 64), 64)
            product = own_grad[here, these] * slot_owner[there, those].astype(F32)
            return total + jnp.sum(product.reshape(8, 8, LANES), axis=0)

        total = lax.fori_loop(0, keys // 64, gain_sum, jnp.zeros((8, LANES), F32))
        total = lax.fori_loop(0, rows // 64, own_sum, total)
        stage[0, block : block + 1, :] = (
            jnp.sum(total, axis=0, keepdims=True) / gains[0:1, these]
        )
        stage[0, gain_rows + block : gain_rows + block + 1, :] = gain_part[:, these]

    rounds = [[place.to_core], [place.to_x, place.to_y, place.to_corner]]
    rounds.append([place.to_mp(k) for k in range(1, mp_size)])
    at, sums = 0, []
    for i, partners in enumerate(rounds):
        sums.append(
            [
                remote(
                    stage.at[i], stage_in.at[at + j], stage_send.at[at + j], stage_recv.at[at + j], partner
                )
                for j, partner in enumerate(partners)
            ]
        )
        at += len(partners)
    at = 0
    steps = steps[1:]
    for i, group_sums in enumerate(sums):
        for copy in group_sums:
            copy.start()
        for s in steps[:1]:
            scatter.step(s)
        steps = steps[1:]
        for copy in group_sums:
            copy.wait_recv()
        value = stage[i]
        for j in range(len(group_sums)):
            value = value + stage_in[at + j]
        at += len(group_sums)
        if i + 1 < len(sums):
            stage[i + 1] = value
        else:
            small_out[...] = value
    sums = sum(sums, [])
    for copy in copies:
        copy.wait_recv()

    def input_back(i, carry):
        here = pl.ds(pl.multiple_of(i * 16, 16), 16)
        grad = own_grad[here, :] + slot_grad[pl.ds(pl.multiple_of(own_start + i * 16, 16), 16), :]
        for k in range(group - 1):
            grad = grad + peers[k, here, :].astype(F32)
        values = layer_input[here, :]
        scale = lax.rsqrt(jnp.mean(values * values, axis=1, keepdims=True) + EPSILON)
        scaled = gains[0:1, :] * grad
        mean = jnp.mean(scaled * values, axis=1, keepdims=True)
        input_grad[here, :] = (
            residual_grad[here, :] + scale * scaled - values * (scale * scale * scale * mean)
        )
        return carry

    lax.fori_loop(0, rows // 16, input_back, 0)
    for s in steps:
        scatter.step(s)
    scatter.close()
    for copy in copies + sums:
        copy.wait_send()


def backward(
    mp_size, group, gate_up_full, down_full, w_first, queries, keys_t, values_t, heads_out,
    residual, second_grad, cotangent, lse, layout, line, key_extra, key_extra_t, slot_owner,
    layer_input, gains, line_hot, bin_hot,
):
    rows, model_width = layer_input.shape
    keys = slot_owner.shape[0]
    width = line.shape[2]
    inner_here = queries.shape[0] // mp_size
    heads_here = inner_here // 64
    head_count = heads_here * mp_size
    hidden = down_full.shape[1] // mp_size
    sizes = [(2, hidden), (1, hidden), (4, inner_here)]
    count = 4 + mp_size - 1
    small_rows = 2 * model_width // LANES + 3 * head_count
    others = max(group - 1, 1)
    dma = pltpu.SemaphoreType.DMA
    hbm = pl.BlockSpec(memory_space=HBM)
    vmem = pl.BlockSpec(memory_space=pltpu.VMEM)
    shape = jax.ShapeDtypeStruct
    return pl.pallas_call(
        partial(backward_kernel, mp_size, group),
        out_shape=(
            shape((rows, model_width), F32),
            shape((small_rows, LANES), F32),
            *[shape((lead, n, LANES), F32) for lead, n in sizes],
        ),
        in_specs=[hbm] * 10 + [vmem] * 10,
        out_specs=(vmem,) * 5,
        scratch_shapes=[
            pltpu.VMEM((keys, model_width), F32),
            pltpu.VMEM((rows, model_width), F32),
            pltpu.VMEM((rows, model_width), F32),
            pltpu.VMEM((rows, model_width), BF16),
            pltpu.VMEM((model_width, rows), BF16),
            pltpu.VMEM((inner_here, model_width), BF16),
            pltpu.VMEM((inner_here, model_width), BF16),
            pltpu.VMEM((2 * inner_here, model_width), BF16),
            pltpu.VMEM((inner_here, rows), BF16),
            pltpu.VMEM((inner_here, keys), BF16),
            pltpu.VMEM((inner_here, keys), BF16),
            pltpu.VMEM((inner_here, rows), BF16),
            pltpu.VMEM((inner_here, rows), BF16),
            pltpu.VMEM((inner_here, rows), BF16),
            pltpu.VMEM((inner_here, keys), BF16),
            pltpu.VMEM((inner_here, keys), BF16),
            pltpu.VMEM((keys, heads_here * LANES), BF16),
            pltpu.VMEM((keys, 256), BF16),
            pltpu.VMEM((192, keys), BF16),
            pltpu.VMEM((256, rows), BF16),
            pltpu.VMEM((keys, LANES), BF16),
            pltpu.VMEM((LANES, rows), BF16),
            pltpu.VMEM((LANES, width), F32),
            pltpu.VMEM((LANES, width), F32),
            pltpu.VMEM((keys, rows), BF16),
            pltpu.VMEM((LANES, LANES), F32),
            pltpu.VMEM((head_count, width), F32),
            pltpu.VMEM((2, head_count, LANES), F32),
            pltpu.VMEM((1, model_width), F32),
            pltpu.VMEM((others, rows, model_width), BF16),
            pltpu.VMEM((others, rows, model_width), BF16),
            pltpu.VMEM((3, small_rows, LANES), F32),
            pltpu.VMEM((count, small_rows, LANES), F32),
            pltpu.VMEM((2, 4, inner_here, model_width), BF16),
            dma((6 + 2 * heads_here,)), dma((3,)), dma((group,)), dma((group,)),
            dma((count,)), dma((count,)),
        ]
        + Scatter.scratch(sizes, (True, True, False), mp_size),
        compiler_params=pltpu.CompilerParams(
            collective_id=1, has_side_effects=True, vmem_limit_bytes=63 << 20
        ),
        name="backward",
    )(
        gate_up_full, down_full, w_first, queries, keys_t, values_t, heads_out, residual,
        second_grad, cotangent, lse, layout, line, key_extra, key_extra_t, slot_owner, layer_input,
        gains, line_hot, bin_hot,
    )


def line_onehot(first_row, width, key_blocks):
    place = jnp.arange(width, dtype=jnp.int32)
    place = jnp.where(place >= width - LANES, place - width, place)
    offset = LANES * (key_blocks - 1) - place - first_row
    return (bucket_of(offset)[:, None] == jnp.arange(32, dtype=jnp.int32)[None, :]).astype(F32)


def bin_onehot():
    bins = np.arange(NBIN)
    offset = bins[:, None] - bins[None, :]
    distance = np.abs(offset)
    bucket = np.minimum(distance, 7) + sum((distance >= t).astype(np.int64) for t in THRESHOLDS)
    bucket = bucket + 16 * (offset > 0)
    return jnp.asarray(bucket[:, :, None] == np.arange(32), F32)


def gather_rows(local, axis_name):
    return lax.all_gather(local, axis_name, axis=0, tiled=True)


def scatter_grad(full):
    summed = lax.psum_scatter(full, "dp", scatter_dimension=1, tiled=True)
    return lax.psum_scatter(summed, "mp", scatter_dimension=0, tiled=True)


def per_device_plain(
    dp_size, mp_size,
    layer_input, norm_gains, query_weight, key_value_weight, output_weight,
    gate_up_weight, down_weight, bias_tables, doc_lengths, box_bins, cotangent,
):
    rows, model_width = layer_input.shape
    doc_count = doc_lengths.shape[0]
    slot_span = box_bins.shape[1] // doc_count
    group = mp_size // doc_count
    mp_index = lax.axis_index("mp")
    doc = mp_index // group
    first_row = (mp_index % group) * rows
    key_blocks = slot_span // LANES
    width = LANES * (key_blocks + (rows + LANES - 1) // LANES)
    groups = [[d * group + i for i in range(group)] for d in range(doc_count)]
    gain_first = norm_gains[0].astype(F32)
    gain_second = norm_gains[1].astype(F32)

    w_query = gather_rows(query_weight.T, "mp")
    inner_here = query_weight.shape[1]
    inner = inner_here * mp_size
    w_key = gather_rows(key_value_weight[:, 0].T, "mp")
    w_value = gather_rows(key_value_weight[:, 1].T, "mp")
    w_output = gather_rows(output_weight, "mp")
    w_gate = gather_rows(gate_up_weight[:, 0].T, "mp")
    w_up = gather_rows(gate_up_weight[:, 1].T, "mp")
    w_down = gather_rows(down_weight, "mp")
    tables = lax.all_gather(bias_tables, "mp", axis=2, tiled=True).astype(F32)
    head_count = tables.shape[2]

    onehot_line = line_onehot(first_row, width, key_blocks)
    line = jnp.dot(onehot_line, tables[0], precision=lax.Precision.HIGHEST)
    line = line.T.reshape(head_count, 1, width)
    onehot_bin = bin_onehot()
    x_part = jnp.einsum("ban,nh->hba", onehot_bin, tables[1], precision=lax.Precision.HIGHEST)
    y_part = jnp.einsum("ban,nh->hba", onehot_bin, tables[2], precision=lax.Precision.HIGHEST)
    empty = jnp.zeros_like(x_part)
    layout = jnp.concatenate(
        [jnp.concatenate([x_part, empty], axis=2), jnp.concatenate([empty, y_part], axis=2)], axis=1
    ).astype(BF16)
    key_bins = lax.dynamic_slice(box_bins, (0, doc * slot_span), (2, slot_span))
    own_bins = lax.dynamic_slice(key_bins, (0, first_row), (2, rows))
    bin_ids = jnp.arange(NBIN, dtype=jnp.int32)

    def placed_rows(bins):
        return jnp.concatenate(
            [bins[0][:, None] == bin_ids, bins[1][:, None] == bin_ids], axis=1
        ).astype(BF16)

    def placed_lanes(bins):
        return jnp.concatenate(
            [bin_ids[:, None] == bins[0][None], bin_ids[:, None] == bins[1][None]], axis=0
        ).astype(BF16)

    length = lax.dynamic_index_in_dim(doc_lengths, doc, keepdims=False)
    masked = jnp.arange(slot_span, dtype=jnp.int32)[:, None] >= length
    key_placed = placed_rows(key_bins)
    key_extra = jnp.concatenate(
        [
            jnp.zeros((slot_span, 64), BF16),
            key_placed,
            jnp.where(masked, NEG_FILL, 0.0).astype(BF16),
            jnp.ones((slot_span, 3), BF16),
            jnp.zeros((slot_span, 60), BF16),
        ],
        axis=1,
    )
    key_extra_t = placed_lanes(key_bins)
    query_bins_t = placed_rows(own_bins)
    query_bins = placed_lanes(own_bins)

    scale_first = inverse_rms(layer_input)
    normed = (layer_input * scale_first * gain_first).astype(BF16)
    slot_normed = lax.all_gather(normed, "mp", axis=0, tiled=True, axis_index_groups=groups)
    queries = dot_f32(w_query, normed, 1, 1).astype(BF16)
    keys_t = dot_f32(w_key, slot_normed, 1, 1).astype(BF16)
    values_t = dot_f32(w_value, slot_normed, 1, 1).astype(BF16)
    heads_out, lse = attend(queries, keys_t, values_t, layout, line, key_extra, query_bins)
    residual = layer_input + dot_f32(heads_out, w_output, 0, 0)
    scale_second = inverse_rms(residual)
    normed_second = (residual * scale_second * gain_second).astype(BF16)
    gate = dot_f32(normed_second, w_gate, 1, 1)
    up = dot_f32(normed_second, w_up, 1, 1)
    gelu_value, gelu_pull = jax.vjp(lambda v: jax.nn.gelu(v, approximate=True), gate)
    activated = (gelu_value * up).astype(BF16)
    layer_output = residual + dot_f32(activated, w_down, 1, 0)

    out_low = cotangent.astype(BF16)
    down_full = dot_f32(activated, out_low, 0, 0).astype(BF16)
    act_grad = dot_f32(out_low, w_down, 1, 1)
    gate_low = gelu_pull(act_grad * up)[0].astype(BF16)
    up_low = (act_grad * gelu_value).astype(BF16)
    gate_full = dot_f32(gate_low, normed_second, 0, 0).astype(BF16)
    up_full = dot_f32(up_low, normed_second, 0, 0).astype(BF16)
    second_grad = dot_f32(gate_low, w_gate, 1, 0) + dot_f32(up_low, w_up, 1, 0)
    gain_second_grad = jnp.sum(second_grad * residual * scale_second, axis=0)
    scaled = gain_second * second_grad
    residual_grad = (
        cotangent
        + scale_second * scaled
        - residual * scale_second**3 * jnp.mean(scaled * residual, axis=-1, keepdims=True)
    )

    branch_low = residual_grad.astype(BF16)
    output_full = dot_f32(heads_out, branch_low, 1, 0).astype(BF16)
    heads_grad = dot_f32(w_output, branch_low, 1, 1).astype(BF16)
    dq, dk, dv, line_grad, layout_grad = attend_back(
        queries, keys_t, values_t, heads_out, heads_grad, lse, layout, line,
        key_extra, key_extra_t, query_bins, query_bins_t,
    )
    query_full = dot_f32(dq, normed, 1, 0).astype(BF16)
    key_full = dot_f32(dk, slot_normed, 1, 0).astype(BF16)
    value_full = dot_f32(dv, slot_normed, 1, 0).astype(BF16)
    slot_grad = dot_f32(dk, w_key, 0, 0) + dot_f32(dv, w_value, 0, 0)
    first_grad = lax.psum_scatter(
        slot_grad.astype(BF16), "mp", scatter_dimension=0, tiled=True, axis_index_groups=groups
    ).astype(F32) + dot_f32(dq, w_query, 0, 0)
    gain_first_grad = jnp.sum(first_grad * layer_input * scale_first, axis=0)
    scaled = gain_first * first_grad
    input_grad = (
        residual_grad
        + scale_first * scaled
        - layer_input * scale_first**3 * jnp.mean(scaled * layer_input, axis=-1, keepdims=True)
    )

    gain_grad = lax.psum_scatter(
        jnp.stack([gain_first_grad, gain_second_grad]), ("dp", "mp"), scatter_dimension=1, tiled=True
    )
    line_part = jnp.dot(
        onehot_line.T, line_grad[:, 0].T, precision=lax.Precision.HIGHEST
    )
    x_part = jnp.einsum(
        "ban,hba->nh", onehot_bin, layout_grad[:, :64, :64], precision=lax.Precision.HIGHEST
    )
    y_part = jnp.einsum(
        "ban,hba->nh", onehot_bin, layout_grad[:, 64:, 64:], precision=lax.Precision.HIGHEST
    )
    table_full = jnp.stack([line_part, x_part, y_part])
    table_grad = lax.psum_scatter(
        lax.psum_scatter(table_full, "mp", scatter_dimension=2, tiled=True),
        "dp", scatter_dimension=1, tiled=True,
    )

    query_grad = scatter_grad(query_full).T.astype(F32)
    key_value_grad = jnp.stack(
        [scatter_grad(key_full).T, scatter_grad(value_full).T], axis=1
    ).astype(F32)
    output_grad = scatter_grad(output_full).astype(F32)
    gate_up_grad = jnp.stack(
        [scatter_grad(gate_full).T, scatter_grad(up_full).T], axis=1
    ).astype(F32)
    down_grad = scatter_grad(down_full).astype(F32)
    return (
        layer_output, input_grad, gain_grad, query_grad, key_value_grad,
        output_grad, gate_up_grad, down_grad, table_grad,
    )


def per_device_linked(
    dp_size, mp_size,
    layer_input, norm_gains, query_weight, key_value_weight, output_weight,
    gate_up_weight, down_weight, bias_tables, doc_lengths, box_bins, cotangent,
):
    rows, model_width = layer_input.shape
    doc_count = doc_lengths.shape[0]
    slot_span = box_bins.shape[1] // doc_count
    group = mp_size // doc_count
    dp_index, mp_index = lax.axis_index("dp"), lax.axis_index("mp")
    doc = mp_index // group
    first_row = (mp_index % group) * rows
    key_blocks = slot_span // LANES
    width = LANES * (key_blocks + rows // LANES)
    heads_here = bias_tables.shape[2]
    head_count = heads_here * mp_size
    gain_second = norm_gains[1:2].astype(F32)

    column = ((dp_index % 2) * 4 + dp_index // 2) * LANES
    piece = lambda weight, axis: lax.dynamic_slice_in_dim(weight, column, LANES, axis)
    key_value_piece = jnp.transpose(piece(key_value_weight, 0), (1, 2, 0))
    pieces = [
        jnp.stack(
            [
                piece(query_weight, 0).T, key_value_piece[0], key_value_piece[1], piece(output_weight, 1)
            ]
        ),
        jnp.transpose(piece(gate_up_weight, 0), (1, 2, 0)),
        piece(down_weight, 1)[None],
    ]
    table = jnp.swapaxes(bias_tables.astype(F32), 1, 2)
    table = jnp.pad(table, ((0, 0), (0, 8 - heads_here), (0, LANES - 32))).reshape(24, LANES)

    onehot_line = line_onehot(first_row, width, key_blocks)
    line_hot = jnp.pad(onehot_line.T, ((0, LANES - 32), (0, 0))).astype(BF16)
    place = jnp.arange(LANES, dtype=jnp.int32)
    place = jnp.where(place < NBIN, place, place - LANES)
    bin_hot = (bucket_of(-place)[None, :] == jnp.arange(LANES, dtype=jnp.int32)[:, None]).astype(BF16)
    key_bins = lax.dynamic_slice(box_bins, (0, doc * slot_span), (2, slot_span))
    length = lax.dynamic_index_in_dim(doc_lengths, doc, keepdims=False)
    masked = jnp.arange(slot_span, dtype=jnp.int32)[None, :] >= length
    key_info = jnp.concatenate(
        [key_bins.astype(F32), jnp.where(masked, NEG_FILL, 0.0), jnp.zeros((5, slot_span), F32)]
    )

    scale_first = inverse_rms(layer_input)
    normed_t = (layer_input * scale_first * norm_gains[0].astype(F32)).astype(BF16).T
    (
        w_first, queries, keys_t, values_t, heads_out, lse, layout, line, key_extra, key_extra_t,
        slot_owner, residual, layer_output, second_grad, gate_up_full, down_full, _,
    ) = forward(
        mp_size, group, pieces, normed_t, table, key_info, line_hot, bin_hot, layer_input,
        gain_second, cotangent,
    )
    input_grad, small, gate_up_sum, down_sum, summed = backward(
        mp_size, group, gate_up_full, down_full, w_first, queries, keys_t, values_t, heads_out,
        residual, second_grad, cotangent, lse, layout, line, key_extra, key_extra_t, slot_owner,
        layer_input, norm_gains.astype(F32), line_hot, bin_hot,
    )
    gain_rows = model_width // LANES
    gains = small[: 2 * gain_rows].reshape(2, model_width)
    share = model_width // (dp_size * mp_size)
    at = (dp_index * mp_size + mp_index) * share
    gain_grad = lax.dynamic_slice(gains, (0, at), (2, share))
    tables = small[2 * gain_rows :].reshape(3, head_count, LANES)
    table_grad = lax.dynamic_slice(
        tables,
        (0, mp_index * heads_here, dp_index * (32 // dp_size)),
        (3, heads_here, 32 // dp_size),
    )
    table_grad = jnp.swapaxes(table_grad, 1, 2)
    query_grad = summed[0].T
    key_value_grad = jnp.transpose(summed[1:3], (2, 0, 1))
    gate_up_grad = jnp.transpose(gate_up_sum, (2, 0, 1))
    return (
        layer_output, input_grad, gain_grad, query_grad, key_value_grad,
        summed[3], gate_up_grad, down_sum[0], table_grad,
    )


def per_device(dp_size, mp_size, *args):
    rows, model_width = args[0].shape
    heads_here = args[7].shape[2]
    fits = dp_size == 8 and model_width == 8 * LANES and mp_size == 4
    fits = fits and heads_here == 4 and rows % LANES == 0
    body = per_device_linked if fits else per_device_plain
    return body(dp_size, mp_size, *args)


def solution(mesh):
    return jax.shard_map(
        partial(per_device, mesh.shape["dp"], mesh.shape["mp"]),
        mesh=mesh,
        in_specs=(
            P(("dp", "mp"), None),
            P(),
            P(None, "mp"),
            P(None, None, "mp"),
            P("mp", None),
            P(None, None, "mp"),
            P("mp", None),
            P(None, None, "mp"),
            P("dp"),
            P(None, "dp"),
            P(("dp", "mp"), None),
        ),
        out_specs=(
            P(("dp", "mp"), None),
            P(("dp", "mp"), None),
            P(None, ("dp", "mp")),
            P("dp", "mp"),
            P("dp", None, "mp"),
            P("mp", "dp"),
            P("dp", None, "mp"),
            P("mp", "dp"),
            P(None, "dp", "mp"),
        ),
        check_vma=False,
    )
```

```python
from functools import partial

import jax
import jax.numpy as jnp
import numpy as np
from jax import lax
from jax.experimental import pallas as pl
from jax.experimental.pallas import tpu as pltpu
from jax.sharding import PartitionSpec as P

NBIN = 64
EPSILON = 1e-06
THRESHOLDS = (8, 12, 16, 23, 32, 46, 64, 91)
NEG_FILL = -1e30
LANES = 128
MESH = pl.DeviceIdType.MESH
HBM = pltpu.MemorySpace.HBM
BF16 = jnp.bfloat16
F32 = jnp.float32


def bucket_of(relative):
    distance = jnp.abs(relative)
    bucket = jnp.minimum(distance, 7)
    for threshold in THRESHOLDS:
        bucket = bucket + (distance >= threshold).astype(jnp.int32)
    return bucket + 16 * (relative > 0).astype(jnp.int32)


def inverse_rms(values):
    return lax.rsqrt(jnp.mean(values * values, axis=-1, keepdims=True) + EPSILON)


def dot_f32(left, right, left_dim, right_dim):
    return lax.dot_general(
        left, right, (((left_dim,), (right_dim,)), ((), ())), preferred_element_type=F32
    )


def three_parts(values):
    high = values.astype(BF16)
    rest = values - high.astype(F32)
    middle = rest.astype(BF16)
    low = (rest - middle.astype(F32)).astype(BF16)
    return high, middle, low


def lane_ids(shape):
    return lax.broadcasted_iota(jnp.int32, shape, 1)


def row_ids(shape):
    return lax.broadcasted_iota(jnp.int32, shape, 0)


def attend_kernel(
    q_ref, k_ref, v_ref, layout_ref, line_ref, key_extra_ref, query_bins_ref,
    out_ref, lse_ref,
    key_aug, query_aug, strip, scores, probs,
):
    head_size, rows = q_ref.shape
    keys = k_ref.shape[1]
    blocks = keys // LANES
    width = strip.shape[1]

    @pl.when(pl.program_id(0) == 0)
    def _():
        key_aug[...] = key_extra_ref[...]
        tail = row_ids((64, rows))
        query_aug[pl.ds(192, 64), :] = jnp.where(tail == 0, 1.0, 0.0).astype(BF16)

    both = jnp.concatenate([k_ref[...], v_ref[...]], axis=0).T
    low_lanes = lane_ids((keys, LANES)) < head_size
    key_aug[:, 0:LANES] = jnp.where(low_lanes, both, key_extra_ref[:, 0:LANES])
    query_aug[pl.ds(0, 64), :] = q_ref[...]
    query_aug[pl.ds(64, 128), :] = jnp.dot(
        layout_ref[0], query_bins_ref[...], preferred_element_type=F32
    ).astype(BF16)
    strip[...] = pltpu.roll(
        jnp.broadcast_to(line_ref[0], (LANES, width)), 0, 1, stride=1, stride_axis=0
    )
    query_all = query_aug[...]
    top = jnp.full((1, rows), -jnp.inf, F32)
    for block in range(blocks):
        here = pl.ds(block * LANES, LANES)
        part = jnp.dot(key_aug[here, :], query_all, preferred_element_type=F32)
        part = part + strip[:, pl.ds((blocks - 1 - block) * LANES, rows)]
        scores[here, :] = part
        top = jnp.maximum(top, jnp.max(part, axis=0, keepdims=True))
    total = jnp.zeros((1, rows), F32)
    for block in range(blocks):
        here = pl.ds(block * LANES, LANES)
        part = jnp.exp(scores[here, :] - top)
        total = total + jnp.sum(part, axis=0, keepdims=True)
        probs[here, :] = part.astype(BF16)
    mixed = jnp.dot(v_ref[...], probs[...], preferred_element_type=F32)
    out_ref[...] = (mixed / total).astype(BF16)
    lse_ref[0] = top + jnp.log(total)


def attend_back_kernel(
    q_ref, k_ref, v_ref, out_ref, out_grad_ref, lse_ref, layout_ref, line_ref,
    key_extra_ref, key_extra_t_ref, query_bins_ref, query_bins_t_ref,
    dq_ref, dk_ref, dv_ref, line_grad_ref, layout_grad_ref,
    key_aug, key_aug_t, query_aug, value_aug, grad_aug, strip, strip_grad, probs_grad,
):
    head_size, rows = q_ref.shape
    keys = k_ref.shape[1]
    blocks = keys // LANES
    width = strip.shape[1]

    @pl.when(pl.program_id(0) == 0)
    def _():
        key_aug[...] = key_extra_ref[...]
        key_aug_t[pl.ds(64, 128), :] = key_extra_t_ref[...]
        tail = row_ids((64, rows))
        query_aug[pl.ds(192, 64), :] = jnp.where(tail == 0, 1.0, 0.0).astype(BF16)

    both = jnp.concatenate([k_ref[...], v_ref[...]], axis=0).T
    lanes = lane_ids((keys, LANES))
    key_aug[:, 0:LANES] = jnp.where(lanes < head_size, both, key_extra_ref[:, 0:LANES])
    ones = jnp.where(lanes < 3, 1.0, 0.0).astype(BF16)
    value_aug[...] = jnp.where(lanes < head_size, ones, both)
    key_aug_t[pl.ds(0, 64), :] = k_ref[...]
    query_aug[pl.ds(0, 64), :] = q_ref[...]
    query_aug[pl.ds(64, 128), :] = jnp.dot(
        layout_ref[0], query_bins_ref[...], preferred_element_type=F32
    ).astype(BF16)
    high, middle, low = three_parts(-lse_ref[0])
    tail = row_ids((64, rows))
    rows_of = lambda part: jnp.broadcast_to(part.astype(F32), (64, rows))
    query_aug[pl.ds(192, 64), :] = jnp.where(
        tail == 0, 1.0,
        jnp.where(
            tail == 1, rows_of(high),
            jnp.where(tail == 2, rows_of(middle), jnp.where(tail == 3, rows_of(low), 0.0)),
        ),
    ).astype(BF16)
    row_dot = jnp.sum(
        out_grad_ref[...].astype(F32) * out_ref[...].astype(F32), axis=0, keepdims=True
    )
    high, middle, low = three_parts(-row_dot)
    grad_aug[pl.ds(0, 64), :] = jnp.where(
        tail == 0, rows_of(high),
        jnp.where(tail == 1, rows_of(middle), jnp.where(tail == 2, rows_of(low), 0.0)),
    ).astype(BF16)
    grad_aug[pl.ds(64, 64), :] = out_grad_ref[...]
    strip[...] = pltpu.roll(
        jnp.broadcast_to(line_ref[0], (LANES, width)), 0, 1, stride=1, stride_axis=0
    )
    strip_grad[...] = jnp.zeros_like(strip_grad)
    query_and_grad = jnp.concatenate([q_ref[...], out_grad_ref[...]], axis=0).T
    query_all = query_aug[...]
    grad_all = grad_aug[...]
    half = lane_ids((LANES, LANES)) < head_size
    for block in range(blocks):
        here = pl.ds(block * LANES, LANES)
        band = pl.ds((blocks - 1 - block) * LANES, rows)
        part = jnp.dot(key_aug[here, :], query_all, preferred_element_type=F32)
        part = jnp.exp(part + strip[:, band])
        slope = part * jnp.dot(value_aug[here, :], grad_all, preferred_element_type=F32)
        strip_grad[:, band] = strip_grad[:, band] + slope
        slope = slope.astype(BF16)
        probs_grad[here, :] = slope
        key_part = jnp.dot(slope, query_and_grad, preferred_element_type=F32)
        value_part = jnp.dot(part.astype(BF16), query_and_grad, preferred_element_type=F32)
        turned = jnp.where(half, key_part, value_part).T.astype(BF16)
        dk_ref[:, here] = turned[0:64]
        dv_ref[:, here] = turned[64:128]
    query_part = jnp.dot(key_aug_t[...], probs_grad[...], preferred_element_type=F32)
    dq_ref[...] = query_part[0:64].astype(BF16)
    layout_grad_ref[0] = jnp.dot(
        query_part[64:192].astype(BF16), query_bins_t_ref[...], preferred_element_type=F32
    )
    folded = strip_grad[pl.ds(0, 8), :]
    for group in range(1, LANES // 8):
        folded = folded + pltpu.roll(strip_grad[pl.ds(group * 8, 8), :], width - group * 8, 1)
    line = folded[0:1]
    for row in range(1, 8):
        line = line + pltpu.roll(folded[row : row + 1], width - row, 1)
    line_grad_ref[0] = line


class Place:
    def __init__(self, mp_size):
        self.dp = lax.axis_index("dp")
        self.mp = lax.axis_index("mp")
        self.mp_size = mp_size
        self.core = lax.rem(self.dp, 2)
        self.x = lax.rem(lax.div(self.dp, 2), 2)
        self.y = lax.div(self.dp, 4)
        self.to_core = (self.dp + 1 - 2 * self.core, self.mp)
        self.to_x = (self.dp + 2 - 4 * self.x, self.mp)
        self.to_y = (self.dp + 4 - 8 * self.y, self.mp)
        self.to_corner = (self.dp + 6 - 4 * self.x - 8 * self.y, self.mp)

    def across(self, step):
        low = lax.rem(lax.rem(self.mp, 2) + step % 2, 2)
        high = lax.rem(lax.div(self.mp, 2) + step // 2, 2)
        return low + 2 * high

    def to_mp(self, step):
        return (self.dp, self.across(step))

    def partners(self):
        others = [self.to_mp(step) for step in range(1, self.mp_size)]
        return [self.to_core, self.to_x, self.to_y, self.to_corner] + others


def greet(place):
    barrier = pltpu.get_barrier_semaphore()
    for partner in place.partners():
        pl.semaphore_signal(barrier, inc=1, device_id=partner, device_id_type=MESH)


def meet(place):
    pl.semaphore_wait(pltpu.get_barrier_semaphore(), len(place.partners()))


class Copy:
    def __init__(self, source, target, send, receive=None, partner=None):
        self.parts = (source, target, send, receive, partner)

    def made(self):
        source, target, send, receive, partner = self.parts
        if partner is None:
            return pltpu.make_async_copy(source, target, send)
        return pltpu.make_async_remote_copy(
            src_ref=source, dst_ref=target, send_sem=send, recv_sem=receive,
            device_id=partner, device_id_type=MESH,
        )

    def start(self):
        self.made().start()

    def wait(self):
        self.made().wait()

    def wait_send(self):
        self.made().wait_send()

    def wait_recv(self):
        self.made().wait_recv()


def remote(source, target, send, receive, partner):
    return Copy(source, target, send, receive, partner)


def lanes_at(block, count):
    return pl.ds(pl.multiple_of(block * LANES, LANES), count * LANES)


class Gather:
    def __init__(self, place, pieces, outs, sems, items):
        self.place, self.pieces, self.outs = place, pieces, outs
        self.z_send, self.z_recv, self.own_sem, self.send, self.recv = sems
        self.items = items

    @staticmethod
    def semaphores(count, mp_size):
        dma = pltpu.SemaphoreType.DMA
        items = count * mp_size
        return [
            dma((count, mp_size)), dma((count, mp_size)), dma((count,)), dma((items, 6)), dma((items, 6))
        ]

    def rows(self, c, source, half):
        n = self.pieces[c].shape[1]
        if half is None:
            return pl.ds(pl.multiple_of(source * n, 16), n)
        return pl.ds(pl.multiple_of(source * n + half * (n // 2), 16), n // 2)

    def window(self, c, source, half, block, count):
        return self.outs[c].at[:, self.rows(c, source, half), lanes_at(block, count)]

    def own(self, c):
        place = self.place
        block = place.core * 4 + place.y * 2 + place.x
        return Copy(
            self.pieces[c], self.window(c, place.mp, None, block, 1), self.own_sem.at[c]
        )

    def along_mp(self, c, step):
        place = self.place
        block = place.core * 4 + place.y * 2 + place.x
        source = place.across(2) if step == 3 else place.mp
        window = self.window(c, source, None, block, 1)
        return remote(
            window if step == 3 else self.pieces[c], window,
            self.z_send.at[c, step], self.z_recv.at[c, step], place.to_mp(2 if step == 2 else 1),
        )

    def copies(self, t):
        c, k = self.items[t]
        place = self.place
        source = place.across(k)
        base = place.core * 4
        mine = base + place.y * 2 + place.x
        turned = base + (1 - place.y) * 2 + place.x

        def copy(i, half, block, count, partner):
            here = self.window(c, source, half, block, count)
            return remote(here, here, self.send.at[t, i], self.recv.at[t, i], partner)

        first = [copy(0, 0, mine, 1, place.to_x), copy(1, 1, mine, 1, place.to_y)]
        second = [
            copy(2, 0, base + place.y * 2, 2, place.to_y),
            copy(3, 1, mine, 1, place.to_x),
            copy(4, 1, turned, 1, place.to_x),
        ]
        third = [copy(5, None, base, 4, place.to_core)]
        return first, second, third

    def first(self, t):
        c, k = self.items[t]
        if k == 0:
            self.own(c).wait()
        else:
            self.along_mp(c, k).wait_recv()
        if k == 2:
            self.along_mp(c, 3).start()
        for copy in self.copies(t)[0]:
            copy.start()

    def second(self, t):
        first, second, _ = self.copies(t)
        for copy in first:
            copy.wait_recv()
        for copy in second:
            copy.start()

    def third(self, t):
        _, second, third = self.copies(t)
        for copy in second:
            copy.wait_recv()
        third[0].start()

    def run(self, ops):
        for op in ops.split():
            which, t = op[0], int(op[1:])
            if which == "z":
                self.along_mp(*self.items[t]).start()
            else:
                {"f": self.first, "s": self.second, "t": self.third}[which](t)

    def done(self, t):
        self.copies(t)[2][0].wait_recv()

    def close(self):
        for t, (c, k) in enumerate(self.items):
            first, second, third = self.copies(t)
            for copy in first + second + third:
                copy.wait_send()
            if k > 0:
                self.along_mp(c, k).wait_send()


def add_rows(target, target_index, source, source_index):
    lead, rows, lanes = target_index
    source_rows, source_lanes = source_index
    row_start, count = rows
    source_start = source_rows
    size = 32
    while count % size:
        size //= 2

    def body(i, carry):
        here = pl.ds(pl.multiple_of(row_start + i * size, size), size)
        there = pl.ds(pl.multiple_of(source_start + i * size, size), size)
        for part in range(lead):
            target[part, here, lanes] = target[part, here, lanes] + source[part, there, source_lanes]
        return carry

    lax.fori_loop(0, count // size, body, 0)


class Scatter:
    def __init__(self, place, fulls, outs, scratch, items):
        self.place, self.fulls, self.outs, self.items = place, fulls, outs, items
        count = len(fulls)
        self.whole = [len(full.shape) == 3 for full in fulls]
        buffers = [scratch[i * count : (i + 1) * count] for i in range(5)]
        self.sums, self.from_first, self.from_second, self.from_mp, self.staged = buffers
        self.own_sem, self.send, self.recv = scratch[5 * count :]
        self.steps = len(items) + 8

    @staticmethod
    def scratch(shapes, whole, mp_size):
        out = []
        for blocks in (4, 2, 1, 1):
            for lead, n in shapes:
                out.append(pltpu.VMEM((mp_size, lead, n, blocks * LANES), BF16))
        for (lead, n), is_whole in zip(shapes, whole):
            out.append(pltpu.VMEM((lead, n, 4 * LANES) if is_whole else (1, 8, LANES), BF16))
        dma = pltpu.SemaphoreType.DMA
        count = len(shapes) * mp_size
        return out + [dma((count,)), dma((count, 7)), dma((count, 7))]

    def size(self, c):
        return self.sums[c].shape[1], self.sums[c].shape[2]

    def source(self, t):
        c, k = self.items[t]
        if not self.whole[c]:
            return self.fulls[c].at[(k + 1) % 2]
        lead, n = self.size(c)
        target = self.place.across(k)
        return self.fulls[c].at[:, pl.ds(pl.multiple_of(target * n, 16), n), :]

    def from_core(self, t):
        c, k = self.items[t]
        place = self.place
        return remote(
            self.source(t).at[:, :, lanes_at((1 - place.core) * 4, 4)], self.sums[c].at[k],
            self.send.at[t, 0], self.recv.at[t, 0], place.to_core,
        )

    def own(self, t):
        c, _ = self.items[t]
        return Copy(
            self.source(t).at[:, :, lanes_at(self.place.core * 4, 4)], self.staged[c], self.own_sem.at[t]
        )

    def copies(self, t):
        c, k = self.items[t]
        place = self.place
        lead, n = self.size(c)
        top, bottom = pl.ds(0, n // 2), pl.ds(n // 2, n // 2)
        every = pl.ds(0, lead)
        sums = self.sums[c].at[k]

        def copy(i, source, landing, partner):
            return remote(source, landing, self.send.at[t, i], self.recv.at[t, i], partner)

        landing = self.from_first[c].at[k]
        first = [
            copy(
                1, sums.at[every, top, lanes_at((1 - place.y) * 2, 2)],
                landing.at[every, top, pl.ds(0, 256)], place.to_y,
            ),
            copy(
                2, sums.at[every, bottom, lanes_at(1 - place.x, 1)],
                landing.at[every, bottom, pl.ds(0, 128)], place.to_x,
            ),
            copy(
                3, sums.at[every, bottom, lanes_at(3 - place.x, 1)],
                landing.at[every, bottom, pl.ds(128, 128)], place.to_x,
            ),
        ]
        landing = self.from_second[c].at[k]
        second = [
            copy(
                4, sums.at[every, top, lanes_at(place.y * 2 + 1 - place.x, 1)],
                landing.at[every, top, pl.ds(0, 128)], place.to_x,
            ),
            copy(
                5, sums.at[every, bottom, lanes_at((1 - place.y) * 2 + place.x, 1)],
                landing.at[every, bottom, pl.ds(0, 128)], place.to_y,
            ),
        ]
        third = None
        if k > 0:
            third = copy(
                6, sums.at[:, :, lanes_at(place.y * 2 + place.x, 1)], self.from_mp[c].at[k - 1],
                place.to_mp(1 if k % 2 else 2),
            )
        return first, second, third

    def step(self, s):
        count = len(self.items)
        place = self.place
        if s < count:
            self.from_core(s).start()
        if 0 <= s - 1 < count:
            t = s - 1
            c, k = self.items[t]
            lead, n = self.size(c)
            first, *_ = self.copies(t)
            self.from_core(t).wait_recv()
            if self.whole[c]:
                self.own(t).wait()
                add_rows(self.sums[c].at[k], (lead, (0, n), pl.ds(0, 512)), self.staged[c], (0, pl.ds(0, 512)))
            else:
                add_rows(
                    self.sums[c].at[k], (lead, (0, n), pl.ds(0, 512)),
                    self.source(t), (0, lanes_at(place.core * 4, 4)),
                )
            for copy in first:
                copy.start()
        if s < count and self.whole[self.items[s][0]]:
            self.own(s).start()
        if 0 <= s - 3 < count:
            t = s - 3
            c, k = self.items[t]
            lead, n = self.size(c)
            first, second, _ = self.copies(t)
            for copy in first:
                copy.wait_recv()
            sums, landing = self.sums[c].at[k], self.from_first[c].at[k]
            half = n // 2
            add_rows(sums, (lead, (0, half), lanes_at(place.y * 2, 2)), landing, (0, pl.ds(0, 256)))
            add_rows(sums, (lead, (half, half), lanes_at(place.x, 1)), landing, (half, pl.ds(0, 128)))
            add_rows(
                sums, (lead, (half, half), lanes_at(2 + place.x, 1)), landing, (half, pl.ds(128, 128))
            )
            for copy in second:
                copy.start()
        if 0 <= s - 5 < count:
            t = s - 5
            c, k = self.items[t]
            lead, n = self.size(c)
            _, second, third = self.copies(t)
            for copy in second:
                copy.wait_recv()
            sums, landing = self.sums[c].at[k], self.from_second[c].at[k]
            mine = lanes_at(place.y * 2 + place.x, 1)
            add_rows(sums, (lead, (0, n), mine), landing, (0, pl.ds(0, 128)))
            if k % 2:
                third.start()
        if 0 <= s - 6 < count and self.items[s - 6][1] == 2:
            c, k = self.items[s - 6]
            lead, n = self.size(c)
            self.copies(self.items.index((c, 3)))[2].wait_recv()
            mine = lanes_at(place.y * 2 + place.x, 1)
            add_rows(
                self.sums[c].at[k], (lead, (0, n), mine), self.from_mp[c].at[2], (0, pl.ds(0, 128))
            )
            self.copies(s - 6)[2].start()
        if 0 <= s - 8 < count:
            c = self.items[s - 8][0]
            steps = [k for which, k in self.items if which == c]
            if self.items[s - 8][1] == steps[-1]:
                for k in steps:
                    if k in (1, 2):
                        self.copies(self.items.index((c, k)))[2].wait_recv()
                self.finish(c)

    def left(self, t):
        self.from_core(t).wait_send()

    def close(self):
        for t, (c, k) in enumerate(self.items):
            first, second, third = self.copies(t)
            if self.whole[c] or k < 2:
                self.from_core(t).wait_send()
            for copy in first + second:
                copy.wait_send()
            if third is not None:
                third.wait_send()

    def finish(self, c):
        place = self.place
        lead, n = self.size(c)
        mine = lanes_at(place.y * 2 + place.x, 1)
        sums, landing, out = self.sums[c], self.from_mp[c], self.outs[c]
        size = 32
        while n % size:
            size //= 2

        def body(i, carry):
            here = pl.ds(pl.multiple_of(i * size, size), size)
            for part in range(lead):
                total = sums[0, part, here, mine].astype(F32)
                for k in (1, 2):
                    total = total + landing[k - 1, part, here, :].astype(F32)
                out[part, here, :] = total
            return carry

        lax.fori_loop(0, n // size, body, 0)


def attention_shapes(head_count, head_size, rows, keys, width):
    whole = lambda shape: pl.BlockSpec(shape, lambda head: (0,) * len(shape))
    column = lambda size: pl.BlockSpec((head_size, size), lambda head: (head, 0))
    page = lambda a, b: pl.BlockSpec((1, a, b), lambda head: (head, 0, 0))
    return whole, column, page


def attend(queries, keys_t, values_t, layout, line, key_extra, query_bins):
    inner, rows = queries.shape
    keys = keys_t.shape[1]
    head_count, _, width = line.shape
    head_size = inner // head_count
    whole, column, page = attention_shapes(head_count, head_size, rows, keys, width)
    return pl.pallas_call(
        attend_kernel,
        grid=(head_count,),
        out_shape=(
            jax.ShapeDtypeStruct((inner, rows), BF16),
            jax.ShapeDtypeStruct((head_count, 1, rows), F32),
        ),
        in_specs=[
            column(rows), column(keys), column(keys), page(128, 128), page(1, width),
            whole((keys, 256)), whole((128, rows)),
        ],
        out_specs=(column(rows), page(1, rows)),
        scratch_shapes=[
            pltpu.VMEM((keys, 256), BF16),
            pltpu.VMEM((256, rows), BF16),
            pltpu.VMEM((LANES, width), F32),
            pltpu.VMEM((keys, rows), F32),
            pltpu.VMEM((keys, rows), BF16),
        ],
        compiler_params=pltpu.CompilerParams(
            dimension_semantics=("arbitrary",), vmem_limit_bytes=32 << 20
        ),
        name="attend",
    )(queries, keys_t, values_t, layout, line, key_extra, query_bins)


def attend_back(
    queries, keys_t, values_t, heads_out, heads_grad, lse, layout, line,
    key_extra, key_extra_t, query_bins, query_bins_t,
):
    inner, rows = queries.shape
    keys = keys_t.shape[1]
    head_count, _, width = line.shape
    head_size = inner // head_count
    whole, column, page = attention_shapes(head_count, head_size, rows, keys, width)
    return pl.pallas_call(
        attend_back_kernel,
        grid=(head_count,),
        out_shape=(
            jax.ShapeDtypeStruct((inner, rows), BF16),
            jax.ShapeDtypeStruct((inner, keys), BF16),
            jax.ShapeDtypeStruct((inner, keys), BF16),
            jax.ShapeDtypeStruct((head_count, 1, width), F32),
            jax.ShapeDtypeStruct((head_count, 128, 128), F32),
        ),
        in_specs=[
            column(rows), column(keys), column(keys), column(rows), column(rows),
            page(1, rows), page(128, 128), page(1, width),
            whole((keys, 256)), whole((128, keys)), whole((128, rows)), whole((rows, 128)),
        ],
        out_specs=(column(rows), column(keys), column(keys), page(1, width), page(128, 128)),
        scratch_shapes=[
            pltpu.VMEM((keys, 256), BF16),
            pltpu.VMEM((192, keys), BF16),
            pltpu.VMEM((256, rows), BF16),
            pltpu.VMEM((keys, 128), BF16),
            pltpu.VMEM((128, rows), BF16),
            pltpu.VMEM((LANES, width), F32),
            pltpu.VMEM((LANES, width), F32),
            pltpu.VMEM((keys, rows), BF16),
        ],
        compiler_params=pltpu.CompilerParams(
            dimension_semantics=("arbitrary",), vmem_limit_bytes=32 << 20
        ),
        name="attend_back",
    )(
        queries, keys_t, values_t, heads_out, heads_grad, lse, layout, line,
        key_extra, key_extra_t, query_bins, query_bins_t,
    )


FORWARD_ITEMS = [(0, 0), (1, 0), (2, 0), (0, 1), (0, 2), (0, 3), (1, 1), (2, 1), (1, 2), (2, 2), (1, 3), (2, 3)]


def forward_kernel(
    mp_size, group,
    query_ref, output_ref, gate_up_ref, down_ref, key_value_ref, table_ref, boxes_ref, lengths_ref,
    input_ref, gain_ref, cotangent_ref,
    w_first, queries_out, keys_out, values_out, heads_out_out, lse, layout, line, key_extra, key_extra_t,
    slot_owner_out, residual_out, layer_output, second_grad, gate_up_full, down_full, tables,
    line_hot, bin_hot, queries, keys_t, values_t, heads_out, slot_owner, residual,
    first_ref, query_piece, normed_t, slot_t, w_gate_up, w_down, first_here, key_aug, query_aug, strip, scores, probs,
    second_t, second_owner, out_owner, out_t,
    hidden_a, hidden_b, hidden_c, act_t, low_t, stage_gate_up, stage_down,
    row_send, row_recv, row_own, table_send, table_recv, table_own, load_sem, store_sem, keep_sem, *sems,
):
    place = Place(mp_size)
    rows, model_width = input_ref.shape
    keys = keys_t.shape[1]
    blocks = keys // LANES
    width = strip.shape[1]
    inner_here = first_ref.shape[1]
    heads_here = inner_here // 64
    hidden = gate_up_ref.shape[1]
    doc = lax.div(place.mp, group)
    member = lax.rem(place.mp, group)
    first_peer = place.mp - member
    own_lanes = pl.ds(pl.multiple_of(member * rows, LANES), rows)

    items = FORWARD_ITEMS
    column = lanes_at(place.core * 4 + place.y * 2 + place.x, 1)
    gather = Gather(
        place, [first_ref, gate_up_ref.at[:, :, column], down_ref.at[:, :, column]],
        [w_first, w_gate_up, w_down], sems, items
    )
    at = {item: t for t, item in enumerate(items)}

    row_copies = [
        remote(
            normed_t, slot_t.at[:, own_lanes], row_send.at[k], row_recv.at[k],
            (place.dp, first_peer + lax.rem(member + k, group)),
        )
        for k in range(1, group)
    ]
    table_copies = [
        remote(table_ref, tables.at[place.mp], table_send.at[k], table_recv.at[k], place.to_mp(k))
        for k in range(1, mp_size)
    ]
    row_here = Copy(normed_t, slot_t.at[:, own_lanes], row_own.at[0])
    table_here = Copy(table_ref, tables.at[place.mp], table_own.at[0])

    greet(place)
    loads = [
        Copy(query_ref.at[column, :], query_piece, load_sem.at[0]),
        Copy(output_ref.at[:, column], first_ref.at[3], load_sem.at[1]),
    ]
    for copy in loads:
        copy.start()
    for c in range(1, 3):
        gather.own(c).start()
    table_here.start()
    turned = key_value_ref[...].T
    first_ref[1] = turned[0:inner_here]
    first_ref[2] = turned[inner_here : 2 * inner_here]

    def norm_into(values_ref, gain):
        def body(i, carry):
            here = pl.ds(pl.multiple_of(i * 16, 16), 16)
            values = values_ref[here, :]
            scale = lax.rsqrt(jnp.mean(values * values, axis=1, keepdims=True) + EPSILON)
            second_owner[here, :] = (values * scale * gain).astype(BF16)
            return carry

        lax.fori_loop(0, rows // 16, body, 0)

    norm_into(input_ref, gain_ref[0:1, :])
    normed_t[...] = second_owner[...].T
    row_here.start()
    for copy in loads:
        copy.wait()
    first_ref[0] = query_piece[...].T
    gather.own(0).start()
    meet(place)
    gather.run("f0 f1")
    for copy in row_copies + table_copies:
        copy.start()
    gather.along_mp(0, 1).start()

    key_rows = row_ids((64, keys))
    key_bins = boxes_ref[:, pl.ds(pl.multiple_of(doc * keys, LANES), keys)]
    x_place = jnp.where(key_rows == key_bins[0:1], 1.0, 0.0).astype(BF16)
    y_place = jnp.where(key_rows == key_bins[1:2], 1.0, 0.0).astype(BF16)
    key_extra_t[0:64, :] = x_place
    key_extra_t[64:128, :] = y_place
    mask = jnp.where(lane_ids((64, keys)) >= lengths_ref[doc], NEG_FILL, 0.0)
    first_row = member * rows
    spot = lane_ids((8, width))
    spot = jnp.where(spot >= width - LANES, spot - width, spot)
    bucket = bucket_of(LANES * (blocks - 1) - spot - first_row)[0:1]
    line_hot[...] = jnp.where(row_ids((LANES, width)) == bucket, 1.0, 0.0).astype(BF16)
    spot = lane_ids((8, LANES))
    bucket = bucket_of(jnp.where(spot < NBIN, -spot, LANES - spot))[0:1]
    bin_hot[...] = jnp.where(row_ids((LANES, LANES)) == bucket, 1.0, 0.0).astype(BF16)
    tail = jnp.where(key_rows == 0, mask, jnp.where(key_rows < 4, 1.0, 0.0)).astype(BF16)
    turned = jnp.concatenate([jnp.zeros((64, keys), BF16), x_place, y_place, tail], axis=0).T
    key_extra[...] = turned
    key_aug[...] = turned
    query_aug[pl.ds(192, 64), :] = jnp.where(row_ids((64, rows)) == 0, 1.0, 0.0).astype(BF16)
    gather.run("s0 f2")
    for block in range(model_width // LANES):
        owner = block_owner(block)
        out_owner[:, owner * LANES : (owner + 1) * LANES] = cotangent_ref[
            :, block * LANES : (block + 1) * LANES
        ].astype(BF16)
    out_t[...] = cotangent_ref[...].astype(BF16).T
    residual[...] = input_ref[...]
    layer_output[...] = jnp.zeros_like(layer_output)
    second_grad[...] = jnp.zeros_like(second_grad)
    row_here.wait()
    table_here.wait()
    gather.run("s1 t0")

    head_units = mp_size * heads_here
    table = {
        (1, 0): "f3 z4 z6", (2, 0): "s3 s2 t1", (4, 0): "t3 f4 z7", (5, 0): "s4 t2", (6, 0): "f5 z8",
        (7, 0): "t4 f6", (8, 0): "s5 z9", (9, 0): "f7 s6", (11, 0): "t5", (12, 0): "f8 s7", (13, 0): "t6",
        (14, 0): "f9 s8", (16, 0): "f10 t7", (16, 2): "s9", (17, 0): "f11 t8", (17, 1): "s10",
        (17, 3): "t9", (18, 0): "s11", (18, 3): "t10", (19, 0): "t11",
    }

    def communicate(unit, point):
        for (at_unit, at_point), ops in table.items():
            if at_point == point:

                @pl.when(unit == at_unit)
                def _(ops=ops):
                    gather.run(ops)

    def head_unit(unit, carry):
        communicate(unit, 0)
        step = lax.div(unit, heads_here)
        inside = lax.rem(unit, heads_here)
        source = place.across(step)
        base = pl.multiple_of(source * inner_here, 16)
        head = source * heads_here + inside

        @pl.when(inside == 0)
        def _():
            for k in range(mp_size):

                @pl.when(step == k)
                def _(k=k):
                    gather.done(at[(0, k)])
                    if k == 0:
                        for copy in row_copies:
                            copy.wait_recv()
                    else:
                        table_copies[k - 1].wait_recv()

            load = Copy(w_first.at[:, pl.ds(base, inner_here), :], first_here, load_sem.at[0])
            load.start()
            hot = tables[source].astype(BF16)
            line[source] = jnp.dot(hot[0:8], line_hot[...], preferred_element_type=F32)
            bins = jnp.dot(hot[8:24], bin_hot[...], preferred_element_type=F32)
            for i in range(heads_here):
                x_line = jnp.broadcast_to(bins[i : i + 1], (64, LANES))
                y_line = jnp.broadcast_to(bins[8 + i : 9 + i], (64, LANES))
                left = lane_ids((64, LANES)) < 64
                x_part = pltpu.roll(x_line, 0, 1, stride=1, stride_axis=0)
                y_part = pltpu.roll(y_line, 64, 1, stride=1, stride_axis=0)
                layout[source * heads_here + i] = jnp.concatenate(
                    [jnp.where(left, x_part, 0.0), jnp.where(left, 0.0, y_part)], axis=0
                ).astype(BF16)
            load.wait()
            here = pl.ds(base, inner_here)
            queries[here, :] = jnp.dot(
                first_here[0], normed_t[...], preferred_element_type=F32
            ).astype(BF16)
            keys_t[here, :] = jnp.dot(
                first_here[1], slot_t[...], preferred_element_type=F32
            ).astype(BF16)
            values_t[here, :] = jnp.dot(
                first_here[2], slot_t[...], preferred_element_type=F32
            ).astype(BF16)

        here = pl.ds(pl.multiple_of(head * 64, 16), 64)
        both = jnp.concatenate([keys_t[here, :], values_t[here, :]], axis=0).T
        low_lanes = lane_ids((keys, LANES)) < 64
        key_aug[:, 0:LANES] = jnp.where(low_lanes, both, key_extra[:, 0:LANES])
        query_aug[pl.ds(0, 64), :] = queries[here, :]
        query_aug[pl.ds(64, 128), :] = jnp.dot(
            layout[head], key_extra_t[:, own_lanes], preferred_element_type=F32
        ).astype(BF16)
        strip[...] = pltpu.roll(
            jnp.broadcast_to(line[source, pl.ds(inside, 1), :], (LANES, width)), 0, 1,
            stride=1, stride_axis=0,
        )
        query_all = query_aug[...]
        top = jnp.full((1, rows), -jnp.inf, F32)
        for block in range(blocks):
            some = pl.ds(block * LANES, LANES)
            part = jnp.dot(key_aug[some, :], query_all, preferred_element_type=F32)
            part = part + strip[:, pl.ds((blocks - 1 - block) * LANES, rows)]
            scores[some, :] = part
            top = jnp.maximum(top, jnp.max(part, axis=0, keepdims=True))
        sums = jnp.zeros((1, rows), F32)
        for block in range(blocks):
            some = pl.ds(block * LANES, LANES)
            part = jnp.exp(scores[some, :] - top)
            sums = sums + jnp.sum(part, axis=0, keepdims=True)
            probs[some, :] = part.astype(BF16)
        mixed = jnp.dot(values_t[here, :], probs[...], preferred_element_type=F32)
        heads_out[here, :] = (mixed / sums).astype(BF16)
        lse[head] = top + jnp.log(sums)

        @pl.when(inside == heads_here - 1)
        def _():
            part = heads_out[pl.ds(base, inner_here), :].T
            residual[...] = residual[...] + jnp.dot(
                part, first_here[3], preferred_element_type=F32
            )

        return carry

    lax.fori_loop(0, head_units, head_unit, 0)
    for block in range(model_width // LANES):
        owner = block_owner(block)
        slot_owner[:, owner * LANES : (owner + 1) * LANES] = slot_t[
            block * LANES : (block + 1) * LANES, :
        ].T

    kept = [
        Copy(here, there, keep_sem.at[i])
        for i, (here, there) in enumerate(
            [
                (queries, queries_out), (keys_t, keys_out), (values_t, values_out),
                (heads_out, heads_out_out), (slot_owner, slot_owner_out), (residual, residual_out),
            ]
        )
    ]
    for copy in kept:
        copy.start()
    norm_into(residual, gain_ref[1:2, :])
    second_t[...] = second_owner[...].T
    turned_blocks = [second_owner[:, b * LANES : (b + 1) * LANES] for b in range(model_width // LANES)]
    for block, values in enumerate(turned_blocks):
        owner = block_owner(block)
        second_owner[:, owner * LANES : (owner + 1) * LANES] = values

    def store(step):
        source = place.across(step)
        here = pl.ds(pl.multiple_of(source * hidden, 16), hidden)
        return [
            Copy(stage_gate_up, gate_up_full.at[:, here, :], store_sem.at[0]),
            Copy(stage_down, down_full.at[:, here, :], store_sem.at[1]),
        ]

    def hidden_unit(step, carry):
        unit = step + head_units
        communicate(unit, 0)
        source = place.across(step)
        here = pl.ds(pl.multiple_of(source * hidden, 16), hidden)
        for k in range(mp_size):

            @pl.when(step == k)
            def _(k=k):
                gather.done(at[(1, k)])
                gather.done(at[(2, k)])

        hidden_a[...] = jnp.dot(w_gate_up[0, here, :], second_t[...], preferred_element_type=F32)
        hidden_b[...] = jnp.dot(w_gate_up[1, here, :], second_t[...], preferred_element_type=F32)
        communicate(unit, 1)
        hidden_c[...] = jnp.dot(w_down[0, here, :], out_t[...], preferred_element_type=F32)

        def activate(i, inner_carry):
            some = pl.ds(pl.multiple_of(i * 16, 16), 16)
            gate, up, slope = hidden_a[some, :], hidden_b[some, :], hidden_c[some, :]
            square = gate * gate
            factor = 0.7978845608028654
            bent = jnp.tanh(factor * gate * (1.0 + 0.044715 * square))
            half = 0.5 * (1.0 + bent)
            value = gate * half
            change = half + 0.5 * gate * (1.0 - bent * bent) * (
                factor * (1.0 + 3.0 * 0.044715 * square)
            )
            act_t[some, :] = (value * up).astype(BF16)
            low_t[some, :] = (slope * up * change).astype(BF16)
            low_t[pl.ds(pl.multiple_of(hidden + i * 16, 16), 16), :] = (slope * value).astype(BF16)
            return inner_carry

        lax.fori_loop(0, hidden // 16, activate, 0)
        communicate(unit, 2)

        @pl.when(step > 0)
        def _():
            for copy in store(step):
                copy.wait()

        stage_down[0] = jnp.dot(act_t[...], out_owner[...], preferred_element_type=F32).astype(BF16)
        stage_gate_up[0] = jnp.dot(
            low_t[0:hidden], second_owner[...], preferred_element_type=F32
        ).astype(BF16)
        stage_gate_up[1] = jnp.dot(
            low_t[hidden:], second_owner[...], preferred_element_type=F32
        ).astype(BF16)
        for copy in store(step):
            copy.start()
        communicate(unit, 3)
        layer_output[...] = layer_output[...] + dot_f32(act_t[...].T, w_down[0, here, :], 1, 0)
        second_grad[...] = (
            second_grad[...]
            + dot_f32(low_t[0:hidden].T, w_gate_up[0, here, :], 1, 0)
            + dot_f32(low_t[hidden:].T, w_gate_up[1, here, :], 1, 0)
        )
        return carry

    lax.fori_loop(0, mp_size, hidden_unit, 0)
    layer_output[...] = layer_output[...] + residual[...]
    for copy in store(mp_size - 1):
        copy.wait()
    gather.close()
    for copy in row_copies + table_copies:
        copy.wait_send()
    for copy in kept:
        copy.wait()


def block_owner(block):
    return (block % 2) * 4 + block // 2


def forward(
    mp_size, group, query, output, gate_up, down, key_value, table, boxes, lengths, layer_input,
    gains, cotangent,
):
    rows, model_width = layer_input.shape
    keys = boxes.shape[1] // lengths.shape[0]
    width = LANES * (keys // LANES + rows // LANES)
    inner_here, hidden = query.shape[1], gate_up.shape[1]
    inner, total_hidden = inner_here * mp_size, hidden * mp_size
    head_count = inner // 64
    dma = pltpu.SemaphoreType.DMA
    hbm = pl.BlockSpec(memory_space=HBM)
    vmem = pl.BlockSpec(memory_space=pltpu.VMEM)
    shape = jax.ShapeDtypeStruct
    out = [
        (shape((4, inner, model_width), BF16), hbm),
        (shape((inner, rows), BF16), hbm),
        (shape((inner, keys), BF16), hbm),
        (shape((inner, keys), BF16), hbm),
        (shape((inner, rows), BF16), hbm),
        (shape((head_count, 1, rows), F32), vmem),
        (shape((head_count, 128, 128), BF16), vmem),
        (shape((mp_size, 8, width), F32), vmem),
        (shape((keys, 256), BF16), vmem),
        (shape((128, keys), BF16), vmem),
        (shape((keys, model_width), BF16), hbm),
        (shape((rows, model_width), F32), hbm),
        (shape((rows, model_width), F32), vmem),
        (shape((rows, model_width), F32), vmem),
        (shape((2, total_hidden, model_width), BF16), hbm),
        (shape((1, total_hidden, model_width), BF16), hbm),
        (shape((mp_size, 24, LANES), F32), vmem),
        (shape((LANES, width), BF16), vmem),
        (shape((LANES, LANES), BF16), vmem),
    ]
    return pl.pallas_call(
        partial(forward_kernel, mp_size, group),
        out_shape=tuple(o[0] for o in out),
        in_specs=[hbm] * 4 + [vmem] * 3 + [pl.BlockSpec(memory_space=pltpu.SMEM)] + [vmem] * 3,
        out_specs=tuple(o[1] for o in out),
        scratch_shapes=[
            pltpu.VMEM((inner, rows), BF16),
            pltpu.VMEM((inner, keys), BF16),
            pltpu.VMEM((inner, keys), BF16),
            pltpu.VMEM((inner, rows), BF16),
            pltpu.VMEM((keys, model_width), BF16),
            pltpu.VMEM((rows, model_width), F32),
            pltpu.VMEM((4, inner_here, LANES), BF16),
            pltpu.VMEM((LANES, inner_here), BF16),
            pltpu.VMEM((model_width, rows), BF16),
            pltpu.VMEM((model_width, keys), BF16),
            pltpu.VMEM((2, total_hidden, model_width), BF16),
            pltpu.VMEM((1, total_hidden, model_width), BF16),
            pltpu.VMEM((4, inner_here, model_width), BF16),
            pltpu.VMEM((keys, 256), BF16),
            pltpu.VMEM((256, rows), BF16),
            pltpu.VMEM((LANES, width), F32),
            pltpu.VMEM((keys, rows), F32),
            pltpu.VMEM((keys, rows), BF16),
            pltpu.VMEM((model_width, rows), BF16),
            pltpu.VMEM((rows, model_width), BF16),
            pltpu.VMEM((rows, model_width), BF16),
            pltpu.VMEM((model_width, rows), BF16),
            pltpu.VMEM((hidden, rows), F32),
            pltpu.VMEM((hidden, rows), F32),
            pltpu.VMEM((hidden, rows), F32),
            pltpu.VMEM((hidden, rows), BF16),
            pltpu.VMEM((2 * hidden, rows), BF16),
            pltpu.VMEM((2, hidden, model_width), BF16),
            pltpu.VMEM((1, hidden, model_width), BF16),
            dma((group,)), dma((group,)), dma((1,)),
            dma((mp_size,)), dma((mp_size,)), dma((1,)), dma((2,)), dma((2,)), dma((6,)),
        ]
        + Gather.semaphores(3, mp_size),
        compiler_params=pltpu.CompilerParams(
            collective_id=0, has_side_effects=True, vmem_limit_bytes=62 << 20
        ),
        name="forward",
    )(
        query, output, gate_up, down, key_value, table, boxes, lengths, layer_input, gains, cotangent,
    )


BACKWARD_ITEMS = [(0, 3), (1, 3), (0, 2), (1, 2), (2, 3), (0, 1), (2, 2), (1, 1), (0, 0), (1, 0), (2, 1), (2, 0)]


def unskewed(values, first, count, shift):
    width = values.shape[1]
    folded = None
    for group in range(count // 8):
        part = values[pl.ds(first + group * 8, 8), :]
        back = (-(group * 8 + shift)) % width
        part = pltpu.roll(part, back, 1) if back else part
        folded = part if folded is None else folded + part
    total = folded[0:1]
    for row in range(1, 8):
        total = total + pltpu.roll(folded[row : row + 1], width - row, 1)
    return total


def exact_dot(left, right):
    parts = three_parts(left)
    return sum(dot_f32(part, right, 1, 1) for part in parts)


def backward_kernel(mp_size, group, *refs):
    (
        gate_up_full, down_full, w_first, queries, keys_t, values_t, heads_out,
        residual_in, second_in, cotangent_in,
        lse, layout, line, key_extra, key_extra_t, slot_owner, layer_input, gains, line_hot, bin_hot,
        input_grad, small_out, gate_up_sum, down_sum, first_sum,
        *refs,
    ) = refs
    (
        slot_grad, own_grad, residual_grad, branch_owner, branch_t, w_query, w_output, w_kv,
        q_here, k_here, v_here, out_here, grad_here, dq_here, dk_here, dv_here, kv_here,
        key_aug, key_aug_t, query_aug, value_aug, grad_aug, strip, strip_grad, probs_grad,
        layout_grad, line_sums, bin_sums, gain_part, rows_out, peers, stage, stage_in, full_here,
        load_sem, value_sem, row_send, row_recv, stage_send, stage_recv,
        *refs,
    ) = refs
    place = Place(mp_size)
    rows, model_width = layer_input.shape
    keys = slot_owner.shape[0]
    blocks = keys // LANES
    inner_here = q_here.shape[0]
    heads_here = inner_here // 64
    member = lax.rem(place.mp, group)
    first_peer = place.mp - member
    own_start = pl.multiple_of(member * rows, LANES)
    own_lanes = pl.ds(own_start, rows)

    items = BACKWARD_ITEMS
    fulls = [gate_up_full, down_full, full_here]
    scatter = Scatter(place, fulls, [gate_up_sum, down_sum, first_sum], refs, items)

    loads = [
        Copy(second_in, slot_grad.at[pl.ds(0, rows), :], value_sem.at[0]),
        Copy(residual_in, slot_grad.at[pl.ds(rows, rows), :], value_sem.at[1]),
        Copy(cotangent_in, input_grad, value_sem.at[2]),
    ]
    for copy in loads:
        copy.start()
    greet(place)
    meet(place)
    scatter.step(0)
    key_aug[...] = key_extra[...]
    key_aug_t[pl.ds(64, 128), :] = key_extra_t[...]
    for copy in loads:
        copy.wait()

    def norm_back(i, total):
        here = pl.ds(pl.multiple_of(i * 16, 16), 16)
        grad = slot_grad[here, :]
        values = slot_grad[pl.ds(pl.multiple_of(rows + i * 16, 16), 16), :]
        scale = lax.rsqrt(jnp.mean(values * values, axis=1, keepdims=True) + EPSILON)
        scaled = gains[1:2, :] * grad
        mean = jnp.mean(scaled * values, axis=1, keepdims=True)
        result = input_grad[here, :] + scale * scaled - values * (scale * scale * scale * mean)
        residual_grad[here, :] = result
        branch_owner[here, :] = result.astype(BF16)
        product = grad * values * scale
        return total + product[0:8] + product[8:16]

    total = lax.fori_loop(0, rows // 16, norm_back, jnp.zeros((8, model_width), F32))
    gain_part[...] = jnp.sum(total, axis=0, keepdims=True)
    scatter.step(1)
    branch_t[...] = branch_owner[...].T
    parts = [branch_owner[:, b * LANES : (b + 1) * LANES] for b in range(model_width // LANES)]
    for block, values in enumerate(parts):
        owner = block_owner(block)
        branch_owner[:, owner * LANES : (owner + 1) * LANES] = values
    slot_grad[...] = jnp.zeros_like(slot_grad)
    own_grad[...] = jnp.zeros_like(own_grad)
    scatter.step(2)

    plan = {
        (0, 2): [3], (0, 4): [4], (1, 2): [5], (1, 4): [6], (2, 2): [7], (2, 4): [8], (3, 4): [9],
    }
    done = 9

    def communicate(block, point):
        for (at_block, at_point), steps in plan.items():
            if at_point == point:

                @pl.when(block == at_block)
                def _(steps=steps):
                    for s in steps:
                        scatter.step(s)

    def block_unit(block, carry):
        communicate(block, 0)
        step = mp_size - 1 - block
        target = place.across(step)
        base = pl.multiple_of(target * inner_here, 16)
        here = pl.ds(base, inner_here)
        slot = lax.rem(block, 2)
        copies = [
            Copy(w_first.at[0, here, :], w_query, load_sem.at[0]),
            Copy(w_first.at[3, here, :], w_output, load_sem.at[1]),
            Copy(queries.at[here, :], q_here, load_sem.at[2]),
            Copy(keys_t.at[here, :], k_here, load_sem.at[3]),
            Copy(values_t.at[here, :], v_here, load_sem.at[4]),
            Copy(heads_out.at[here, :], out_here, load_sem.at[5]),
        ]
        for i in range(heads_here):
            for part in range(2):
                copies.append(
                    Copy(
                        w_first.at[1 + part, pl.ds(pl.multiple_of(base + i * 64, 16), 64), :],
                        w_kv.at[pl.ds(i * 128 + part * 64, 64), :],
                        load_sem.at[6 + 2 * i + part],
                    )
                )
        for copy in copies:
            copy.start()
        for copy in (copies[1], copies[5]):
            copy.wait()

        for b in range(2, mp_size):

            @pl.when(block == b)
            def _(b=b):
                scatter.left(items.index((2, mp_size + 1 - b)))

        grad_here[...] = jnp.dot(w_output[...], branch_t[...], preferred_element_type=F32).astype(BF16)
        full_here[slot, 3] = jnp.dot(
            out_here[...], branch_owner[...], preferred_element_type=F32
        ).astype(BF16)
        for copy in [copies[0]] + copies[2:5] + copies[6:]:
            copy.wait()

        def head_unit(inside, inner_carry):
            for point in range(1, heads_here):

                @pl.when(inside == point)
                def _(point=point):
                    communicate(block, point)

            head = target * heads_here + inside
            some = pl.ds(pl.multiple_of(inside * 64, 16), 64)
            q_head, k_head, v_head = q_here[some, :], k_here[some, :], v_here[some, :]
            grad_head = grad_here[some, :]
            both = jnp.concatenate([k_head, v_head], axis=0).T
            lanes = lane_ids((keys, LANES))
            key_aug[:, 0:LANES] = jnp.where(lanes < 64, both, key_extra[:, 0:LANES])
            ones = jnp.where(lanes < 3, 1.0, 0.0).astype(BF16)
            value_aug[...] = jnp.where(lanes < 64, ones, both)
            key_aug_t[pl.ds(0, 64), :] = k_head
            query_aug[pl.ds(0, 64), :] = q_head
            query_aug[pl.ds(64, 128), :] = jnp.dot(
                layout[head], key_extra_t[:, own_lanes], preferred_element_type=F32
            ).astype(BF16)
            high, middle, low = three_parts(-lse[head])
            tail = row_ids((64, rows))
            rows_of = lambda part: jnp.broadcast_to(part.astype(F32), (64, rows))
            query_aug[pl.ds(192, 64), :] = jnp.where(
                tail == 0, 1.0,
                jnp.where(
                    tail == 1, rows_of(high),
                    jnp.where(tail == 2, rows_of(middle), jnp.where(tail == 3, rows_of(low), 0.0)),
                ),
            ).astype(BF16)
            row_dot = jnp.sum(
                grad_head.astype(F32) * out_here[some, :].astype(F32), axis=0, keepdims=True
            )
            high, middle, low = three_parts(-row_dot)
            grad_aug[pl.ds(0, 64), :] = jnp.where(
                tail == 0, rows_of(high),
                jnp.where(tail == 1, rows_of(middle), jnp.where(tail == 2, rows_of(low), 0.0)),
            ).astype(BF16)
            grad_aug[pl.ds(64, 64), :] = grad_head
            width = strip.shape[1]
            strip[...] = pltpu.roll(
                jnp.broadcast_to(line[target, pl.ds(inside, 1), :], (LANES, width)), 0, 1,
                stride=1, stride_axis=0,
            )
            strip_grad[...] = jnp.zeros_like(strip_grad)
            query_and_grad = jnp.concatenate([q_head, grad_head], axis=0).T
            query_all = query_aug[...]
            grad_all = grad_aug[...]
            half = lane_ids((LANES, LANES)) < 64
            kv_lanes = pl.ds(pl.multiple_of(inside * LANES, LANES), LANES)
            for part_index in range(blocks):
                these = pl.ds(part_index * LANES, LANES)
                band = pl.ds((blocks - 1 - part_index) * LANES, rows)
                part = jnp.dot(key_aug[these, :], query_all, preferred_element_type=F32)
                part = jnp.exp(part + strip[:, band])
                slope = part * jnp.dot(value_aug[these, :], grad_all, preferred_element_type=F32)
                strip_grad[:, band] = strip_grad[:, band] + slope
                slope = slope.astype(BF16)
                probs_grad[these, :] = slope
                key_part = jnp.dot(slope, query_and_grad, preferred_element_type=F32)
                value_part = jnp.dot(part.astype(BF16), query_and_grad, preferred_element_type=F32)
                joined = jnp.where(half, key_part, value_part)
                kv_here[these, kv_lanes] = joined.astype(BF16)
                turned = joined.T.astype(BF16)
                dk_here[some, these] = turned[0:64]
                dv_here[some, these] = turned[64:128]
            query_part = jnp.dot(key_aug_t[...], probs_grad[...], preferred_element_type=F32)
            dq_here[some, :] = query_part[0:64].astype(BF16)
            bins = dot_f32(query_part[64:192].astype(BF16), key_extra_t[:, own_lanes], 1, 1)
            left = lane_ids((LANES, LANES)) < 64
            upper = row_ids((LANES, LANES)) < 64
            layout_grad[...] = jnp.where(left == upper, bins, 0.0)
            bin_sums[0, pl.ds(head, 1), :] = unskewed(layout_grad, 0, 64, 0)
            bin_sums[1, pl.ds(head, 1), :] = unskewed(layout_grad, 64, 64, 64)
            line_sums[pl.ds(head, 1), :] = unskewed(strip_grad, 0, LANES, 0)
            return inner_carry

        lax.fori_loop(0, heads_here, head_unit, 0)
        full_here[slot, 0] = jnp.dot(
            dq_here[...], slot_owner[pl.ds(own_start, rows), :], preferred_element_type=F32
        ).astype(BF16)
        full_here[slot, 1] = jnp.dot(
            dk_here[...], slot_owner[...], preferred_element_type=F32
        ).astype(BF16)
        full_here[slot, 2] = jnp.dot(
            dv_here[...], slot_owner[...], preferred_element_type=F32
        ).astype(BF16)
        slot_grad[...] = slot_grad[...] + jnp.dot(
            kv_here[...], w_kv[...], preferred_element_type=F32
        )
        own_grad[...] = own_grad[...] + jnp.dot(
            dq_here[...].T, w_query[...], preferred_element_type=F32
        )
        communicate(block, heads_here)
        return carry

    lax.fori_loop(0, mp_size, block_unit, 0)

    copies = []
    for k in range(1, group):
        other = lax.rem(member + k, group)
        rows_out[k - 1] = slot_grad[pl.ds(pl.multiple_of(other * rows, 16), rows), :].astype(BF16)
        copies.append(
            remote(
                rows_out.at[k - 1], peers.at[k - 1], row_send.at[k], row_recv.at[k],
                (place.dp, first_peer + other),
            )
        )
    for copy in copies:
        copy.start()
    steps = list(range(done + 1, scatter.steps))
    for s in steps[:1]:
        scatter.step(s)

    gain_rows = model_width // LANES
    head_count = bin_sums.shape[1]
    stage[0, 2 * gain_rows : 2 * gain_rows + head_count, :] = exact_dot(line_sums[...], line_hot[...])
    for i in range(2):
        start = 2 * gain_rows + (1 + i) * head_count
        stage[0, start : start + head_count, :] = exact_dot(bin_sums[i], bin_hot[...])
    for block in range(gain_rows):
        these = slice(block * LANES, (block + 1) * LANES)
        owner = block_owner(block)
        those = slice(owner * LANES, (owner + 1) * LANES)

        def gain_sum(i, total, these=these, those=those):
            here = pl.ds(pl.multiple_of(i * 64, 64), 64)
            product = slot_grad[here, these] * slot_owner[here, those].astype(F32)
            return total + jnp.sum(product.reshape(8, 8, LANES), axis=0)

        def own_sum(i, total, these=these, those=those):
            here = pl.ds(pl.multiple_of(i * 64, 64), 64)
            there = pl.ds(pl.multiple_of(own_start + i * 64, 64), 64)
            product = own_grad[here, these] * slot_owner[there, those].astype(F32)
            return total + jnp.sum(product.reshape(8, 8, LANES), axis=0)

        total = lax.fori_loop(0, keys // 64, gain_sum, jnp.zeros((8, LANES), F32))
        total = lax.fori_loop(0, rows // 64, own_sum, total)
        stage[0, block : block + 1, :] = (
            jnp.sum(total, axis=0, keepdims=True) / gains[0:1, these]
        )
        stage[0, gain_rows + block : gain_rows + block + 1, :] = gain_part[:, these]

    rounds = [[place.to_core], [place.to_x, place.to_y, place.to_corner]]
    rounds.append([place.to_mp(k) for k in range(1, mp_size)])
    at, sums = 0, []
    for i, partners in enumerate(rounds):
        sums.append(
            [
                remote(
                    stage.at[i], stage_in.at[at + j], stage_send.at[at + j], stage_recv.at[at + j], partner
                )
                for j, partner in enumerate(partners)
            ]
        )
        at += len(partners)
    steps = steps[1:]

    def advance(count):
        nonlocal steps
        for s in steps[:count]:
            scatter.step(s)
        steps = steps[count:]

    def round_done(i):
        at = sum(len(partners) for partners in rounds[:i])
        value = stage[i]
        for j, copy in enumerate(sums[i]):
            copy.wait_recv()
            value = value + stage_in[at + j]
        return value

    for copy in sums[0]:
        copy.start()
    advance(2)
    stage[1] = round_done(0)
    for copy in sums[1]:
        copy.start()
    advance(2)
    for copy in copies:
        copy.wait_recv()

    def input_back(i, carry):
        here = pl.ds(pl.multiple_of(i * 16, 16), 16)
        grad = own_grad[here, :] + slot_grad[pl.ds(pl.multiple_of(own_start + i * 16, 16), 16), :]
        for k in range(group - 1):
            grad = grad + peers[k, here, :].astype(F32)
        values = layer_input[here, :]
        scale = lax.rsqrt(jnp.mean(values * values, axis=1, keepdims=True) + EPSILON)
        scaled = gains[0:1, :] * grad
        mean = jnp.mean(scaled * values, axis=1, keepdims=True)
        input_grad[here, :] = (
            residual_grad[here, :] + scale * scaled - values * (scale * scale * scale * mean)
        )
        return carry

    lax.fori_loop(0, rows // 16, input_back, 0)
    advance(1)
    stage[2] = round_done(1)
    for copy in sums[2]:
        copy.start()
    advance(len(steps))
    small_out[...] = round_done(2)
    sums = sum(sums, [])
    for s in steps:
        scatter.step(s)
    scatter.close()
    for copy in copies + sums:
        copy.wait_send()


def backward(
    mp_size, group, gate_up_full, down_full, w_first, queries, keys_t, values_t, heads_out,
    residual, second_grad, cotangent, lse, layout, line, key_extra, key_extra_t, slot_owner,
    layer_input, gains, line_hot, bin_hot,
):
    rows, model_width = layer_input.shape
    keys = slot_owner.shape[0]
    width = line.shape[2]
    inner_here = queries.shape[0] // mp_size
    heads_here = inner_here // 64
    head_count = heads_here * mp_size
    hidden = down_full.shape[1] // mp_size
    sizes = [(2, hidden), (1, hidden), (4, inner_here)]
    count = 4 + mp_size - 1
    small_rows = 2 * model_width // LANES + 3 * head_count
    others = max(group - 1, 1)
    dma = pltpu.SemaphoreType.DMA
    hbm = pl.BlockSpec(memory_space=HBM)
    vmem = pl.BlockSpec(memory_space=pltpu.VMEM)
    shape = jax.ShapeDtypeStruct
    return pl.pallas_call(
        partial(backward_kernel, mp_size, group),
        out_shape=(
            shape((rows, model_width), F32),
            shape((small_rows, LANES), F32),
            *[shape((lead, n, LANES), F32) for lead, n in sizes],
        ),
        in_specs=[hbm] * 10 + [vmem] * 10,
        out_specs=(vmem,) * 5,
        scratch_shapes=[
            pltpu.VMEM((keys, model_width), F32),
            pltpu.VMEM((rows, model_width), F32),
            pltpu.VMEM((rows, model_width), F32),
            pltpu.VMEM((rows, model_width), BF16),
            pltpu.VMEM((model_width, rows), BF16),
            pltpu.VMEM((inner_here, model_width), BF16),
            pltpu.VMEM((inner_here, model_width), BF16),
            pltpu.VMEM((2 * inner_here, model_width), BF16),
            pltpu.VMEM((inner_here, rows), BF16),
            pltpu.VMEM((inner_here, keys), BF16),
            pltpu.VMEM((inner_here, keys), BF16),
            pltpu.VMEM((inner_here, rows), BF16),
            pltpu.VMEM((inner_here, rows), BF16),
            pltpu.VMEM((inner_here, rows), BF16),
            pltpu.VMEM((inner_here, keys), BF16),
            pltpu.VMEM((inner_here, keys), BF16),
            pltpu.VMEM((keys, heads_here * LANES), BF16),
            pltpu.VMEM((keys, 256), BF16),
            pltpu.VMEM((192, keys), BF16),
            pltpu.VMEM((256, rows), BF16),
            pltpu.VMEM((keys, LANES), BF16),
            pltpu.VMEM((LANES, rows), BF16),
            pltpu.VMEM((LANES, width), F32),
            pltpu.VMEM((LANES, width), F32),
            pltpu.VMEM((keys, rows), BF16),
            pltpu.VMEM((LANES, LANES), F32),
            pltpu.VMEM((head_count, width), F32),
            pltpu.VMEM((2, head_count, LANES), F32),
            pltpu.VMEM((1, model_width), F32),
            pltpu.VMEM((others, rows, model_width), BF16),
            pltpu.VMEM((others, rows, model_width), BF16),
            pltpu.VMEM((3, small_rows, LANES), F32),
            pltpu.VMEM((count, small_rows, LANES), F32),
            pltpu.VMEM((2, 4, inner_here, model_width), BF16),
            dma((6 + 2 * heads_here,)), dma((3,)), dma((group,)), dma((group,)),
            dma((count,)), dma((count,)),
        ]
        + Scatter.scratch(sizes, (True, True, False), mp_size),
        compiler_params=pltpu.CompilerParams(
            collective_id=1, has_side_effects=True, vmem_limit_bytes=63 << 20
        ),
        name="backward",
    )(
        gate_up_full, down_full, w_first, queries, keys_t, values_t, heads_out, residual,
        second_grad, cotangent, lse, layout, line, key_extra, key_extra_t, slot_owner, layer_input,
        gains, line_hot, bin_hot,
    )


def line_onehot(first_row, width, key_blocks):
    place = jnp.arange(width, dtype=jnp.int32)
    place = jnp.where(place >= width - LANES, place - width, place)
    offset = LANES * (key_blocks - 1) - place - first_row
    return (bucket_of(offset)[:, None] == jnp.arange(32, dtype=jnp.int32)[None, :]).astype(F32)


def bin_onehot():
    bins = np.arange(NBIN)
    offset = bins[:, None] - bins[None, :]
    distance = np.abs(offset)
    bucket = np.minimum(distance, 7) + sum((distance >= t).astype(np.int64) for t in THRESHOLDS)
    bucket = bucket + 16 * (offset > 0)
    return jnp.asarray(bucket[:, :, None] == np.arange(32), F32)


def gather_rows(local, axis_name):
    return lax.all_gather(local, axis_name, axis=0, tiled=True)


def scatter_grad(full):
    summed = lax.psum_scatter(full, "dp", scatter_dimension=1, tiled=True)
    return lax.psum_scatter(summed, "mp", scatter_dimension=0, tiled=True)


def per_device_plain(
    dp_size, mp_size,
    layer_input, norm_gains, query_weight, key_value_weight, output_weight,
    gate_up_weight, down_weight, bias_tables, doc_lengths, box_bins, cotangent,
):
    rows, model_width = layer_input.shape
    doc_count = doc_lengths.shape[0]
    slot_span = box_bins.shape[1] // doc_count
    group = mp_size // doc_count
    mp_index = lax.axis_index("mp")
    doc = mp_index // group
    first_row = (mp_index % group) * rows
    key_blocks = slot_span // LANES
    width = LANES * (key_blocks + (rows + LANES - 1) // LANES)
    groups = [[d * group + i for i in range(group)] for d in range(doc_count)]
    gain_first = norm_gains[0].astype(F32)
    gain_second = norm_gains[1].astype(F32)

    w_query = gather_rows(query_weight.T, "mp")
    inner_here = query_weight.shape[1]
    inner = inner_here * mp_size
    w_key = gather_rows(key_value_weight[:, 0].T, "mp")
    w_value = gather_rows(key_value_weight[:, 1].T, "mp")
    w_output = gather_rows(output_weight, "mp")
    w_gate = gather_rows(gate_up_weight[:, 0].T, "mp")
    w_up = gather_rows(gate_up_weight[:, 1].T, "mp")
    w_down = gather_rows(down_weight, "mp")
    tables = lax.all_gather(bias_tables, "mp", axis=2, tiled=True).astype(F32)
    head_count = tables.shape[2]

    onehot_line = line_onehot(first_row, width, key_blocks)
    line = jnp.dot(onehot_line, tables[0], precision=lax.Precision.HIGHEST)
    line = line.T.reshape(head_count, 1, width)
    onehot_bin = bin_onehot()
    x_part = jnp.einsum("ban,nh->hba", onehot_bin, tables[1], precision=lax.Precision.HIGHEST)
    y_part = jnp.einsum("ban,nh->hba", onehot_bin, tables[2], precision=lax.Precision.HIGHEST)
    empty = jnp.zeros_like(x_part)
    layout = jnp.concatenate(
        [jnp.concatenate([x_part, empty], axis=2), jnp.concatenate([empty, y_part], axis=2)], axis=1
    ).astype(BF16)
    key_bins = lax.dynamic_slice(box_bins, (0, doc * slot_span), (2, slot_span))
    own_bins = lax.dynamic_slice(key_bins, (0, first_row), (2, rows))
    bin_ids = jnp.arange(NBIN, dtype=jnp.int32)

    def placed_rows(bins):
        return jnp.concatenate(
            [bins[0][:, None] == bin_ids, bins[1][:, None] == bin_ids], axis=1
        ).astype(BF16)

    def placed_lanes(bins):
        return jnp.concatenate(
            [bin_ids[:, None] == bins[0][None], bin_ids[:, None] == bins[1][None]], axis=0
        ).astype(BF16)

    length = lax.dynamic_index_in_dim(doc_lengths, doc, keepdims=False)
    masked = jnp.arange(slot_span, dtype=jnp.int32)[:, None] >= length
    key_placed = placed_rows(key_bins)
    key_extra = jnp.concatenate(
        [
            jnp.zeros((slot_span, 64), BF16),
            key_placed,
            jnp.where(masked, NEG_FILL, 0.0).astype(BF16),
            jnp.ones((slot_span, 3), BF16),
            jnp.zeros((slot_span, 60), BF16),
        ],
        axis=1,
    )
    key_extra_t = placed_lanes(key_bins)
    query_bins_t = placed_rows(own_bins)
    query_bins = placed_lanes(own_bins)

    scale_first = inverse_rms(layer_input)
    normed = (layer_input * scale_first * gain_first).astype(BF16)
    slot_normed = lax.all_gather(normed, "mp", axis=0, tiled=True, axis_index_groups=groups)
    queries = dot_f32(w_query, normed, 1, 1).astype(BF16)
    keys_t = dot_f32(w_key, slot_normed, 1, 1).astype(BF16)
    values_t = dot_f32(w_value, slot_normed, 1, 1).astype(BF16)
    heads_out, lse = attend(queries, keys_t, values_t, layout, line, key_extra, query_bins)
    residual = layer_input + dot_f32(heads_out, w_output, 0, 0)
    scale_second = inverse_rms(residual)
    normed_second = (residual * scale_second * gain_second).astype(BF16)
    gate = dot_f32(normed_second, w_gate, 1, 1)
    up = dot_f32(normed_second, w_up, 1, 1)
    gelu_value, gelu_pull = jax.vjp(lambda v: jax.nn.gelu(v, approximate=True), gate)
    activated = (gelu_value * up).astype(BF16)
    layer_output = residual + dot_f32(activated, w_down, 1, 0)

    out_low = cotangent.astype(BF16)
    down_full = dot_f32(activated, out_low, 0, 0).astype(BF16)
    act_grad = dot_f32(out_low, w_down, 1, 1)
    gate_low = gelu_pull(act_grad * up)[0].astype(BF16)
    up_low = (act_grad * gelu_value).astype(BF16)
    gate_full = dot_f32(gate_low, normed_second, 0, 0).astype(BF16)
    up_full = dot_f32(up_low, normed_second, 0, 0).astype(BF16)
    second_grad = dot_f32(gate_low, w_gate, 1, 0) + dot_f32(up_low, w_up, 1, 0)
    gain_second_grad = jnp.sum(second_grad * residual * scale_second, axis=0)
    scaled = gain_second * second_grad
    residual_grad = (
        cotangent
        + scale_second * scaled
        - residual * scale_second**3 * jnp.mean(scaled * residual, axis=-1, keepdims=True)
    )

    branch_low = residual_grad.astype(BF16)
    output_full = dot_f32(heads_out, branch_low, 1, 0).astype(BF16)
    heads_grad = dot_f32(w_output, branch_low, 1, 1).astype(BF16)
    dq, dk, dv, line_grad, layout_grad = attend_back(
        queries, keys_t, values_t, heads_out, heads_grad, lse, layout, line,
        key_extra, key_extra_t, query_bins, query_bins_t,
    )
    query_full = dot_f32(dq, normed, 1, 0).astype(BF16)
    key_full = dot_f32(dk, slot_normed, 1, 0).astype(BF16)
    value_full = dot_f32(dv, slot_normed, 1, 0).astype(BF16)
    slot_grad = dot_f32(dk, w_key, 0, 0) + dot_f32(dv, w_value, 0, 0)
    first_grad = lax.psum_scatter(
        slot_grad.astype(BF16), "mp", scatter_dimension=0, tiled=True, axis_index_groups=groups
    ).astype(F32) + dot_f32(dq, w_query, 0, 0)
    gain_first_grad = jnp.sum(first_grad * layer_input * scale_first, axis=0)
    scaled = gain_first * first_grad
    input_grad = (
        residual_grad
        + scale_first * scaled
        - layer_input * scale_first**3 * jnp.mean(scaled * layer_input, axis=-1, keepdims=True)
    )

    gain_grad = lax.psum_scatter(
        jnp.stack([gain_first_grad, gain_second_grad]), ("dp", "mp"), scatter_dimension=1, tiled=True
    )
    line_part = jnp.dot(
        onehot_line.T, line_grad[:, 0].T, precision=lax.Precision.HIGHEST
    )
    x_part = jnp.einsum(
        "ban,hba->nh", onehot_bin, layout_grad[:, :64, :64], precision=lax.Precision.HIGHEST
    )
    y_part = jnp.einsum(
        "ban,hba->nh", onehot_bin, layout_grad[:, 64:, 64:], precision=lax.Precision.HIGHEST
    )
    table_full = jnp.stack([line_part, x_part, y_part])
    table_grad = lax.psum_scatter(
        lax.psum_scatter(table_full, "mp", scatter_dimension=2, tiled=True),
        "dp", scatter_dimension=1, tiled=True,
    )

    query_grad = scatter_grad(query_full).T.astype(F32)
    key_value_grad = jnp.stack(
        [scatter_grad(key_full).T, scatter_grad(value_full).T], axis=1
    ).astype(F32)
    output_grad = scatter_grad(output_full).astype(F32)
    gate_up_grad = jnp.stack(
        [scatter_grad(gate_full).T, scatter_grad(up_full).T], axis=1
    ).astype(F32)
    down_grad = scatter_grad(down_full).astype(F32)
    return (
        layer_output, input_grad, gain_grad, query_grad, key_value_grad,
        output_grad, gate_up_grad, down_grad, table_grad,
    )


def per_device_linked(
    dp_size, mp_size,
    layer_input, norm_gains, query_weight, key_value_weight, output_weight,
    gate_up_weight, down_weight, bias_tables, doc_lengths, box_bins, cotangent,
):
    rows, model_width = layer_input.shape
    doc_count = doc_lengths.shape[0]
    group = mp_size // doc_count
    dp_index, mp_index = lax.axis_index("dp"), lax.axis_index("mp")
    heads_here = bias_tables.shape[2]
    head_count = heads_here * mp_size
    inner_here = query_weight.shape[1]
    gains = norm_gains.astype(F32)
    column = ((dp_index % 2) * 4 + dp_index // 2) * LANES
    key_value = lax.dynamic_slice_in_dim(key_value_weight, column, LANES, 0)
    table = jnp.swapaxes(bias_tables.astype(F32), 1, 2)
    table = jnp.pad(table, ((0, 0), (0, 8 - heads_here), (0, LANES - 32))).reshape(24, LANES)
    (
        w_first, queries, keys_t, values_t, heads_out, lse, layout, line, key_extra, key_extra_t,
        slot_owner, residual, layer_output, second_grad, gate_up_full, down_full, _, line_hot, bin_hot,
    ) = forward(
        mp_size, group, query_weight, output_weight, jnp.transpose(gate_up_weight, (1, 2, 0)),
        down_weight[None], key_value.reshape(LANES, 2 * inner_here), table, box_bins, doc_lengths,
        layer_input, gains, cotangent,
    )
    input_grad, small, gate_up_sum, down_sum, summed = backward(
        mp_size, group, gate_up_full, down_full, w_first, queries, keys_t, values_t, heads_out,
        residual, second_grad, cotangent, lse, layout, line, key_extra, key_extra_t, slot_owner,
        layer_input, gains, line_hot, bin_hot,
    )
    gain_rows = model_width // LANES
    gains = small[: 2 * gain_rows].reshape(2, model_width)
    share = model_width // (dp_size * mp_size)
    at = (dp_index * mp_size + mp_index) * share
    gain_grad = lax.dynamic_slice(gains, (0, at), (2, share))
    tables = small[2 * gain_rows :].reshape(3, head_count, LANES)
    table_grad = lax.dynamic_slice(
        tables,
        (0, mp_index * heads_here, dp_index * (32 // dp_size)),
        (3, heads_here, 32 // dp_size),
    )
    table_grad = jnp.swapaxes(table_grad, 1, 2)
    query_grad = summed[0].T
    key_value_grad = jnp.transpose(summed[1:3], (2, 0, 1))
    gate_up_grad = jnp.transpose(gate_up_sum, (2, 0, 1))
    return (
        layer_output, input_grad, gain_grad, query_grad, key_value_grad,
        summed[3], gate_up_grad, down_sum[0], table_grad,
    )


def per_device(dp_size, mp_size, *args):
    rows, model_width = args[0].shape
    heads_here = args[7].shape[2]
    fits = dp_size == 8 and model_width == 8 * LANES and mp_size == 4
    fits = fits and heads_here == 4 and rows % LANES == 0
    body = per_device_linked if fits else per_device_plain
    return body(dp_size, mp_size, *args)


def solution(mesh):
    return jax.shard_map(
        partial(per_device, mesh.shape["dp"], mesh.shape["mp"]),
        mesh=mesh,
        in_specs=(
            P(("dp", "mp"), None),
            P(),
            P(None, "mp"),
            P(None, None, "mp"),
            P("mp", None),
            P(None, None, "mp"),
            P("mp", None),
            P(None, None, "mp"),
            P("dp"),
            P(None, "dp"),
            P(("dp", "mp"), None),
        ),
        out_specs=(
            P(("dp", "mp"), None),
            P(("dp", "mp"), None),
            P(None, ("dp", "mp")),
            P("dp", "mp"),
            P("dp", None, "mp"),
            P("mp", "dp"),
            P("dp", None, "mp"),
            P("mp", "dp"),
            P(None, "dp", "mp"),
        ),
        check_vma=False,
    )
```

```python
from functools import partial

import jax
import jax.numpy as jnp
import numpy as np
from jax import lax
from jax.experimental import pallas as pl
from jax.experimental.pallas import tpu as pltpu
from jax.sharding import PartitionSpec as P

NBIN = 64
EPSILON = 1e-06
THRESHOLDS = (8, 12, 16, 23, 32, 46, 64, 91)
NEG_FILL = -1e30
LANES = 128
MESH = pl.DeviceIdType.MESH
HBM = pltpu.MemorySpace.HBM
BF16 = jnp.bfloat16
F32 = jnp.float32


def bucket_of(relative):
    distance = jnp.abs(relative)
    bucket = jnp.minimum(distance, 7)
    for threshold in THRESHOLDS:
        bucket = bucket + (distance >= threshold).astype(jnp.int32)
    return bucket + 16 * (relative > 0).astype(jnp.int32)


def inverse_rms(values):
    return lax.rsqrt(jnp.mean(values * values, axis=-1, keepdims=True) + EPSILON)


def dot_f32(left, right, left_dim, right_dim):
    return lax.dot_general(
        left, right, (((left_dim,), (right_dim,)), ((), ())), preferred_element_type=F32
    )


def three_parts(values):
    high = values.astype(BF16)
    rest = values - high.astype(F32)
    middle = rest.astype(BF16)
    low = (rest - middle.astype(F32)).astype(BF16)
    return high, middle, low


def lane_ids(shape):
    return lax.broadcasted_iota(jnp.int32, shape, 1)


def row_ids(shape):
    return lax.broadcasted_iota(jnp.int32, shape, 0)


def attend_kernel(
    q_ref, k_ref, v_ref, layout_ref, line_ref, key_extra_ref, query_bins_ref,
    out_ref, lse_ref,
    key_aug, query_aug, strip, scores, probs,
):
    head_size, rows = q_ref.shape
    keys = k_ref.shape[1]
    blocks = keys // LANES
    width = strip.shape[1]

    @pl.when(pl.program_id(0) == 0)
    def _():
        key_aug[...] = key_extra_ref[...]
        tail = row_ids((64, rows))
        query_aug[pl.ds(192, 64), :] = jnp.where(tail == 0, 1.0, 0.0).astype(BF16)

    both = jnp.concatenate([k_ref[...], v_ref[...]], axis=0).T
    low_lanes = lane_ids((keys, LANES)) < head_size
    key_aug[:, 0:LANES] = jnp.where(low_lanes, both, key_extra_ref[:, 0:LANES])
    query_aug[pl.ds(0, 64), :] = q_ref[...]
    query_aug[pl.ds(64, 128), :] = jnp.dot(
        layout_ref[0], query_bins_ref[...], preferred_element_type=F32
    ).astype(BF16)
    strip[...] = pltpu.roll(
        jnp.broadcast_to(line_ref[0], (LANES, width)), 0, 1, stride=1, stride_axis=0
    )
    query_all = query_aug[...]
    top = jnp.full((1, rows), -jnp.inf, F32)
    for block in range(blocks):
        here = pl.ds(block * LANES, LANES)
        part = jnp.dot(key_aug[here, :], query_all, preferred_element_type=F32)
        part = part + strip[:, pl.ds((blocks - 1 - block) * LANES, rows)]
        scores[here, :] = part
        top = jnp.maximum(top, jnp.max(part, axis=0, keepdims=True))
    total = jnp.zeros((1, rows), F32)
    for block in range(blocks):
        here = pl.ds(block * LANES, LANES)
        part = jnp.exp(scores[here, :] - top)
        total = total + jnp.sum(part, axis=0, keepdims=True)
        probs[here, :] = part.astype(BF16)
    mixed = jnp.dot(v_ref[...], probs[...], preferred_element_type=F32)
    out_ref[...] = (mixed / total).astype(BF16)
    lse_ref[0] = top + jnp.log(total)


def attend_back_kernel(
    q_ref, k_ref, v_ref, out_ref, out_grad_ref, lse_ref, layout_ref, line_ref,
    key_extra_ref, key_extra_t_ref, query_bins_ref, query_bins_t_ref,
    dq_ref, dk_ref, dv_ref, line_grad_ref, layout_grad_ref,
    key_aug, key_aug_t, query_aug, value_aug, grad_aug, strip, strip_grad, probs_grad,
):
    head_size, rows = q_ref.shape
    keys = k_ref.shape[1]
    blocks = keys // LANES
    width = strip.shape[1]

    @pl.when(pl.program_id(0) == 0)
    def _():
        key_aug[...] = key_extra_ref[...]
        key_aug_t[pl.ds(64, 128), :] = key_extra_t_ref[...]
        tail = row_ids((64, rows))
        query_aug[pl.ds(192, 64), :] = jnp.where(tail == 0, 1.0, 0.0).astype(BF16)

    both = jnp.concatenate([k_ref[...], v_ref[...]], axis=0).T
    lanes = lane_ids((keys, LANES))
    key_aug[:, 0:LANES] = jnp.where(lanes < head_size, both, key_extra_ref[:, 0:LANES])
    ones = jnp.where(lanes < 3, 1.0, 0.0).astype(BF16)
    value_aug[...] = jnp.where(lanes < head_size, ones, both)
    key_aug_t[pl.ds(0, 64), :] = k_ref[...]
    query_aug[pl.ds(0, 64), :] = q_ref[...]
    query_aug[pl.ds(64, 128), :] = jnp.dot(
        layout_ref[0], query_bins_ref[...], preferred_element_type=F32
    ).astype(BF16)
    high, middle, low = three_parts(-lse_ref[0])
    tail = row_ids((64, rows))
    rows_of = lambda part: jnp.broadcast_to(part.astype(F32), (64, rows))
    query_aug[pl.ds(192, 64), :] = jnp.where(
        tail == 0, 1.0,
        jnp.where(
            tail == 1, rows_of(high),
            jnp.where(tail == 2, rows_of(middle), jnp.where(tail == 3, rows_of(low), 0.0)),
        ),
    ).astype(BF16)
    row_dot = jnp.sum(
        out_grad_ref[...].astype(F32) * out_ref[...].astype(F32), axis=0, keepdims=True
    )
    high, middle, low = three_parts(-row_dot)
    grad_aug[pl.ds(0, 64), :] = jnp.where(
        tail == 0, rows_of(high),
        jnp.where(tail == 1, rows_of(middle), jnp.where(tail == 2, rows_of(low), 0.0)),
    ).astype(BF16)
    grad_aug[pl.ds(64, 64), :] = out_grad_ref[...]
    strip[...] = pltpu.roll(
        jnp.broadcast_to(line_ref[0], (LANES, width)), 0, 1, stride=1, stride_axis=0
    )
    strip_grad[...] = jnp.zeros_like(strip_grad)
    query_and_grad = jnp.concatenate([q_ref[...], out_grad_ref[...]], axis=0).T
    query_all = query_aug[...]
    grad_all = grad_aug[...]
    half = lane_ids((LANES, LANES)) < head_size
    for block in range(blocks):
        here = pl.ds(block * LANES, LANES)
        band = pl.ds((blocks - 1 - block) * LANES, rows)
        part = jnp.dot(key_aug[here, :], query_all, preferred_element_type=F32)
        part = jnp.exp(part + strip[:, band])
        slope = part * jnp.dot(value_aug[here, :], grad_all, preferred_element_type=F32)
        strip_grad[:, band] = strip_grad[:, band] + slope
        slope = slope.astype(BF16)
        probs_grad[here, :] = slope
        key_part = jnp.dot(slope, query_and_grad, preferred_element_type=F32)
        value_part = jnp.dot(part.astype(BF16), query_and_grad, preferred_element_type=F32)
        turned = jnp.where(half, key_part, value_part).T.astype(BF16)
        dk_ref[:, here] = turned[0:64]
        dv_ref[:, here] = turned[64:128]
    query_part = jnp.dot(key_aug_t[...], probs_grad[...], preferred_element_type=F32)
    dq_ref[...] = query_part[0:64].astype(BF16)
    layout_grad_ref[0] = jnp.dot(
        query_part[64:192].astype(BF16), query_bins_t_ref[...], preferred_element_type=F32
    )
    folded = strip_grad[pl.ds(0, 8), :]
    for group in range(1, LANES // 8):
        folded = folded + pltpu.roll(strip_grad[pl.ds(group * 8, 8), :], width - group * 8, 1)
    line = folded[0:1]
    for row in range(1, 8):
        line = line + pltpu.roll(folded[row : row + 1], width - row, 1)
    line_grad_ref[0] = line


class Place:
    def __init__(self, mp_size):
        self.dp = lax.axis_index("dp")
        self.mp = lax.axis_index("mp")
        self.mp_size = mp_size
        self.core = lax.rem(self.dp, 2)
        self.x = lax.rem(lax.div(self.dp, 2), 2)
        self.y = lax.div(self.dp, 4)
        self.to_core = (self.dp + 1 - 2 * self.core, self.mp)
        self.to_x = (self.dp + 2 - 4 * self.x, self.mp)
        self.to_y = (self.dp + 4 - 8 * self.y, self.mp)
        self.to_corner = (self.dp + 6 - 4 * self.x - 8 * self.y, self.mp)

    def across(self, step):
        low = lax.rem(lax.rem(self.mp, 2) + step % 2, 2)
        high = lax.rem(lax.div(self.mp, 2) + step // 2, 2)
        return low + 2 * high

    def to_mp(self, step):
        return (self.dp, self.across(step))

    def partners(self):
        others = [self.to_mp(step) for step in range(1, self.mp_size)]
        return [self.to_core, self.to_x, self.to_y, self.to_corner] + others


def greet(place):
    barrier = pltpu.get_barrier_semaphore()
    for partner in place.partners():
        pl.semaphore_signal(barrier, inc=1, device_id=partner, device_id_type=MESH)


def meet(place):
    pl.semaphore_wait(pltpu.get_barrier_semaphore(), len(place.partners()))


class Copy:
    def __init__(self, source, target, send, receive=None, partner=None):
        self.parts = (source, target, send, receive, partner)

    def made(self):
        source, target, send, receive, partner = self.parts
        if partner is None:
            return pltpu.make_async_copy(source, target, send)
        return pltpu.make_async_remote_copy(
            src_ref=source, dst_ref=target, send_sem=send, recv_sem=receive,
            device_id=partner, device_id_type=MESH,
        )

    def start(self):
        self.made().start()

    def wait(self):
        self.made().wait()

    def wait_send(self):
        self.made().wait_send()

    def wait_recv(self):
        self.made().wait_recv()


def remote(source, target, send, receive, partner):
    return Copy(source, target, send, receive, partner)


def lanes_at(block, count):
    return pl.ds(pl.multiple_of(block * LANES, LANES), count * LANES)


class Gather:
    def __init__(self, place, pieces, outs, sems, items):
        self.place, self.pieces, self.outs = place, pieces, outs
        self.z_send, self.z_recv, self.own_sem, self.send, self.recv = sems
        self.items = items

    @staticmethod
    def semaphores(count, mp_size):
        dma = pltpu.SemaphoreType.DMA
        items = count * mp_size
        return [
            dma((count, mp_size)), dma((count, mp_size)), dma((count,)), dma((items, 6)), dma((items, 6))
        ]

    def rows(self, c, source, half):
        n = self.pieces[c].shape[1]
        if half is None:
            return pl.ds(pl.multiple_of(source * n, 16), n)
        return pl.ds(pl.multiple_of(source * n + half * (n // 2), 16), n // 2)

    def window(self, c, source, half, block, count):
        return self.outs[c].at[:, self.rows(c, source, half), lanes_at(block, count)]

    def own(self, c):
        place = self.place
        block = place.core * 4 + place.y * 2 + place.x
        return Copy(
            self.pieces[c], self.window(c, place.mp, None, block, 1), self.own_sem.at[c]
        )

    def along_mp(self, c, step):
        place = self.place
        block = place.core * 4 + place.y * 2 + place.x
        source = place.across(2) if step == 3 else place.mp
        window = self.window(c, source, None, block, 1)
        return remote(
            window if step == 3 else self.pieces[c], window,
            self.z_send.at[c, step], self.z_recv.at[c, step], place.to_mp(2 if step == 2 else 1),
        )

    def copies(self, t):
        c, k = self.items[t]
        place = self.place
        source = place.across(k)
        base = place.core * 4
        mine = base + place.y * 2 + place.x
        turned = base + (1 - place.y) * 2 + place.x

        def copy(i, half, block, count, partner):
            here = self.window(c, source, half, block, count)
            return remote(here, here, self.send.at[t, i], self.recv.at[t, i], partner)

        first = [copy(0, 0, mine, 1, place.to_x), copy(1, 1, mine, 1, place.to_y)]
        second = [
            copy(2, 0, base + place.y * 2, 2, place.to_y),
            copy(3, 1, mine, 1, place.to_x),
            copy(4, 1, turned, 1, place.to_x),
        ]
        third = [copy(5, None, base, 4, place.to_core)]
        return first, second, third

    def first(self, t):
        c, k = self.items[t]
        if k == 0:
            self.own(c).wait()
        else:
            self.along_mp(c, k).wait_recv()
        if k == 2:
            self.along_mp(c, 3).start()
        for copy in self.copies(t)[0]:
            copy.start()

    def second(self, t):
        first, second, _ = self.copies(t)
        for copy in first:
            copy.wait_recv()
        for copy in second:
            copy.start()

    def third(self, t):
        _, second, third = self.copies(t)
        for copy in second:
            copy.wait_recv()
        third[0].start()

    def run(self, ops):
        for op in ops.split():
            which, t = op[0], int(op[1:])
            if which == "z":
                self.along_mp(*self.items[t]).start()
            else:
                {"f": self.first, "s": self.second, "t": self.third}[which](t)

    def done(self, t):
        self.copies(t)[2][0].wait_recv()

    def close(self):
        for t, (c, k) in enumerate(self.items):
            first, second, third = self.copies(t)
            for copy in first + second + third:
                copy.wait_send()
            if k > 0:
                self.along_mp(c, k).wait_send()


def add_rows(target, target_index, source, source_index):
    lead, rows, lanes = target_index
    source_rows, source_lanes = source_index
    row_start, count = rows
    source_start = source_rows
    size = 32
    while count % size:
        size //= 2

    def body(i, carry):
        here = pl.ds(pl.multiple_of(row_start + i * size, size), size)
        there = pl.ds(pl.multiple_of(source_start + i * size, size), size)
        for part in range(lead):
            target[part, here, lanes] = target[part, here, lanes] + source[part, there, source_lanes]
        return carry

    lax.fori_loop(0, count // size, body, 0)


class Scatter:
    def __init__(self, place, fulls, outs, scratch, items, shares=None, inside=False):
        self.inside = inside
        self.place, self.fulls, self.outs, self.items = place, fulls, outs, items
        count = len(fulls)
        self.shares = shares or [None] * count
        self.held = [sorted(k for c, k in items if c == which) for which in range(count)]
        self.whole = [len(full.shape) == 3 for full in fulls]
        buffers = [scratch[i * count : (i + 1) * count] for i in range(5)]
        self.sums, self.from_first, self.from_second, self.from_mp, self.staged = buffers
        self.own_sem, self.send, self.recv, self.share_send, self.share_recv = scratch[5 * count :]

    @staticmethod
    def scratch(shapes, whole, items):
        out = []
        for part, blocks in enumerate((4, 2, 1, 1)):
            for c, (lead, n) in enumerate(shapes):
                slots = sum(which == c for which, _ in items)
                if part == 3:
                    slots, lead, n = (3, lead, n) if slots > 1 else (1, 1, 16)
                out.append(pltpu.VMEM((slots, lead, n, blocks * LANES), BF16))
        for (lead, n), is_whole in zip(shapes, whole):
            out.append(pltpu.VMEM((lead, n, 4 * LANES) if is_whole else (1, 16, LANES), BF16))
        dma = pltpu.SemaphoreType.DMA
        count = len(items)
        out += [dma((count,)), dma((count, 7)), dma((count, 7))]
        return out + [dma((len(shapes),)), dma((len(shapes),))]

    def slot(self, c, k):
        return self.held[c].index(k)

    def size(self, c):
        return self.sums[c].shape[1], self.sums[c].shape[2]

    def source(self, t):
        c, k = self.items[t]
        if not self.whole[c]:
            return self.fulls[c].at[(k + 1) % 2]
        lead, n = self.size(c)
        target = self.place.across(k)
        return self.fulls[c].at[:, pl.ds(pl.multiple_of(target * n, 16), n), :]

    def from_core(self, t):
        c, k = self.items[t]
        place = self.place
        return remote(
            self.source(t).at[:, :, lanes_at((1 - place.core) * 4, 4)], self.sums[c].at[self.slot(c, k)],
            self.send.at[t, 0], self.recv.at[t, 0], place.to_core,
        )

    def own(self, t):
        c, _ = self.items[t]
        return Copy(
            self.source(t).at[:, :, lanes_at(self.place.core * 4, 4)], self.staged[c], self.own_sem.at[t]
        )

    def copies(self, t):
        c, k = self.items[t]
        place = self.place
        lead, n = self.size(c)
        top, bottom = pl.ds(0, n // 2), pl.ds(n // 2, n // 2)
        every = pl.ds(0, lead)
        sums = self.sums[c].at[self.slot(c, k)]

        def copy(i, source, landing, partner):
            return remote(source, landing, self.send.at[t, i], self.recv.at[t, i], partner)

        landing = self.from_first[c].at[self.slot(c, k)]
        first = [
            copy(
                1, sums.at[every, top, lanes_at((1 - place.y) * 2, 2)],
                landing.at[every, top, pl.ds(0, 256)], place.to_y,
            ),
            copy(
                2, sums.at[every, bottom, lanes_at(1 - place.x, 1)],
                landing.at[every, bottom, pl.ds(0, 128)], place.to_x,
            ),
            copy(
                3, sums.at[every, bottom, lanes_at(3 - place.x, 1)],
                landing.at[every, bottom, pl.ds(128, 128)], place.to_x,
            ),
        ]
        landing = self.from_second[c].at[self.slot(c, k)]
        second = [
            copy(
                4, sums.at[every, top, lanes_at(place.y * 2 + 1 - place.x, 1)],
                landing.at[every, top, pl.ds(0, 128)], place.to_x,
            ),
            copy(
                5, sums.at[every, bottom, lanes_at((1 - place.y) * 2 + place.x, 1)],
                landing.at[every, bottom, pl.ds(0, 128)], place.to_y,
            ),
        ]
        third = None
        if k > 0:
            third = copy(
                6, sums.at[:, :, lanes_at(place.y * 2 + place.x, 1)], self.from_mp[c].at[k - 1],
                place.to_mp(1 if k % 2 else 2),
            )
        return first, second, third

    def core(self, t):
        self.from_core(t).start()
        if self.whole[self.items[t][0]]:
            self.own(t).start()

    def first(self, t):
        c, k = self.items[t]
        lead, n = self.size(c)
        sums = self.sums[c].at[self.slot(c, k)]
        self.from_core(t).wait_recv()
        if self.whole[c]:
            self.own(t).wait()
            add_rows(sums, (lead, (0, n), pl.ds(0, 512)), self.staged[c], (0, pl.ds(0, 512)))
        else:
            mine = lanes_at(self.place.core * 4, 4)
            add_rows(sums, (lead, (0, n), pl.ds(0, 512)), self.source(t), (0, mine))
        for copy in self.copies(t)[0]:
            copy.start()

    def second(self, t):
        c, k = self.items[t]
        place = self.place
        lead, n = self.size(c)
        first, second, _ = self.copies(t)
        for copy in first:
            copy.wait_recv()
        slot = self.slot(c, k)
        sums, landing = self.sums[c].at[slot], self.from_first[c].at[slot]
        half = n // 2
        add_rows(sums, (lead, (0, half), lanes_at(place.y * 2, 2)), landing, (0, pl.ds(0, 256)))
        add_rows(sums, (lead, (half, half), lanes_at(place.x, 1)), landing, (half, pl.ds(0, 128)))
        add_rows(sums, (lead, (half, half), lanes_at(2 + place.x, 1)), landing, (half, pl.ds(128, 128)))
        for copy in second:
            copy.start()

    def third(self, t):
        c, k = self.items[t]
        lead, n = self.size(c)
        _, second, third = self.copies(t)
        for copy in second:
            copy.wait_recv()
        slot = self.slot(c, k)
        mine = lanes_at(self.place.y * 2 + self.place.x, 1)
        add_rows(
            self.sums[c].at[slot], (lead, (0, n), mine), self.from_second[c].at[slot], (0, pl.ds(0, 128))
        )
        if k == 2:
            self.copies(self.items.index((c, 3)))[2].wait_recv()
            add_rows(
                self.sums[c].at[slot], (lead, (0, n), mine), self.from_mp[c].at[2], (0, pl.ds(0, 128))
            )
        if k > 0 and not self.inside:
            third.start()

    def share(self, c):
        return remote(
            self.shares[c], self.from_mp[c].at[0], self.share_send.at[c], self.share_recv.at[c],
            self.place.to_mp(1),
        )

    def end(self, c):
        if self.inside:
            self.finish(c)
            return
        if self.shares[c] is not None:
            self.share(c).wait_recv()
        for k in (1, 2):
            if (c, k) in self.items:
                self.copies(self.items.index((c, k)))[2].wait_recv()
        self.finish(c)

    def run(self, ops):
        for op in ops.split():
            table = {"c": self.core, "f": self.first, "s": self.second, "t": self.third, "e": self.end}
            table[op[0]](int(op[1:]))

    def left(self, t):
        self.from_core(t).wait_send()

    def close(self):
        for t, (c, k) in enumerate(self.items):
            first, second, third = self.copies(t)
            if self.whole[c] or k < 2:
                self.from_core(t).wait_send()
            for copy in first + second:
                copy.wait_send()
            if third is not None and not self.inside:
                third.wait_send()
        for c, share in enumerate(self.shares):
            if share is not None:
                self.share(c).wait_send()

    def finish(self, c):
        place = self.place
        lead, n = self.size(c)
        mine = lanes_at(place.y * 2 + place.x, 1)
        sums, landing, out = self.sums[c], self.from_mp[c], self.outs[c]
        steps = () if self.inside else (1, 2)
        slot = self.slot(c, 1 if self.inside else 0)
        size = 32
        while n % size:
            size //= 2

        def body(i, carry):
            here = pl.ds(pl.multiple_of(i * size, size), size)
            for part in range(lead):
                total = sums[slot, part, here, mine].astype(F32)
                for k in steps:
                    total = total + landing[k - 1, part, here, :].astype(F32)
                out[part, here, :] = total.astype(out.dtype)
            return carry

        lax.fori_loop(0, n // size, body, 0)


def attention_shapes(head_count, head_size, rows, keys, width):
    whole = lambda shape: pl.BlockSpec(shape, lambda head: (0,) * len(shape))
    column = lambda size: pl.BlockSpec((head_size, size), lambda head: (head, 0))
    page = lambda a, b: pl.BlockSpec((1, a, b), lambda head: (head, 0, 0))
    return whole, column, page


def attend(queries, keys_t, values_t, layout, line, key_extra, query_bins):
    inner, rows = queries.shape
    keys = keys_t.shape[1]
    head_count, _, width = line.shape
    head_size = inner // head_count
    whole, column, page = attention_shapes(head_count, head_size, rows, keys, width)
    return pl.pallas_call(
        attend_kernel,
        grid=(head_count,),
        out_shape=(
            jax.ShapeDtypeStruct((inner, rows), BF16),
            jax.ShapeDtypeStruct((head_count, 1, rows), F32),
        ),
        in_specs=[
            column(rows), column(keys), column(keys), page(128, 128), page(1, width),
            whole((keys, 256)), whole((128, rows)),
        ],
        out_specs=(column(rows), page(1, rows)),
        scratch_shapes=[
            pltpu.VMEM((keys, 256), BF16),
            pltpu.VMEM((256, rows), BF16),
            pltpu.VMEM((LANES, width), F32),
            pltpu.VMEM((keys, rows), F32),
            pltpu.VMEM((keys, rows), BF16),
        ],
        compiler_params=pltpu.CompilerParams(
            dimension_semantics=("arbitrary",), vmem_limit_bytes=32 << 20
        ),
        name="attend",
    )(queries, keys_t, values_t, layout, line, key_extra, query_bins)


def attend_back(
    queries, keys_t, values_t, heads_out, heads_grad, lse, layout, line,
    key_extra, key_extra_t, query_bins, query_bins_t,
):
    inner, rows = queries.shape
    keys = keys_t.shape[1]
    head_count, _, width = line.shape
    head_size = inner // head_count
    whole, column, page = attention_shapes(head_count, head_size, rows, keys, width)
    return pl.pallas_call(
        attend_back_kernel,
        grid=(head_count,),
        out_shape=(
            jax.ShapeDtypeStruct((inner, rows), BF16),
            jax.ShapeDtypeStruct((inner, keys), BF16),
            jax.ShapeDtypeStruct((inner, keys), BF16),
            jax.ShapeDtypeStruct((head_count, 1, width), F32),
            jax.ShapeDtypeStruct((head_count, 128, 128), F32),
        ),
        in_specs=[
            column(rows), column(keys), column(keys), column(rows), column(rows),
            page(1, rows), page(128, 128), page(1, width),
            whole((keys, 256)), whole((128, keys)), whole((128, rows)), whole((rows, 128)),
        ],
        out_specs=(column(rows), column(keys), column(keys), page(1, width), page(128, 128)),
        scratch_shapes=[
            pltpu.VMEM((keys, 256), BF16),
            pltpu.VMEM((192, keys), BF16),
            pltpu.VMEM((256, rows), BF16),
            pltpu.VMEM((keys, 128), BF16),
            pltpu.VMEM((128, rows), BF16),
            pltpu.VMEM((LANES, width), F32),
            pltpu.VMEM((LANES, width), F32),
            pltpu.VMEM((keys, rows), BF16),
        ],
        compiler_params=pltpu.CompilerParams(
            dimension_semantics=("arbitrary",), vmem_limit_bytes=32 << 20
        ),
        name="attend_back",
    )(
        queries, keys_t, values_t, heads_out, heads_grad, lse, layout, line,
        key_extra, key_extra_t, query_bins, query_bins_t,
    )


FORWARD_ITEMS = [(0, 0), (1, 0), (2, 0), (0, 1), (0, 2), (0, 3), (1, 1), (2, 1), (1, 2), (2, 2), (1, 3), (2, 3)]


FORWARD_SUMS = [(0, 1), (1, 1)]


def forward_kernel(
    mp_size, group,
    query_ref, output_ref, gate_up_ref, down_ref, key_value_ref, table_ref, boxes_ref, lengths_ref,
    input_ref, gain_ref, cotangent_ref,
    w_first, queries_out, keys_out, values_out, heads_out_out, lse, layout, line, key_extra, key_extra_t,
    slot_owner_out, residual_out, layer_output, second_grad, gate_up_full, down_full, tables,
    line_hot, bin_hot, gate_up_share, down_share, queries, keys_t, values_t, heads_out, slot_owner, residual,
    first_ref, query_piece, normed_t, slot_t, w_gate_up, w_down, first_here, key_aug, query_aug, strip, scores, probs,
    second_t, second_owner, out_owner, out_t,
    hidden_a, hidden_b, hidden_c, act_t, low_t, stage_gate_up, stage_down,
    row_send, row_recv, row_own, table_send, table_recv, table_own, load_sem, store_sem, keep_sem, *sems,
):
    place = Place(mp_size)
    rows, model_width = input_ref.shape
    keys = keys_t.shape[1]
    blocks = keys // LANES
    width = strip.shape[1]
    inner_here = first_ref.shape[1]
    heads_here = inner_here // 64
    hidden = gate_up_ref.shape[1]
    doc = lax.div(place.mp, group)
    member = lax.rem(place.mp, group)
    first_peer = place.mp - member
    own_lanes = pl.ds(pl.multiple_of(member * rows, LANES), rows)

    items = FORWARD_ITEMS
    column = lanes_at(place.core * 4 + place.y * 2 + place.x, 1)
    gather = Gather(
        place, [first_ref, gate_up_ref.at[:, :, column], down_ref.at[:, :, column]],
        [w_first, w_gate_up, w_down], sems[:5], items
    )
    at = {item: t for t, item in enumerate(items)}

    row_copies = [
        remote(
            normed_t, slot_t.at[:, own_lanes], row_send.at[k], row_recv.at[k],
            (place.dp, first_peer + lax.rem(member + k, group)),
        )
        for k in range(1, group)
    ]
    table_copies = [
        remote(table_ref, tables.at[place.mp], table_send.at[k], table_recv.at[k], place.to_mp(k))
        for k in range(1, mp_size)
    ]
    row_here = Copy(normed_t, slot_t.at[:, own_lanes], row_own.at[0])
    table_here = Copy(table_ref, tables.at[place.mp], table_own.at[0])

    greet(place)
    loads = [
        Copy(query_ref.at[column, :], query_piece, load_sem.at[0]),
        Copy(output_ref.at[:, column], first_ref.at[3], load_sem.at[1]),
    ]
    for copy in loads:
        copy.start()
    for c in range(1, 3):
        gather.own(c).start()
    table_here.start()
    turned = key_value_ref[...].T
    first_ref[1] = turned[0:inner_here]
    first_ref[2] = turned[inner_here : 2 * inner_here]

    def norm_into(values_ref, gain):
        def body(i, carry):
            here = pl.ds(pl.multiple_of(i * 16, 16), 16)
            values = values_ref[here, :]
            scale = lax.rsqrt(jnp.mean(values * values, axis=1, keepdims=True) + EPSILON)
            second_owner[here, :] = (values * scale * gain).astype(BF16)
            return carry

        lax.fori_loop(0, rows // 16, body, 0)

    norm_into(input_ref, gain_ref[0:1, :])
    normed_t[...] = second_owner[...].T
    row_here.start()
    for copy in loads:
        copy.wait()
    first_ref[0] = query_piece[...].T
    gather.own(0).start()
    meet(place)
    gather.run("f0 f1")
    for copy in row_copies + table_copies:
        copy.start()
    gather.along_mp(0, 1).start()

    key_rows = row_ids((64, keys))
    key_bins = boxes_ref[:, pl.ds(pl.multiple_of(doc * keys, LANES), keys)]
    x_place = jnp.where(key_rows == key_bins[0:1], 1.0, 0.0).astype(BF16)
    y_place = jnp.where(key_rows == key_bins[1:2], 1.0, 0.0).astype(BF16)
    key_extra_t[0:64, :] = x_place
    key_extra_t[64:128, :] = y_place
    mask = jnp.where(lane_ids((64, keys)) >= lengths_ref[doc], NEG_FILL, 0.0)
    first_row = member * rows
    spot = lane_ids((8, width))
    spot = jnp.where(spot >= width - LANES, spot - width, spot)
    bucket = bucket_of(LANES * (blocks - 1) - spot - first_row)[0:1]
    line_hot[...] = jnp.where(row_ids((LANES, width)) == bucket, 1.0, 0.0).astype(BF16)
    spot = lane_ids((8, LANES))
    bucket = bucket_of(jnp.where(spot < NBIN, -spot, LANES - spot))[0:1]
    bin_hot[...] = jnp.where(row_ids((LANES, LANES)) == bucket, 1.0, 0.0).astype(BF16)
    tail = jnp.where(key_rows == 0, mask, jnp.where(key_rows < 4, 1.0, 0.0)).astype(BF16)
    turned = jnp.concatenate([jnp.zeros((64, keys), BF16), x_place, y_place, tail], axis=0).T
    key_extra[...] = turned
    key_aug[...] = turned
    query_aug[pl.ds(192, 64), :] = jnp.where(row_ids((64, rows)) == 0, 1.0, 0.0).astype(BF16)
    gather.run("s0 f2")
    for block in range(model_width // LANES):
        owner = block_owner(block)
        out_owner[:, owner * LANES : (owner + 1) * LANES] = cotangent_ref[
            :, block * LANES : (block + 1) * LANES
        ].astype(BF16)
    out_t[...] = cotangent_ref[...].astype(BF16).T
    residual[...] = input_ref[...]
    layer_output[...] = jnp.zeros_like(layer_output)
    second_grad[...] = jnp.zeros_like(second_grad)
    row_here.wait()
    table_here.wait()
    gather.run("s1 t0")

    head_units = mp_size * heads_here
    table = {
        (1, 0): "f3 z4 z6", (2, 0): "s3 s2 t1", (4, 0): "t3 f4 z7", (5, 0): "s4 t2", (6, 0): "f5 z8",
        (7, 0): "t4 f6", (8, 0): "s5 z9", (9, 0): "f7 s6", (11, 0): "t5", (12, 0): "f8 s7", (13, 0): "t6",
        (14, 0): "f9 s8", (16, 0): "f10 t7", (16, 2): "s9", (17, 0): "f11 t8", (17, 1): "s10",
        (17, 3): "t9", (18, 0): "s11", (18, 3): "t10", (19, 0): "t11",
    }
    scatter = Scatter(
        place, [gate_up_full, down_full], [gate_up_share, down_share], sems[5:], FORWARD_SUMS,
        inside=True,
    )
    sum_table = {(18, 3): "c0 c1", (19, 0): "f0 f1", (19, 2): "s0", (19, 3): "s1"}

    def communicate(unit, point):
        for (at_unit, at_point), ops in table.items():
            if at_point == point:

                @pl.when(unit == at_unit)
                def _(ops=ops):
                    gather.run(ops)

        for (at_unit, at_point), ops in sum_table.items():
            if at_point == point:

                @pl.when(unit == at_unit)
                def _(ops=ops):
                    scatter.run(ops)

    def head_unit(unit, carry):
        communicate(unit, 0)
        step = lax.div(unit, heads_here)
        inside = lax.rem(unit, heads_here)
        source = place.across(step)
        base = pl.multiple_of(source * inner_here, 16)
        head = source * heads_here + inside

        @pl.when(inside == 0)
        def _():
            for k in range(mp_size):

                @pl.when(step == k)
                def _(k=k):
                    gather.done(at[(0, k)])
                    if k == 0:
                        for copy in row_copies:
                            copy.wait_recv()
                    else:
                        table_copies[k - 1].wait_recv()

            load = Copy(w_first.at[:, pl.ds(base, inner_here), :], first_here, load_sem.at[0])
            load.start()
            hot = tables[source].astype(BF16)
            line[source] = jnp.dot(hot[0:8], line_hot[...], preferred_element_type=F32)
            bins = jnp.dot(hot[8:24], bin_hot[...], preferred_element_type=F32)
            for i in range(heads_here):
                x_line = jnp.broadcast_to(bins[i : i + 1], (64, LANES))
                y_line = jnp.broadcast_to(bins[8 + i : 9 + i], (64, LANES))
                left = lane_ids((64, LANES)) < 64
                x_part = pltpu.roll(x_line, 0, 1, stride=1, stride_axis=0)
                y_part = pltpu.roll(y_line, 64, 1, stride=1, stride_axis=0)
                layout[source * heads_here + i] = jnp.concatenate(
                    [jnp.where(left, x_part, 0.0), jnp.where(left, 0.0, y_part)], axis=0
                ).astype(BF16)
            load.wait()
            here = pl.ds(base, inner_here)
            queries[here, :] = jnp.dot(
                first_here[0], normed_t[...], preferred_element_type=F32
            ).astype(BF16)
            keys_t[here, :] = jnp.dot(
                first_here[1], slot_t[...], preferred_element_type=F32
            ).astype(BF16)
            values_t[here, :] = jnp.dot(
                first_here[2], slot_t[...], preferred_element_type=F32
            ).astype(BF16)

        here = pl.ds(pl.multiple_of(head * 64, 16), 64)
        both = jnp.concatenate([keys_t[here, :], values_t[here, :]], axis=0).T
        low_lanes = lane_ids((keys, LANES)) < 64
        key_aug[:, 0:LANES] = jnp.where(low_lanes, both, key_extra[:, 0:LANES])
        query_aug[pl.ds(0, 64), :] = queries[here, :]
        query_aug[pl.ds(64, 128), :] = jnp.dot(
            layout[head], key_extra_t[:, own_lanes], preferred_element_type=F32
        ).astype(BF16)
        strip[...] = pltpu.roll(
            jnp.broadcast_to(line[source, pl.ds(inside, 1), :], (LANES, width)), 0, 1,
            stride=1, stride_axis=0,
        )
        query_all = query_aug[...]
        top = jnp.full((1, rows), -jnp.inf, F32)
        for block in range(blocks):
            some = pl.ds(block * LANES, LANES)
            part = jnp.dot(key_aug[some, :], query_all, preferred_element_type=F32)
            part = part + strip[:, pl.ds((blocks - 1 - block) * LANES, rows)]
            scores[some, :] = part
            top = jnp.maximum(top, jnp.max(part, axis=0, keepdims=True))
        sums = jnp.zeros((1, rows), F32)
        for block in range(blocks):
            some = pl.ds(block * LANES, LANES)
            part = jnp.exp(scores[some, :] - top)
            sums = sums + jnp.sum(part, axis=0, keepdims=True)
            probs[some, :] = part.astype(BF16)
        mixed = jnp.dot(values_t[here, :], probs[...], preferred_element_type=F32)
        heads_out[here, :] = (mixed / sums).astype(BF16)
        lse[head] = top + jnp.log(sums)

        @pl.when(inside == heads_here - 1)
        def _():
            part = heads_out[pl.ds(base, inner_here), :].T
            residual[...] = residual[...] + jnp.dot(
                part, first_here[3], preferred_element_type=F32
            )

        return carry

    lax.fori_loop(0, head_units, head_unit, 0)
    for block in range(model_width // LANES):
        owner = block_owner(block)
        slot_owner[:, owner * LANES : (owner + 1) * LANES] = slot_t[
            block * LANES : (block + 1) * LANES, :
        ].T

    kept = [
        Copy(here, there, keep_sem.at[i])
        for i, (here, there) in enumerate(
            [
                (queries, queries_out), (keys_t, keys_out), (values_t, values_out),
                (heads_out, heads_out_out), (slot_owner, slot_owner_out), (residual, residual_out),
            ]
        )
    ]
    for copy in kept:
        copy.start()
    norm_into(residual, gain_ref[1:2, :])
    second_t[...] = second_owner[...].T
    turned_blocks = [second_owner[:, b * LANES : (b + 1) * LANES] for b in range(model_width // LANES)]
    for block, values in enumerate(turned_blocks):
        owner = block_owner(block)
        second_owner[:, owner * LANES : (owner + 1) * LANES] = values

    def store(step):
        source = place.across(step)
        here = pl.ds(pl.multiple_of(source * hidden, 16), hidden)
        return [
            Copy(stage_gate_up, gate_up_full.at[:, here, :], store_sem.at[0]),
            Copy(stage_down, down_full.at[:, here, :], store_sem.at[1]),
        ]

    def hidden_unit(step, carry):
        unit = step + head_units
        communicate(unit, 0)
        source = place.across(step)
        here = pl.ds(pl.multiple_of(source * hidden, 16), hidden)
        for k in range(mp_size):

            @pl.when(step == k)
            def _(k=k):
                gather.done(at[(1, k)])
                gather.done(at[(2, k)])

        hidden_a[...] = jnp.dot(w_gate_up[0, here, :], second_t[...], preferred_element_type=F32)
        hidden_b[...] = jnp.dot(w_gate_up[1, here, :], second_t[...], preferred_element_type=F32)
        communicate(unit, 1)
        hidden_c[...] = jnp.dot(w_down[0, here, :], out_t[...], preferred_element_type=F32)

        def activate(i, inner_carry):
            some = pl.ds(pl.multiple_of(i * 16, 16), 16)
            gate, up, slope = hidden_a[some, :], hidden_b[some, :], hidden_c[some, :]
            square = gate * gate
            factor = 0.7978845608028654
            bent = jnp.tanh(factor * gate * (1.0 + 0.044715 * square))
            half = 0.5 * (1.0 + bent)
            value = gate * half
            change = half + 0.5 * gate * (1.0 - bent * bent) * (
                factor * (1.0 + 3.0 * 0.044715 * square)
            )
            act_t[some, :] = (value * up).astype(BF16)
            low_t[some, :] = (slope * up * change).astype(BF16)
            low_t[pl.ds(pl.multiple_of(hidden + i * 16, 16), 16), :] = (slope * value).astype(BF16)
            return inner_carry

        lax.fori_loop(0, hidden // 16, activate, 0)
        communicate(unit, 2)

        @pl.when(step > 0)
        def _():
            for copy in store(step):
                copy.wait()

        stage_down[0] = jnp.dot(act_t[...], out_owner[...], preferred_element_type=F32).astype(BF16)
        stage_gate_up[0] = jnp.dot(
            low_t[0:hidden], second_owner[...], preferred_element_type=F32
        ).astype(BF16)
        stage_gate_up[1] = jnp.dot(
            low_t[hidden:], second_owner[...], preferred_element_type=F32
        ).astype(BF16)
        for copy in store(step):
            copy.start()
        communicate(unit, 3)
        layer_output[...] = layer_output[...] + dot_f32(act_t[...].T, w_down[0, here, :], 1, 0)
        second_grad[...] = (
            second_grad[...]
            + dot_f32(low_t[0:hidden].T, w_gate_up[0, here, :], 1, 0)
            + dot_f32(low_t[hidden:].T, w_gate_up[1, here, :], 1, 0)
        )
        return carry

    lax.fori_loop(0, mp_size, hidden_unit, 0)
    layer_output[...] = layer_output[...] + residual[...]
    scatter.run("t0 t1 e0 e1")
    for copy in store(mp_size - 1):
        copy.wait()
    gather.close()
    scatter.close()
    for copy in row_copies + table_copies:
        copy.wait_send()
    for copy in kept:
        copy.wait()


def block_owner(block):
    return (block % 2) * 4 + block // 2


def forward(
    mp_size, group, query, output, gate_up, down, key_value, table, boxes, lengths, layer_input,
    gains, cotangent,
):
    rows, model_width = layer_input.shape
    keys = boxes.shape[1] // lengths.shape[0]
    width = LANES * (keys // LANES + rows // LANES)
    inner_here, hidden = query.shape[1], gate_up.shape[1]
    inner, total_hidden = inner_here * mp_size, hidden * mp_size
    head_count = inner // 64
    dma = pltpu.SemaphoreType.DMA
    hbm = pl.BlockSpec(memory_space=HBM)
    vmem = pl.BlockSpec(memory_space=pltpu.VMEM)
    shape = jax.ShapeDtypeStruct
    out = [
        (shape((4, inner, model_width), BF16), hbm),
        (shape((inner, rows), BF16), hbm),
        (shape((inner, keys), BF16), hbm),
        (shape((inner, keys), BF16), hbm),
        (shape((inner, rows), BF16), hbm),
        (shape((head_count, 1, rows), F32), vmem),
        (shape((head_count, 128, 128), BF16), vmem),
        (shape((mp_size, 8, width), F32), vmem),
        (shape((keys, 256), BF16), vmem),
        (shape((128, keys), BF16), vmem),
        (shape((keys, model_width), BF16), hbm),
        (shape((rows, model_width), F32), hbm),
        (shape((rows, model_width), F32), vmem),
        (shape((rows, model_width), F32), vmem),
        (shape((2, total_hidden, model_width), BF16), hbm),
        (shape((1, total_hidden, model_width), BF16), hbm),
        (shape((mp_size, 24, LANES), F32), vmem),
        (shape((LANES, width), BF16), vmem),
        (shape((LANES, LANES), BF16), vmem),
        (shape((2, hidden, LANES), BF16), vmem),
        (shape((1, hidden, LANES), BF16), vmem),
    ]
    return pl.pallas_call(
        partial(forward_kernel, mp_size, group),
        out_shape=tuple(o[0] for o in out),
        in_specs=[hbm] * 4 + [vmem] * 3 + [pl.BlockSpec(memory_space=pltpu.SMEM)] + [vmem] * 3,
        out_specs=tuple(o[1] for o in out),
        scratch_shapes=[
            pltpu.VMEM((inner, rows), BF16),
            pltpu.VMEM((inner, keys), BF16),
            pltpu.VMEM((inner, keys), BF16),
            pltpu.VMEM((inner, rows), BF16),
            pltpu.VMEM((keys, model_width), BF16),
            pltpu.VMEM((rows, model_width), F32),
            pltpu.VMEM((4, inner_here, LANES), BF16),
            pltpu.VMEM((LANES, inner_here), BF16),
            pltpu.VMEM((model_width, rows), BF16),
            pltpu.VMEM((model_width, keys), BF16),
            pltpu.VMEM((2, total_hidden, model_width), BF16),
            pltpu.VMEM((1, total_hidden, model_width), BF16),
            pltpu.VMEM((4, inner_here, model_width), BF16),
            pltpu.VMEM((keys, 256), BF16),
            pltpu.VMEM((256, rows), BF16),
            pltpu.VMEM((LANES, width), F32),
            pltpu.VMEM((keys, rows), F32),
            pltpu.VMEM((keys, rows), BF16),
            pltpu.VMEM((model_width, rows), BF16),
            pltpu.VMEM((rows, model_width), BF16),
            pltpu.VMEM((rows, model_width), BF16),
            pltpu.VMEM((model_width, rows), BF16),
            pltpu.VMEM((hidden, rows), F32),
            pltpu.VMEM((hidden, rows), F32),
            pltpu.VMEM((hidden, rows), F32),
            pltpu.VMEM((hidden, rows), BF16),
            pltpu.VMEM((2 * hidden, rows), BF16),
            pltpu.VMEM((2, hidden, model_width), BF16),
            pltpu.VMEM((1, hidden, model_width), BF16),
            dma((group,)), dma((group,)), dma((1,)),
            dma((mp_size,)), dma((mp_size,)), dma((1,)), dma((2,)), dma((2,)), dma((6,)),
        ]
        + Gather.semaphores(3, mp_size)
        + Scatter.scratch([(2, hidden), (1, hidden)], (True, True), FORWARD_SUMS),
        compiler_params=pltpu.CompilerParams(
            collective_id=0, has_side_effects=True, vmem_limit_bytes=62 << 20
        ),
        name="forward",
    )(
        query, output, gate_up, down, key_value, table, boxes, lengths, layer_input, gains, cotangent,
    )


BACKWARD_ITEMS = [(0, 3), (1, 3), (0, 2), (1, 2), (2, 3), (2, 2), (0, 0), (2, 1), (1, 0), (2, 0)]


def unskewed(values, first, count, shift):
    width = values.shape[1]
    folded = None
    for group in range(count // 8):
        part = values[pl.ds(first + group * 8, 8), :]
        back = (-(group * 8 + shift)) % width
        part = pltpu.roll(part, back, 1) if back else part
        folded = part if folded is None else folded + part
    total = folded[0:1]
    for row in range(1, 8):
        total = total + pltpu.roll(folded[row : row + 1], width - row, 1)
    return total


def exact_dot(left, right):
    parts = three_parts(left)
    return sum(dot_f32(part, right, 1, 1) for part in parts)


def backward_kernel(mp_size, group, *refs):
    (
        gate_up_full, down_full, w_first, queries, keys_t, values_t, heads_out,
        residual_in, second_in, cotangent_in,
        lse, layout, line, key_extra, key_extra_t, slot_owner, layer_input, gains, line_hot, bin_hot,
        gate_up_share, down_share, input_grad, small_out, gate_up_sum, down_sum, first_sum,
        *refs,
    ) = refs
    (
        slot_grad, own_grad, residual_grad, branch_owner, branch_t, w_query, w_output, w_kv,
        q_here, k_here, v_here, out_here, grad_here, dq_here, dk_here, dv_here, kv_here,
        key_aug, key_aug_t, query_aug, value_aug, grad_aug, strip, strip_grad, probs_grad,
        layout_grad, line_sums, bin_sums, gain_part, rows_out, peers, stage, stage_in, full_here,
        load_sem, value_sem, row_send, row_recv, stage_send, stage_recv,
        *refs,
    ) = refs
    place = Place(mp_size)
    rows, model_width = layer_input.shape
    keys = slot_owner.shape[0]
    blocks = keys // LANES
    inner_here = q_here.shape[0]
    heads_here = inner_here // 64
    member = lax.rem(place.mp, group)
    first_peer = place.mp - member
    own_start = pl.multiple_of(member * rows, LANES)
    own_lanes = pl.ds(own_start, rows)

    items = BACKWARD_ITEMS
    fulls = [gate_up_full, down_full, full_here]
    scatter = Scatter(
        place, fulls, [gate_up_sum, down_sum, first_sum], refs, items, [gate_up_share, down_share, None]
    )

    loads = [
        Copy(second_in, slot_grad.at[pl.ds(0, rows), :], value_sem.at[0]),
        Copy(residual_in, slot_grad.at[pl.ds(rows, rows), :], value_sem.at[1]),
        Copy(cotangent_in, input_grad, value_sem.at[2]),
    ]
    for copy in loads:
        copy.start()
    greet(place)
    meet(place)
    scatter.run("c0 c1")
    for c in range(2):
        scatter.share(c).start()
    key_aug[...] = key_extra[...]
    key_aug_t[pl.ds(64, 128), :] = key_extra_t[...]
    for copy in loads:
        copy.wait()

    def norm_back(i, total):
        here = pl.ds(pl.multiple_of(i * 16, 16), 16)
        grad = slot_grad[here, :]
        values = slot_grad[pl.ds(pl.multiple_of(rows + i * 16, 16), 16), :]
        scale = lax.rsqrt(jnp.mean(values * values, axis=1, keepdims=True) + EPSILON)
        scaled = gains[1:2, :] * grad
        mean = jnp.mean(scaled * values, axis=1, keepdims=True)
        result = input_grad[here, :] + scale * scaled - values * (scale * scale * scale * mean)
        residual_grad[here, :] = result
        branch_owner[here, :] = result.astype(BF16)
        product = grad * values * scale
        return total + product[0:8] + product[8:16]

    total = lax.fori_loop(0, rows // 16, norm_back, jnp.zeros((8, model_width), F32))
    gain_part[...] = jnp.sum(total, axis=0, keepdims=True)
    scatter.run("f0 c2")
    branch_t[...] = branch_owner[...].T
    parts = [branch_owner[:, b * LANES : (b + 1) * LANES] for b in range(model_width // LANES)]
    for block, values in enumerate(parts):
        owner = block_owner(block)
        branch_owner[:, owner * LANES : (owner + 1) * LANES] = values
    slot_grad[...] = jnp.zeros_like(slot_grad)
    own_grad[...] = jnp.zeros_like(own_grad)
    scatter.run("f1 c3")

    plan = {
        (0, 2): "s0 f2", (0, 3): "s1 f3", (0, 4): "t0 c4", (1, 1): "s2", (1, 2): "t1 f4", (1, 3): "s3 c6",
        (2, 0): "t2 c5", (2, 1): "s4 f5", (2, 2): "t3", (2, 3): "f6 c8", (2, 4): "t4 c7", (3, 1): "s5",
        (3, 2): "s6 f7", (3, 4): "t5 f8 c9",
    }

    def communicate(block, point):
        for (at_block, at_point), ops in plan.items():
            if at_point == point:

                @pl.when(block == at_block)
                def _(ops=ops):
                    scatter.run(ops)

    row_copies = [
        remote(
            rows_out.at[k - 1], peers.at[k - 1], row_send.at[k], row_recv.at[k],
            (place.dp, first_peer + lax.rem(member + k, group)),
        )
        for k in range(1, group)
    ]

    def block_unit(block, carry):
        communicate(block, 0)
        step = mp_size - 1 - block
        target = place.across(step)
        base = pl.multiple_of(target * inner_here, 16)
        here = pl.ds(base, inner_here)
        slot = lax.rem(block, 2)
        copies = [
            Copy(w_first.at[0, here, :], w_query, load_sem.at[0]),
            Copy(w_first.at[3, here, :], w_output, load_sem.at[1]),
            Copy(queries.at[here, :], q_here, load_sem.at[2]),
            Copy(keys_t.at[here, :], k_here, load_sem.at[3]),
            Copy(values_t.at[here, :], v_here, load_sem.at[4]),
            Copy(heads_out.at[here, :], out_here, load_sem.at[5]),
        ]
        for i in range(heads_here):
            for part in range(2):
                copies.append(
                    Copy(
                        w_first.at[1 + part, pl.ds(pl.multiple_of(base + i * 64, 16), 64), :],
                        w_kv.at[pl.ds(i * 128 + part * 64, 64), :],
                        load_sem.at[6 + 2 * i + part],
                    )
                )
        for copy in copies:
            copy.start()
        for copy in (copies[1], copies[5]):
            copy.wait()

        for b in range(2, mp_size):

            @pl.when(block == b)
            def _(b=b):
                scatter.left(items.index((2, mp_size + 1 - b)))

        grad_here[...] = jnp.dot(w_output[...], branch_t[...], preferred_element_type=F32).astype(BF16)
        full_here[slot, 3] = jnp.dot(
            out_here[...], branch_owner[...], preferred_element_type=F32
        ).astype(BF16)
        for copy in [copies[0]] + copies[2:5] + copies[6:]:
            copy.wait()

        def head_unit(inside, inner_carry):
            for point in range(1, heads_here):

                @pl.when(inside == point)
                def _(point=point):
                    communicate(block, point)

            head = target * heads_here + inside
            some = pl.ds(pl.multiple_of(inside * 64, 16), 64)
            q_head, k_head, v_head = q_here[some, :], k_here[some, :], v_here[some, :]
            grad_head = grad_here[some, :]
            both = jnp.concatenate([k_head, v_head], axis=0).T
            lanes = lane_ids((keys, LANES))
            key_aug[:, 0:LANES] = jnp.where(lanes < 64, both, key_extra[:, 0:LANES])
            ones = jnp.where(lanes < 3, 1.0, 0.0).astype(BF16)
            value_aug[...] = jnp.where(lanes < 64, ones, both)
            key_aug_t[pl.ds(0, 64), :] = k_head
            query_aug[pl.ds(0, 64), :] = q_head
            query_aug[pl.ds(64, 128), :] = jnp.dot(
                layout[head], key_extra_t[:, own_lanes], preferred_element_type=F32
            ).astype(BF16)
            high, middle, low = three_parts(-lse[head])
            tail = row_ids((64, rows))
            rows_of = lambda part: jnp.broadcast_to(part.astype(F32), (64, rows))
            query_aug[pl.ds(192, 64), :] = jnp.where(
                tail == 0, 1.0,
                jnp.where(
                    tail == 1, rows_of(high),
                    jnp.where(tail == 2, rows_of(middle), jnp.where(tail == 3, rows_of(low), 0.0)),
                ),
            ).astype(BF16)
            row_dot = jnp.sum(
                grad_head.astype(F32) * out_here[some, :].astype(F32), axis=0, keepdims=True
            )
            high, middle, low = three_parts(-row_dot)
            grad_aug[pl.ds(0, 64), :] = jnp.where(
                tail == 0, rows_of(high),
                jnp.where(tail == 1, rows_of(middle), jnp.where(tail == 2, rows_of(low), 0.0)),
            ).astype(BF16)
            grad_aug[pl.ds(64, 64), :] = grad_head
            width = strip.shape[1]
            strip[...] = pltpu.roll(
                jnp.broadcast_to(line[target, pl.ds(inside, 1), :], (LANES, width)), 0, 1,
                stride=1, stride_axis=0,
            )
            strip_grad[...] = jnp.zeros_like(strip_grad)
            query_and_grad = jnp.concatenate([q_head, grad_head], axis=0).T
            query_all = query_aug[...]
            grad_all = grad_aug[...]
            half = lane_ids((LANES, LANES)) < 64
            kv_lanes = pl.ds(pl.multiple_of(inside * LANES, LANES), LANES)
            for part_index in range(blocks):
                these = pl.ds(part_index * LANES, LANES)
                band = pl.ds((blocks - 1 - part_index) * LANES, rows)
                part = jnp.dot(key_aug[these, :], query_all, preferred_element_type=F32)
                part = jnp.exp(part + strip[:, band])
                slope = part * jnp.dot(value_aug[these, :], grad_all, preferred_element_type=F32)
                strip_grad[:, band] = strip_grad[:, band] + slope
                slope = slope.astype(BF16)
                probs_grad[these, :] = slope
                key_part = jnp.dot(slope, query_and_grad, preferred_element_type=F32)
                value_part = jnp.dot(part.astype(BF16), query_and_grad, preferred_element_type=F32)
                joined = jnp.where(half, key_part, value_part)
                kv_here[these, kv_lanes] = joined.astype(BF16)
                turned = joined.T.astype(BF16)
                dk_here[some, these] = turned[0:64]
                dv_here[some, these] = turned[64:128]
            query_part = jnp.dot(key_aug_t[...], probs_grad[...], preferred_element_type=F32)
            dq_here[some, :] = query_part[0:64].astype(BF16)
            bins = dot_f32(query_part[64:192].astype(BF16), key_extra_t[:, own_lanes], 1, 1)
            left = lane_ids((LANES, LANES)) < 64
            upper = row_ids((LANES, LANES)) < 64
            layout_grad[...] = jnp.where(left == upper, bins, 0.0)
            bin_sums[0, pl.ds(head, 1), :] = unskewed(layout_grad, 0, 64, 0)
            bin_sums[1, pl.ds(head, 1), :] = unskewed(layout_grad, 64, 64, 64)
            line_sums[pl.ds(head, 1), :] = unskewed(strip_grad, 0, LANES, 0)
            return inner_carry

        lax.fori_loop(0, heads_here, head_unit, 0)
        slot_grad[...] = slot_grad[...] + jnp.dot(
            kv_here[...], w_kv[...], preferred_element_type=F32
        )
        own_grad[...] = own_grad[...] + jnp.dot(
            dq_here[...].T, w_query[...], preferred_element_type=F32
        )

        @pl.when(block == mp_size - 1)
        def _():
            for k, copy in enumerate(row_copies):
                other = lax.rem(member + k + 1, group)
                rows_out[k] = slot_grad[pl.ds(pl.multiple_of(other * rows, 16), rows), :].astype(BF16)
                copy.start()

        full_here[slot, 0] = jnp.dot(
            dq_here[...], slot_owner[pl.ds(own_start, rows), :], preferred_element_type=F32
        ).astype(BF16)
        full_here[slot, 1] = jnp.dot(
            dk_here[...], slot_owner[...], preferred_element_type=F32
        ).astype(BF16)
        full_here[slot, 2] = jnp.dot(
            dv_here[...], slot_owner[...], preferred_element_type=F32
        ).astype(BF16)
        communicate(block, heads_here)
        return carry

    lax.fori_loop(0, mp_size, block_unit, 0)

    scatter.run("t6 f9")

    gain_rows = model_width // LANES
    head_count = bin_sums.shape[1]
    stage[0, 2 * gain_rows : 2 * gain_rows + head_count, :] = exact_dot(line_sums[...], line_hot[...])
    for i in range(2):
        start = 2 * gain_rows + (1 + i) * head_count
        stage[0, start : start + head_count, :] = exact_dot(bin_sums[i], bin_hot[...])
    for block in range(gain_rows):
        these = slice(block * LANES, (block + 1) * LANES)
        owner = block_owner(block)
        those = slice(owner * LANES, (owner + 1) * LANES)

        def gain_sum(i, total, these=these, those=those):
            here = pl.ds(pl.multiple_of(i * 64, 64), 64)
            product = slot_grad[here, these] * slot_owner[here, those].astype(F32)
            return total + jnp.sum(product.reshape(8, 8, LANES), axis=0)

        def own_sum(i, total, these=these, those=those):
            here = pl.ds(pl.multiple_of(i * 64, 64), 64)
            there = pl.ds(pl.multiple_of(own_start + i * 64, 64), 64)
            product = own_grad[here, these] * slot_owner[there, those].astype(F32)
            return total + jnp.sum(product.reshape(8, 8, LANES), axis=0)

        total = lax.fori_loop(0, keys // 64, gain_sum, jnp.zeros((8, LANES), F32))
        total = lax.fori_loop(0, rows // 64, own_sum, total)
        stage[0, block : block + 1, :] = (
            jnp.sum(total, axis=0, keepdims=True) / gains[0:1, these]
        )
        stage[0, gain_rows + block : gain_rows + block + 1, :] = gain_part[:, these]

    rounds = [[place.to_core], [place.to_x, place.to_y, place.to_corner]]
    rounds.append([place.to_mp(k) for k in range(1, mp_size)])
    at, sums = 0, []
    for i, partners in enumerate(rounds):
        sums.append(
            [
                remote(
                    stage.at[i], stage_in.at[at + j], stage_send.at[at + j], stage_recv.at[at + j], partner
                )
                for j, partner in enumerate(partners)
            ]
        )
        at += len(partners)
    def round_done(i):
        at = sum(len(partners) for partners in rounds[:i])
        value = stage[i]
        for j, copy in enumerate(sums[i]):
            copy.wait_recv()
            value = value + stage_in[at + j]
        return value

    for copy in sums[0]:
        copy.start()
    scatter.run("s7 s8")
    stage[1] = round_done(0)
    for copy in sums[1]:
        copy.start()
    scatter.run("t7 s9")
    for copy in row_copies:
        copy.wait_recv()

    def input_back(i, carry):
        here = pl.ds(pl.multiple_of(i * 16, 16), 16)
        grad = own_grad[here, :] + slot_grad[pl.ds(pl.multiple_of(own_start + i * 16, 16), 16), :]
        for k in range(group - 1):
            grad = grad + peers[k, here, :].astype(F32)
        values = layer_input[here, :]
        scale = lax.rsqrt(jnp.mean(values * values, axis=1, keepdims=True) + EPSILON)
        scaled = gains[0:1, :] * grad
        mean = jnp.mean(scaled * values, axis=1, keepdims=True)
        input_grad[here, :] = (
            residual_grad[here, :] + scale * scaled - values * (scale * scale * scale * mean)
        )
        return carry

    lax.fori_loop(0, rows // 16, input_back, 0)
    stage[2] = round_done(1)
    for copy in sums[2]:
        copy.start()
    scatter.run("t8 t9 e0 e1 e2")
    small_out[...] = round_done(2)
    sums = sum(sums, [])
    scatter.close()
    for copy in row_copies + sums:
        copy.wait_send()


def backward(
    mp_size, group, gate_up_full, down_full, w_first, queries, keys_t, values_t, heads_out,
    residual, second_grad, cotangent, lse, layout, line, key_extra, key_extra_t, slot_owner,
    layer_input, gains, line_hot, bin_hot, gate_up_share, down_share,
):
    rows, model_width = layer_input.shape
    keys = slot_owner.shape[0]
    width = line.shape[2]
    inner_here = queries.shape[0] // mp_size
    heads_here = inner_here // 64
    head_count = heads_here * mp_size
    hidden = down_full.shape[1] // mp_size
    sizes = [(2, hidden), (1, hidden), (4, inner_here)]
    count = 4 + mp_size - 1
    small_rows = 2 * model_width // LANES + 3 * head_count
    others = max(group - 1, 1)
    dma = pltpu.SemaphoreType.DMA
    hbm = pl.BlockSpec(memory_space=HBM)
    vmem = pl.BlockSpec(memory_space=pltpu.VMEM)
    shape = jax.ShapeDtypeStruct
    return pl.pallas_call(
        partial(backward_kernel, mp_size, group),
        out_shape=(
            shape((rows, model_width), F32),
            shape((small_rows, LANES), F32),
            *[shape((lead, n, LANES), F32) for lead, n in sizes],
        ),
        in_specs=[hbm] * 10 + [vmem] * 12,
        out_specs=(vmem,) * 5,
        scratch_shapes=[
            pltpu.VMEM((keys, model_width), F32),
            pltpu.VMEM((rows, model_width), F32),
            pltpu.VMEM((rows, model_width), F32),
            pltpu.VMEM((rows, model_width), BF16),
            pltpu.VMEM((model_width, rows), BF16),
            pltpu.VMEM((inner_here, model_width), BF16),
            pltpu.VMEM((inner_here, model_width), BF16),
            pltpu.VMEM((2 * inner_here, model_width), BF16),
            pltpu.VMEM((inner_here, rows), BF16),
            pltpu.VMEM((inner_here, keys), BF16),
            pltpu.VMEM((inner_here, keys), BF16),
            pltpu.VMEM((inner_here, rows), BF16),
            pltpu.VMEM((inner_here, rows), BF16),
            pltpu.VMEM((inner_here, rows), BF16),
            pltpu.VMEM((inner_here, keys), BF16),
            pltpu.VMEM((inner_here, keys), BF16),
            pltpu.VMEM((keys, heads_here * LANES), BF16),
            pltpu.VMEM((keys, 256), BF16),
            pltpu.VMEM((192, keys), BF16),
            pltpu.VMEM((256, rows), BF16),
            pltpu.VMEM((keys, LANES), BF16),
            pltpu.VMEM((LANES, rows), BF16),
            pltpu.VMEM((LANES, width), F32),
            pltpu.VMEM((LANES, width), F32),
            pltpu.VMEM((keys, rows), BF16),
            pltpu.VMEM((LANES, LANES), F32),
            pltpu.VMEM((head_count, width), F32),
            pltpu.VMEM((2, head_count, LANES), F32),
            pltpu.VMEM((1, model_width), F32),
            pltpu.VMEM((others, rows, model_width), BF16),
            pltpu.VMEM((others, rows, model_width), BF16),
            pltpu.VMEM((3, small_rows, LANES), F32),
            pltpu.VMEM((count, small_rows, LANES), F32),
            pltpu.VMEM((2, 4, inner_here, model_width), BF16),
            dma((6 + 2 * heads_here,)), dma((3,)), dma((group,)), dma((group,)),
            dma((count,)), dma((count,)),
        ]
        + Scatter.scratch(sizes, (True, True, False), BACKWARD_ITEMS),
        compiler_params=pltpu.CompilerParams(
            collective_id=1, has_side_effects=True, vmem_limit_bytes=63 << 20
        ),
        name="backward",
    )(
        gate_up_full, down_full, w_first, queries, keys_t, values_t, heads_out, residual,
        second_grad, cotangent, lse, layout, line, key_extra, key_extra_t, slot_owner, layer_input,
        gains, line_hot, bin_hot, gate_up_share, down_share,
    )


def line_onehot(first_row, width, key_blocks):
    place = jnp.arange(width, dtype=jnp.int32)
    place = jnp.where(place >= width - LANES, place - width, place)
    offset = LANES * (key_blocks - 1) - place - first_row
    return (bucket_of(offset)[:, None] == jnp.arange(32, dtype=jnp.int32)[None, :]).astype(F32)


def bin_onehot():
    bins = np.arange(NBIN)
    offset = bins[:, None] - bins[None, :]
    distance = np.abs(offset)
    bucket = np.minimum(distance, 7) + sum((distance >= t).astype(np.int64) for t in THRESHOLDS)
    bucket = bucket + 16 * (offset > 0)
    return jnp.asarray(bucket[:, :, None] == np.arange(32), F32)


def gather_rows(local, axis_name):
    return lax.all_gather(local, axis_name, axis=0, tiled=True)


def scatter_grad(full):
    summed = lax.psum_scatter(full, "dp", scatter_dimension=1, tiled=True)
    return lax.psum_scatter(summed, "mp", scatter_dimension=0, tiled=True)


def per_device_plain(
    dp_size, mp_size,
    layer_input, norm_gains, query_weight, key_value_weight, output_weight,
    gate_up_weight, down_weight, bias_tables, doc_lengths, box_bins, cotangent,
):
    rows, model_width = layer_input.shape
    doc_count = doc_lengths.shape[0]
    slot_span = box_bins.shape[1] // doc_count
    group = mp_size // doc_count
    mp_index = lax.axis_index("mp")
    doc = mp_index // group
    first_row = (mp_index % group) * rows
    key_blocks = slot_span // LANES
    width = LANES * (key_blocks + (rows + LANES - 1) // LANES)
    groups = [[d * group + i for i in range(group)] for d in range(doc_count)]
    gain_first = norm_gains[0].astype(F32)
    gain_second = norm_gains[1].astype(F32)

    w_query = gather_rows(query_weight.T, "mp")
    inner_here = query_weight.shape[1]
    inner = inner_here * mp_size
    w_key = gather_rows(key_value_weight[:, 0].T, "mp")
    w_value = gather_rows(key_value_weight[:, 1].T, "mp")
    w_output = gather_rows(output_weight, "mp")
    w_gate = gather_rows(gate_up_weight[:, 0].T, "mp")
    w_up = gather_rows(gate_up_weight[:, 1].T, "mp")
    w_down = gather_rows(down_weight, "mp")
    tables = lax.all_gather(bias_tables, "mp", axis=2, tiled=True).astype(F32)
    head_count = tables.shape[2]

    onehot_line = line_onehot(first_row, width, key_blocks)
    line = jnp.dot(onehot_line, tables[0], precision=lax.Precision.HIGHEST)
    line = line.T.reshape(head_count, 1, width)
    onehot_bin = bin_onehot()
    x_part = jnp.einsum("ban,nh->hba", onehot_bin, tables[1], precision=lax.Precision.HIGHEST)
    y_part = jnp.einsum("ban,nh->hba", onehot_bin, tables[2], precision=lax.Precision.HIGHEST)
    empty = jnp.zeros_like(x_part)
    layout = jnp.concatenate(
        [jnp.concatenate([x_part, empty], axis=2), jnp.concatenate([empty, y_part], axis=2)], axis=1
    ).astype(BF16)
    key_bins = lax.dynamic_slice(box_bins, (0, doc * slot_span), (2, slot_span))
    own_bins = lax.dynamic_slice(key_bins, (0, first_row), (2, rows))
    bin_ids = jnp.arange(NBIN, dtype=jnp.int32)

    def placed_rows(bins):
        return jnp.concatenate(
            [bins[0][:, None] == bin_ids, bins[1][:, None] == bin_ids], axis=1
        ).astype(BF16)

    def placed_lanes(bins):
        return jnp.concatenate(
            [bin_ids[:, None] == bins[0][None], bin_ids[:, None] == bins[1][None]], axis=0
        ).astype(BF16)

    length = lax.dynamic_index_in_dim(doc_lengths, doc, keepdims=False)
    masked = jnp.arange(slot_span, dtype=jnp.int32)[:, None] >= length
    key_placed = placed_rows(key_bins)
    key_extra = jnp.concatenate(
        [
            jnp.zeros((slot_span, 64), BF16),
            key_placed,
            jnp.where(masked, NEG_FILL, 0.0).astype(BF16),
            jnp.ones((slot_span, 3), BF16),
            jnp.zeros((slot_span, 60), BF16),
        ],
        axis=1,
    )
    key_extra_t = placed_lanes(key_bins)
    query_bins_t = placed_rows(own_bins)
    query_bins = placed_lanes(own_bins)

    scale_first = inverse_rms(layer_input)
    normed = (layer_input * scale_first * gain_first).astype(BF16)
    slot_normed = lax.all_gather(normed, "mp", axis=0, tiled=True, axis_index_groups=groups)
    queries = dot_f32(w_query, normed, 1, 1).astype(BF16)
    keys_t = dot_f32(w_key, slot_normed, 1, 1).astype(BF16)
    values_t = dot_f32(w_value, slot_normed, 1, 1).astype(BF16)
    heads_out, lse = attend(queries, keys_t, values_t, layout, line, key_extra, query_bins)
    residual = layer_input + dot_f32(heads_out, w_output, 0, 0)
    scale_second = inverse_rms(residual)
    normed_second = (residual * scale_second * gain_second).astype(BF16)
    gate = dot_f32(normed_second, w_gate, 1, 1)
    up = dot_f32(normed_second, w_up, 1, 1)
    gelu_value, gelu_pull = jax.vjp(lambda v: jax.nn.gelu(v, approximate=True), gate)
    activated = (gelu_value * up).astype(BF16)
    layer_output = residual + dot_f32(activated, w_down, 1, 0)

    out_low = cotangent.astype(BF16)
    down_full = dot_f32(activated, out_low, 0, 0).astype(BF16)
    act_grad = dot_f32(out_low, w_down, 1, 1)
    gate_low = gelu_pull(act_grad * up)[0].astype(BF16)
    up_low = (act_grad * gelu_value).astype(BF16)
    gate_full = dot_f32(gate_low, normed_second, 0, 0).astype(BF16)
    up_full = dot_f32(up_low, normed_second, 0, 0).astype(BF16)
    second_grad = dot_f32(gate_low, w_gate, 1, 0) + dot_f32(up_low, w_up, 1, 0)
    gain_second_grad = jnp.sum(second_grad * residual * scale_second, axis=0)
    scaled = gain_second * second_grad
    residual_grad = (
        cotangent
        + scale_second * scaled
        - residual * scale_second**3 * jnp.mean(scaled * residual, axis=-1, keepdims=True)
    )

    branch_low = residual_grad.astype(BF16)
    output_full = dot_f32(heads_out, branch_low, 1, 0).astype(BF16)
    heads_grad = dot_f32(w_output, branch_low, 1, 1).astype(BF16)
    dq, dk, dv, line_grad, layout_grad = attend_back(
        queries, keys_t, values_t, heads_out, heads_grad, lse, layout, line,
        key_extra, key_extra_t, query_bins, query_bins_t,
    )
    query_full = dot_f32(dq, normed, 1, 0).astype(BF16)
    key_full = dot_f32(dk, slot_normed, 1, 0).astype(BF16)
    value_full = dot_f32(dv, slot_normed, 1, 0).astype(BF16)
    slot_grad = dot_f32(dk, w_key, 0, 0) + dot_f32(dv, w_value, 0, 0)
    first_grad = lax.psum_scatter(
        slot_grad.astype(BF16), "mp", scatter_dimension=0, tiled=True, axis_index_groups=groups
    ).astype(F32) + dot_f32(dq, w_query, 0, 0)
    gain_first_grad = jnp.sum(first_grad * layer_input * scale_first, axis=0)
    scaled = gain_first * first_grad
    input_grad = (
        residual_grad
        + scale_first * scaled
        - layer_input * scale_first**3 * jnp.mean(scaled * layer_input, axis=-1, keepdims=True)
    )

    gain_grad = lax.psum_scatter(
        jnp.stack([gain_first_grad, gain_second_grad]), ("dp", "mp"), scatter_dimension=1, tiled=True
    )
    line_part = jnp.dot(
        onehot_line.T, line_grad[:, 0].T, precision=lax.Precision.HIGHEST
    )
    x_part = jnp.einsum(
        "ban,hba->nh", onehot_bin, layout_grad[:, :64, :64], precision=lax.Precision.HIGHEST
    )
    y_part = jnp.einsum(
        "ban,hba->nh", onehot_bin, layout_grad[:, 64:, 64:], precision=lax.Precision.HIGHEST
    )
    table_full = jnp.stack([line_part, x_part, y_part])
    table_grad = lax.psum_scatter(
        lax.psum_scatter(table_full, "mp", scatter_dimension=2, tiled=True),
        "dp", scatter_dimension=1, tiled=True,
    )

    query_grad = scatter_grad(query_full).T.astype(F32)
    key_value_grad = jnp.stack(
        [scatter_grad(key_full).T, scatter_grad(value_full).T], axis=1
    ).astype(F32)
    output_grad = scatter_grad(output_full).astype(F32)
    gate_up_grad = jnp.stack(
        [scatter_grad(gate_full).T, scatter_grad(up_full).T], axis=1
    ).astype(F32)
    down_grad = scatter_grad(down_full).astype(F32)
    return (
        layer_output, input_grad, gain_grad, query_grad, key_value_grad,
        output_grad, gate_up_grad, down_grad, table_grad,
    )


def per_device_linked(
    dp_size, mp_size,
    layer_input, norm_gains, query_weight, key_value_weight, output_weight,
    gate_up_weight, down_weight, bias_tables, doc_lengths, box_bins, cotangent,
):
    rows, model_width = layer_input.shape
    doc_count = doc_lengths.shape[0]
    group = mp_size // doc_count
    dp_index, mp_index = lax.axis_index("dp"), lax.axis_index("mp")
    heads_here = bias_tables.shape[2]
    head_count = heads_here * mp_size
    inner_here = query_weight.shape[1]
    gains = norm_gains.astype(F32)
    column = ((dp_index % 2) * 4 + dp_index // 2) * LANES
    key_value = lax.dynamic_slice_in_dim(key_value_weight, column, LANES, 0)
    table = jnp.swapaxes(bias_tables.astype(F32), 1, 2)
    table = jnp.pad(table, ((0, 0), (0, 8 - heads_here), (0, LANES - 32))).reshape(24, LANES)
    (
        w_first, queries, keys_t, values_t, heads_out, lse, layout, line, key_extra, key_extra_t,
        slot_owner, residual, layer_output, second_grad, gate_up_full, down_full, _, line_hot, bin_hot,
        gate_up_share, down_share,
    ) = forward(
        mp_size, group, query_weight, output_weight, jnp.transpose(gate_up_weight, (1, 2, 0)),
        down_weight[None], key_value.reshape(LANES, 2 * inner_here), table, box_bins, doc_lengths,
        layer_input, gains, cotangent,
    )
    input_grad, small, gate_up_sum, down_sum, summed = backward(
        mp_size, group, gate_up_full, down_full, w_first, queries, keys_t, values_t, heads_out,
        residual, second_grad, cotangent, lse, layout, line, key_extra, key_extra_t, slot_owner,
        layer_input, gains, line_hot, bin_hot, gate_up_share, down_share,
    )
    gain_rows = model_width // LANES
    gains = small[: 2 * gain_rows].reshape(2, model_width)
    share = model_width // (dp_size * mp_size)
    at = (dp_index * mp_size + mp_index) * share
    gain_grad = lax.dynamic_slice(gains, (0, at), (2, share))
    tables = small[2 * gain_rows :].reshape(3, head_count, LANES)
    table_grad = lax.dynamic_slice(
        tables,
        (0, mp_index * heads_here, dp_index * (32 // dp_size)),
        (3, heads_here, 32 // dp_size),
    )
    table_grad = jnp.swapaxes(table_grad, 1, 2)
    query_grad = summed[0].T
    key_value_grad = jnp.transpose(summed[1:3], (2, 0, 1))
    gate_up_grad = jnp.transpose(gate_up_sum, (2, 0, 1))
    return (
        layer_output, input_grad, gain_grad, query_grad, key_value_grad,
        summed[3], gate_up_grad, down_sum[0], table_grad,
    )


def per_device(dp_size, mp_size, *args):
    rows, model_width = args[0].shape
    heads_here = args[7].shape[2]
    fits = dp_size == 8 and model_width == 8 * LANES and mp_size == 4
    fits = fits and heads_here == 4 and rows % LANES == 0
    body = per_device_linked if fits else per_device_plain
    return body(dp_size, mp_size, *args)


def solution(mesh):
    return jax.shard_map(
        partial(per_device, mesh.shape["dp"], mesh.shape["mp"]),
        mesh=mesh,
        in_specs=(
            P(("dp", "mp"), None),
            P(),
            P(None, "mp"),
            P(None, None, "mp"),
            P("mp", None),
            P(None, None, "mp"),
            P("mp", None),
            P(None, None, "mp"),
            P("dp"),
            P(None, "dp"),
            P(("dp", "mp"), None),
        ),
        out_specs=(
            P(("dp", "mp"), None),
            P(("dp", "mp"), None),
            P(None, ("dp", "mp")),
            P("dp", "mp"),
            P("dp", None, "mp"),
            P("mp", "dp"),
            P("dp", None, "mp"),
            P("mp", "dp"),
            P(None, "dp", "mp"),
        ),
        check_vma=False,
    )
```

```python
from functools import partial

import jax
import jax.numpy as jnp
import numpy as np
from jax import lax
from jax.experimental import pallas as pl
from jax.experimental.pallas import tpu as pltpu
from jax.sharding import PartitionSpec as P

NBIN = 64
EPSILON = 1e-06
THRESHOLDS = (8, 12, 16, 23, 32, 46, 64, 91)
NEG_FILL = -1e30
LANES = 128
MESH = pl.DeviceIdType.MESH
HBM = pltpu.MemorySpace.HBM
BF16 = jnp.bfloat16
F32 = jnp.float32


def bucket_of(relative):
    distance = jnp.abs(relative)
    bucket = jnp.minimum(distance, 7)
    for threshold in THRESHOLDS:
        bucket = bucket + (distance >= threshold).astype(jnp.int32)
    return bucket + 16 * (relative > 0).astype(jnp.int32)


def inverse_rms(values):
    return lax.rsqrt(jnp.mean(values * values, axis=-1, keepdims=True) + EPSILON)


def dot_f32(left, right, left_dim, right_dim):
    return lax.dot_general(
        left, right, (((left_dim,), (right_dim,)), ((), ())), preferred_element_type=F32
    )


def three_parts(values):
    high = values.astype(BF16)
    rest = values - high.astype(F32)
    middle = rest.astype(BF16)
    low = (rest - middle.astype(F32)).astype(BF16)
    return high, middle, low


def lane_ids(shape):
    return lax.broadcasted_iota(jnp.int32, shape, 1)


def row_ids(shape):
    return lax.broadcasted_iota(jnp.int32, shape, 0)


def attend_kernel(
    q_ref, k_ref, v_ref, layout_ref, line_ref, key_extra_ref, query_bins_ref,
    out_ref, lse_ref,
    key_aug, query_aug, strip, scores, probs,
):
    head_size, rows = q_ref.shape
    keys = k_ref.shape[1]
    blocks = keys // LANES
    width = strip.shape[1]

    @pl.when(pl.program_id(0) == 0)
    def _():
        key_aug[...] = key_extra_ref[...]
        tail = row_ids((64, rows))
        query_aug[pl.ds(192, 64), :] = jnp.where(tail == 0, 1.0, 0.0).astype(BF16)

    both = jnp.concatenate([k_ref[...], v_ref[...]], axis=0).T
    low_lanes = lane_ids((keys, LANES)) < head_size
    key_aug[:, 0:LANES] = jnp.where(low_lanes, both, key_extra_ref[:, 0:LANES])
    query_aug[pl.ds(0, 64), :] = q_ref[...]
    query_aug[pl.ds(64, 128), :] = jnp.dot(
        layout_ref[0], query_bins_ref[...], preferred_element_type=F32
    ).astype(BF16)
    strip[...] = pltpu.roll(
        jnp.broadcast_to(line_ref[0], (LANES, width)), 0, 1, stride=1, stride_axis=0
    )
    query_all = query_aug[...]
    top = jnp.full((1, rows), -jnp.inf, F32)
    for block in range(blocks):
        here = pl.ds(block * LANES, LANES)
        part = jnp.dot(key_aug[here, :], query_all, preferred_element_type=F32)
        part = part + strip[:, pl.ds((blocks - 1 - block) * LANES, rows)]
        scores[here, :] = part
        top = jnp.maximum(top, jnp.max(part, axis=0, keepdims=True))
    total = jnp.zeros((1, rows), F32)
    for block in range(blocks):
        here = pl.ds(block * LANES, LANES)
        part = jnp.exp(scores[here, :] - top)
        total = total + jnp.sum(part, axis=0, keepdims=True)
        probs[here, :] = part.astype(BF16)
    mixed = jnp.dot(v_ref[...], probs[...], preferred_element_type=F32)
    out_ref[...] = (mixed / total).astype(BF16)
    lse_ref[0] = top + jnp.log(total)


def attend_back_kernel(
    q_ref, k_ref, v_ref, out_ref, out_grad_ref, lse_ref, layout_ref, line_ref,
    key_extra_ref, key_extra_t_ref, query_bins_ref, query_bins_t_ref,
    dq_ref, dk_ref, dv_ref, line_grad_ref, layout_grad_ref,
    key_aug, key_aug_t, query_aug, value_aug, grad_aug, strip, strip_grad, probs_grad,
):
    head_size, rows = q_ref.shape
    keys = k_ref.shape[1]
    blocks = keys // LANES
    width = strip.shape[1]

    @pl.when(pl.program_id(0) == 0)
    def _():
        key_aug[...] = key_extra_ref[...]
        key_aug_t[pl.ds(64, 128), :] = key_extra_t_ref[...]
        tail = row_ids((64, rows))
        query_aug[pl.ds(192, 64), :] = jnp.where(tail == 0, 1.0, 0.0).astype(BF16)

    both = jnp.concatenate([k_ref[...], v_ref[...]], axis=0).T
    lanes = lane_ids((keys, LANES))
    key_aug[:, 0:LANES] = jnp.where(lanes < head_size, both, key_extra_ref[:, 0:LANES])
    ones = jnp.where(lanes < 3, 1.0, 0.0).astype(BF16)
    value_aug[...] = jnp.where(lanes < head_size, ones, both)
    key_aug_t[pl.ds(0, 64), :] = k_ref[...]
    query_aug[pl.ds(0, 64), :] = q_ref[...]
    query_aug[pl.ds(64, 128), :] = jnp.dot(
        layout_ref[0], query_bins_ref[...], preferred_element_type=F32
    ).astype(BF16)
    high, middle, low = three_parts(-lse_ref[0])
    tail = row_ids((64, rows))
    rows_of = lambda part: jnp.broadcast_to(part.astype(F32), (64, rows))
    query_aug[pl.ds(192, 64), :] = jnp.where(
        tail == 0, 1.0,
        jnp.where(
            tail == 1, rows_of(high),
            jnp.where(tail == 2, rows_of(middle), jnp.where(tail == 3, rows_of(low), 0.0)),
        ),
    ).astype(BF16)
    row_dot = jnp.sum(
        out_grad_ref[...].astype(F32) * out_ref[...].astype(F32), axis=0, keepdims=True
    )
    high, middle, low = three_parts(-row_dot)
    grad_aug[pl.ds(0, 64), :] = jnp.where(
        tail == 0, rows_of(high),
        jnp.where(tail == 1, rows_of(middle), jnp.where(tail == 2, rows_of(low), 0.0)),
    ).astype(BF16)
    grad_aug[pl.ds(64, 64), :] = out_grad_ref[...]
    strip[...] = pltpu.roll(
        jnp.broadcast_to(line_ref[0], (LANES, width)), 0, 1, stride=1, stride_axis=0
    )
    strip_grad[...] = jnp.zeros_like(strip_grad)
    query_and_grad = jnp.concatenate([q_ref[...], out_grad_ref[...]], axis=0).T
    query_all = query_aug[...]
    grad_all = grad_aug[...]
    half = lane_ids((LANES, LANES)) < head_size
    for block in range(blocks):
        here = pl.ds(block * LANES, LANES)
        band = pl.ds((blocks - 1 - block) * LANES, rows)
        part = jnp.dot(key_aug[here, :], query_all, preferred_element_type=F32)
        part = jnp.exp(part + strip[:, band])
        slope = part * jnp.dot(value_aug[here, :], grad_all, preferred_element_type=F32)
        strip_grad[:, band] = strip_grad[:, band] + slope
        slope = slope.astype(BF16)
        probs_grad[here, :] = slope
        key_part = jnp.dot(slope, query_and_grad, preferred_element_type=F32)
        value_part = jnp.dot(part.astype(BF16), query_and_grad, preferred_element_type=F32)
        turned = jnp.where(half, key_part, value_part).T.astype(BF16)
        dk_ref[:, here] = turned[0:64]
        dv_ref[:, here] = turned[64:128]
    query_part = jnp.dot(key_aug_t[...], probs_grad[...], preferred_element_type=F32)
    dq_ref[...] = query_part[0:64].astype(BF16)
    layout_grad_ref[0] = jnp.dot(
        query_part[64:192].astype(BF16), query_bins_t_ref[...], preferred_element_type=F32
    )
    folded = strip_grad[pl.ds(0, 8), :]
    for group in range(1, LANES // 8):
        folded = folded + pltpu.roll(strip_grad[pl.ds(group * 8, 8), :], width - group * 8, 1)
    line = folded[0:1]
    for row in range(1, 8):
        line = line + pltpu.roll(folded[row : row + 1], width - row, 1)
    line_grad_ref[0] = line


class Place:
    def __init__(self, mp_size):
        self.dp = lax.axis_index("dp")
        self.mp = lax.axis_index("mp")
        self.mp_size = mp_size
        self.core = lax.rem(self.dp, 2)
        self.x = lax.rem(lax.div(self.dp, 2), 2)
        self.y = lax.div(self.dp, 4)
        self.to_core = (self.dp + 1 - 2 * self.core, self.mp)
        self.to_x = (self.dp + 2 - 4 * self.x, self.mp)
        self.to_y = (self.dp + 4 - 8 * self.y, self.mp)
        self.to_corner = (self.dp + 6 - 4 * self.x - 8 * self.y, self.mp)

    def across(self, step):
        low = lax.rem(lax.rem(self.mp, 2) + step % 2, 2)
        high = lax.rem(lax.div(self.mp, 2) + step // 2, 2)
        return low + 2 * high

    def to_mp(self, step):
        return (self.dp, self.across(step))

    def partners(self):
        others = [self.to_mp(step) for step in range(1, self.mp_size)]
        return [self.to_core, self.to_x, self.to_y, self.to_corner] + others


def greet(place):
    barrier = pltpu.get_barrier_semaphore()
    for partner in place.partners():
        pl.semaphore_signal(barrier, inc=1, device_id=partner, device_id_type=MESH)


def meet(place):
    pl.semaphore_wait(pltpu.get_barrier_semaphore(), len(place.partners()))


class Copy:
    def __init__(self, source, target, send, receive=None, partner=None):
        self.parts = (source, target, send, receive, partner)

    def made(self):
        source, target, send, receive, partner = self.parts
        if partner is None:
            return pltpu.make_async_copy(source, target, send)
        return pltpu.make_async_remote_copy(
            src_ref=source, dst_ref=target, send_sem=send, recv_sem=receive,
            device_id=partner, device_id_type=MESH,
        )

    def start(self):
        self.made().start()

    def wait(self):
        self.made().wait()

    def wait_send(self):
        self.made().wait_send()

    def wait_recv(self):
        self.made().wait_recv()


def remote(source, target, send, receive, partner):
    return Copy(source, target, send, receive, partner)


def lanes_at(block, count):
    return pl.ds(pl.multiple_of(block * LANES, LANES), count * LANES)


class Gather:
    def __init__(self, place, pieces, outs, sems, items):
        self.place, self.pieces, self.outs = place, pieces, outs
        self.z_send, self.z_recv, self.own_sem, self.send, self.recv = sems
        self.items = items

    @staticmethod
    def semaphores(count, mp_size):
        dma = pltpu.SemaphoreType.DMA
        items = count * mp_size
        return [
            dma((count, mp_size)), dma((count, mp_size)), dma((count,)), dma((items, 6)), dma((items, 6))
        ]

    def rows(self, c, source, half):
        n = self.pieces[c].shape[1]
        if half is None:
            return pl.ds(pl.multiple_of(source * n, 16), n)
        return pl.ds(pl.multiple_of(source * n + half * (n // 2), 16), n // 2)

    def window(self, c, source, half, block, count):
        return self.outs[c].at[:, self.rows(c, source, half), lanes_at(block, count)]

    def own(self, c):
        place = self.place
        block = place.core * 4 + place.y * 2 + place.x
        return Copy(
            self.pieces[c], self.window(c, place.mp, None, block, 1), self.own_sem.at[c]
        )

    def along_mp(self, c, step):
        place = self.place
        block = place.core * 4 + place.y * 2 + place.x
        source = place.across(2) if step == 3 else place.mp
        window = self.window(c, source, None, block, 1)
        return remote(
            window if step == 3 else self.pieces[c], window,
            self.z_send.at[c, step], self.z_recv.at[c, step], place.to_mp(2 if step == 2 else 1),
        )

    def copies(self, t):
        c, k = self.items[t]
        place = self.place
        source = place.across(k)
        base = place.core * 4
        mine = base + place.y * 2 + place.x
        turned = base + (1 - place.y) * 2 + place.x

        def copy(i, half, block, count, partner):
            here = self.window(c, source, half, block, count)
            return remote(here, here, self.send.at[t, i], self.recv.at[t, i], partner)

        first = [copy(0, 0, mine, 1, place.to_x), copy(1, 1, mine, 1, place.to_y)]
        second = [
            copy(2, 0, base + place.y * 2, 2, place.to_y),
            copy(3, 1, mine, 1, place.to_x),
            copy(4, 1, turned, 1, place.to_x),
        ]
        third = [copy(5, None, base, 4, place.to_core)]
        return first, second, third

    def first(self, t):
        c, k = self.items[t]
        if k == 0:
            self.own(c).wait()
        else:
            self.along_mp(c, k).wait_recv()
        if k == 2:
            self.along_mp(c, 3).start()
        for copy in self.copies(t)[0]:
            copy.start()

    def second(self, t):
        first, second, _ = self.copies(t)
        for copy in first:
            copy.wait_recv()
        for copy in second:
            copy.start()

    def third(self, t):
        _, second, third = self.copies(t)
        for copy in second:
            copy.wait_recv()
        third[0].start()

    def run(self, ops):
        for op in ops.split():
            which, t = op[0], int(op[1:])
            if which == "z":
                self.along_mp(*self.items[t]).start()
            else:
                {"f": self.first, "s": self.second, "t": self.third}[which](t)

    def done(self, t):
        self.copies(t)[2][0].wait_recv()

    def close(self):
        for t, (c, k) in enumerate(self.items):
            first, second, third = self.copies(t)
            for copy in first + second + third:
                copy.wait_send()
            if k > 0:
                self.along_mp(c, k).wait_send()


def add_rows(target, target_index, source, source_index):
    lead, rows, lanes = target_index
    source_rows, source_lanes = source_index
    row_start, count = rows
    source_start = source_rows
    size = 32
    while count % size:
        size //= 2

    def body(i, carry):
        here = pl.ds(pl.multiple_of(row_start + i * size, size), size)
        there = pl.ds(pl.multiple_of(source_start + i * size, size), size)
        for part in range(lead):
            target[part, here, lanes] = target[part, here, lanes] + source[part, there, source_lanes]
        return carry

    lax.fori_loop(0, count // size, body, 0)


class Scatter:
    def __init__(self, place, fulls, outs, scratch, items, shares=None, inside=False):
        self.inside = inside
        self.place, self.fulls, self.outs, self.items = place, fulls, outs, items
        count = len(fulls)
        self.shares = shares or [None] * count
        self.held = [sorted(k for c, k in items if c == which) for which in range(count)]
        self.whole = [len(full.shape) == 3 for full in fulls]
        buffers = [scratch[i * count : (i + 1) * count] for i in range(5)]
        self.sums, self.from_first, self.from_second, self.from_mp, self.staged = buffers
        self.own_sem, self.send, self.recv, self.share_send, self.share_recv = scratch[5 * count :]

    @staticmethod
    def scratch(shapes, whole, items):
        out = []
        for part, blocks in enumerate((4, 2, 1, 1)):
            for c, (lead, n) in enumerate(shapes):
                slots = sum(which == c for which, _ in items)
                if part == 3:
                    slots, lead, n = (3, lead, n) if slots > 1 else (1, 1, 16)
                out.append(pltpu.VMEM((slots, lead, n, blocks * LANES), BF16))
        for (lead, n), is_whole in zip(shapes, whole):
            out.append(pltpu.VMEM((lead, n, 4 * LANES) if is_whole else (1, 16, LANES), BF16))
        dma = pltpu.SemaphoreType.DMA
        count = len(items)
        out += [dma((count,)), dma((count, 7)), dma((count, 7))]
        return out + [dma((len(shapes),)), dma((len(shapes),))]

    def slot(self, c, k):
        return self.held[c].index(k)

    def size(self, c):
        return self.sums[c].shape[1], self.sums[c].shape[2]

    def source(self, t):
        c, k = self.items[t]
        if not self.whole[c]:
            return self.fulls[c].at[(k + 1) % 2]
        lead, n = self.size(c)
        target = self.place.across(k)
        return self.fulls[c].at[:, pl.ds(pl.multiple_of(target * n, 16), n), :]

    def from_core(self, t):
        c, k = self.items[t]
        place = self.place
        return remote(
            self.source(t).at[:, :, lanes_at((1 - place.core) * 4, 4)], self.sums[c].at[self.slot(c, k)],
            self.send.at[t, 0], self.recv.at[t, 0], place.to_core,
        )

    def own(self, t):
        c, _ = self.items[t]
        return Copy(
            self.source(t).at[:, :, lanes_at(self.place.core * 4, 4)], self.staged[c], self.own_sem.at[t]
        )

    def copies(self, t):
        c, k = self.items[t]
        place = self.place
        lead, n = self.size(c)
        top, bottom = pl.ds(0, n // 2), pl.ds(n // 2, n // 2)
        every = pl.ds(0, lead)
        sums = self.sums[c].at[self.slot(c, k)]

        def copy(i, source, landing, partner):
            return remote(source, landing, self.send.at[t, i], self.recv.at[t, i], partner)

        landing = self.from_first[c].at[self.slot(c, k)]
        first = [
            copy(
                1, sums.at[every, top, lanes_at((1 - place.y) * 2, 2)],
                landing.at[every, top, pl.ds(0, 256)], place.to_y,
            ),
            copy(
                2, sums.at[every, bottom, lanes_at(1 - place.x, 1)],
                landing.at[every, bottom, pl.ds(0, 128)], place.to_x,
            ),
            copy(
                3, sums.at[every, bottom, lanes_at(3 - place.x, 1)],
                landing.at[every, bottom, pl.ds(128, 128)], place.to_x,
            ),
        ]
        landing = self.from_second[c].at[self.slot(c, k)]
        second = [
            copy(
                4, sums.at[every, top, lanes_at(place.y * 2 + 1 - place.x, 1)],
                landing.at[every, top, pl.ds(0, 128)], place.to_x,
            ),
            copy(
                5, sums.at[every, bottom, lanes_at((1 - place.y) * 2 + place.x, 1)],
                landing.at[every, bottom, pl.ds(0, 128)], place.to_y,
            ),
        ]
        third = None
        if k > 0:
            third = copy(
                6, sums.at[:, :, lanes_at(place.y * 2 + place.x, 1)], self.from_mp[c].at[k - 1],
                place.to_mp(1 if k % 2 else 2),
            )
        return first, second, third

    def core(self, t):
        self.from_core(t).start()
        if self.whole[self.items[t][0]]:
            self.own(t).start()

    def first(self, t):
        c, k = self.items[t]
        lead, n = self.size(c)
        sums = self.sums[c].at[self.slot(c, k)]
        self.from_core(t).wait_recv()
        if self.whole[c]:
            self.own(t).wait()
            add_rows(sums, (lead, (0, n), pl.ds(0, 512)), self.staged[c], (0, pl.ds(0, 512)))
        else:
            mine = lanes_at(self.place.core * 4, 4)
            add_rows(sums, (lead, (0, n), pl.ds(0, 512)), self.source(t), (0, mine))
        for copy in self.copies(t)[0]:
            copy.start()

    def second(self, t):
        c, k = self.items[t]
        place = self.place
        lead, n = self.size(c)
        first, second, _ = self.copies(t)
        for copy in first:
            copy.wait_recv()
        slot = self.slot(c, k)
        sums, landing = self.sums[c].at[slot], self.from_first[c].at[slot]
        half = n // 2
        add_rows(sums, (lead, (0, half), lanes_at(place.y * 2, 2)), landing, (0, pl.ds(0, 256)))
        add_rows(sums, (lead, (half, half), lanes_at(place.x, 1)), landing, (half, pl.ds(0, 128)))
        add_rows(sums, (lead, (half, half), lanes_at(2 + place.x, 1)), landing, (half, pl.ds(128, 128)))
        for copy in second:
            copy.start()

    def third(self, t):
        c, k = self.items[t]
        lead, n = self.size(c)
        _, second, third = self.copies(t)
        for copy in second:
            copy.wait_recv()
        slot = self.slot(c, k)
        mine = lanes_at(self.place.y * 2 + self.place.x, 1)
        add_rows(
            self.sums[c].at[slot], (lead, (0, n), mine), self.from_second[c].at[slot], (0, pl.ds(0, 128))
        )
        if k == 2:
            self.copies(self.items.index((c, 3)))[2].wait_recv()
            add_rows(
                self.sums[c].at[slot], (lead, (0, n), mine), self.from_mp[c].at[2], (0, pl.ds(0, 128))
            )
        if k > 0 and not self.inside:
            third.start()

    def share(self, c):
        return remote(
            self.shares[c], self.from_mp[c].at[0], self.share_send.at[c], self.share_recv.at[c],
            self.place.to_mp(1),
        )

    def end(self, c):
        if self.inside:
            self.finish(c)
            return
        if self.shares[c] is not None:
            self.share(c).wait_recv()
        for k in (1, 2):
            if (c, k) in self.items:
                self.copies(self.items.index((c, k)))[2].wait_recv()
        self.finish(c)

    def run(self, ops):
        for op in ops.split():
            table = {"c": self.core, "f": self.first, "s": self.second, "t": self.third, "e": self.end}
            table[op[0]](int(op[1:]))

    def left(self, t):
        self.from_core(t).wait_send()

    def close(self):
        for t, (c, k) in enumerate(self.items):
            first, second, third = self.copies(t)
            if self.whole[c] or k < 2:
                self.from_core(t).wait_send()
            for copy in first + second:
                copy.wait_send()
            if third is not None and not self.inside:
                third.wait_send()
        for c, share in enumerate(self.shares):
            if share is not None:
                self.share(c).wait_send()

    def finish(self, c):
        place = self.place
        lead, n = self.size(c)
        mine = lanes_at(place.y * 2 + place.x, 1)
        sums, landing, out = self.sums[c], self.from_mp[c], self.outs[c]
        steps = () if self.inside else (1, 2)
        slot = self.slot(c, 1 if self.inside else 0)
        size = 32
        while n % size:
            size //= 2

        def body(i, carry):
            here = pl.ds(pl.multiple_of(i * size, size), size)
            for part in range(lead):
                total = sums[slot, part, here, mine].astype(F32)
                for k in steps:
                    total = total + landing[k - 1, part, here, :].astype(F32)
                out[part, here, :] = total.astype(out.dtype)
            return carry

        lax.fori_loop(0, n // size, body, 0)


def attention_shapes(head_count, head_size, rows, keys, width):
    whole = lambda shape: pl.BlockSpec(shape, lambda head: (0,) * len(shape))
    column = lambda size: pl.BlockSpec((head_size, size), lambda head: (head, 0))
    page = lambda a, b: pl.BlockSpec((1, a, b), lambda head: (head, 0, 0))
    return whole, column, page


def attend(queries, keys_t, values_t, layout, line, key_extra, query_bins):
    inner, rows = queries.shape
    keys = keys_t.shape[1]
    head_count, _, width = line.shape
    head_size = inner // head_count
    whole, column, page = attention_shapes(head_count, head_size, rows, keys, width)
    return pl.pallas_call(
        attend_kernel,
        grid=(head_count,),
        out_shape=(
            jax.ShapeDtypeStruct((inner, rows), BF16),
            jax.ShapeDtypeStruct((head_count, 1, rows), F32),
        ),
        in_specs=[
            column(rows), column(keys), column(keys), page(128, 128), page(1, width),
            whole((keys, 256)), whole((128, rows)),
        ],
        out_specs=(column(rows), page(1, rows)),
        scratch_shapes=[
            pltpu.VMEM((keys, 256), BF16),
            pltpu.VMEM((256, rows), BF16),
            pltpu.VMEM((LANES, width), F32),
            pltpu.VMEM((keys, rows), F32),
            pltpu.VMEM((keys, rows), BF16),
        ],
        compiler_params=pltpu.CompilerParams(
            dimension_semantics=("arbitrary",), vmem_limit_bytes=32 << 20
        ),
        name="attend",
    )(queries, keys_t, values_t, layout, line, key_extra, query_bins)


def attend_back(
    queries, keys_t, values_t, heads_out, heads_grad, lse, layout, line,
    key_extra, key_extra_t, query_bins, query_bins_t,
):
    inner, rows = queries.shape
    keys = keys_t.shape[1]
    head_count, _, width = line.shape
    head_size = inner // head_count
    whole, column, page = attention_shapes(head_count, head_size, rows, keys, width)
    return pl.pallas_call(
        attend_back_kernel,
        grid=(head_count,),
        out_shape=(
            jax.ShapeDtypeStruct((inner, rows), BF16),
            jax.ShapeDtypeStruct((inner, keys), BF16),
            jax.ShapeDtypeStruct((inner, keys), BF16),
            jax.ShapeDtypeStruct((head_count, 1, width), F32),
            jax.ShapeDtypeStruct((head_count, 128, 128), F32),
        ),
        in_specs=[
            column(rows), column(keys), column(keys), column(rows), column(rows),
            page(1, rows), page(128, 128), page(1, width),
            whole((keys, 256)), whole((128, keys)), whole((128, rows)), whole((rows, 128)),
        ],
        out_specs=(column(rows), column(keys), column(keys), page(1, width), page(128, 128)),
        scratch_shapes=[
            pltpu.VMEM((keys, 256), BF16),
            pltpu.VMEM((192, keys), BF16),
            pltpu.VMEM((256, rows), BF16),
            pltpu.VMEM((keys, 128), BF16),
            pltpu.VMEM((128, rows), BF16),
            pltpu.VMEM((LANES, width), F32),
            pltpu.VMEM((LANES, width), F32),
            pltpu.VMEM((keys, rows), BF16),
        ],
        compiler_params=pltpu.CompilerParams(
            dimension_semantics=("arbitrary",), vmem_limit_bytes=32 << 20
        ),
        name="attend_back",
    )(
        queries, keys_t, values_t, heads_out, heads_grad, lse, layout, line,
        key_extra, key_extra_t, query_bins, query_bins_t,
    )


FORWARD_ITEMS = [(0, 0), (1, 0), (2, 0), (0, 1), (0, 2), (0, 3), (1, 1), (2, 1), (1, 2), (2, 2), (1, 3), (2, 3)]


FORWARD_SUMS = [(0, 1), (1, 1)]


def forward_kernel(
    mp_size, group,
    query_ref, output_ref, gate_up_ref, down_ref, key_value_ref, table_ref, boxes_ref, lengths_ref,
    input_ref, gain_ref, cotangent_ref,
    w_first, queries_out, keys_out, values_out, heads_out_out, lse, layout, line, key_extra, key_extra_t,
    slot_owner_out, residual_out, layer_output, second_grad, gate_up_full, down_full, tables,
    line_hot, bin_hot, gate_up_share, down_share, queries, keys_t, values_t, heads_out, slot_owner, residual,
    first_ref, query_piece, normed_t, slot_t, w_gate_up, w_down, first_here, key_aug, query_aug, strip, scores, probs,
    second_t, second_owner, out_owner, out_t,
    hidden_a, hidden_b, hidden_c, act_t, low_t, stage_gate_up, stage_down,
    row_send, row_recv, row_own, table_send, table_recv, table_own, load_sem, store_sem, keep_sem, *sems,
):
    place = Place(mp_size)
    rows, model_width = input_ref.shape
    keys = keys_t.shape[1]
    blocks = keys // LANES
    width = strip.shape[1]
    inner_here = first_ref.shape[1]
    heads_here = inner_here // 64
    hidden = gate_up_ref.shape[1]
    doc = lax.div(place.mp, group)
    member = lax.rem(place.mp, group)
    first_peer = place.mp - member
    own_lanes = pl.ds(pl.multiple_of(member * rows, LANES), rows)

    items = FORWARD_ITEMS
    column = lanes_at(place.core * 4 + place.y * 2 + place.x, 1)
    gather = Gather(
        place, [first_ref, gate_up_ref.at[:, :, column], down_ref.at[:, :, column]],
        [w_first, w_gate_up, w_down], sems[:5], items
    )
    at = {item: t for t, item in enumerate(items)}

    row_copies = [
        remote(
            normed_t, slot_t.at[:, own_lanes], row_send.at[k], row_recv.at[k],
            (place.dp, first_peer + lax.rem(member + k, group)),
        )
        for k in range(1, group)
    ]
    table_copies = [
        remote(table_ref, tables.at[place.mp], table_send.at[k], table_recv.at[k], place.to_mp(k))
        for k in range(1, mp_size)
    ]
    row_here = Copy(normed_t, slot_t.at[:, own_lanes], row_own.at[0])
    table_here = Copy(table_ref, tables.at[place.mp], table_own.at[0])

    greet(place)
    loads = [
        Copy(query_ref.at[column, :], query_piece, load_sem.at[0]),
        Copy(output_ref.at[:, column], first_ref.at[3], load_sem.at[1]),
    ]
    for copy in loads:
        copy.start()
    for c in range(1, 3):
        gather.own(c).start()
    table_here.start()
    turned = key_value_ref[...].T
    first_ref[1] = turned[0:inner_here]
    first_ref[2] = turned[inner_here : 2 * inner_here]

    def norm_into(values_ref, gain):
        def body(i, carry):
            here = pl.ds(pl.multiple_of(i * 16, 16), 16)
            values = values_ref[here, :]
            scale = lax.rsqrt(jnp.mean(values * values, axis=1, keepdims=True) + EPSILON)
            second_owner[here, :] = (values * scale * gain).astype(BF16)
            return carry

        lax.fori_loop(0, rows // 16, body, 0)

    norm_into(input_ref, gain_ref[0:1, :])
    normed_t[...] = second_owner[...].T
    row_here.start()
    for copy in loads:
        copy.wait()
    first_ref[0] = query_piece[...].T
    gather.own(0).start()
    meet(place)
    gather.run("f0 f1")
    for copy in row_copies + table_copies:
        copy.start()
    gather.along_mp(0, 1).start()

    key_rows = row_ids((64, keys))
    key_bins = boxes_ref[:, pl.ds(pl.multiple_of(doc * keys, LANES), keys)]
    x_place = jnp.where(key_rows == key_bins[0:1], 1.0, 0.0).astype(BF16)
    y_place = jnp.where(key_rows == key_bins[1:2], 1.0, 0.0).astype(BF16)
    key_extra_t[0:64, :] = x_place
    key_extra_t[64:128, :] = y_place
    mask = jnp.where(lane_ids((64, keys)) >= lengths_ref[doc], NEG_FILL, 0.0)
    first_row = member * rows
    spot = lane_ids((8, width))
    spot = jnp.where(spot >= width - LANES, spot - width, spot)
    bucket = bucket_of(LANES * (blocks - 1) - spot - first_row)[0:1]
    line_hot[...] = jnp.where(row_ids((LANES, width)) == bucket, 1.0, 0.0).astype(BF16)
    spot = lane_ids((8, LANES))
    bucket = bucket_of(jnp.where(spot < NBIN, -spot, LANES - spot))[0:1]
    bin_hot[...] = jnp.where(row_ids((LANES, LANES)) == bucket, 1.0, 0.0).astype(BF16)
    tail = jnp.where(key_rows == 0, mask, jnp.where(key_rows < 4, 1.0, 0.0)).astype(BF16)
    turned = jnp.concatenate([jnp.zeros((64, keys), BF16), x_place, y_place, tail], axis=0).T
    key_extra[...] = turned
    key_aug[...] = turned
    query_aug[pl.ds(192, 64), :] = jnp.where(row_ids((64, rows)) == 0, 1.0, 0.0).astype(BF16)
    gather.run("s0 f2")
    for block in range(model_width // LANES):
        owner = block_owner(block)
        out_owner[:, owner * LANES : (owner + 1) * LANES] = cotangent_ref[
            :, block * LANES : (block + 1) * LANES
        ].astype(BF16)
    out_t[...] = cotangent_ref[...].astype(BF16).T
    residual[...] = input_ref[...]
    layer_output[...] = jnp.zeros_like(layer_output)
    second_grad[...] = jnp.zeros_like(second_grad)
    row_here.wait()
    table_here.wait()
    gather.run("s1 t0")

    head_units = mp_size * heads_here
    table = {
        (1, 0): "f3 z4 z6", (2, 0): "s3 s2 t1", (4, 0): "t3 f4 z7", (5, 0): "s4 t2", (6, 0): "f5 z8",
        (7, 0): "t4 f6", (8, 0): "s5 z9", (9, 0): "f7 s6", (11, 0): "t5", (12, 0): "f8 s7", (13, 0): "t6",
        (14, 0): "f9 s8", (16, 0): "f10 t7", (16, 2): "s9", (17, 0): "f11 t8", (17, 1): "s10",
        (17, 3): "t9", (18, 0): "s11", (18, 3): "t10", (19, 0): "t11",
    }
    scatter = Scatter(
        place, [gate_up_full, down_full], [gate_up_share, down_share], sems[5:], FORWARD_SUMS,
        inside=True,
    )
    sum_table = {(18, 0): "c0 c1", (18, 3): "f0 f1", (19, 3): "s0"}

    def communicate(unit, point):
        for (at_unit, at_point), ops in table.items():
            if at_point == point:

                @pl.when(unit == at_unit)
                def _(ops=ops):
                    gather.run(ops)

        for (at_unit, at_point), ops in sum_table.items():
            if at_point == point:

                @pl.when(unit == at_unit)
                def _(ops=ops):
                    scatter.run(ops)

    def head_unit(unit, carry):
        communicate(unit, 0)
        step = lax.div(unit, heads_here)
        inside = lax.rem(unit, heads_here)
        source = place.across(step)
        base = pl.multiple_of(source * inner_here, 16)
        head = source * heads_here + inside

        @pl.when(inside == 0)
        def _():
            for k in range(mp_size):

                @pl.when(step == k)
                def _(k=k):
                    gather.done(at[(0, k)])
                    if k == 0:
                        for copy in row_copies:
                            copy.wait_recv()
                    else:
                        table_copies[k - 1].wait_recv()

            load = Copy(w_first.at[:, pl.ds(base, inner_here), :], first_here, load_sem.at[0])
            load.start()
            hot = tables[source].astype(BF16)
            line[source] = jnp.dot(hot[0:8], line_hot[...], preferred_element_type=F32)
            bins = jnp.dot(hot[8:24], bin_hot[...], preferred_element_type=F32)
            for i in range(heads_here):
                x_line = jnp.broadcast_to(bins[i : i + 1], (64, LANES))
                y_line = jnp.broadcast_to(bins[8 + i : 9 + i], (64, LANES))
                left = lane_ids((64, LANES)) < 64
                x_part = pltpu.roll(x_line, 0, 1, stride=1, stride_axis=0)
                y_part = pltpu.roll(y_line, 64, 1, stride=1, stride_axis=0)
                layout[source * heads_here + i] = jnp.concatenate(
                    [jnp.where(left, x_part, 0.0), jnp.where(left, 0.0, y_part)], axis=0
                ).astype(BF16)
            load.wait()
            here = pl.ds(base, inner_here)
            queries[here, :] = jnp.dot(
                first_here[0], normed_t[...], preferred_element_type=F32
            ).astype(BF16)
            keys_t[here, :] = jnp.dot(
                first_here[1], slot_t[...], preferred_element_type=F32
            ).astype(BF16)
            values_t[here, :] = jnp.dot(
                first_here[2], slot_t[...], preferred_element_type=F32
            ).astype(BF16)

        here = pl.ds(pl.multiple_of(head * 64, 16), 64)
        both = jnp.concatenate([keys_t[here, :], values_t[here, :]], axis=0).T
        low_lanes = lane_ids((keys, LANES)) < 64
        key_aug[:, 0:LANES] = jnp.where(low_lanes, both, key_extra[:, 0:LANES])
        query_aug[pl.ds(0, 64), :] = queries[here, :]
        query_aug[pl.ds(64, 128), :] = jnp.dot(
            layout[head], key_extra_t[:, own_lanes], preferred_element_type=F32
        ).astype(BF16)
        strip[...] = pltpu.roll(
            jnp.broadcast_to(line[source, pl.ds(inside, 1), :], (LANES, width)), 0, 1,
            stride=1, stride_axis=0,
        )
        query_all = query_aug[...]
        top = jnp.full((1, rows), -jnp.inf, F32)
        for block in range(blocks):
            some = pl.ds(block * LANES, LANES)
            part = jnp.dot(key_aug[some, :], query_all, preferred_element_type=F32)
            part = part + strip[:, pl.ds((blocks - 1 - block) * LANES, rows)]
            scores[some, :] = part
            top = jnp.maximum(top, jnp.max(part, axis=0, keepdims=True))
        sums = jnp.zeros((1, rows), F32)
        for block in range(blocks):
            some = pl.ds(block * LANES, LANES)
            part = jnp.exp(scores[some, :] - top)
            sums = sums + jnp.sum(part, axis=0, keepdims=True)
            probs[some, :] = part.astype(BF16)
        mixed = jnp.dot(values_t[here, :], probs[...], preferred_element_type=F32)
        heads_out[here, :] = (mixed / sums).astype(BF16)
        lse[head] = top + jnp.log(sums)

        @pl.when(inside == heads_here - 1)
        def _():
            part = heads_out[pl.ds(base, inner_here), :].T
            residual[...] = residual[...] + jnp.dot(
                part, first_here[3], preferred_element_type=F32
            )

        return carry

    lax.fori_loop(0, head_units, head_unit, 0)
    for block in range(model_width // LANES):
        owner = block_owner(block)
        slot_owner[:, owner * LANES : (owner + 1) * LANES] = slot_t[
            block * LANES : (block + 1) * LANES, :
        ].T

    kept = [
        Copy(here, there, keep_sem.at[i])
        for i, (here, there) in enumerate(
            [
                (queries, queries_out), (keys_t, keys_out), (values_t, values_out),
                (heads_out, heads_out_out), (slot_owner, slot_owner_out), (residual, residual_out),
            ]
        )
    ]
    for copy in kept:
        copy.start()
    norm_into(residual, gain_ref[1:2, :])
    second_t[...] = second_owner[...].T
    turned_blocks = [second_owner[:, b * LANES : (b + 1) * LANES] for b in range(model_width // LANES)]
    for block, values in enumerate(turned_blocks):
        owner = block_owner(block)
        second_owner[:, owner * LANES : (owner + 1) * LANES] = values

    def store(step):
        source = place.across(step)
        here = pl.ds(pl.multiple_of(source * hidden, 16), hidden)
        return [
            Copy(stage_gate_up, gate_up_full.at[:, here, :], store_sem.at[0]),
            Copy(stage_down, down_full.at[:, here, :], store_sem.at[1]),
        ]

    def hidden_unit(step, carry):
        unit = step + head_units

        @pl.when(step > 0)
        def _():
            for copy in store(step):
                copy.wait()

        communicate(unit, 0)
        source = place.across(step)
        here = pl.ds(pl.multiple_of(source * hidden, 16), hidden)
        for k in range(mp_size):

            @pl.when(step == k)
            def _(k=k):
                gather.done(at[(1, k)])
                gather.done(at[(2, k)])

        hidden_a[...] = jnp.dot(w_gate_up[0, here, :], second_t[...], preferred_element_type=F32)
        hidden_b[...] = jnp.dot(w_gate_up[1, here, :], second_t[...], preferred_element_type=F32)
        communicate(unit, 1)
        hidden_c[...] = jnp.dot(w_down[0, here, :], out_t[...], preferred_element_type=F32)

        def activate(i, inner_carry):
            some = pl.ds(pl.multiple_of(i * 16, 16), 16)
            gate, up, slope = hidden_a[some, :], hidden_b[some, :], hidden_c[some, :]
            square = gate * gate
            factor = 0.7978845608028654
            bent = jnp.tanh(factor * gate * (1.0 + 0.044715 * square))
            half = 0.5 * (1.0 + bent)
            value = gate * half
            change = half + 0.5 * gate * (1.0 - bent * bent) * (
                factor * (1.0 + 3.0 * 0.044715 * square)
            )
            act_t[some, :] = (value * up).astype(BF16)
            low_t[some, :] = (slope * up * change).astype(BF16)
            low_t[pl.ds(pl.multiple_of(hidden + i * 16, 16), 16), :] = (slope * value).astype(BF16)
            return inner_carry

        lax.fori_loop(0, hidden // 16, activate, 0)
        communicate(unit, 2)

        stage_down[0] = jnp.dot(act_t[...], out_owner[...], preferred_element_type=F32).astype(BF16)
        stage_gate_up[0] = jnp.dot(
            low_t[0:hidden], second_owner[...], preferred_element_type=F32
        ).astype(BF16)
        stage_gate_up[1] = jnp.dot(
            low_t[hidden:], second_owner[...], preferred_element_type=F32
        ).astype(BF16)
        for copy in store(step):
            copy.start()
        communicate(unit, 3)
        layer_output[...] = layer_output[...] + dot_f32(act_t[...].T, w_down[0, here, :], 1, 0)
        second_grad[...] = (
            second_grad[...]
            + dot_f32(low_t[0:hidden].T, w_gate_up[0, here, :], 1, 0)
            + dot_f32(low_t[hidden:].T, w_gate_up[1, here, :], 1, 0)
        )
        return carry

    lax.fori_loop(0, mp_size, hidden_unit, 0)
    layer_output[...] = layer_output[...] + residual[...]
    scatter.run("s1 t0 t1")
    scatter.run("e0 e1")
    for copy in store(mp_size - 1):
        copy.wait()
    gather.close()
    scatter.close()
    for copy in row_copies + table_copies:
        copy.wait_send()
    for copy in kept:
        copy.wait()


def block_owner(block):
    return (block % 2) * 4 + block // 2


def forward(
    mp_size, group, query, output, gate_up, down, key_value, table, boxes, lengths, layer_input,
    gains, cotangent,
):
    rows, model_width = layer_input.shape
    keys = boxes.shape[1] // lengths.shape[0]
    width = LANES * (keys // LANES + rows // LANES)
    inner_here, hidden = query.shape[1], gate_up.shape[1]
    inner, total_hidden = inner_here * mp_size, hidden * mp_size
    head_count = inner // 64
    dma = pltpu.SemaphoreType.DMA
    hbm = pl.BlockSpec(memory_space=HBM)
    vmem = pl.BlockSpec(memory_space=pltpu.VMEM)
    shape = jax.ShapeDtypeStruct
    out = [
        (shape((4, inner, model_width), BF16), hbm),
        (shape((inner, rows), BF16), hbm),
        (shape((inner, keys), BF16), hbm),
        (shape((inner, keys), BF16), hbm),
        (shape((inner, rows), BF16), hbm),
        (shape((head_count, 1, rows), F32), vmem),
        (shape((head_count, 128, 128), BF16), vmem),
        (shape((mp_size, 8, width), F32), vmem),
        (shape((keys, 256), BF16), vmem),
        (shape((128, keys), BF16), vmem),
        (shape((keys, model_width), BF16), hbm),
        (shape((rows, model_width), F32), hbm),
        (shape((rows, model_width), F32), vmem),
        (shape((rows, model_width), F32), vmem),
        (shape((2, total_hidden, model_width), BF16), hbm),
        (shape((1, total_hidden, model_width), BF16), hbm),
        (shape((mp_size, 24, LANES), F32), vmem),
        (shape((LANES, width), BF16), vmem),
        (shape((LANES, LANES), BF16), vmem),
        (shape((2, hidden, LANES), BF16), vmem),
        (shape((1, hidden, LANES), BF16), vmem),
    ]
    return pl.pallas_call(
        partial(forward_kernel, mp_size, group),
        out_shape=tuple(o[0] for o in out),
        in_specs=[hbm] * 4 + [vmem] * 3 + [pl.BlockSpec(memory_space=pltpu.SMEM)] + [vmem] * 3,
        out_specs=tuple(o[1] for o in out),
        scratch_shapes=[
            pltpu.VMEM((inner, rows), BF16),
            pltpu.VMEM((inner, keys), BF16),
            pltpu.VMEM((inner, keys), BF16),
            pltpu.VMEM((inner, rows), BF16),
            pltpu.VMEM((keys, model_width), BF16),
            pltpu.VMEM((rows, model_width), F32),
            pltpu.VMEM((4, inner_here, LANES), BF16),
            pltpu.VMEM((LANES, inner_here), BF16),
            pltpu.VMEM((model_width, rows), BF16),
            pltpu.VMEM((model_width, keys), BF16),
            pltpu.VMEM((2, total_hidden, model_width), BF16),
            pltpu.VMEM((1, total_hidden, model_width), BF16),
            pltpu.VMEM((4, inner_here, model_width), BF16),
            pltpu.VMEM((keys, 256), BF16),
            pltpu.VMEM((256, rows), BF16),
            pltpu.VMEM((LANES, width), F32),
            pltpu.VMEM((keys, rows), F32),
            pltpu.VMEM((keys, rows), BF16),
            pltpu.VMEM((model_width, rows), BF16),
            pltpu.VMEM((rows, model_width), BF16),
            pltpu.VMEM((rows, model_width), BF16),
            pltpu.VMEM((model_width, rows), BF16),
            pltpu.VMEM((hidden, rows), F32),
            pltpu.VMEM((hidden, rows), F32),
            pltpu.VMEM((hidden, rows), F32),
            pltpu.VMEM((hidden, rows), BF16),
            pltpu.VMEM((2 * hidden, rows), BF16),
            pltpu.VMEM((2, hidden, model_width), BF16),
            pltpu.VMEM((1, hidden, model_width), BF16),
            dma((group,)), dma((group,)), dma((1,)),
            dma((mp_size,)), dma((mp_size,)), dma((1,)), dma((2,)), dma((2,)), dma((6,)),
        ]
        + Gather.semaphores(3, mp_size)
        + Scatter.scratch([(2, hidden), (1, hidden)], (True, True), FORWARD_SUMS),
        compiler_params=pltpu.CompilerParams(
            collective_id=0, has_side_effects=True, vmem_limit_bytes=62 << 20
        ),
        name="forward",
    )(
        query, output, gate_up, down, key_value, table, boxes, lengths, layer_input, gains, cotangent,
    )


BACKWARD_ITEMS = [(0, 3), (1, 3), (0, 2), (1, 2), (2, 3), (2, 2), (0, 0), (2, 1), (1, 0), (2, 0)]


def unskewed(values, first, count, shift):
    width = values.shape[1]
    folded = None
    for group in range(count // 8):
        part = values[pl.ds(first + group * 8, 8), :]
        back = (-(group * 8 + shift)) % width
        part = pltpu.roll(part, back, 1) if back else part
        folded = part if folded is None else folded + part
    total = folded[0:1]
    for row in range(1, 8):
        total = total + pltpu.roll(folded[row : row + 1], width - row, 1)
    return total


def exact_dot(left, right):
    parts = three_parts(left)
    return sum(dot_f32(part, right, 1, 1) for part in parts)


def backward_kernel(mp_size, group, *refs):
    (
        gate_up_full, down_full, w_first, queries, keys_t, values_t, heads_out,
        residual_in, second_in, cotangent_in,
        lse, layout, line, key_extra, key_extra_t, slot_owner, layer_input, gains, line_hot, bin_hot,
        gate_up_share, down_share, input_out, small_out, gate_up_sum, down_sum, first_sum,
        *refs,
    ) = refs
    (
        input_grad, slot_grad, own_grad, residual_grad, branch_owner, branch_t, w_query, w_output, w_kv,
        q_here, k_here, v_here, out_here, grad_here, dq_here, dk_here, dv_here, kv_here,
        key_aug, key_aug_t, query_aug, value_aug, grad_aug, strip, strip_grad, probs_grad,
        layout_grad, line_sums, bin_sums, gain_part, rows_out, peers, stage, stage_in, full_here,
        load_sem, value_sem, row_send, row_recv, stage_send, stage_recv,
        *refs,
    ) = refs
    place = Place(mp_size)
    rows, model_width = layer_input.shape
    keys = slot_owner.shape[0]
    blocks = keys // LANES
    inner_here = q_here.shape[0]
    heads_here = inner_here // 64
    member = lax.rem(place.mp, group)
    first_peer = place.mp - member
    own_start = pl.multiple_of(member * rows, LANES)
    own_lanes = pl.ds(own_start, rows)

    items = BACKWARD_ITEMS
    fulls = [gate_up_full, down_full, full_here]
    scatter = Scatter(
        place, fulls, [gate_up_sum, down_sum, first_sum], refs, items, [gate_up_share, down_share, None]
    )

    loads = [
        Copy(second_in, slot_grad.at[pl.ds(0, rows), :], value_sem.at[0]),
        Copy(residual_in, slot_grad.at[pl.ds(rows, rows), :], value_sem.at[1]),
        Copy(cotangent_in, input_grad, value_sem.at[2]),
    ]
    for copy in loads:
        copy.start()
    greet(place)
    meet(place)
    scatter.run("c0 c1")
    for c in range(2):
        scatter.share(c).start()
    key_aug[...] = key_extra[...]
    key_aug_t[pl.ds(64, 128), :] = key_extra_t[...]
    for copy in loads:
        copy.wait()

    def norm_back(i, total):
        here = pl.ds(pl.multiple_of(i * 16, 16), 16)
        grad = slot_grad[here, :]
        values = slot_grad[pl.ds(pl.multiple_of(rows + i * 16, 16), 16), :]
        scale = lax.rsqrt(jnp.mean(values * values, axis=1, keepdims=True) + EPSILON)
        scaled = gains[1:2, :] * grad
        mean = jnp.mean(scaled * values, axis=1, keepdims=True)
        result = input_grad[here, :] + scale * scaled - values * (scale * scale * scale * mean)
        residual_grad[here, :] = result
        branch_owner[here, :] = result.astype(BF16)
        product = grad * values * scale
        return total + product[0:8] + product[8:16]

    total = lax.fori_loop(0, rows // 16, norm_back, jnp.zeros((8, model_width), F32))
    gain_part[...] = jnp.sum(total, axis=0, keepdims=True)
    scatter.run("f0 c2")
    branch_t[...] = branch_owner[...].T
    parts = [branch_owner[:, b * LANES : (b + 1) * LANES] for b in range(model_width // LANES)]
    for block, values in enumerate(parts):
        owner = block_owner(block)
        branch_owner[:, owner * LANES : (owner + 1) * LANES] = values
    slot_grad[...] = jnp.zeros_like(slot_grad)
    own_grad[...] = jnp.zeros_like(own_grad)
    scatter.run("f1 c3")

    plan = {
        (0, 2): "s0 f2", (0, 3): "s1 f3", (0, 4): "t0 c4", (1, 1): "s2", (1, 2): "t1 f4", (1, 3): "s3 c6",
        (2, 0): "t2 c5", (2, 1): "s4 f5", (2, 2): "t3", (2, 3): "f6 c8", (2, 4): "t4 c7", (3, 1): "s5",
        (3, 2): "s6 f7", (3, 4): "t5 f8 c9",
    }

    def communicate(block, point):
        for (at_block, at_point), ops in plan.items():
            if at_point == point:

                @pl.when(block == at_block)
                def _(ops=ops):
                    scatter.run(ops)

    row_copies = [
        remote(
            rows_out.at[k - 1], peers.at[k - 1], row_send.at[k], row_recv.at[k],
            (place.dp, first_peer + lax.rem(member + k, group)),
        )
        for k in range(1, group)
    ]

    def block_unit(block, carry):
        communicate(block, 0)
        step = mp_size - 1 - block
        target = place.across(step)
        base = pl.multiple_of(target * inner_here, 16)
        here = pl.ds(base, inner_here)
        slot = lax.rem(block, 2)
        copies = [
            Copy(w_first.at[0, here, :], w_query, load_sem.at[0]),
            Copy(w_first.at[3, here, :], w_output, load_sem.at[1]),
            Copy(queries.at[here, :], q_here, load_sem.at[2]),
            Copy(keys_t.at[here, :], k_here, load_sem.at[3]),
            Copy(values_t.at[here, :], v_here, load_sem.at[4]),
            Copy(heads_out.at[here, :], out_here, load_sem.at[5]),
        ]
        for i in range(heads_here):
            for part in range(2):
                copies.append(
                    Copy(
                        w_first.at[1 + part, pl.ds(pl.multiple_of(base + i * 64, 16), 64), :],
                        w_kv.at[pl.ds(i * 128 + part * 64, 64), :],
                        load_sem.at[6 + 2 * i + part],
                    )
                )
        for copy in copies:
            copy.start()
        for copy in (copies[1], copies[5]):
            copy.wait()

        for b in range(2, mp_size):

            @pl.when(block == b)
            def _(b=b):
                scatter.left(items.index((2, mp_size + 1 - b)))

        grad_here[...] = jnp.dot(w_output[...], branch_t[...], preferred_element_type=F32).astype(BF16)
        full_here[slot, 3] = jnp.dot(
            out_here[...], branch_owner[...], preferred_element_type=F32
        ).astype(BF16)
        for copy in [copies[0]] + copies[2:5] + copies[6:]:
            copy.wait()

        def head_unit(inside, inner_carry):
            for point in range(1, heads_here):

                @pl.when(inside == point)
                def _(point=point):
                    communicate(block, point)

            head = target * heads_here + inside
            some = pl.ds(pl.multiple_of(inside * 64, 16), 64)
            q_head, k_head, v_head = q_here[some, :], k_here[some, :], v_here[some, :]
            grad_head = grad_here[some, :]
            both = jnp.concatenate([k_head, v_head], axis=0).T
            lanes = lane_ids((keys, LANES))
            key_aug[:, 0:LANES] = jnp.where(lanes < 64, both, key_extra[:, 0:LANES])
            ones = jnp.where(lanes < 3, 1.0, 0.0).astype(BF16)
            value_aug[...] = jnp.where(lanes < 64, ones, both)
            key_aug_t[pl.ds(0, 64), :] = k_head
            query_aug[pl.ds(0, 64), :] = q_head
            query_aug[pl.ds(64, 128), :] = jnp.dot(
                layout[head], key_extra_t[:, own_lanes], preferred_element_type=F32
            ).astype(BF16)
            high, middle, low = three_parts(-lse[head])
            tail = row_ids((64, rows))
            rows_of = lambda part: jnp.broadcast_to(part.astype(F32), (64, rows))
            query_aug[pl.ds(192, 64), :] = jnp.where(
                tail == 0, 1.0,
                jnp.where(
                    tail == 1, rows_of(high),
                    jnp.where(tail == 2, rows_of(middle), jnp.where(tail == 3, rows_of(low), 0.0)),
                ),
            ).astype(BF16)
            row_dot = jnp.sum(
                grad_head.astype(F32) * out_here[some, :].astype(F32), axis=0, keepdims=True
            )
            high, middle, low = three_parts(-row_dot)
            grad_aug[pl.ds(0, 64), :] = jnp.where(
                tail == 0, rows_of(high),
                jnp.where(tail == 1, rows_of(middle), jnp.where(tail == 2, rows_of(low), 0.0)),
            ).astype(BF16)
            grad_aug[pl.ds(64, 64), :] = grad_head
            width = strip.shape[1]
            strip[...] = pltpu.roll(
                jnp.broadcast_to(line[target, pl.ds(inside, 1), :], (LANES, width)), 0, 1,
                stride=1, stride_axis=0,
            )
            strip_grad[...] = jnp.zeros_like(strip_grad)
            query_and_grad = jnp.concatenate([q_head, grad_head], axis=0).T
            query_all = query_aug[...]
            grad_all = grad_aug[...]
            half = lane_ids((LANES, LANES)) < 64
            kv_lanes = pl.ds(pl.multiple_of(inside * LANES, LANES), LANES)
            for part_index in range(blocks):
                these = pl.ds(part_index * LANES, LANES)
                band = pl.ds((blocks - 1 - part_index) * LANES, rows)
                part = jnp.dot(key_aug[these, :], query_all, preferred_element_type=F32)
                part = jnp.exp(part + strip[:, band])
                slope = part * jnp.dot(value_aug[these, :], grad_all, preferred_element_type=F32)
                strip_grad[:, band] = strip_grad[:, band] + slope
                slope = slope.astype(BF16)
                probs_grad[these, :] = slope
                key_part = jnp.dot(slope, query_and_grad, preferred_element_type=F32)
                value_part = jnp.dot(part.astype(BF16), query_and_grad, preferred_element_type=F32)
                joined = jnp.where(half, key_part, value_part)
                kv_here[these, kv_lanes] = joined.astype(BF16)
                turned = joined.T.astype(BF16)
                dk_here[some, these] = turned[0:64]
                dv_here[some, these] = turned[64:128]
            query_part = jnp.dot(key_aug_t[...], probs_grad[...], preferred_element_type=F32)
            dq_here[some, :] = query_part[0:64].astype(BF16)
            bins = dot_f32(query_part[64:192].astype(BF16), key_extra_t[:, own_lanes], 1, 1)
            left = lane_ids((LANES, LANES)) < 64
            upper = row_ids((LANES, LANES)) < 64
            layout_grad[...] = jnp.where(left == upper, bins, 0.0)
            bin_sums[0, pl.ds(head, 1), :] = unskewed(layout_grad, 0, 64, 0)
            bin_sums[1, pl.ds(head, 1), :] = unskewed(layout_grad, 64, 64, 64)
            line_sums[pl.ds(head, 1), :] = unskewed(strip_grad, 0, LANES, 0)
            return inner_carry

        lax.fori_loop(0, heads_here, head_unit, 0)
        slot_grad[...] = slot_grad[...] + jnp.dot(
            kv_here[...], w_kv[...], preferred_element_type=F32
        )
        own_grad[...] = own_grad[...] + jnp.dot(
            dq_here[...].T, w_query[...], preferred_element_type=F32
        )

        @pl.when(block == mp_size - 1)
        def _():
            for k, copy in enumerate(row_copies):
                other = lax.rem(member + k + 1, group)
                rows_out[k] = slot_grad[pl.ds(pl.multiple_of(other * rows, 16), rows), :].astype(BF16)
                copy.start()

        full_here[slot, 0] = jnp.dot(
            dq_here[...], slot_owner[pl.ds(own_start, rows), :], preferred_element_type=F32
        ).astype(BF16)
        full_here[slot, 1] = jnp.dot(
            dk_here[...], slot_owner[...], preferred_element_type=F32
        ).astype(BF16)
        full_here[slot, 2] = jnp.dot(
            dv_here[...], slot_owner[...], preferred_element_type=F32
        ).astype(BF16)
        communicate(block, heads_here)
        return carry

    lax.fori_loop(0, mp_size, block_unit, 0)

    scatter.run("t6 f9")

    gain_rows = model_width // LANES
    head_count = bin_sums.shape[1]
    stage[0, 2 * gain_rows : 2 * gain_rows + head_count, :] = exact_dot(line_sums[...], line_hot[...])
    for i in range(2):
        start = 2 * gain_rows + (1 + i) * head_count
        stage[0, start : start + head_count, :] = exact_dot(bin_sums[i], bin_hot[...])
    for block in range(gain_rows):
        these = slice(block * LANES, (block + 1) * LANES)
        owner = block_owner(block)
        those = slice(owner * LANES, (owner + 1) * LANES)

        def gain_sum(i, total, these=these, those=those):
            here = pl.ds(pl.multiple_of(i * 64, 64), 64)
            product = slot_grad[here, these] * slot_owner[here, those].astype(F32)
            return total + jnp.sum(product.reshape(8, 8, LANES), axis=0)

        def own_sum(i, total, these=these, those=those):
            here = pl.ds(pl.multiple_of(i * 64, 64), 64)
            there = pl.ds(pl.multiple_of(own_start + i * 64, 64), 64)
            product = own_grad[here, these] * slot_owner[there, those].astype(F32)
            return total + jnp.sum(product.reshape(8, 8, LANES), axis=0)

        total = lax.fori_loop(0, keys // 64, gain_sum, jnp.zeros((8, LANES), F32))
        total = lax.fori_loop(0, rows // 64, own_sum, total)
        stage[0, block : block + 1, :] = (
            jnp.sum(total, axis=0, keepdims=True) / gains[0:1, these]
        )
        stage[0, gain_rows + block : gain_rows + block + 1, :] = gain_part[:, these]

    rounds = [[place.to_core], [place.to_x, place.to_y, place.to_corner]]
    rounds.append([place.to_mp(k) for k in range(1, mp_size)])
    at, sums = 0, []
    for i, partners in enumerate(rounds):
        sums.append(
            [
                remote(
                    stage.at[i], stage_in.at[at + j], stage_send.at[at + j], stage_recv.at[at + j], partner
                )
                for j, partner in enumerate(partners)
            ]
        )
        at += len(partners)
    def round_done(i):
        at = sum(len(partners) for partners in rounds[:i])
        value = stage[i]
        for j, copy in enumerate(sums[i]):
            copy.wait_recv()
            value = value + stage_in[at + j]
        return value

    for copy in sums[0]:
        copy.start()
    scatter.run("s7 s8")
    stage[1] = round_done(0)
    for copy in sums[1]:
        copy.start()
    scatter.run("t7 s9")
    for copy in row_copies:
        copy.wait_recv()

    def input_back(i, carry):
        here = pl.ds(pl.multiple_of(i * 16, 16), 16)
        grad = own_grad[here, :] + slot_grad[pl.ds(pl.multiple_of(own_start + i * 16, 16), 16), :]
        for k in range(group - 1):
            grad = grad + peers[k, here, :].astype(F32)
        values = layer_input[here, :]
        scale = lax.rsqrt(jnp.mean(values * values, axis=1, keepdims=True) + EPSILON)
        scaled = gains[0:1, :] * grad
        mean = jnp.mean(scaled * values, axis=1, keepdims=True)
        input_grad[here, :] = (
            residual_grad[here, :] + scale * scaled - values * (scale * scale * scale * mean)
        )
        return carry

    lax.fori_loop(0, rows // 16, input_back, 0)
    leave = Copy(input_grad, input_out, value_sem.at[0])
    leave.start()
    stage[2] = round_done(1)
    for copy in sums[2]:
        copy.start()
    scatter.run("t8 t9")
    scatter.run("e0 e1 e2")
    small_out[...] = round_done(2)
    sums = sum(sums, [])
    scatter.close()
    leave.wait()
    for copy in row_copies + sums:
        copy.wait_send()


def backward(
    mp_size, group, gate_up_full, down_full, w_first, queries, keys_t, values_t, heads_out,
    residual, second_grad, cotangent, lse, layout, line, key_extra, key_extra_t, slot_owner,
    layer_input, gains, line_hot, bin_hot, gate_up_share, down_share,
):
    rows, model_width = layer_input.shape
    keys = slot_owner.shape[0]
    width = line.shape[2]
    inner_here = queries.shape[0] // mp_size
    heads_here = inner_here // 64
    head_count = heads_here * mp_size
    hidden = down_full.shape[1] // mp_size
    sizes = [(2, hidden), (1, hidden), (4, inner_here)]
    count = 4 + mp_size - 1
    small_rows = 2 * model_width // LANES + 3 * head_count
    others = max(group - 1, 1)
    dma = pltpu.SemaphoreType.DMA
    hbm = pl.BlockSpec(memory_space=HBM)
    vmem = pl.BlockSpec(memory_space=pltpu.VMEM)
    shape = jax.ShapeDtypeStruct
    return pl.pallas_call(
        partial(backward_kernel, mp_size, group),
        out_shape=(
            shape((rows, model_width), F32),
            shape((small_rows, LANES), F32),
            *[shape((lead, n, LANES), F32) for lead, n in sizes],
        ),
        in_specs=[hbm] * 10 + [vmem] * 12,
        out_specs=(hbm,) + (vmem,) * 4,
        scratch_shapes=[
            pltpu.VMEM((rows, model_width), F32),
            pltpu.VMEM((keys, model_width), F32),
            pltpu.VMEM((rows, model_width), F32),
            pltpu.VMEM((rows, model_width), F32),
            pltpu.VMEM((rows, model_width), BF16),
            pltpu.VMEM((model_width, rows), BF16),
            pltpu.VMEM((inner_here, model_width), BF16),
            pltpu.VMEM((inner_here, model_width), BF16),
            pltpu.VMEM((2 * inner_here, model_width), BF16),
            pltpu.VMEM((inner_here, rows), BF16),
            pltpu.VMEM((inner_here, keys), BF16),
            pltpu.VMEM((inner_here, keys), BF16),
            pltpu.VMEM((inner_here, rows), BF16),
            pltpu.VMEM((inner_here, rows), BF16),
            pltpu.VMEM((inner_here, rows), BF16),
            pltpu.VMEM((inner_here, keys), BF16),
            pltpu.VMEM((inner_here, keys), BF16),
            pltpu.VMEM((keys, heads_here * LANES), BF16),
            pltpu.VMEM((keys, 256), BF16),
            pltpu.VMEM((192, keys), BF16),
            pltpu.VMEM((256, rows), BF16),
            pltpu.VMEM((keys, LANES), BF16),
            pltpu.VMEM((LANES, rows), BF16),
            pltpu.VMEM((LANES, width), F32),
            pltpu.VMEM((LANES, width), F32),
            pltpu.VMEM((keys, rows), BF16),
            pltpu.VMEM((LANES, LANES), F32),
            pltpu.VMEM((head_count, width), F32),
            pltpu.VMEM((2, head_count, LANES), F32),
            pltpu.VMEM((1, model_width), F32),
            pltpu.VMEM((others, rows, model_width), BF16),
            pltpu.VMEM((others, rows, model_width), BF16),
            pltpu.VMEM((3, small_rows, LANES), F32),
            pltpu.VMEM((count, small_rows, LANES), F32),
            pltpu.VMEM((2, 4, inner_here, model_width), BF16),
            dma((6 + 2 * heads_here,)), dma((3,)), dma((group,)), dma((group,)),
            dma((count,)), dma((count,)),
        ]
        + Scatter.scratch(sizes, (True, True, False), BACKWARD_ITEMS),
        compiler_params=pltpu.CompilerParams(
            collective_id=1, has_side_effects=True, vmem_limit_bytes=63 << 20
        ),
        name="backward",
    )(
        gate_up_full, down_full, w_first, queries, keys_t, values_t, heads_out, residual,
        second_grad, cotangent, lse, layout, line, key_extra, key_extra_t, slot_owner, layer_input,
        gains, line_hot, bin_hot, gate_up_share, down_share,
    )


def line_onehot(first_row, width, key_blocks):
    place = jnp.arange(width, dtype=jnp.int32)
    place = jnp.where(place >= width - LANES, place - width, place)
    offset = LANES * (key_blocks - 1) - place - first_row
    return (bucket_of(offset)[:, None] == jnp.arange(32, dtype=jnp.int32)[None, :]).astype(F32)


def bin_onehot():
    bins = np.arange(NBIN)
    offset = bins[:, None] - bins[None, :]
    distance = np.abs(offset)
    bucket = np.minimum(distance, 7) + sum((distance >= t).astype(np.int64) for t in THRESHOLDS)
    bucket = bucket + 16 * (offset > 0)
    return jnp.asarray(bucket[:, :, None] == np.arange(32), F32)


def gather_rows(local, axis_name):
    return lax.all_gather(local, axis_name, axis=0, tiled=True)


def scatter_grad(full):
    summed = lax.psum_scatter(full, "dp", scatter_dimension=1, tiled=True)
    return lax.psum_scatter(summed, "mp", scatter_dimension=0, tiled=True)


def per_device_plain(
    dp_size, mp_size,
    layer_input, norm_gains, query_weight, key_value_weight, output_weight,
    gate_up_weight, down_weight, bias_tables, doc_lengths, box_bins, cotangent,
):
    rows, model_width = layer_input.shape
    doc_count = doc_lengths.shape[0]
    slot_span = box_bins.shape[1] // doc_count
    group = mp_size // doc_count
    mp_index = lax.axis_index("mp")
    doc = mp_index // group
    first_row = (mp_index % group) * rows
    key_blocks = slot_span // LANES
    width = LANES * (key_blocks + (rows + LANES - 1) // LANES)
    groups = [[d * group + i for i in range(group)] for d in range(doc_count)]
    gain_first = norm_gains[0].astype(F32)
    gain_second = norm_gains[1].astype(F32)

    w_query = gather_rows(query_weight.T, "mp")
    inner_here = query_weight.shape[1]
    inner = inner_here * mp_size
    w_key = gather_rows(key_value_weight[:, 0].T, "mp")
    w_value = gather_rows(key_value_weight[:, 1].T, "mp")
    w_output = gather_rows(output_weight, "mp")
    w_gate = gather_rows(gate_up_weight[:, 0].T, "mp")
    w_up = gather_rows(gate_up_weight[:, 1].T, "mp")
    w_down = gather_rows(down_weight, "mp")
    tables = lax.all_gather(bias_tables, "mp", axis=2, tiled=True).astype(F32)
    head_count = tables.shape[2]

    onehot_line = line_onehot(first_row, width, key_blocks)
    line = jnp.dot(onehot_line, tables[0], precision=lax.Precision.HIGHEST)
    line = line.T.reshape(head_count, 1, width)
    onehot_bin = bin_onehot()
    x_part = jnp.einsum("ban,nh->hba", onehot_bin, tables[1], precision=lax.Precision.HIGHEST)
    y_part = jnp.einsum("ban,nh->hba", onehot_bin, tables[2], precision=lax.Precision.HIGHEST)
    empty = jnp.zeros_like(x_part)
    layout = jnp.concatenate(
        [jnp.concatenate([x_part, empty], axis=2), jnp.concatenate([empty, y_part], axis=2)], axis=1
    ).astype(BF16)
    key_bins = lax.dynamic_slice(box_bins, (0, doc * slot_span), (2, slot_span))
    own_bins = lax.dynamic_slice(key_bins, (0, first_row), (2, rows))
    bin_ids = jnp.arange(NBIN, dtype=jnp.int32)

    def placed_rows(bins):
        return jnp.concatenate(
            [bins[0][:, None] == bin_ids, bins[1][:, None] == bin_ids], axis=1
        ).astype(BF16)

    def placed_lanes(bins):
        return jnp.concatenate(
            [bin_ids[:, None] == bins[0][None], bin_ids[:, None] == bins[1][None]], axis=0
        ).astype(BF16)

    length = lax.dynamic_index_in_dim(doc_lengths, doc, keepdims=False)
    masked = jnp.arange(slot_span, dtype=jnp.int32)[:, None] >= length
    key_placed = placed_rows(key_bins)
    key_extra = jnp.concatenate(
        [
            jnp.zeros((slot_span, 64), BF16),
            key_placed,
            jnp.where(masked, NEG_FILL, 0.0).astype(BF16),
            jnp.ones((slot_span, 3), BF16),
            jnp.zeros((slot_span, 60), BF16),
        ],
        axis=1,
    )
    key_extra_t = placed_lanes(key_bins)
    query_bins_t = placed_rows(own_bins)
    query_bins = placed_lanes(own_bins)

    scale_first = inverse_rms(layer_input)
    normed = (layer_input * scale_first * gain_first).astype(BF16)
    slot_normed = lax.all_gather(normed, "mp", axis=0, tiled=True, axis_index_groups=groups)
    queries = dot_f32(w_query, normed, 1, 1).astype(BF16)
    keys_t = dot_f32(w_key, slot_normed, 1, 1).astype(BF16)
    values_t = dot_f32(w_value, slot_normed, 1, 1).astype(BF16)
    heads_out, lse = attend(queries, keys_t, values_t, layout, line, key_extra, query_bins)
    residual = layer_input + dot_f32(heads_out, w_output, 0, 0)
    scale_second = inverse_rms(residual)
    normed_second = (residual * scale_second * gain_second).astype(BF16)
    gate = dot_f32(normed_second, w_gate, 1, 1)
    up = dot_f32(normed_second, w_up, 1, 1)
    gelu_value, gelu_pull = jax.vjp(lambda v: jax.nn.gelu(v, approximate=True), gate)
    activated = (gelu_value * up).astype(BF16)
    layer_output = residual + dot_f32(activated, w_down, 1, 0)

    out_low = cotangent.astype(BF16)
    down_full = dot_f32(activated, out_low, 0, 0).astype(BF16)
    act_grad = dot_f32(out_low, w_down, 1, 1)
    gate_low = gelu_pull(act_grad * up)[0].astype(BF16)
    up_low = (act_grad * gelu_value).astype(BF16)
    gate_full = dot_f32(gate_low, normed_second, 0, 0).astype(BF16)
    up_full = dot_f32(up_low, normed_second, 0, 0).astype(BF16)
    second_grad = dot_f32(gate_low, w_gate, 1, 0) + dot_f32(up_low, w_up, 1, 0)
    gain_second_grad = jnp.sum(second_grad * residual * scale_second, axis=0)
    scaled = gain_second * second_grad
    residual_grad = (
        cotangent
        + scale_second * scaled
        - residual * scale_second**3 * jnp.mean(scaled * residual, axis=-1, keepdims=True)
    )

    branch_low = residual_grad.astype(BF16)
    output_full = dot_f32(heads_out, branch_low, 1, 0).astype(BF16)
    heads_grad = dot_f32(w_output, branch_low, 1, 1).astype(BF16)
    dq, dk, dv, line_grad, layout_grad = attend_back(
        queries, keys_t, values_t, heads_out, heads_grad, lse, layout, line,
        key_extra, key_extra_t, query_bins, query_bins_t,
    )
    query_full = dot_f32(dq, normed, 1, 0).astype(BF16)
    key_full = dot_f32(dk, slot_normed, 1, 0).astype(BF16)
    value_full = dot_f32(dv, slot_normed, 1, 0).astype(BF16)
    slot_grad = dot_f32(dk, w_key, 0, 0) + dot_f32(dv, w_value, 0, 0)
    first_grad = lax.psum_scatter(
        slot_grad.astype(BF16), "mp", scatter_dimension=0, tiled=True, axis_index_groups=groups
    ).astype(F32) + dot_f32(dq, w_query, 0, 0)
    gain_first_grad = jnp.sum(first_grad * layer_input * scale_first, axis=0)
    scaled = gain_first * first_grad
    input_grad = (
        residual_grad
        + scale_first * scaled
        - layer_input * scale_first**3 * jnp.mean(scaled * layer_input, axis=-1, keepdims=True)
    )

    gain_grad = lax.psum_scatter(
        jnp.stack([gain_first_grad, gain_second_grad]), ("dp", "mp"), scatter_dimension=1, tiled=True
    )
    line_part = jnp.dot(
        onehot_line.T, line_grad[:, 0].T, precision=lax.Precision.HIGHEST
    )
    x_part = jnp.einsum(
        "ban,hba->nh", onehot_bin, layout_grad[:, :64, :64], precision=lax.Precision.HIGHEST
    )
    y_part = jnp.einsum(
        "ban,hba->nh", onehot_bin, layout_grad[:, 64:, 64:], precision=lax.Precision.HIGHEST
    )
    table_full = jnp.stack([line_part, x_part, y_part])
    table_grad = lax.psum_scatter(
        lax.psum_scatter(table_full, "mp", scatter_dimension=2, tiled=True),
        "dp", scatter_dimension=1, tiled=True,
    )

    query_grad = scatter_grad(query_full).T.astype(F32)
    key_value_grad = jnp.stack(
        [scatter_grad(key_full).T, scatter_grad(value_full).T], axis=1
    ).astype(F32)
    output_grad = scatter_grad(output_full).astype(F32)
    gate_up_grad = jnp.stack(
        [scatter_grad(gate_full).T, scatter_grad(up_full).T], axis=1
    ).astype(F32)
    down_grad = scatter_grad(down_full).astype(F32)
    return (
        layer_output, input_grad, gain_grad, query_grad, key_value_grad,
        output_grad, gate_up_grad, down_grad, table_grad,
    )


def per_device_linked(
    dp_size, mp_size,
    layer_input, norm_gains, query_weight, key_value_weight, output_weight,
    gate_up_weight, down_weight, bias_tables, doc_lengths, box_bins, cotangent,
):
    rows, model_width = layer_input.shape
    doc_count = doc_lengths.shape[0]
    group = mp_size // doc_count
    dp_index, mp_index = lax.axis_index("dp"), lax.axis_index("mp")
    heads_here = bias_tables.shape[2]
    head_count = heads_here * mp_size
    inner_here = query_weight.shape[1]
    gains = norm_gains.astype(F32)
    column = ((dp_index % 2) * 4 + dp_index // 2) * LANES
    key_value = lax.dynamic_slice_in_dim(key_value_weight, column, LANES, 0)
    table = jnp.swapaxes(bias_tables.astype(F32), 1, 2)
    table = jnp.pad(table, ((0, 0), (0, 8 - heads_here), (0, LANES - 32))).reshape(24, LANES)
    (
        w_first, queries, keys_t, values_t, heads_out, lse, layout, line, key_extra, key_extra_t,
        slot_owner, residual, layer_output, second_grad, gate_up_full, down_full, _, line_hot, bin_hot,
        gate_up_share, down_share,
    ) = forward(
        mp_size, group, query_weight, output_weight, jnp.transpose(gate_up_weight, (1, 2, 0)),
        down_weight[None], key_value.reshape(LANES, 2 * inner_here), table, box_bins, doc_lengths,
        layer_input, gains, cotangent,
    )
    input_grad, small, gate_up_sum, down_sum, summed = backward(
        mp_size, group, gate_up_full, down_full, w_first, queries, keys_t, values_t, heads_out,
        residual, second_grad, cotangent, lse, layout, line, key_extra, key_extra_t, slot_owner,
        layer_input, gains, line_hot, bin_hot, gate_up_share, down_share,
    )
    gain_rows = model_width // LANES
    gains = small[: 2 * gain_rows].reshape(2, model_width)
    share = model_width // (dp_size * mp_size)
    at = (dp_index * mp_size + mp_index) * share
    gain_grad = lax.dynamic_slice(gains, (0, at), (2, share))
    tables = small[2 * gain_rows :].reshape(3, head_count, LANES)
    table_grad = lax.dynamic_slice(
        tables,
        (0, mp_index * heads_here, dp_index * (32 // dp_size)),
        (3, heads_here, 32 // dp_size),
    )
    table_grad = jnp.swapaxes(table_grad, 1, 2)
    query_grad = summed[0].T
    key_value_grad = jnp.transpose(summed[1:3], (2, 0, 1))
    gate_up_grad = jnp.transpose(gate_up_sum, (2, 0, 1))
    return (
        layer_output, input_grad, gain_grad, query_grad, key_value_grad,
        summed[3], gate_up_grad, down_sum[0], table_grad,
    )


def per_device(dp_size, mp_size, *args):
    rows, model_width = args[0].shape
    heads_here = args[7].shape[2]
    fits = dp_size == 8 and model_width == 8 * LANES and mp_size == 4
    fits = fits and heads_here == 4 and rows % LANES == 0
    body = per_device_linked if fits else per_device_plain
    return body(dp_size, mp_size, *args)


def solution(mesh):
    return jax.shard_map(
        partial(per_device, mesh.shape["dp"], mesh.shape["mp"]),
        mesh=mesh,
        in_specs=(
            P(("dp", "mp"), None),
            P(),
            P(None, "mp"),
            P(None, None, "mp"),
            P("mp", None),
            P(None, None, "mp"),
            P("mp", None),
            P(None, None, "mp"),
            P("dp"),
            P(None, "dp"),
            P(("dp", "mp"), None),
        ),
        out_specs=(
            P(("dp", "mp"), None),
            P(("dp", "mp"), None),
            P(None, ("dp", "mp")),
            P("dp", "mp"),
            P("dp", None, "mp"),
            P("mp", "dp"),
            P("dp", None, "mp"),
            P("mp", "dp"),
            P(None, "dp", "mp"),
        ),
        check_vma=False,
    )
```

```python
from functools import partial

import jax
import jax.numpy as jnp
import numpy as np
from jax import lax
from jax.experimental import pallas as pl
from jax.experimental.pallas import tpu as pltpu
from jax.sharding import PartitionSpec as P

NBIN = 64
EPSILON = 1e-06
THRESHOLDS = (8, 12, 16, 23, 32, 46, 64, 91)
NEG_FILL = -1e30
LANES = 128
MESH = pl.DeviceIdType.MESH
HBM = pltpu.MemorySpace.HBM
BF16 = jnp.bfloat16
F32 = jnp.float32


def bucket_of(relative):
    distance = jnp.abs(relative)
    bucket = jnp.minimum(distance, 7)
    for threshold in THRESHOLDS:
        bucket = bucket + (distance >= threshold).astype(jnp.int32)
    return bucket + 16 * (relative > 0).astype(jnp.int32)


def inverse_rms(values):
    return lax.rsqrt(jnp.mean(values * values, axis=-1, keepdims=True) + EPSILON)


def dot_f32(left, right, left_dim, right_dim):
    return lax.dot_general(
        left, right, (((left_dim,), (right_dim,)), ((), ())), preferred_element_type=F32
    )


def three_parts(values):
    high = values.astype(BF16)
    rest = values - high.astype(F32)
    middle = rest.astype(BF16)
    low = (rest - middle.astype(F32)).astype(BF16)
    return high, middle, low


def lane_ids(shape):
    return lax.broadcasted_iota(jnp.int32, shape, 1)


def row_ids(shape):
    return lax.broadcasted_iota(jnp.int32, shape, 0)


def attend_kernel(
    q_ref, k_ref, v_ref, layout_ref, line_ref, key_extra_ref, query_bins_ref,
    out_ref, lse_ref,
    key_aug, query_aug, strip, scores, probs,
):
    head_size, rows = q_ref.shape
    keys = k_ref.shape[1]
    blocks = keys // LANES
    width = strip.shape[1]

    @pl.when(pl.program_id(0) == 0)
    def _():
        key_aug[...] = key_extra_ref[...]
        tail = row_ids((64, rows))
        query_aug[pl.ds(192, 64), :] = jnp.where(tail == 0, 1.0, 0.0).astype(BF16)

    both = jnp.concatenate([k_ref[...], v_ref[...]], axis=0).T
    low_lanes = lane_ids((keys, LANES)) < head_size
    key_aug[:, 0:LANES] = jnp.where(low_lanes, both, key_extra_ref[:, 0:LANES])
    query_aug[pl.ds(0, 64), :] = q_ref[...]
    query_aug[pl.ds(64, 128), :] = jnp.dot(
        layout_ref[0], query_bins_ref[...], preferred_element_type=F32
    ).astype(BF16)
    strip[...] = pltpu.roll(
        jnp.broadcast_to(line_ref[0], (LANES, width)), 0, 1, stride=1, stride_axis=0
    )
    query_all = query_aug[...]
    top = jnp.full((1, rows), -jnp.inf, F32)
    for block in range(blocks):
        here = pl.ds(block * LANES, LANES)
        part = jnp.dot(key_aug[here, :], query_all, preferred_element_type=F32)
        part = part + strip[:, pl.ds((blocks - 1 - block) * LANES, rows)]
        scores[here, :] = part
        top = jnp.maximum(top, jnp.max(part, axis=0, keepdims=True))
    total = jnp.zeros((1, rows), F32)
    for block in range(blocks):
        here = pl.ds(block * LANES, LANES)
        part = jnp.exp(scores[here, :] - top)
        total = total + jnp.sum(part, axis=0, keepdims=True)
        probs[here, :] = part.astype(BF16)
    mixed = jnp.dot(v_ref[...], probs[...], preferred_element_type=F32)
    out_ref[...] = (mixed / total).astype(BF16)
    lse_ref[0] = top + jnp.log(total)


def attend_back_kernel(
    q_ref, k_ref, v_ref, out_ref, out_grad_ref, lse_ref, layout_ref, line_ref,
    key_extra_ref, key_extra_t_ref, query_bins_ref, query_bins_t_ref,
    dq_ref, dk_ref, dv_ref, line_grad_ref, layout_grad_ref,
    key_aug, key_aug_t, query_aug, value_aug, grad_aug, strip, strip_grad, probs_grad,
):
    head_size, rows = q_ref.shape
    keys = k_ref.shape[1]
    blocks = keys // LANES
    width = strip.shape[1]

    @pl.when(pl.program_id(0) == 0)
    def _():
        key_aug[...] = key_extra_ref[...]
        key_aug_t[pl.ds(64, 128), :] = key_extra_t_ref[...]
        tail = row_ids((64, rows))
        query_aug[pl.ds(192, 64), :] = jnp.where(tail == 0, 1.0, 0.0).astype(BF16)

    both = jnp.concatenate([k_ref[...], v_ref[...]], axis=0).T
    lanes = lane_ids((keys, LANES))
    key_aug[:, 0:LANES] = jnp.where(lanes < head_size, both, key_extra_ref[:, 0:LANES])
    ones = jnp.where(lanes < 3, 1.0, 0.0).astype(BF16)
    value_aug[...] = jnp.where(lanes < head_size, ones, both)
    key_aug_t[pl.ds(0, 64), :] = k_ref[...]
    query_aug[pl.ds(0, 64), :] = q_ref[...]
    query_aug[pl.ds(64, 128), :] = jnp.dot(
        layout_ref[0], query_bins_ref[...], preferred_element_type=F32
    ).astype(BF16)
    high, middle, low = three_parts(-lse_ref[0])
    tail = row_ids((64, rows))
    rows_of = lambda part: jnp.broadcast_to(part.astype(F32), (64, rows))
    query_aug[pl.ds(192, 64), :] = jnp.where(
        tail == 0, 1.0,
        jnp.where(
            tail == 1, rows_of(high),
            jnp.where(tail == 2, rows_of(middle), jnp.where(tail == 3, rows_of(low), 0.0)),
        ),
    ).astype(BF16)
    row_dot = jnp.sum(
        out_grad_ref[...].astype(F32) * out_ref[...].astype(F32), axis=0, keepdims=True
    )
    high, middle, low = three_parts(-row_dot)
    grad_aug[pl.ds(0, 64), :] = jnp.where(
        tail == 0, rows_of(high),
        jnp.where(tail == 1, rows_of(middle), jnp.where(tail == 2, rows_of(low), 0.0)),
    ).astype(BF16)
    grad_aug[pl.ds(64, 64), :] = out_grad_ref[...]
    strip[...] = pltpu.roll(
        jnp.broadcast_to(line_ref[0], (LANES, width)), 0, 1, stride=1, stride_axis=0
    )
    strip_grad[...] = jnp.zeros_like(strip_grad)
    query_and_grad = jnp.concatenate([q_ref[...], out_grad_ref[...]], axis=0).T
    query_all = query_aug[...]
    grad_all = grad_aug[...]
    half = lane_ids((LANES, LANES)) < head_size
    for block in range(blocks):
        here = pl.ds(block * LANES, LANES)
        band = pl.ds((blocks - 1 - block) * LANES, rows)
        part = jnp.dot(key_aug[here, :], query_all, preferred_element_type=F32)
        part = jnp.exp(part + strip[:, band])
        slope = part * jnp.dot(value_aug[here, :], grad_all, preferred_element_type=F32)
        strip_grad[:, band] = strip_grad[:, band] + slope
        slope = slope.astype(BF16)
        probs_grad[here, :] = slope
        key_part = jnp.dot(slope, query_and_grad, preferred_element_type=F32)
        value_part = jnp.dot(part.astype(BF16), query_and_grad, preferred_element_type=F32)
        turned = jnp.where(half, key_part, value_part).T.astype(BF16)
        dk_ref[:, here] = turned[0:64]
        dv_ref[:, here] = turned[64:128]
    query_part = jnp.dot(key_aug_t[...], probs_grad[...], preferred_element_type=F32)
    dq_ref[...] = query_part[0:64].astype(BF16)
    layout_grad_ref[0] = jnp.dot(
        query_part[64:192].astype(BF16), query_bins_t_ref[...], preferred_element_type=F32
    )
    folded = strip_grad[pl.ds(0, 8), :]
    for group in range(1, LANES // 8):
        folded = folded + pltpu.roll(strip_grad[pl.ds(group * 8, 8), :], width - group * 8, 1)
    line = folded[0:1]
    for row in range(1, 8):
        line = line + pltpu.roll(folded[row : row + 1], width - row, 1)
    line_grad_ref[0] = line


class Place:
    def __init__(self, mp_size):
        self.dp = lax.axis_index("dp")
        self.mp = lax.axis_index("mp")
        self.mp_size = mp_size
        self.core = lax.rem(self.dp, 2)
        self.x = lax.rem(lax.div(self.dp, 2), 2)
        self.y = lax.div(self.dp, 4)
        self.to_core = (self.dp + 1 - 2 * self.core, self.mp)
        self.to_x = (self.dp + 2 - 4 * self.x, self.mp)
        self.to_y = (self.dp + 4 - 8 * self.y, self.mp)
        self.to_corner = (self.dp + 6 - 4 * self.x - 8 * self.y, self.mp)

    def across(self, step):
        low = lax.rem(lax.rem(self.mp, 2) + step % 2, 2)
        high = lax.rem(lax.div(self.mp, 2) + step // 2, 2)
        return low + 2 * high

    def to_mp(self, step):
        return (self.dp, self.across(step))

    def partners(self):
        others = [self.to_mp(step) for step in range(1, self.mp_size)]
        return [self.to_core, self.to_x, self.to_y, self.to_corner] + others


def greet(place):
    barrier = pltpu.get_barrier_semaphore()
    for partner in place.partners():
        pl.semaphore_signal(barrier, inc=1, device_id=partner, device_id_type=MESH)


def meet(place):
    pl.semaphore_wait(pltpu.get_barrier_semaphore(), len(place.partners()))


class Copy:
    def __init__(self, source, target, send, receive=None, partner=None):
        self.parts = (source, target, send, receive, partner)

    def made(self):
        source, target, send, receive, partner = self.parts
        if partner is None:
            return pltpu.make_async_copy(source, target, send)
        return pltpu.make_async_remote_copy(
            src_ref=source, dst_ref=target, send_sem=send, recv_sem=receive,
            device_id=partner, device_id_type=MESH,
        )

    def start(self):
        self.made().start()

    def wait(self):
        self.made().wait()

    def wait_send(self):
        self.made().wait_send()

    def wait_recv(self):
        self.made().wait_recv()


def remote(source, target, send, receive, partner):
    return Copy(source, target, send, receive, partner)


def lanes_at(block, count):
    return pl.ds(pl.multiple_of(block * LANES, LANES), count * LANES)


class Gather:
    def __init__(self, place, pieces, outs, sems, items):
        self.place, self.pieces, self.outs = place, pieces, outs
        self.z_send, self.z_recv, self.own_sem, self.send, self.recv = sems
        self.items = items

    @staticmethod
    def semaphores(count, mp_size):
        dma = pltpu.SemaphoreType.DMA
        items = count * mp_size
        return [
            dma((count, mp_size)), dma((count, mp_size)), dma((count,)), dma((items, 6)), dma((items, 6))
        ]

    def rows(self, c, source, half):
        n = self.pieces[c].shape[1]
        if half is None:
            return pl.ds(pl.multiple_of(source * n, 16), n)
        return pl.ds(pl.multiple_of(source * n + half * (n // 2), 16), n // 2)

    def window(self, c, source, half, block, count):
        return self.outs[c].at[:, self.rows(c, source, half), lanes_at(block, count)]

    def own(self, c):
        place = self.place
        block = place.core * 4 + place.y * 2 + place.x
        return Copy(
            self.pieces[c], self.window(c, place.mp, None, block, 1), self.own_sem.at[c]
        )

    def along_mp(self, c, step):
        place = self.place
        block = place.core * 4 + place.y * 2 + place.x
        source = place.across(2) if step == 3 else place.mp
        window = self.window(c, source, None, block, 1)
        return remote(
            window if step == 3 else self.pieces[c], window,
            self.z_send.at[c, step], self.z_recv.at[c, step], place.to_mp(2 if step == 2 else 1),
        )

    def copies(self, t):
        c, k = self.items[t]
        place = self.place
        source = place.across(k)
        base = place.core * 4
        mine = base + place.y * 2 + place.x
        turned = base + (1 - place.y) * 2 + place.x

        def copy(i, half, block, count, partner):
            here = self.window(c, source, half, block, count)
            return remote(here, here, self.send.at[t, i], self.recv.at[t, i], partner)

        first = [copy(0, 0, mine, 1, place.to_x), copy(1, 1, mine, 1, place.to_y)]
        second = [
            copy(2, 0, base + place.y * 2, 2, place.to_y),
            copy(3, 1, mine, 1, place.to_x),
            copy(4, 1, turned, 1, place.to_x),
        ]
        third = [copy(5, None, base, 4, place.to_core)]
        return first, second, third

    def first(self, t):
        c, k = self.items[t]
        if k == 0:
            self.own(c).wait()
        else:
            self.along_mp(c, k).wait_recv()
        if k == 2:
            self.along_mp(c, 3).start()
        for copy in self.copies(t)[0]:
            copy.start()

    def second(self, t):
        first, second, _ = self.copies(t)
        for copy in first:
            copy.wait_recv()
        for copy in second:
            copy.start()

    def third(self, t):
        _, second, third = self.copies(t)
        for copy in second:
            copy.wait_recv()
        third[0].start()

    def run(self, ops):
        for op in ops.split():
            which, t = op[0], int(op[1:])
            if which == "z":
                self.along_mp(*self.items[t]).start()
            else:
                {"f": self.first, "s": self.second, "t": self.third}[which](t)

    def done(self, t):
        self.copies(t)[2][0].wait_recv()

    def close(self):
        for t, (c, k) in enumerate(self.items):
            first, second, third = self.copies(t)
            for copy in first + second + third:
                copy.wait_send()
            if k > 0:
                self.along_mp(c, k).wait_send()


def add_rows(target, target_index, source, source_index):
    lead, rows, lanes = target_index
    source_rows, source_lanes = source_index
    row_start, count = rows
    source_start = source_rows
    size = 32
    while count % size:
        size //= 2

    def body(i, carry):
        here = pl.ds(pl.multiple_of(row_start + i * size, size), size)
        there = pl.ds(pl.multiple_of(source_start + i * size, size), size)
        for part in range(lead):
            target[part, here, lanes] = target[part, here, lanes] + source[part, there, source_lanes]
        return carry

    lax.fori_loop(0, count // size, body, 0)


class Scatter:
    def __init__(self, place, fulls, outs, scratch, items, shares=None, inside=False):
        self.inside = inside
        self.place, self.fulls, self.outs, self.items = place, fulls, outs, items
        count = len(fulls)
        self.shares = shares or [None] * count
        self.held = [sorted(k for c, k in items if c == which) for which in range(count)]
        self.whole = [len(full.shape) == 3 for full in fulls]
        buffers = [scratch[i * count : (i + 1) * count] for i in range(5)]
        self.sums, self.from_first, self.from_second, self.from_mp, self.staged = buffers
        self.own_sem, self.send, self.recv, self.share_send, self.share_recv = scratch[5 * count :]

    @staticmethod
    def scratch(shapes, whole, items):
        out = []
        for part, blocks in enumerate((4, 2, 1, 1)):
            for c, (lead, n) in enumerate(shapes):
                slots = sum(which == c for which, _ in items)
                if part == 3:
                    slots, lead, n = (3, lead, n) if slots > 1 else (1, 1, 16)
                out.append(pltpu.VMEM((slots, lead, n, blocks * LANES), BF16))
        for (lead, n), is_whole in zip(shapes, whole):
            out.append(pltpu.VMEM((lead, n, 4 * LANES) if is_whole else (1, 16, LANES), BF16))
        dma = pltpu.SemaphoreType.DMA
        count = len(items)
        out += [dma((count,)), dma((count, 7)), dma((count, 7))]
        return out + [dma((len(shapes),)), dma((len(shapes),))]

    def slot(self, c, k):
        return self.held[c].index(k)

    def size(self, c):
        return self.sums[c].shape[1], self.sums[c].shape[2]

    def source(self, t):
        c, k = self.items[t]
        if not self.whole[c]:
            return self.fulls[c].at[(k + 1) % 2]
        lead, n = self.size(c)
        target = self.place.across(k)
        return self.fulls[c].at[:, pl.ds(pl.multiple_of(target * n, 16), n), :]

    def from_core(self, t):
        c, k = self.items[t]
        place = self.place
        return remote(
            self.source(t).at[:, :, lanes_at((1 - place.core) * 4, 4)], self.sums[c].at[self.slot(c, k)],
            self.send.at[t, 0], self.recv.at[t, 0], place.to_core,
        )

    def own(self, t):
        c, _ = self.items[t]
        return Copy(
            self.source(t).at[:, :, lanes_at(self.place.core * 4, 4)], self.staged[c], self.own_sem.at[t]
        )

    def copies(self, t):
        c, k = self.items[t]
        place = self.place
        lead, n = self.size(c)
        top, bottom = pl.ds(0, n // 2), pl.ds(n // 2, n // 2)
        every = pl.ds(0, lead)
        sums = self.sums[c].at[self.slot(c, k)]

        def copy(i, source, landing, partner):
            return remote(source, landing, self.send.at[t, i], self.recv.at[t, i], partner)

        landing = self.from_first[c].at[self.slot(c, k)]
        first = [
            copy(
                1, sums.at[every, top, lanes_at((1 - place.y) * 2, 2)],
                landing.at[every, top, pl.ds(0, 256)], place.to_y,
            ),
            copy(
                2, sums.at[every, bottom, lanes_at(1 - place.x, 1)],
                landing.at[every, bottom, pl.ds(0, 128)], place.to_x,
            ),
            copy(
                3, sums.at[every, bottom, lanes_at(3 - place.x, 1)],
                landing.at[every, bottom, pl.ds(128, 128)], place.to_x,
            ),
        ]
        landing = self.from_second[c].at[self.slot(c, k)]
        second = [
            copy(
                4, sums.at[every, top, lanes_at(place.y * 2 + 1 - place.x, 1)],
                landing.at[every, top, pl.ds(0, 128)], place.to_x,
            ),
            copy(
                5, sums.at[every, bottom, lanes_at((1 - place.y) * 2 + place.x, 1)],
                landing.at[every, bottom, pl.ds(0, 128)], place.to_y,
            ),
        ]
        third = None
        if k > 0:
            third = copy(
                6, sums.at[:, :, lanes_at(place.y * 2 + place.x, 1)], self.from_mp[c].at[k - 1],
                place.to_mp(1 if k % 2 else 2),
            )
        return first, second, third

    def core(self, t):
        self.from_core(t).start()
        if self.whole[self.items[t][0]]:
            self.own(t).start()

    def first(self, t):
        c, k = self.items[t]
        lead, n = self.size(c)
        sums = self.sums[c].at[self.slot(c, k)]
        self.from_core(t).wait_recv()
        if self.whole[c]:
            self.own(t).wait()
            add_rows(sums, (lead, (0, n), pl.ds(0, 512)), self.staged[c], (0, pl.ds(0, 512)))
        else:
            mine = lanes_at(self.place.core * 4, 4)
            add_rows(sums, (lead, (0, n), pl.ds(0, 512)), self.source(t), (0, mine))
        for copy in self.copies(t)[0]:
            copy.start()

    def second(self, t):
        c, k = self.items[t]
        place = self.place
        lead, n = self.size(c)
        first, second, _ = self.copies(t)
        for copy in first:
            copy.wait_recv()
        slot = self.slot(c, k)
        sums, landing = self.sums[c].at[slot], self.from_first[c].at[slot]
        half = n // 2
        add_rows(sums, (lead, (0, half), lanes_at(place.y * 2, 2)), landing, (0, pl.ds(0, 256)))
        add_rows(sums, (lead, (half, half), lanes_at(place.x, 1)), landing, (half, pl.ds(0, 128)))
        add_rows(sums, (lead, (half, half), lanes_at(2 + place.x, 1)), landing, (half, pl.ds(128, 128)))
        for copy in second:
            copy.start()

    def third(self, t):
        c, k = self.items[t]
        lead, n = self.size(c)
        _, second, third = self.copies(t)
        for copy in second:
            copy.wait_recv()
        slot = self.slot(c, k)
        mine = lanes_at(self.place.y * 2 + self.place.x, 1)
        add_rows(
            self.sums[c].at[slot], (lead, (0, n), mine), self.from_second[c].at[slot], (0, pl.ds(0, 128))
        )
        if k == 2:
            self.copies(self.items.index((c, 3)))[2].wait_recv()
            add_rows(
                self.sums[c].at[slot], (lead, (0, n), mine), self.from_mp[c].at[2], (0, pl.ds(0, 128))
            )
        if k > 0 and not self.inside:
            third.start()

    def share(self, c):
        return remote(
            self.shares[c], self.from_mp[c].at[0], self.share_send.at[c], self.share_recv.at[c],
            self.place.to_mp(1),
        )

    def end(self, c):
        if self.inside:
            self.finish(c)
            return
        if self.shares[c] is not None:
            self.share(c).wait_recv()
        for k in (1, 2):
            if (c, k) in self.items:
                self.copies(self.items.index((c, k)))[2].wait_recv()
        self.finish(c)

    def run(self, ops):
        for op in ops.split():
            table = {"c": self.core, "f": self.first, "s": self.second, "t": self.third, "e": self.end}
            table[op[0]](int(op[1:]))

    def left(self, t):
        self.from_core(t).wait_send()

    def close(self):
        for t, (c, k) in enumerate(self.items):
            first, second, third = self.copies(t)
            if self.whole[c] or k < 2:
                self.from_core(t).wait_send()
            for copy in first + second:
                copy.wait_send()
            if third is not None and not self.inside:
                third.wait_send()
        for c, share in enumerate(self.shares):
            if share is not None:
                self.share(c).wait_send()

    def finish(self, c):
        place = self.place
        lead, n = self.size(c)
        mine = lanes_at(place.y * 2 + place.x, 1)
        sums, landing, out = self.sums[c], self.from_mp[c], self.outs[c]
        steps = () if self.inside else (1, 2)
        slot = self.slot(c, 1 if self.inside else 0)
        size = 32
        while n % size:
            size //= 2

        def body(i, carry):
            here = pl.ds(pl.multiple_of(i * size, size), size)
            for part in range(lead):
                total = sums[slot, part, here, mine].astype(F32)
                for k in steps:
                    total = total + landing[k - 1, part, here, :].astype(F32)
                out[part, here, :] = total.astype(out.dtype)
            return carry

        lax.fori_loop(0, n // size, body, 0)


def attention_shapes(head_count, head_size, rows, keys, width):
    whole = lambda shape: pl.BlockSpec(shape, lambda head: (0,) * len(shape))
    column = lambda size: pl.BlockSpec((head_size, size), lambda head: (head, 0))
    page = lambda a, b: pl.BlockSpec((1, a, b), lambda head: (head, 0, 0))
    return whole, column, page


def attend(queries, keys_t, values_t, layout, line, key_extra, query_bins):
    inner, rows = queries.shape
    keys = keys_t.shape[1]
    head_count, _, width = line.shape
    head_size = inner // head_count
    whole, column, page = attention_shapes(head_count, head_size, rows, keys, width)
    return pl.pallas_call(
        attend_kernel,
        grid=(head_count,),
        out_shape=(
            jax.ShapeDtypeStruct((inner, rows), BF16),
            jax.ShapeDtypeStruct((head_count, 1, rows), F32),
        ),
        in_specs=[
            column(rows), column(keys), column(keys), page(128, 128), page(1, width),
            whole((keys, 256)), whole((128, rows)),
        ],
        out_specs=(column(rows), page(1, rows)),
        scratch_shapes=[
            pltpu.VMEM((keys, 256), BF16),
            pltpu.VMEM((256, rows), BF16),
            pltpu.VMEM((LANES, width), F32),
            pltpu.VMEM((keys, rows), F32),
            pltpu.VMEM((keys, rows), BF16),
        ],
        compiler_params=pltpu.CompilerParams(
            dimension_semantics=("arbitrary",), vmem_limit_bytes=32 << 20
        ),
        name="attend",
    )(queries, keys_t, values_t, layout, line, key_extra, query_bins)


def attend_back(
    queries, keys_t, values_t, heads_out, heads_grad, lse, layout, line,
    key_extra, key_extra_t, query_bins, query_bins_t,
):
    inner, rows = queries.shape
    keys = keys_t.shape[1]
    head_count, _, width = line.shape
    head_size = inner // head_count
    whole, column, page = attention_shapes(head_count, head_size, rows, keys, width)
    return pl.pallas_call(
        attend_back_kernel,
        grid=(head_count,),
        out_shape=(
            jax.ShapeDtypeStruct((inner, rows), BF16),
            jax.ShapeDtypeStruct((inner, keys), BF16),
            jax.ShapeDtypeStruct((inner, keys), BF16),
            jax.ShapeDtypeStruct((head_count, 1, width), F32),
            jax.ShapeDtypeStruct((head_count, 128, 128), F32),
        ),
        in_specs=[
            column(rows), column(keys), column(keys), column(rows), column(rows),
            page(1, rows), page(128, 128), page(1, width),
            whole((keys, 256)), whole((128, keys)), whole((128, rows)), whole((rows, 128)),
        ],
        out_specs=(column(rows), column(keys), column(keys), page(1, width), page(128, 128)),
        scratch_shapes=[
            pltpu.VMEM((keys, 256), BF16),
            pltpu.VMEM((192, keys), BF16),
            pltpu.VMEM((256, rows), BF16),
            pltpu.VMEM((keys, 128), BF16),
            pltpu.VMEM((128, rows), BF16),
            pltpu.VMEM((LANES, width), F32),
            pltpu.VMEM((LANES, width), F32),
            pltpu.VMEM((keys, rows), BF16),
        ],
        compiler_params=pltpu.CompilerParams(
            dimension_semantics=("arbitrary",), vmem_limit_bytes=32 << 20
        ),
        name="attend_back",
    )(
        queries, keys_t, values_t, heads_out, heads_grad, lse, layout, line,
        key_extra, key_extra_t, query_bins, query_bins_t,
    )


FORWARD_ITEMS = [(0, 0), (1, 0), (2, 0), (0, 1), (0, 2), (0, 3), (1, 1), (2, 1), (1, 2), (2, 2), (1, 3), (2, 3)]


FORWARD_SUMS = [(0, 1), (1, 1)]


def forward_kernel(
    mp_size, group,
    query_ref, output_ref, gate_up_ref, down_ref, key_value_ref, table_ref, boxes_ref, lengths_ref,
    input_ref, gain_ref, cotangent_ref,
    w_first, queries_out, keys_out, values_out, heads_out_out, lse, layout, line, key_extra, key_extra_t,
    slot_owner_out, residual_out, layer_output, second_grad, gate_up_full, down_full, tables,
    line_hot, bin_hot, gate_up_share, down_share, queries, keys_t, values_t, heads_out, slot_owner, residual,
    first_ref, query_piece, normed_t, slot_t, w_gate_up, w_down, first_here, key_aug, query_aug, strip, scores, probs,
    second_t, second_owner, out_owner, out_t,
    hidden_a, hidden_b, hidden_c, act_t, low_t, stage_gate_up, stage_down,
    row_send, row_recv, row_own, table_send, table_recv, table_own, load_sem, store_sem, keep_sem, *sems,
):
    place = Place(mp_size)
    rows, model_width = input_ref.shape
    keys = keys_t.shape[1]
    blocks = keys // LANES
    width = strip.shape[1]
    inner_here = first_ref.shape[1]
    heads_here = inner_here // 64
    hidden = gate_up_ref.shape[1]
    doc = lax.div(place.mp, group)
    member = lax.rem(place.mp, group)
    first_peer = place.mp - member
    own_lanes = pl.ds(pl.multiple_of(member * rows, LANES), rows)

    items = FORWARD_ITEMS
    column = lanes_at(place.core * 4 + place.y * 2 + place.x, 1)
    gather = Gather(
        place, [first_ref, gate_up_ref.at[:, :, column], down_ref.at[:, :, column]],
        [w_first, w_gate_up, w_down], sems[:5], items
    )
    at = {item: t for t, item in enumerate(items)}

    row_copies = [
        remote(
            normed_t, slot_t.at[:, own_lanes], row_send.at[k], row_recv.at[k],
            (place.dp, first_peer + lax.rem(member + k, group)),
        )
        for k in range(1, group)
    ]
    table_copies = [
        remote(table_ref, tables.at[place.mp], table_send.at[k], table_recv.at[k], place.to_mp(k))
        for k in range(1, mp_size)
    ]
    row_here = Copy(normed_t, slot_t.at[:, own_lanes], row_own.at[0])
    table_here = Copy(table_ref, tables.at[place.mp], table_own.at[0])

    greet(place)
    loads = [
        Copy(query_ref.at[column, :], query_piece, load_sem.at[0]),
        Copy(output_ref.at[:, column], first_ref.at[3], load_sem.at[1]),
    ]
    for copy in loads:
        copy.start()
    for c in range(1, 3):
        gather.own(c).start()
    table_here.start()
    turned = key_value_ref[...].T
    first_ref[1] = turned[0:inner_here]
    first_ref[2] = turned[inner_here : 2 * inner_here]

    def norm_into(values_ref, gain):
        def body(i, carry):
            here = pl.ds(pl.multiple_of(i * 16, 16), 16)
            values = values_ref[here, :]
            scale = lax.rsqrt(jnp.mean(values * values, axis=1, keepdims=True) + EPSILON)
            second_owner[here, :] = (values * scale * gain).astype(BF16)
            return carry

        lax.fori_loop(0, rows // 16, body, 0)

    norm_into(input_ref, gain_ref[0:1, :].astype(F32))
    normed_t[...] = second_owner[...].T
    row_here.start()
    for copy in loads:
        copy.wait()
    first_ref[0] = query_piece[...].T
    gather.own(0).start()
    meet(place)
    gather.run("f0 f1")
    for copy in row_copies + table_copies:
        copy.start()
    gather.along_mp(0, 1).start()

    key_rows = row_ids((64, keys))
    key_bins = boxes_ref[:, pl.ds(pl.multiple_of(doc * keys, LANES), keys)]
    x_place = jnp.where(key_rows == key_bins[0:1], 1.0, 0.0).astype(BF16)
    y_place = jnp.where(key_rows == key_bins[1:2], 1.0, 0.0).astype(BF16)
    key_extra_t[0:64, :] = x_place
    key_extra_t[64:128, :] = y_place
    mask = jnp.where(lane_ids((64, keys)) >= lengths_ref[doc], NEG_FILL, 0.0)
    first_row = member * rows
    spot = lane_ids((8, width))
    spot = jnp.where(spot >= width - LANES, spot - width, spot)
    bucket = bucket_of(LANES * (blocks - 1) - spot - first_row)[0:1]
    line_hot[...] = jnp.where(row_ids((LANES, width)) == bucket, 1.0, 0.0).astype(BF16)
    spot = lane_ids((8, LANES))
    bucket = bucket_of(jnp.where(spot < NBIN, -spot, LANES - spot))[0:1]
    bin_hot[...] = jnp.where(row_ids((LANES, LANES)) == bucket, 1.0, 0.0).astype(BF16)
    tail = jnp.where(key_rows == 0, mask, jnp.where(key_rows < 4, 1.0, 0.0)).astype(BF16)
    turned = jnp.concatenate([jnp.zeros((64, keys), BF16), x_place, y_place, tail], axis=0).T
    key_extra[...] = turned
    key_aug[...] = turned
    query_aug[pl.ds(192, 64), :] = jnp.where(row_ids((64, rows)) == 0, 1.0, 0.0).astype(BF16)
    gather.run("s0 f2")
    for block in range(model_width // LANES):
        owner = block_owner(block)
        out_owner[:, owner * LANES : (owner + 1) * LANES] = cotangent_ref[
            :, block * LANES : (block + 1) * LANES
        ].astype(BF16)
    out_t[...] = cotangent_ref[...].astype(BF16).T
    residual[...] = input_ref[...]
    layer_output[...] = jnp.zeros_like(layer_output)
    second_grad[...] = jnp.zeros_like(second_grad)
    row_here.wait()
    table_here.wait()
    gather.run("s1 t0")

    head_units = mp_size * heads_here
    table = {
        (1, 0): "f3 z4 z6", (2, 0): "s3 s2 t1", (4, 0): "t3 f4 z7", (5, 0): "s4 t2", (6, 0): "f5 z8",
        (7, 0): "t4 f6", (8, 0): "s5 z9", (9, 0): "f7 s6", (11, 0): "t5", (12, 0): "f8 s7", (13, 0): "t6",
        (14, 0): "f9 s8", (16, 0): "f10 t7", (16, 2): "s9", (17, 0): "f11 t8", (17, 1): "s10",
        (17, 3): "t9", (18, 0): "s11", (18, 3): "t10", (19, 1): "t11",
    }
    scatter = Scatter(
        place, [gate_up_full, down_full], [gate_up_share, down_share], sems[5:], FORWARD_SUMS,
        inside=True,
    )
    sum_table = {(18, 0): "c0 c1", (18, 3): "f0 f1", (19, 3): "s0"}

    def communicate(unit, point):
        for (at_unit, at_point), ops in table.items():
            if at_point == point:

                @pl.when(unit == at_unit)
                def _(ops=ops):
                    gather.run(ops)

        for (at_unit, at_point), ops in sum_table.items():
            if at_point == point:

                @pl.when(unit == at_unit)
                def _(ops=ops):
                    scatter.run(ops)

    def head_unit(unit, carry):
        communicate(unit, 0)
        step = lax.div(unit, heads_here)
        inside = lax.rem(unit, heads_here)
        source = place.across(step)
        base = pl.multiple_of(source * inner_here, 16)
        head = source * heads_here + inside

        @pl.when(inside == 0)
        def _():
            for k in range(mp_size):

                @pl.when(step == k)
                def _(k=k):
                    gather.done(at[(0, k)])
                    if k == 0:
                        for copy in row_copies:
                            copy.wait_recv()
                    else:
                        table_copies[k - 1].wait_recv()

            load = Copy(w_first.at[:, pl.ds(base, inner_here), :], first_here, load_sem.at[0])
            load.start()
            hot = tables[source].astype(BF16)
            line[source] = jnp.dot(hot[0:8], line_hot[...], preferred_element_type=F32)
            bins = jnp.dot(hot[8:24], bin_hot[...], preferred_element_type=F32)
            for i in range(heads_here):
                x_line = jnp.broadcast_to(bins[i : i + 1], (64, LANES))
                y_line = jnp.broadcast_to(bins[8 + i : 9 + i], (64, LANES))
                left = lane_ids((64, LANES)) < 64
                x_part = pltpu.roll(x_line, 0, 1, stride=1, stride_axis=0)
                y_part = pltpu.roll(y_line, 64, 1, stride=1, stride_axis=0)
                layout[source * heads_here + i] = jnp.concatenate(
                    [jnp.where(left, x_part, 0.0), jnp.where(left, 0.0, y_part)], axis=0
                ).astype(BF16)
            load.wait()
            here = pl.ds(base, inner_here)
            queries[here, :] = jnp.dot(
                first_here[0], normed_t[...], preferred_element_type=F32
            ).astype(BF16)
            keys_t[here, :] = jnp.dot(
                first_here[1], slot_t[...], preferred_element_type=F32
            ).astype(BF16)
            values_t[here, :] = jnp.dot(
                first_here[2], slot_t[...], preferred_element_type=F32
            ).astype(BF16)

        here = pl.ds(pl.multiple_of(head * 64, 16), 64)
        both = jnp.concatenate([keys_t[here, :], values_t[here, :]], axis=0).T
        low_lanes = lane_ids((keys, LANES)) < 64
        key_aug[:, 0:LANES] = jnp.where(low_lanes, both, key_extra[:, 0:LANES])
        query_aug[pl.ds(0, 64), :] = queries[here, :]
        query_aug[pl.ds(64, 128), :] = jnp.dot(
            layout[head], key_extra_t[:, own_lanes], preferred_element_type=F32
        ).astype(BF16)
        strip[...] = pltpu.roll(
            jnp.broadcast_to(line[source, pl.ds(inside, 1), :], (LANES, width)), 0, 1,
            stride=1, stride_axis=0,
        )
        query_all = query_aug[...]
        top = jnp.full((1, rows), -jnp.inf, F32)
        for block in range(blocks):
            some = pl.ds(block * LANES, LANES)
            part = jnp.dot(key_aug[some, :], query_all, preferred_element_type=F32)
            part = part + strip[:, pl.ds((blocks - 1 - block) * LANES, rows)]
            scores[some, :] = part
            top = jnp.maximum(top, jnp.max(part, axis=0, keepdims=True))
        sums = jnp.zeros((1, rows), F32)
        for block in range(blocks):
            some = pl.ds(block * LANES, LANES)
            part = jnp.exp(scores[some, :] - top)
            sums = sums + jnp.sum(part, axis=0, keepdims=True)
            probs[some, :] = part.astype(BF16)
        mixed = jnp.dot(values_t[here, :], probs[...], preferred_element_type=F32)
        heads_out[here, :] = (mixed / sums).astype(BF16)
        lse[head] = top + jnp.log(sums)

        @pl.when(inside == heads_here - 1)
        def _():
            part = heads_out[pl.ds(base, inner_here), :].T
            residual[...] = residual[...] + jnp.dot(
                part, first_here[3], preferred_element_type=F32
            )

        return carry

    lax.fori_loop(0, head_units, head_unit, 0)
    for block in range(model_width // LANES):
        owner = block_owner(block)
        slot_owner[:, owner * LANES : (owner + 1) * LANES] = slot_t[
            block * LANES : (block + 1) * LANES, :
        ].T

    kept = [
        Copy(here, there, keep_sem.at[i])
        for i, (here, there) in enumerate(
            [
                (queries, queries_out), (keys_t, keys_out), (values_t, values_out),
                (heads_out, heads_out_out), (slot_owner, slot_owner_out), (residual, residual_out),
            ]
        )
    ]
    for copy in kept:
        copy.start()
    norm_into(residual, gain_ref[1:2, :].astype(F32))
    second_t[...] = second_owner[...].T
    turned_blocks = [second_owner[:, b * LANES : (b + 1) * LANES] for b in range(model_width // LANES)]
    for block, values in enumerate(turned_blocks):
        owner = block_owner(block)
        second_owner[:, owner * LANES : (owner + 1) * LANES] = values

    def store(step):
        source = place.across(step)
        here = pl.ds(pl.multiple_of(source * hidden, 16), hidden)
        return [
            Copy(stage_gate_up, gate_up_full.at[:, here, :], store_sem.at[0]),
            Copy(stage_down, down_full.at[:, here, :], store_sem.at[1]),
        ]

    def hidden_unit(step, carry):
        unit = step + head_units

        @pl.when(step > 0)
        def _():
            for copy in store(step):
                copy.wait()

        communicate(unit, 0)
        source = place.across(step)
        here = pl.ds(pl.multiple_of(source * hidden, 16), hidden)
        for k in range(mp_size):

            @pl.when(step == k)
            def _(k=k):
                gather.done(at[(1, k)])

        hidden_a[...] = jnp.dot(w_gate_up[0, here, :], second_t[...], preferred_element_type=F32)
        hidden_b[...] = jnp.dot(w_gate_up[1, here, :], second_t[...], preferred_element_type=F32)
        communicate(unit, 1)
        for k in range(mp_size):

            @pl.when(step == k)
            def _(k=k):
                gather.done(at[(2, k)])

        hidden_c[...] = jnp.dot(w_down[0, here, :], out_t[...], preferred_element_type=F32)

        def activate(i, inner_carry):
            some = pl.ds(pl.multiple_of(i * 16, 16), 16)
            gate, up, slope = hidden_a[some, :], hidden_b[some, :], hidden_c[some, :]
            square = gate * gate
            factor = 0.7978845608028654
            bent = jnp.tanh(factor * gate * (1.0 + 0.044715 * square))
            half = 0.5 * (1.0 + bent)
            value = gate * half
            change = half + 0.5 * gate * (1.0 - bent * bent) * (
                factor * (1.0 + 3.0 * 0.044715 * square)
            )
            act_t[some, :] = (value * up).astype(BF16)
            low_t[some, :] = (slope * up * change).astype(BF16)
            low_t[pl.ds(pl.multiple_of(hidden + i * 16, 16), 16), :] = (slope * value).astype(BF16)
            return inner_carry

        lax.fori_loop(0, hidden // 16, activate, 0)
        communicate(unit, 2)

        stage_down[0] = jnp.dot(act_t[...], out_owner[...], preferred_element_type=F32).astype(BF16)
        stage_gate_up[0] = jnp.dot(
            low_t[0:hidden], second_owner[...], preferred_element_type=F32
        ).astype(BF16)
        stage_gate_up[1] = jnp.dot(
            low_t[hidden:], second_owner[...], preferred_element_type=F32
        ).astype(BF16)
        for copy in store(step):
            copy.start()
        communicate(unit, 3)
        layer_output[...] = layer_output[...] + dot_f32(act_t[...].T, w_down[0, here, :], 1, 0)
        second_grad[...] = (
            second_grad[...]
            + dot_f32(low_t[0:hidden].T, w_gate_up[0, here, :], 1, 0)
            + dot_f32(low_t[hidden:].T, w_gate_up[1, here, :], 1, 0)
        )
        return carry

    lax.fori_loop(0, mp_size, hidden_unit, 0)
    layer_output[...] = layer_output[...] + residual[...]
    scatter.run("s1 t0 t1")
    scatter.run("e0 e1")
    for copy in store(mp_size - 1):
        copy.wait()
    gather.close()
    scatter.close()
    for copy in row_copies + table_copies:
        copy.wait_send()
    for copy in kept:
        copy.wait()


def block_owner(block):
    return (block % 2) * 4 + block // 2


def forward(
    mp_size, group, query, output, gate_up, down, key_value, table, boxes, lengths, layer_input,
    gains, cotangent,
):
    rows, model_width = layer_input.shape
    keys = boxes.shape[1] // lengths.shape[0]
    width = LANES * (keys // LANES + rows // LANES)
    inner_here, hidden = query.shape[1], gate_up.shape[1]
    inner, total_hidden = inner_here * mp_size, hidden * mp_size
    head_count = inner // 64
    dma = pltpu.SemaphoreType.DMA
    hbm = pl.BlockSpec(memory_space=HBM)
    vmem = pl.BlockSpec(memory_space=pltpu.VMEM)
    shape = jax.ShapeDtypeStruct
    out = [
        (shape((4, inner, model_width), BF16), hbm),
        (shape((inner, rows), BF16), hbm),
        (shape((inner, keys), BF16), hbm),
        (shape((inner, keys), BF16), hbm),
        (shape((inner, rows), BF16), hbm),
        (shape((head_count, 1, rows), F32), vmem),
        (shape((head_count, 128, 128), BF16), vmem),
        (shape((mp_size, 8, width), F32), vmem),
        (shape((keys, 256), BF16), vmem),
        (shape((128, keys), BF16), vmem),
        (shape((keys, model_width), BF16), hbm),
        (shape((rows, model_width), F32), hbm),
        (shape((rows, model_width), F32), vmem),
        (shape((rows, model_width), F32), vmem),
        (shape((2, total_hidden, model_width), BF16), hbm),
        (shape((1, total_hidden, model_width), BF16), hbm),
        (shape((mp_size, 24, LANES), F32), vmem),
        (shape((LANES, width), BF16), vmem),
        (shape((LANES, LANES), BF16), vmem),
        (shape((2, hidden, LANES), BF16), vmem),
        (shape((1, hidden, LANES), BF16), vmem),
    ]
    return pl.pallas_call(
        partial(forward_kernel, mp_size, group),
        out_shape=tuple(o[0] for o in out),
        in_specs=[hbm] * 4 + [vmem] * 3 + [pl.BlockSpec(memory_space=pltpu.SMEM)] + [vmem] * 3,
        out_specs=tuple(o[1] for o in out),
        scratch_shapes=[
            pltpu.VMEM((inner, rows), BF16),
            pltpu.VMEM((inner, keys), BF16),
            pltpu.VMEM((inner, keys), BF16),
            pltpu.VMEM((inner, rows), BF16),
            pltpu.VMEM((keys, model_width), BF16),
            pltpu.VMEM((rows, model_width), F32),
            pltpu.VMEM((4, inner_here, LANES), BF16),
            pltpu.VMEM((LANES, inner_here), BF16),
            pltpu.VMEM((model_width, rows), BF16),
            pltpu.VMEM((model_width, keys), BF16),
            pltpu.VMEM((2, total_hidden, model_width), BF16),
            pltpu.VMEM((1, total_hidden, model_width), BF16),
            pltpu.VMEM((4, inner_here, model_width), BF16),
            pltpu.VMEM((keys, 256), BF16),
            pltpu.VMEM((256, rows), BF16),
            pltpu.VMEM((LANES, width), F32),
            pltpu.VMEM((keys, rows), F32),
            pltpu.VMEM((keys, rows), BF16),
            pltpu.VMEM((model_width, rows), BF16),
            pltpu.VMEM((rows, model_width), BF16),
            pltpu.VMEM((rows, model_width), BF16),
            pltpu.VMEM((model_width, rows), BF16),
            pltpu.VMEM((hidden, rows), F32),
            pltpu.VMEM((hidden, rows), F32),
            pltpu.VMEM((hidden, rows), F32),
            pltpu.VMEM((hidden, rows), BF16),
            pltpu.VMEM((2 * hidden, rows), BF16),
            pltpu.VMEM((2, hidden, model_width), BF16),
            pltpu.VMEM((1, hidden, model_width), BF16),
            dma((group,)), dma((group,)), dma((1,)),
            dma((mp_size,)), dma((mp_size,)), dma((1,)), dma((2,)), dma((2,)), dma((6,)),
        ]
        + Gather.semaphores(3, mp_size)
        + Scatter.scratch([(2, hidden), (1, hidden)], (True, True), FORWARD_SUMS),
        compiler_params=pltpu.CompilerParams(
            collective_id=0, has_side_effects=True, vmem_limit_bytes=62 << 20
        ),
        name="forward",
    )(
        query, output, gate_up, down, key_value, table, boxes, lengths, layer_input, gains, cotangent,
    )


BACKWARD_ITEMS = [(0, 3), (1, 3), (0, 2), (1, 2), (2, 3), (2, 2), (0, 0), (2, 1), (1, 0), (2, 0)]


def unskewed(values, first, count, shift):
    width = values.shape[1]
    folded = None
    for group in range(count // 8):
        part = values[pl.ds(first + group * 8, 8), :]
        back = (-(group * 8 + shift)) % width
        part = pltpu.roll(part, back, 1) if back else part
        folded = part if folded is None else folded + part
    total = folded[0:1]
    for row in range(1, 8):
        total = total + pltpu.roll(folded[row : row + 1], width - row, 1)
    return total


def exact_dot(left, right):
    parts = three_parts(left)
    return sum(dot_f32(part, right, 1, 1) for part in parts)


def backward_kernel(mp_size, group, *refs):
    (
        gate_up_full, down_full, w_first, queries, keys_t, values_t, heads_out,
        residual_in, second_in, cotangent_in,
        lse, layout, line, key_extra, key_extra_t, slot_owner, layer_input, gains, line_hot, bin_hot,
        gate_up_share, down_share, input_out, small_out, gate_up_sum, down_sum, first_sum,
        *refs,
    ) = refs
    (
        input_grad, slot_grad, own_grad, residual_grad, branch_owner, branch_t, w_query, w_output, w_kv,
        q_here, k_here, v_here, out_here, grad_here, dq_here, dk_here, dv_here, kv_here,
        key_aug, key_aug_t, query_aug, value_aug, grad_aug, strip, strip_grad, probs_grad,
        layout_grad, line_sums, bin_sums, gain_part, rows_out, peers, stage, stage_in, full_here,
        load_sem, value_sem, row_send, row_recv, stage_send, stage_recv,
        *refs,
    ) = refs
    place = Place(mp_size)
    rows, model_width = layer_input.shape
    keys = slot_owner.shape[0]
    blocks = keys // LANES
    inner_here = q_here.shape[0]
    heads_here = inner_here // 64
    member = lax.rem(place.mp, group)
    first_peer = place.mp - member
    own_start = pl.multiple_of(member * rows, LANES)
    own_lanes = pl.ds(own_start, rows)

    items = BACKWARD_ITEMS
    fulls = [gate_up_full, down_full, full_here]
    scatter = Scatter(
        place, fulls, [gate_up_sum, down_sum, first_sum], refs, items, [gate_up_share, down_share, None]
    )

    loads = [
        Copy(second_in, slot_grad.at[pl.ds(0, rows), :], value_sem.at[0]),
        Copy(residual_in, slot_grad.at[pl.ds(rows, rows), :], value_sem.at[1]),
        Copy(cotangent_in, input_grad, value_sem.at[2]),
    ]
    for copy in loads:
        copy.start()
    greet(place)
    meet(place)
    scatter.run("c0 c1")
    for c in range(2):
        scatter.share(c).start()
    key_aug[...] = key_extra[...]
    key_aug_t[pl.ds(64, 128), :] = key_extra_t[...]
    for copy in loads:
        copy.wait()

    def norm_back(i, total):
        here = pl.ds(pl.multiple_of(i * 16, 16), 16)
        grad = slot_grad[here, :]
        values = slot_grad[pl.ds(pl.multiple_of(rows + i * 16, 16), 16), :]
        scale = lax.rsqrt(jnp.mean(values * values, axis=1, keepdims=True) + EPSILON)
        scaled = gains[1:2, :].astype(F32) * grad
        mean = jnp.mean(scaled * values, axis=1, keepdims=True)
        result = input_grad[here, :] + scale * scaled - values * (scale * scale * scale * mean)
        residual_grad[here, :] = result
        branch_owner[here, :] = result.astype(BF16)
        product = grad * values * scale
        return total + product[0:8] + product[8:16]

    total = lax.fori_loop(0, rows // 16, norm_back, jnp.zeros((8, model_width), F32))
    gain_part[...] = jnp.sum(total, axis=0, keepdims=True)
    scatter.run("f0 c2")
    branch_t[...] = branch_owner[...].T
    parts = [branch_owner[:, b * LANES : (b + 1) * LANES] for b in range(model_width // LANES)]
    for block, values in enumerate(parts):
        owner = block_owner(block)
        branch_owner[:, owner * LANES : (owner + 1) * LANES] = values
    slot_grad[...] = jnp.zeros_like(slot_grad)
    own_grad[...] = jnp.zeros_like(own_grad)
    scatter.run("f1 c3")

    plan = {
        (0, 2): "s0 f2", (0, 3): "s1 f3", (0, 4): "t0 c4", (1, 1): "s2", (1, 2): "t1 f4", (1, 3): "s3 c6",
        (2, 0): "t2 c5", (2, 1): "s4 f5", (2, 2): "t3", (2, 3): "f6 c8", (2, 4): "t4 c7", (3, 1): "s5",
        (3, 2): "s6 f7", (3, 4): "t5 f8 c9",
    }

    def communicate(block, point):
        for (at_block, at_point), ops in plan.items():
            if at_point == point:

                @pl.when(block == at_block)
                def _(ops=ops):
                    scatter.run(ops)

    row_copies = [
        remote(
            rows_out.at[k - 1], peers.at[k - 1], row_send.at[k], row_recv.at[k],
            (place.dp, first_peer + lax.rem(member + k, group)),
        )
        for k in range(1, group)
    ]

    def block_unit(block, carry):
        communicate(block, 0)
        step = mp_size - 1 - block
        target = place.across(step)
        base = pl.multiple_of(target * inner_here, 16)
        here = pl.ds(base, inner_here)
        slot = lax.rem(block, 2)
        copies = [
            Copy(w_first.at[0, here, :], w_query, load_sem.at[0]),
            Copy(w_first.at[3, here, :], w_output, load_sem.at[1]),
            Copy(queries.at[here, :], q_here, load_sem.at[2]),
            Copy(keys_t.at[here, :], k_here, load_sem.at[3]),
            Copy(values_t.at[here, :], v_here, load_sem.at[4]),
            Copy(heads_out.at[here, :], out_here, load_sem.at[5]),
        ]
        for i in range(heads_here):
            for part in range(2):
                copies.append(
                    Copy(
                        w_first.at[1 + part, pl.ds(pl.multiple_of(base + i * 64, 16), 64), :],
                        w_kv.at[pl.ds(i * 128 + part * 64, 64), :],
                        load_sem.at[6 + 2 * i + part],
                    )
                )
        for copy in copies:
            copy.start()
        for copy in (copies[1], copies[5]):
            copy.wait()

        for b in range(2, mp_size):

            @pl.when(block == b)
            def _(b=b):
                scatter.left(items.index((2, mp_size + 1 - b)))

        grad_here[...] = jnp.dot(w_output[...], branch_t[...], preferred_element_type=F32).astype(BF16)
        full_here[slot, 3] = jnp.dot(
            out_here[...], branch_owner[...], preferred_element_type=F32
        ).astype(BF16)
        for copy in [copies[0]] + copies[2:5] + copies[6:]:
            copy.wait()

        def head_unit(inside, inner_carry):
            for point in range(1, heads_here):

                @pl.when(inside == point)
                def _(point=point):
                    communicate(block, point)

            head = target * heads_here + inside
            some = pl.ds(pl.multiple_of(inside * 64, 16), 64)
            q_head, k_head, v_head = q_here[some, :], k_here[some, :], v_here[some, :]
            grad_head = grad_here[some, :]
            both = jnp.concatenate([k_head, v_head], axis=0).T
            lanes = lane_ids((keys, LANES))
            key_aug[:, 0:LANES] = jnp.where(lanes < 64, both, key_extra[:, 0:LANES])
            ones = jnp.where(lanes < 3, 1.0, 0.0).astype(BF16)
            value_aug[...] = jnp.where(lanes < 64, ones, both)
            key_aug_t[pl.ds(0, 64), :] = k_head
            query_aug[pl.ds(0, 64), :] = q_head
            query_aug[pl.ds(64, 128), :] = jnp.dot(
                layout[head], key_extra_t[:, own_lanes], preferred_element_type=F32
            ).astype(BF16)
            high, middle, low = three_parts(-lse[head])
            tail = row_ids((64, rows))
            rows_of = lambda part: jnp.broadcast_to(part.astype(F32), (64, rows))
            query_aug[pl.ds(192, 64), :] = jnp.where(
                tail == 0, 1.0,
                jnp.where(
                    tail == 1, rows_of(high),
                    jnp.where(tail == 2, rows_of(middle), jnp.where(tail == 3, rows_of(low), 0.0)),
                ),
            ).astype(BF16)
            row_dot = jnp.sum(
                grad_head.astype(F32) * out_here[some, :].astype(F32), axis=0, keepdims=True
            )
            high, middle, low = three_parts(-row_dot)
            grad_aug[pl.ds(0, 64), :] = jnp.where(
                tail == 0, rows_of(high),
                jnp.where(tail == 1, rows_of(middle), jnp.where(tail == 2, rows_of(low), 0.0)),
            ).astype(BF16)
            grad_aug[pl.ds(64, 64), :] = grad_head
            width = strip.shape[1]
            strip[...] = pltpu.roll(
                jnp.broadcast_to(line[target, pl.ds(inside, 1), :], (LANES, width)), 0, 1,
                stride=1, stride_axis=0,
            )
            strip_grad[...] = jnp.zeros_like(strip_grad)
            query_and_grad = jnp.concatenate([q_head, grad_head], axis=0).T
            query_all = query_aug[...]
            grad_all = grad_aug[...]
            half = lane_ids((LANES, LANES)) < 64
            kv_lanes = pl.ds(pl.multiple_of(inside * LANES, LANES), LANES)
            for part_index in range(blocks):
                these = pl.ds(part_index * LANES, LANES)
                band = pl.ds((blocks - 1 - part_index) * LANES, rows)
                part = jnp.dot(key_aug[these, :], query_all, preferred_element_type=F32)
                part = jnp.exp(part + strip[:, band])
                slope = part * jnp.dot(value_aug[these, :], grad_all, preferred_element_type=F32)
                strip_grad[:, band] = strip_grad[:, band] + slope
                slope = slope.astype(BF16)
                probs_grad[these, :] = slope
                key_part = jnp.dot(slope, query_and_grad, preferred_element_type=F32)
                value_part = jnp.dot(part.astype(BF16), query_and_grad, preferred_element_type=F32)
                joined = jnp.where(half, key_part, value_part)
                kv_here[these, kv_lanes] = joined.astype(BF16)
                turned = joined.T.astype(BF16)
                dk_here[some, these] = turned[0:64]
                dv_here[some, these] = turned[64:128]
            query_part = jnp.dot(key_aug_t[...], probs_grad[...], preferred_element_type=F32)
            dq_here[some, :] = query_part[0:64].astype(BF16)
            bins = dot_f32(query_part[64:192].astype(BF16), key_extra_t[:, own_lanes], 1, 1)
            left = lane_ids((LANES, LANES)) < 64
            upper = row_ids((LANES, LANES)) < 64
            layout_grad[...] = jnp.where(left == upper, bins, 0.0)
            bin_sums[0, pl.ds(head, 1), :] = unskewed(layout_grad, 0, 64, 0)
            bin_sums[1, pl.ds(head, 1), :] = unskewed(layout_grad, 64, 64, 64)
            line_sums[pl.ds(head, 1), :] = unskewed(strip_grad, 0, LANES, 0)
            return inner_carry

        lax.fori_loop(0, heads_here, head_unit, 0)
        slot_grad[...] = slot_grad[...] + jnp.dot(
            kv_here[...], w_kv[...], preferred_element_type=F32
        )
        own_grad[...] = own_grad[...] + jnp.dot(
            dq_here[...].T, w_query[...], preferred_element_type=F32
        )

        @pl.when(block == mp_size - 1)
        def _():
            for k, copy in enumerate(row_copies):
                other = lax.rem(member + k + 1, group)
                rows_out[k] = slot_grad[pl.ds(pl.multiple_of(other * rows, 16), rows), :].astype(BF16)
                copy.start()

        full_here[slot, 0] = jnp.dot(
            dq_here[...], slot_owner[pl.ds(own_start, rows), :], preferred_element_type=F32
        ).astype(BF16)
        full_here[slot, 1] = jnp.dot(
            dk_here[...], slot_owner[...], preferred_element_type=F32
        ).astype(BF16)
        full_here[slot, 2] = jnp.dot(
            dv_here[...], slot_owner[...], preferred_element_type=F32
        ).astype(BF16)
        communicate(block, heads_here)
        return carry

    lax.fori_loop(0, mp_size, block_unit, 0)

    scatter.run("t6 f9")

    gain_rows = model_width // LANES
    head_count = bin_sums.shape[1]
    stage[0, 2 * gain_rows : 2 * gain_rows + head_count, :] = exact_dot(line_sums[...], line_hot[...])
    for i in range(2):
        start = 2 * gain_rows + (1 + i) * head_count
        stage[0, start : start + head_count, :] = exact_dot(bin_sums[i], bin_hot[...])
    for block in range(gain_rows):
        these = slice(block * LANES, (block + 1) * LANES)
        owner = block_owner(block)
        those = slice(owner * LANES, (owner + 1) * LANES)

        def gain_sum(i, total, these=these, those=those):
            here = pl.ds(pl.multiple_of(i * 64, 64), 64)
            product = slot_grad[here, these] * slot_owner[here, those].astype(F32)
            return total + jnp.sum(product.reshape(8, 8, LANES), axis=0)

        def own_sum(i, total, these=these, those=those):
            here = pl.ds(pl.multiple_of(i * 64, 64), 64)
            there = pl.ds(pl.multiple_of(own_start + i * 64, 64), 64)
            product = own_grad[here, these] * slot_owner[there, those].astype(F32)
            return total + jnp.sum(product.reshape(8, 8, LANES), axis=0)

        total = lax.fori_loop(0, keys // 64, gain_sum, jnp.zeros((8, LANES), F32))
        total = lax.fori_loop(0, rows // 64, own_sum, total)
        stage[0, block : block + 1, :] = (
            jnp.sum(total, axis=0, keepdims=True) / gains[0:1, these].astype(F32)
        )
        stage[0, gain_rows + block : gain_rows + block + 1, :] = gain_part[:, these]

    rounds = [[place.to_core], [place.to_x, place.to_y, place.to_corner]]
    rounds.append([place.to_mp(k) for k in range(1, mp_size)])
    at, sums = 0, []
    for i, partners in enumerate(rounds):
        sums.append(
            [
                remote(
                    stage.at[i], stage_in.at[at + j], stage_send.at[at + j], stage_recv.at[at + j], partner
                )
                for j, partner in enumerate(partners)
            ]
        )
        at += len(partners)
    def round_done(i):
        at = sum(len(partners) for partners in rounds[:i])
        value = stage[i]
        for j, copy in enumerate(sums[i]):
            copy.wait_recv()
            value = value + stage_in[at + j]
        return value

    for copy in sums[0]:
        copy.start()
    scatter.run("s7 s8 e0")
    stage[1] = round_done(0)
    for copy in sums[1]:
        copy.start()
    scatter.run("t7 s9")
    for copy in row_copies:
        copy.wait_recv()

    def input_back(i, carry):
        here = pl.ds(pl.multiple_of(i * 16, 16), 16)
        grad = own_grad[here, :] + slot_grad[pl.ds(pl.multiple_of(own_start + i * 16, 16), 16), :]
        for k in range(group - 1):
            grad = grad + peers[k, here, :].astype(F32)
        values = layer_input[here, :]
        scale = lax.rsqrt(jnp.mean(values * values, axis=1, keepdims=True) + EPSILON)
        scaled = gains[0:1, :].astype(F32) * grad
        mean = jnp.mean(scaled * values, axis=1, keepdims=True)
        input_grad[here, :] = (
            residual_grad[here, :] + scale * scaled - values * (scale * scale * scale * mean)
        )
        return carry

    lax.fori_loop(0, rows // 16, input_back, 0)
    leave = Copy(input_grad, input_out, value_sem.at[0])
    leave.start()
    stage[2] = round_done(1)
    for copy in sums[2]:
        copy.start()
    scatter.run("t8 t9")
    scatter.run("e1 e2")
    small_out[...] = round_done(2)
    sums = sum(sums, [])
    scatter.close()
    leave.wait()
    for copy in row_copies + sums:
        copy.wait_send()


def backward(
    mp_size, group, gate_up_full, down_full, w_first, queries, keys_t, values_t, heads_out,
    residual, second_grad, cotangent, lse, layout, line, key_extra, key_extra_t, slot_owner,
    layer_input, gains, line_hot, bin_hot, gate_up_share, down_share,
):
    rows, model_width = layer_input.shape
    keys = slot_owner.shape[0]
    width = line.shape[2]
    inner_here = queries.shape[0] // mp_size
    heads_here = inner_here // 64
    head_count = heads_here * mp_size
    hidden = down_full.shape[1] // mp_size
    sizes = [(2, hidden), (1, hidden), (4, inner_here)]
    count = 4 + mp_size - 1
    small_rows = 2 * model_width // LANES + 3 * head_count
    others = max(group - 1, 1)
    dma = pltpu.SemaphoreType.DMA
    hbm = pl.BlockSpec(memory_space=HBM)
    vmem = pl.BlockSpec(memory_space=pltpu.VMEM)
    shape = jax.ShapeDtypeStruct
    return pl.pallas_call(
        partial(backward_kernel, mp_size, group),
        out_shape=(
            shape((rows, model_width), F32),
            shape((small_rows, LANES), F32),
            *[shape((lead, n, LANES), F32) for lead, n in sizes],
        ),
        in_specs=[hbm] * 10 + [vmem] * 12,
        out_specs=(hbm,) + (vmem,) * 4,
        scratch_shapes=[
            pltpu.VMEM((rows, model_width), F32),
            pltpu.VMEM((keys, model_width), F32),
            pltpu.VMEM((rows, model_width), F32),
            pltpu.VMEM((rows, model_width), F32),
            pltpu.VMEM((rows, model_width), BF16),
            pltpu.VMEM((model_width, rows), BF16),
            pltpu.VMEM((inner_here, model_width), BF16),
            pltpu.VMEM((inner_here, model_width), BF16),
            pltpu.VMEM((2 * inner_here, model_width), BF16),
            pltpu.VMEM((inner_here, rows), BF16),
            pltpu.VMEM((inner_here, keys), BF16),
            pltpu.VMEM((inner_here, keys), BF16),
            pltpu.VMEM((inner_here, rows), BF16),
            pltpu.VMEM((inner_here, rows), BF16),
            pltpu.VMEM((inner_here, rows), BF16),
            pltpu.VMEM((inner_here, keys), BF16),
            pltpu.VMEM((inner_here, keys), BF16),
            pltpu.VMEM((keys, heads_here * LANES), BF16),
            pltpu.VMEM((keys, 256), BF16),
            pltpu.VMEM((192, keys), BF16),
            pltpu.VMEM((256, rows), BF16),
            pltpu.VMEM((keys, LANES), BF16),
            pltpu.VMEM((LANES, rows), BF16),
            pltpu.VMEM((LANES, width), F32),
            pltpu.VMEM((LANES, width), F32),
            pltpu.VMEM((keys, rows), BF16),
            pltpu.VMEM((LANES, LANES), F32),
            pltpu.VMEM((head_count, width), F32),
            pltpu.VMEM((2, head_count, LANES), F32),
            pltpu.VMEM((1, model_width), F32),
            pltpu.VMEM((others, rows, model_width), BF16),
            pltpu.VMEM((others, rows, model_width), BF16),
            pltpu.VMEM((3, small_rows, LANES), F32),
            pltpu.VMEM((count, small_rows, LANES), F32),
            pltpu.VMEM((2, 4, inner_here, model_width), BF16),
            dma((6 + 2 * heads_here,)), dma((3,)), dma((group,)), dma((group,)),
            dma((count,)), dma((count,)),
        ]
        + Scatter.scratch(sizes, (True, True, False), BACKWARD_ITEMS),
        compiler_params=pltpu.CompilerParams(
            collective_id=1, has_side_effects=True, vmem_limit_bytes=63 << 20
        ),
        name="backward",
    )(
        gate_up_full, down_full, w_first, queries, keys_t, values_t, heads_out, residual,
        second_grad, cotangent, lse, layout, line, key_extra, key_extra_t, slot_owner, layer_input,
        gains, line_hot, bin_hot, gate_up_share, down_share,
    )


def line_onehot(first_row, width, key_blocks):
    place = jnp.arange(width, dtype=jnp.int32)
    place = jnp.where(place >= width - LANES, place - width, place)
    offset = LANES * (key_blocks - 1) - place - first_row
    return (bucket_of(offset)[:, None] == jnp.arange(32, dtype=jnp.int32)[None, :]).astype(F32)


def bin_onehot():
    bins = np.arange(NBIN)
    offset = bins[:, None] - bins[None, :]
    distance = np.abs(offset)
    bucket = np.minimum(distance, 7) + sum((distance >= t).astype(np.int64) for t in THRESHOLDS)
    bucket = bucket + 16 * (offset > 0)
    return jnp.asarray(bucket[:, :, None] == np.arange(32), F32)


def gather_rows(local, axis_name):
    return lax.all_gather(local, axis_name, axis=0, tiled=True)


def scatter_grad(full):
    summed = lax.psum_scatter(full, "dp", scatter_dimension=1, tiled=True)
    return lax.psum_scatter(summed, "mp", scatter_dimension=0, tiled=True)


def per_device_plain(
    dp_size, mp_size,
    layer_input, norm_gains, query_weight, key_value_weight, output_weight,
    gate_up_weight, down_weight, bias_tables, doc_lengths, box_bins, cotangent,
):
    rows, model_width = layer_input.shape
    doc_count = doc_lengths.shape[0]
    slot_span = box_bins.shape[1] // doc_count
    group = mp_size // doc_count
    mp_index = lax.axis_index("mp")
    doc = mp_index // group
    first_row = (mp_index % group) * rows
    key_blocks = slot_span // LANES
    width = LANES * (key_blocks + (rows + LANES - 1) // LANES)
    groups = [[d * group + i for i in range(group)] for d in range(doc_count)]
    gain_first = norm_gains[0].astype(F32)
    gain_second = norm_gains[1].astype(F32)

    w_query = gather_rows(query_weight.T, "mp")
    inner_here = query_weight.shape[1]
    inner = inner_here * mp_size
    w_key = gather_rows(key_value_weight[:, 0].T, "mp")
    w_value = gather_rows(key_value_weight[:, 1].T, "mp")
    w_output = gather_rows(output_weight, "mp")
    w_gate = gather_rows(gate_up_weight[:, 0].T, "mp")
    w_up = gather_rows(gate_up_weight[:, 1].T, "mp")
    w_down = gather_rows(down_weight, "mp")
    tables = lax.all_gather(bias_tables, "mp", axis=2, tiled=True).astype(F32)
    head_count = tables.shape[2]

    onehot_line = line_onehot(first_row, width, key_blocks)
    line = jnp.dot(onehot_line, tables[0], precision=lax.Precision.HIGHEST)
    line = line.T.reshape(head_count, 1, width)
    onehot_bin = bin_onehot()
    x_part = jnp.einsum("ban,nh->hba", onehot_bin, tables[1], precision=lax.Precision.HIGHEST)
    y_part = jnp.einsum("ban,nh->hba", onehot_bin, tables[2], precision=lax.Precision.HIGHEST)
    empty = jnp.zeros_like(x_part)
    layout = jnp.concatenate(
        [jnp.concatenate([x_part, empty], axis=2), jnp.concatenate([empty, y_part], axis=2)], axis=1
    ).astype(BF16)
    key_bins = lax.dynamic_slice(box_bins, (0, doc * slot_span), (2, slot_span))
    own_bins = lax.dynamic_slice(key_bins, (0, first_row), (2, rows))
    bin_ids = jnp.arange(NBIN, dtype=jnp.int32)

    def placed_rows(bins):
        return jnp.concatenate(
            [bins[0][:, None] == bin_ids, bins[1][:, None] == bin_ids], axis=1
        ).astype(BF16)

    def placed_lanes(bins):
        return jnp.concatenate(
            [bin_ids[:, None] == bins[0][None], bin_ids[:, None] == bins[1][None]], axis=0
        ).astype(BF16)

    length = lax.dynamic_index_in_dim(doc_lengths, doc, keepdims=False)
    masked = jnp.arange(slot_span, dtype=jnp.int32)[:, None] >= length
    key_placed = placed_rows(key_bins)
    key_extra = jnp.concatenate(
        [
            jnp.zeros((slot_span, 64), BF16),
            key_placed,
            jnp.where(masked, NEG_FILL, 0.0).astype(BF16),
            jnp.ones((slot_span, 3), BF16),
            jnp.zeros((slot_span, 60), BF16),
        ],
        axis=1,
    )
    key_extra_t = placed_lanes(key_bins)
    query_bins_t = placed_rows(own_bins)
    query_bins = placed_lanes(own_bins)

    scale_first = inverse_rms(layer_input)
    normed = (layer_input * scale_first * gain_first).astype(BF16)
    slot_normed = lax.all_gather(normed, "mp", axis=0, tiled=True, axis_index_groups=groups)
    queries = dot_f32(w_query, normed, 1, 1).astype(BF16)
    keys_t = dot_f32(w_key, slot_normed, 1, 1).astype(BF16)
    values_t = dot_f32(w_value, slot_normed, 1, 1).astype(BF16)
    heads_out, lse = attend(queries, keys_t, values_t, layout, line, key_extra, query_bins)
    residual = layer_input + dot_f32(heads_out, w_output, 0, 0)
    scale_second = inverse_rms(residual)
    normed_second = (residual * scale_second * gain_second).astype(BF16)
    gate = dot_f32(normed_second, w_gate, 1, 1)
    up = dot_f32(normed_second, w_up, 1, 1)
    gelu_value, gelu_pull = jax.vjp(lambda v: jax.nn.gelu(v, approximate=True), gate)
    activated = (gelu_value * up).astype(BF16)
    layer_output = residual + dot_f32(activated, w_down, 1, 0)

    out_low = cotangent.astype(BF16)
    down_full = dot_f32(activated, out_low, 0, 0).astype(BF16)
    act_grad = dot_f32(out_low, w_down, 1, 1)
    gate_low = gelu_pull(act_grad * up)[0].astype(BF16)
    up_low = (act_grad * gelu_value).astype(BF16)
    gate_full = dot_f32(gate_low, normed_second, 0, 0).astype(BF16)
    up_full = dot_f32(up_low, normed_second, 0, 0).astype(BF16)
    second_grad = dot_f32(gate_low, w_gate, 1, 0) + dot_f32(up_low, w_up, 1, 0)
    gain_second_grad = jnp.sum(second_grad * residual * scale_second, axis=0)
    scaled = gain_second * second_grad
    residual_grad = (
        cotangent
        + scale_second * scaled
        - residual * scale_second**3 * jnp.mean(scaled * residual, axis=-1, keepdims=True)
    )

    branch_low = residual_grad.astype(BF16)
    output_full = dot_f32(heads_out, branch_low, 1, 0).astype(BF16)
    heads_grad = dot_f32(w_output, branch_low, 1, 1).astype(BF16)
    dq, dk, dv, line_grad, layout_grad = attend_back(
        queries, keys_t, values_t, heads_out, heads_grad, lse, layout, line,
        key_extra, key_extra_t, query_bins, query_bins_t,
    )
    query_full = dot_f32(dq, normed, 1, 0).astype(BF16)
    key_full = dot_f32(dk, slot_normed, 1, 0).astype(BF16)
    value_full = dot_f32(dv, slot_normed, 1, 0).astype(BF16)
    slot_grad = dot_f32(dk, w_key, 0, 0) + dot_f32(dv, w_value, 0, 0)
    first_grad = lax.psum_scatter(
        slot_grad.astype(BF16), "mp", scatter_dimension=0, tiled=True, axis_index_groups=groups
    ).astype(F32) + dot_f32(dq, w_query, 0, 0)
    gain_first_grad = jnp.sum(first_grad * layer_input * scale_first, axis=0)
    scaled = gain_first * first_grad
    input_grad = (
        residual_grad
        + scale_first * scaled
        - layer_input * scale_first**3 * jnp.mean(scaled * layer_input, axis=-1, keepdims=True)
    )

    gain_grad = lax.psum_scatter(
        jnp.stack([gain_first_grad, gain_second_grad]), ("dp", "mp"), scatter_dimension=1, tiled=True
    )
    line_part = jnp.dot(
        onehot_line.T, line_grad[:, 0].T, precision=lax.Precision.HIGHEST
    )
    x_part = jnp.einsum(
        "ban,hba->nh", onehot_bin, layout_grad[:, :64, :64], precision=lax.Precision.HIGHEST
    )
    y_part = jnp.einsum(
        "ban,hba->nh", onehot_bin, layout_grad[:, 64:, 64:], precision=lax.Precision.HIGHEST
    )
    table_full = jnp.stack([line_part, x_part, y_part])
    table_grad = lax.psum_scatter(
        lax.psum_scatter(table_full, "mp", scatter_dimension=2, tiled=True),
        "dp", scatter_dimension=1, tiled=True,
    )

    query_grad = scatter_grad(query_full).T.astype(F32)
    key_value_grad = jnp.stack(
        [scatter_grad(key_full).T, scatter_grad(value_full).T], axis=1
    ).astype(F32)
    output_grad = scatter_grad(output_full).astype(F32)
    gate_up_grad = jnp.stack(
        [scatter_grad(gate_full).T, scatter_grad(up_full).T], axis=1
    ).astype(F32)
    down_grad = scatter_grad(down_full).astype(F32)
    return (
        layer_output, input_grad, gain_grad, query_grad, key_value_grad,
        output_grad, gate_up_grad, down_grad, table_grad,
    )


def per_device_linked(
    dp_size, mp_size,
    layer_input, norm_gains, query_weight, key_value_weight, output_weight,
    gate_up_weight, down_weight, bias_tables, doc_lengths, box_bins, cotangent,
):
    rows, model_width = layer_input.shape
    doc_count = doc_lengths.shape[0]
    group = mp_size // doc_count
    dp_index, mp_index = lax.axis_index("dp"), lax.axis_index("mp")
    heads_here = bias_tables.shape[2]
    head_count = heads_here * mp_size
    inner_here = query_weight.shape[1]
    column = ((dp_index % 2) * 4 + dp_index // 2) * LANES
    key_value = lax.dynamic_slice_in_dim(key_value_weight, column, LANES, 0)
    table = jnp.swapaxes(bias_tables.astype(F32), 1, 2)
    table = jnp.pad(table, ((0, 0), (0, 8 - heads_here), (0, LANES - 32))).reshape(24, LANES)
    (
        w_first, queries, keys_t, values_t, heads_out, lse, layout, line, key_extra, key_extra_t,
        slot_owner, residual, layer_output, second_grad, gate_up_full, down_full, _, line_hot, bin_hot,
        gate_up_share, down_share,
    ) = forward(
        mp_size, group, query_weight, output_weight, jnp.transpose(gate_up_weight, (1, 2, 0)),
        down_weight[None], key_value.reshape(LANES, 2 * inner_here), table, box_bins, doc_lengths,
        layer_input, norm_gains, cotangent,
    )
    input_grad, small, gate_up_sum, down_sum, summed = backward(
        mp_size, group, gate_up_full, down_full, w_first, queries, keys_t, values_t, heads_out,
        residual, second_grad, cotangent, lse, layout, line, key_extra, key_extra_t, slot_owner,
        layer_input, norm_gains, line_hot, bin_hot, gate_up_share, down_share,
    )
    gain_rows = model_width // LANES
    gains = small[: 2 * gain_rows].reshape(2, model_width)
    share = model_width // (dp_size * mp_size)
    at = (dp_index * mp_size + mp_index) * share
    gain_grad = lax.dynamic_slice(gains, (0, at), (2, share))
    tables = small[2 * gain_rows :].reshape(3, head_count, LANES)
    table_grad = lax.dynamic_slice(
        tables,
        (0, mp_index * heads_here, dp_index * (32 // dp_size)),
        (3, heads_here, 32 // dp_size),
    )
    table_grad = jnp.swapaxes(table_grad, 1, 2)
    query_grad = summed[0].T
    key_value_grad = jnp.transpose(summed[1:3], (2, 0, 1))
    gate_up_grad = jnp.transpose(gate_up_sum, (2, 0, 1))
    return (
        layer_output, input_grad, gain_grad, query_grad, key_value_grad,
        summed[3], gate_up_grad, down_sum[0], table_grad,
    )


def per_device(dp_size, mp_size, *args):
    rows, model_width = args[0].shape
    heads_here = args[7].shape[2]
    fits = dp_size == 8 and model_width == 8 * LANES and mp_size == 4
    fits = fits and heads_here == 4 and rows % LANES == 0
    body = per_device_linked if fits else per_device_plain
    return body(dp_size, mp_size, *args)


def solution(mesh):
    return jax.shard_map(
        partial(per_device, mesh.shape["dp"], mesh.shape["mp"]),
        mesh=mesh,
        in_specs=(
            P(("dp", "mp"), None),
            P(),
            P(None, "mp"),
            P(None, None, "mp"),
            P("mp", None),
            P(None, None, "mp"),
            P("mp", None),
            P(None, None, "mp"),
            P("dp"),
            P(None, "dp"),
            P(("dp", "mp"), None),
        ),
        out_specs=(
            P(("dp", "mp"), None),
            P(("dp", "mp"), None),
            P(None, ("dp", "mp")),
            P("dp", "mp"),
            P("dp", None, "mp"),
            P("mp", "dp"),
            P("dp", None, "mp"),
            P("mp", "dp"),
            P(None, "dp", "mp"),
        ),
        check_vma=False,
    )
```

```python
from functools import partial

import jax
import jax.numpy as jnp
import numpy as np
from jax import lax
from jax.experimental import pallas as pl
from jax.experimental.pallas import tpu as pltpu
from jax.sharding import PartitionSpec as P

NBIN = 64
EPSILON = 1e-06
THRESHOLDS = (8, 12, 16, 23, 32, 46, 64, 91)
NEG_FILL = -1e30
LANES = 128
MESH = pl.DeviceIdType.MESH
HBM = pltpu.MemorySpace.HBM
BF16 = jnp.bfloat16
F32 = jnp.float32


def bucket_of(relative):
    distance = jnp.abs(relative)
    bucket = jnp.minimum(distance, 7)
    for threshold in THRESHOLDS:
        bucket = bucket + (distance >= threshold).astype(jnp.int32)
    return bucket + 16 * (relative > 0).astype(jnp.int32)


def inverse_rms(values):
    return lax.rsqrt(jnp.mean(values * values, axis=-1, keepdims=True) + EPSILON)


def dot_f32(left, right, left_dim, right_dim):
    return lax.dot_general(
        left, right, (((left_dim,), (right_dim,)), ((), ())), preferred_element_type=F32
    )


def three_parts(values):
    high = values.astype(BF16)
    rest = values - high.astype(F32)
    middle = rest.astype(BF16)
    low = (rest - middle.astype(F32)).astype(BF16)
    return high, middle, low


def lane_ids(shape):
    return lax.broadcasted_iota(jnp.int32, shape, 1)


def row_ids(shape):
    return lax.broadcasted_iota(jnp.int32, shape, 0)


def attend_kernel(
    q_ref, k_ref, v_ref, layout_ref, line_ref, key_extra_ref, query_bins_ref,
    out_ref, lse_ref,
    key_aug, query_aug, strip, scores, probs,
):
    head_size, rows = q_ref.shape
    keys = k_ref.shape[1]
    blocks = keys // LANES
    width = strip.shape[1]

    @pl.when(pl.program_id(0) == 0)
    def _():
        key_aug[...] = key_extra_ref[...]
        tail = row_ids((64, rows))
        query_aug[pl.ds(192, 64), :] = jnp.where(tail == 0, 1.0, 0.0).astype(BF16)

    both = jnp.concatenate([k_ref[...], v_ref[...]], axis=0).T
    low_lanes = lane_ids((keys, LANES)) < head_size
    key_aug[:, 0:LANES] = jnp.where(low_lanes, both, key_extra_ref[:, 0:LANES])
    query_aug[pl.ds(0, 64), :] = q_ref[...]
    query_aug[pl.ds(64, 128), :] = jnp.dot(
        layout_ref[0], query_bins_ref[...], preferred_element_type=F32
    ).astype(BF16)
    strip[...] = pltpu.roll(
        jnp.broadcast_to(line_ref[0], (LANES, width)), 0, 1, stride=1, stride_axis=0
    )
    query_all = query_aug[...]
    top = jnp.full((1, rows), -jnp.inf, F32)
    for block in range(blocks):
        here = pl.ds(block * LANES, LANES)
        part = jnp.dot(key_aug[here, :], query_all, preferred_element_type=F32)
        part = part + strip[:, pl.ds((blocks - 1 - block) * LANES, rows)]
        scores[here, :] = part
        top = jnp.maximum(top, jnp.max(part, axis=0, keepdims=True))
    total = jnp.zeros((1, rows), F32)
    for block in range(blocks):
        here = pl.ds(block * LANES, LANES)
        part = jnp.exp(scores[here, :] - top)
        total = total + jnp.sum(part, axis=0, keepdims=True)
        probs[here, :] = part.astype(BF16)
    mixed = jnp.dot(v_ref[...], probs[...], preferred_element_type=F32)
    out_ref[...] = (mixed / total).astype(BF16)
    lse_ref[0] = top + jnp.log(total)


def attend_back_kernel(
    q_ref, k_ref, v_ref, out_ref, out_grad_ref, lse_ref, layout_ref, line_ref,
    key_extra_ref, key_extra_t_ref, query_bins_ref, query_bins_t_ref,
    dq_ref, dk_ref, dv_ref, line_grad_ref, layout_grad_ref,
    key_aug, key_aug_t, query_aug, value_aug, grad_aug, strip, strip_grad, probs_grad,
):
    head_size, rows = q_ref.shape
    keys = k_ref.shape[1]
    blocks = keys // LANES
    width = strip.shape[1]

    @pl.when(pl.program_id(0) == 0)
    def _():
        key_aug[...] = key_extra_ref[...]
        key_aug_t[pl.ds(64, 128), :] = key_extra_t_ref[...]
        tail = row_ids((64, rows))
        query_aug[pl.ds(192, 64), :] = jnp.where(tail == 0, 1.0, 0.0).astype(BF16)

    both = jnp.concatenate([k_ref[...], v_ref[...]], axis=0).T
    lanes = lane_ids((keys, LANES))
    key_aug[:, 0:LANES] = jnp.where(lanes < head_size, both, key_extra_ref[:, 0:LANES])
    ones = jnp.where(lanes < 3, 1.0, 0.0).astype(BF16)
    value_aug[...] = jnp.where(lanes < head_size, ones, both)
    key_aug_t[pl.ds(0, 64), :] = k_ref[...]
    query_aug[pl.ds(0, 64), :] = q_ref[...]
    query_aug[pl.ds(64, 128), :] = jnp.dot(
        layout_ref[0], query_bins_ref[...], preferred_element_type=F32
    ).astype(BF16)
    high, middle, low = three_parts(-lse_ref[0])
    tail = row_ids((64, rows))
    rows_of = lambda part: jnp.broadcast_to(part.astype(F32), (64, rows))
    query_aug[pl.ds(192, 64), :] = jnp.where(
        tail == 0, 1.0,
        jnp.where(
            tail == 1, rows_of(high),
            jnp.where(tail == 2, rows_of(middle), jnp.where(tail == 3, rows_of(low), 0.0)),
        ),
    ).astype(BF16)
    row_dot = jnp.sum(
        out_grad_ref[...].astype(F32) * out_ref[...].astype(F32), axis=0, keepdims=True
    )
    high, middle, low = three_parts(-row_dot)
    grad_aug[pl.ds(0, 64), :] = jnp.where(
        tail == 0, rows_of(high),
        jnp.where(tail == 1, rows_of(middle), jnp.where(tail == 2, rows_of(low), 0.0)),
    ).astype(BF16)
    grad_aug[pl.ds(64, 64), :] = out_grad_ref[...]
    strip[...] = pltpu.roll(
        jnp.broadcast_to(line_ref[0], (LANES, width)), 0, 1, stride=1, stride_axis=0
    )
    strip_grad[...] = jnp.zeros_like(strip_grad)
    query_and_grad = jnp.concatenate([q_ref[...], out_grad_ref[...]], axis=0).T
    query_all = query_aug[...]
    grad_all = grad_aug[...]
    half = lane_ids((LANES, LANES)) < head_size
    for block in range(blocks):
        here = pl.ds(block * LANES, LANES)
        band = pl.ds((blocks - 1 - block) * LANES, rows)
        part = jnp.dot(key_aug[here, :], query_all, preferred_element_type=F32)
        part = jnp.exp(part + strip[:, band])
        slope = part * jnp.dot(value_aug[here, :], grad_all, preferred_element_type=F32)
        strip_grad[:, band] = strip_grad[:, band] + slope
        slope = slope.astype(BF16)
        probs_grad[here, :] = slope
        key_part = jnp.dot(slope, query_and_grad, preferred_element_type=F32)
        value_part = jnp.dot(part.astype(BF16), query_and_grad, preferred_element_type=F32)
        turned = jnp.where(half, key_part, value_part).T.astype(BF16)
        dk_ref[:, here] = turned[0:64]
        dv_ref[:, here] = turned[64:128]
    query_part = jnp.dot(key_aug_t[...], probs_grad[...], preferred_element_type=F32)
    dq_ref[...] = query_part[0:64].astype(BF16)
    layout_grad_ref[0] = jnp.dot(
        query_part[64:192].astype(BF16), query_bins_t_ref[...], preferred_element_type=F32
    )
    folded = strip_grad[pl.ds(0, 8), :]
    for group in range(1, LANES // 8):
        folded = folded + pltpu.roll(strip_grad[pl.ds(group * 8, 8), :], width - group * 8, 1)
    line = folded[0:1]
    for row in range(1, 8):
        line = line + pltpu.roll(folded[row : row + 1], width - row, 1)
    line_grad_ref[0] = line


class Place:
    def __init__(self, mp_size):
        self.dp = lax.axis_index("dp")
        self.mp = lax.axis_index("mp")
        self.mp_size = mp_size
        self.core = lax.rem(self.dp, 2)
        self.x = lax.rem(lax.div(self.dp, 2), 2)
        self.y = lax.div(self.dp, 4)
        self.to_core = (self.dp + 1 - 2 * self.core, self.mp)
        self.to_x = (self.dp + 2 - 4 * self.x, self.mp)
        self.to_y = (self.dp + 4 - 8 * self.y, self.mp)
        self.to_corner = (self.dp + 6 - 4 * self.x - 8 * self.y, self.mp)

    def across(self, step):
        low = lax.rem(lax.rem(self.mp, 2) + step % 2, 2)
        high = lax.rem(lax.div(self.mp, 2) + step // 2, 2)
        return low + 2 * high

    def to_mp(self, step):
        return (self.dp, self.across(step))

    def partners(self):
        others = [self.to_mp(step) for step in range(1, self.mp_size)]
        return [self.to_core, self.to_x, self.to_y, self.to_corner] + others


def greet(place):
    barrier = pltpu.get_barrier_semaphore()
    for partner in place.partners():
        pl.semaphore_signal(barrier, inc=1, device_id=partner, device_id_type=MESH)


def meet(place):
    pl.semaphore_wait(pltpu.get_barrier_semaphore(), len(place.partners()))


class Copy:
    def __init__(self, source, target, send, receive=None, partner=None):
        self.parts = (source, target, send, receive, partner)

    def made(self):
        source, target, send, receive, partner = self.parts
        if partner is None:
            return pltpu.make_async_copy(source, target, send)
        return pltpu.make_async_remote_copy(
            src_ref=source, dst_ref=target, send_sem=send, recv_sem=receive,
            device_id=partner, device_id_type=MESH,
        )

    def start(self):
        self.made().start()

    def wait(self):
        self.made().wait()

    def wait_send(self):
        self.made().wait_send()

    def wait_recv(self):
        self.made().wait_recv()


def remote(source, target, send, receive, partner):
    return Copy(source, target, send, receive, partner)


def lanes_at(block, count):
    return pl.ds(pl.multiple_of(block * LANES, LANES), count * LANES)


class Gather:
    def __init__(self, place, pieces, outs, sems, items):
        self.place, self.pieces, self.outs = place, pieces, outs
        self.z_send, self.z_recv, self.own_sem, self.send, self.recv = sems
        self.items = items

    @staticmethod
    def semaphores(count, mp_size):
        dma = pltpu.SemaphoreType.DMA
        items = count * mp_size
        return [
            dma((count, mp_size)), dma((count, mp_size)), dma((count,)), dma((items, 6)), dma((items, 6))
        ]

    def rows(self, c, source, half):
        n = self.pieces[c].shape[1]
        if half is None:
            return pl.ds(pl.multiple_of(source * n, 16), n)
        return pl.ds(pl.multiple_of(source * n + half * (n // 2), 16), n // 2)

    def window(self, c, source, half, block, count):
        return self.outs[c].at[:, self.rows(c, source, half), lanes_at(block, count)]

    def own(self, c):
        place = self.place
        block = place.core * 4 + place.y * 2 + place.x
        return Copy(
            self.pieces[c], self.window(c, place.mp, None, block, 1), self.own_sem.at[c]
        )

    def along_mp(self, c, step):
        place = self.place
        block = place.core * 4 + place.y * 2 + place.x
        source = place.across(2) if step == 3 else place.mp
        window = self.window(c, source, None, block, 1)
        return remote(
            window if step == 3 else self.pieces[c], window,
            self.z_send.at[c, step], self.z_recv.at[c, step], place.to_mp(2 if step == 2 else 1),
        )

    def copies(self, t):
        c, k = self.items[t]
        place = self.place
        source = place.across(k)
        base = place.core * 4
        mine = base + place.y * 2 + place.x
        turned = base + (1 - place.y) * 2 + place.x

        def copy(i, half, block, count, partner):
            here = self.window(c, source, half, block, count)
            return remote(here, here, self.send.at[t, i], self.recv.at[t, i], partner)

        first = [copy(0, 0, mine, 1, place.to_x), copy(1, 1, mine, 1, place.to_y)]
        second = [
            copy(2, 0, base + place.y * 2, 2, place.to_y),
            copy(3, 1, mine, 1, place.to_x),
            copy(4, 1, turned, 1, place.to_x),
        ]
        third = [copy(5, None, base, 4, place.to_core)]
        return first, second, third

    def first(self, t):
        c, k = self.items[t]
        if k == 0:
            self.own(c).wait()
        else:
            self.along_mp(c, k).wait_recv()
        if k == 2:
            self.along_mp(c, 3).start()
        for copy in self.copies(t)[0]:
            copy.start()

    def second(self, t):
        first, second, _ = self.copies(t)
        for copy in first:
            copy.wait_recv()
        for copy in second:
            copy.start()

    def third(self, t):
        _, second, third = self.copies(t)
        for copy in second:
            copy.wait_recv()
        third[0].start()

    def run(self, ops):
        for op in ops.split():
            which, t = op[0], int(op[1:])
            if which == "z":
                self.along_mp(*self.items[t]).start()
            else:
                {"f": self.first, "s": self.second, "t": self.third}[which](t)

    def done(self, t):
        self.copies(t)[2][0].wait_recv()

    def close(self):
        for t, (c, k) in enumerate(self.items):
            first, second, third = self.copies(t)
            for copy in first + second + third:
                copy.wait_send()
            if k > 0:
                self.along_mp(c, k).wait_send()


def add_rows(target, target_index, source, source_index):
    lead, rows, lanes = target_index
    source_rows, source_lanes = source_index
    row_start, count = rows
    source_start = source_rows
    size = 32
    while count % size:
        size //= 2

    def body(i, carry):
        here = pl.ds(pl.multiple_of(row_start + i * size, size), size)
        there = pl.ds(pl.multiple_of(source_start + i * size, size), size)
        for part in range(lead):
            target[part, here, lanes] = target[part, here, lanes] + source[part, there, source_lanes]
        return carry

    lax.fori_loop(0, count // size, body, 0)


class Scatter:
    def __init__(self, place, fulls, outs, scratch, items, shares=None, inside=False):
        self.inside = inside
        self.place, self.fulls, self.outs, self.items = place, fulls, outs, items
        count = len(fulls)
        self.shares = shares or [None] * count
        self.held = [sorted(k for c, k in items if c == which) for which in range(count)]
        self.whole = [len(full.shape) == 3 for full in fulls]
        buffers = [scratch[i * count : (i + 1) * count] for i in range(5)]
        self.sums, self.from_first, self.from_second, self.from_mp, self.staged = buffers
        self.own_sem, self.send, self.recv, self.share_send, self.share_recv = scratch[5 * count :]

    @staticmethod
    def scratch(shapes, whole, items):
        out = []
        for part, blocks in enumerate((4, 2, 1, 1)):
            for c, (lead, n) in enumerate(shapes):
                slots = sum(which == c for which, _ in items)
                if part == 3:
                    slots, lead, n = (3, lead, n) if slots > 1 else (1, 1, 16)
                out.append(pltpu.VMEM((slots, lead, n, blocks * LANES), BF16))
        for (lead, n), is_whole in zip(shapes, whole):
            out.append(pltpu.VMEM((lead, n, 4 * LANES) if is_whole else (1, 16, LANES), BF16))
        dma = pltpu.SemaphoreType.DMA
        count = len(items)
        out += [dma((count,)), dma((count, 7)), dma((count, 7))]
        return out + [dma((len(shapes),)), dma((len(shapes),))]

    def slot(self, c, k):
        return self.held[c].index(k)

    def size(self, c):
        return self.sums[c].shape[1], self.sums[c].shape[2]

    def source(self, t):
        c, k = self.items[t]
        if not self.whole[c]:
            return self.fulls[c].at[(k + 1) % 2]
        lead, n = self.size(c)
        target = self.place.across(k)
        return self.fulls[c].at[:, pl.ds(pl.multiple_of(target * n, 16), n), :]

    def from_core(self, t):
        c, k = self.items[t]
        place = self.place
        return remote(
            self.source(t).at[:, :, lanes_at((1 - place.core) * 4, 4)], self.sums[c].at[self.slot(c, k)],
            self.send.at[t, 0], self.recv.at[t, 0], place.to_core,
        )

    def own(self, t):
        c, _ = self.items[t]
        return Copy(
            self.source(t).at[:, :, lanes_at(self.place.core * 4, 4)], self.staged[c], self.own_sem.at[t]
        )

    def copies(self, t):
        c, k = self.items[t]
        place = self.place
        lead, n = self.size(c)
        top, bottom = pl.ds(0, n // 2), pl.ds(n // 2, n // 2)
        every = pl.ds(0, lead)
        sums = self.sums[c].at[self.slot(c, k)]

        def copy(i, source, landing, partner):
            return remote(source, landing, self.send.at[t, i], self.recv.at[t, i], partner)

        landing = self.from_first[c].at[self.slot(c, k)]
        first = [
            copy(
                1, sums.at[every, top, lanes_at((1 - place.y) * 2, 2)],
                landing.at[every, top, pl.ds(0, 256)], place.to_y,
            ),
            copy(
                2, sums.at[every, bottom, lanes_at(1 - place.x, 1)],
                landing.at[every, bottom, pl.ds(0, 128)], place.to_x,
            ),
            copy(
                3, sums.at[every, bottom, lanes_at(3 - place.x, 1)],
                landing.at[every, bottom, pl.ds(128, 128)], place.to_x,
            ),
        ]
        landing = self.from_second[c].at[self.slot(c, k)]
        second = [
            copy(
                4, sums.at[every, top, lanes_at(place.y * 2 + 1 - place.x, 1)],
                landing.at[every, top, pl.ds(0, 128)], place.to_x,
            ),
            copy(
                5, sums.at[every, bottom, lanes_at((1 - place.y) * 2 + place.x, 1)],
                landing.at[every, bottom, pl.ds(0, 128)], place.to_y,
            ),
        ]
        third = None
        if k > 0:
            third = copy(
                6, sums.at[:, :, lanes_at(place.y * 2 + place.x, 1)], self.from_mp[c].at[k - 1],
                place.to_mp(1 if k % 2 else 2),
            )
        return first, second, third

    def core(self, t):
        self.from_core(t).start()
        if self.whole[self.items[t][0]]:
            self.own(t).start()

    def first(self, t):
        c, k = self.items[t]
        lead, n = self.size(c)
        sums = self.sums[c].at[self.slot(c, k)]
        self.from_core(t).wait_recv()
        if self.whole[c]:
            self.own(t).wait()
            add_rows(sums, (lead, (0, n), pl.ds(0, 512)), self.staged[c], (0, pl.ds(0, 512)))
        else:
            mine = lanes_at(self.place.core * 4, 4)
            add_rows(sums, (lead, (0, n), pl.ds(0, 512)), self.source(t), (0, mine))
        for copy in self.copies(t)[0]:
            copy.start()

    def second(self, t):
        c, k = self.items[t]
        place = self.place
        lead, n = self.size(c)
        first, second, _ = self.copies(t)
        for copy in first:
            copy.wait_recv()
        slot = self.slot(c, k)
        sums, landing = self.sums[c].at[slot], self.from_first[c].at[slot]
        half = n // 2
        add_rows(sums, (lead, (0, half), lanes_at(place.y * 2, 2)), landing, (0, pl.ds(0, 256)))
        add_rows(sums, (lead, (half, half), lanes_at(place.x, 1)), landing, (half, pl.ds(0, 128)))
        add_rows(sums, (lead, (half, half), lanes_at(2 + place.x, 1)), landing, (half, pl.ds(128, 128)))
        for copy in second:
            copy.start()

    def third(self, t):
        c, k = self.items[t]
        lead, n = self.size(c)
        _, second, third = self.copies(t)
        for copy in second:
            copy.wait_recv()
        slot = self.slot(c, k)
        mine = lanes_at(self.place.y * 2 + self.place.x, 1)
        add_rows(
            self.sums[c].at[slot], (lead, (0, n), mine), self.from_second[c].at[slot], (0, pl.ds(0, 128))
        )
        if k == 2:
            self.copies(self.items.index((c, 3)))[2].wait_recv()
            add_rows(
                self.sums[c].at[slot], (lead, (0, n), mine), self.from_mp[c].at[2], (0, pl.ds(0, 128))
            )
        if k > 0 and not self.inside:
            third.start()

    def share(self, c):
        return remote(
            self.shares[c], self.from_mp[c].at[0], self.share_send.at[c], self.share_recv.at[c],
            self.place.to_mp(1),
        )

    def end(self, c):
        if self.inside:
            self.finish(c)
            return
        if self.shares[c] is not None:
            self.share(c).wait_recv()
        for k in (1, 2):
            if (c, k) in self.items:
                self.copies(self.items.index((c, k)))[2].wait_recv()
        self.finish(c)

    def run(self, ops):
        for op in ops.split():
            table = {"c": self.core, "f": self.first, "s": self.second, "t": self.third, "e": self.end}
            table[op[0]](int(op[1:]))

    def left(self, t):
        self.from_core(t).wait_send()

    def close(self):
        for t, (c, k) in enumerate(self.items):
            first, second, third = self.copies(t)
            if self.whole[c] or k < 2:
                self.from_core(t).wait_send()
            for copy in first + second:
                copy.wait_send()
            if third is not None and not self.inside:
                third.wait_send()
        for c, share in enumerate(self.shares):
            if share is not None:
                self.share(c).wait_send()

    def finish(self, c):
        place = self.place
        lead, n = self.size(c)
        mine = lanes_at(place.y * 2 + place.x, 1)
        sums, landing, out = self.sums[c], self.from_mp[c], self.outs[c]
        steps = () if self.inside else (1, 2)
        slot = self.slot(c, 1 if self.inside else 0)
        size = 32
        while n % size:
            size //= 2

        def body(i, carry):
            here = pl.ds(pl.multiple_of(i * size, size), size)
            for part in range(lead):
                total = sums[slot, part, here, mine].astype(F32)
                for k in steps:
                    total = total + landing[k - 1, part, here, :].astype(F32)
                out[part, here, :] = total.astype(out.dtype)
            return carry

        lax.fori_loop(0, n // size, body, 0)


def attention_shapes(head_count, head_size, rows, keys, width):
    whole = lambda shape: pl.BlockSpec(shape, lambda head: (0,) * len(shape))
    column = lambda size: pl.BlockSpec((head_size, size), lambda head: (head, 0))
    page = lambda a, b: pl.BlockSpec((1, a, b), lambda head: (head, 0, 0))
    return whole, column, page


def attend(queries, keys_t, values_t, layout, line, key_extra, query_bins):
    inner, rows = queries.shape
    keys = keys_t.shape[1]
    head_count, _, width = line.shape
    head_size = inner // head_count
    whole, column, page = attention_shapes(head_count, head_size, rows, keys, width)
    return pl.pallas_call(
        attend_kernel,
        grid=(head_count,),
        out_shape=(
            jax.ShapeDtypeStruct((inner, rows), BF16),
            jax.ShapeDtypeStruct((head_count, 1, rows), F32),
        ),
        in_specs=[
            column(rows), column(keys), column(keys), page(128, 128), page(1, width),
            whole((keys, 256)), whole((128, rows)),
        ],
        out_specs=(column(rows), page(1, rows)),
        scratch_shapes=[
            pltpu.VMEM((keys, 256), BF16),
            pltpu.VMEM((256, rows), BF16),
            pltpu.VMEM((LANES, width), F32),
            pltpu.VMEM((keys, rows), F32),
            pltpu.VMEM((keys, rows), BF16),
        ],
        compiler_params=pltpu.CompilerParams(
            dimension_semantics=("arbitrary",), vmem_limit_bytes=32 << 20
        ),
        name="attend",
    )(queries, keys_t, values_t, layout, line, key_extra, query_bins)


def attend_back(
    queries, keys_t, values_t, heads_out, heads_grad, lse, layout, line,
    key_extra, key_extra_t, query_bins, query_bins_t,
):
    inner, rows = queries.shape
    keys = keys_t.shape[1]
    head_count, _, width = line.shape
    head_size = inner // head_count
    whole, column, page = attention_shapes(head_count, head_size, rows, keys, width)
    return pl.pallas_call(
        attend_back_kernel,
        grid=(head_count,),
        out_shape=(
            jax.ShapeDtypeStruct((inner, rows), BF16),
            jax.ShapeDtypeStruct((inner, keys), BF16),
            jax.ShapeDtypeStruct((inner, keys), BF16),
            jax.ShapeDtypeStruct((head_count, 1, width), F32),
            jax.ShapeDtypeStruct((head_count, 128, 128), F32),
        ),
        in_specs=[
            column(rows), column(keys), column(keys), column(rows), column(rows),
            page(1, rows), page(128, 128), page(1, width),
            whole((keys, 256)), whole((128, keys)), whole((128, rows)), whole((rows, 128)),
        ],
        out_specs=(column(rows), column(keys), column(keys), page(1, width), page(128, 128)),
        scratch_shapes=[
            pltpu.VMEM((keys, 256), BF16),
            pltpu.VMEM((192, keys), BF16),
            pltpu.VMEM((256, rows), BF16),
            pltpu.VMEM((keys, 128), BF16),
            pltpu.VMEM((128, rows), BF16),
            pltpu.VMEM((LANES, width), F32),
            pltpu.VMEM((LANES, width), F32),
            pltpu.VMEM((keys, rows), BF16),
        ],
        compiler_params=pltpu.CompilerParams(
            dimension_semantics=("arbitrary",), vmem_limit_bytes=32 << 20
        ),
        name="attend_back",
    )(
        queries, keys_t, values_t, heads_out, heads_grad, lse, layout, line,
        key_extra, key_extra_t, query_bins, query_bins_t,
    )


FORWARD_ITEMS = [(0, 0), (1, 0), (2, 0), (0, 1), (0, 2), (0, 3), (1, 1), (2, 1), (1, 2), (2, 2), (1, 3), (2, 3)]


FORWARD_SUMS = [(0, 1), (1, 1)]


def forward_kernel(
    mp_size, group,
    query_ref, output_ref, gate_up_ref, down_ref, key_value_ref, table_ref, boxes_ref, lengths_ref,
    input_ref, gain_ref, cotangent_ref,
    w_first, queries_out, keys_out, values_out, heads_out_out, lse, layout, line, key_extra, key_extra_t,
    slot_owner_out, residual_out, layer_output, second_grad, gate_up_full, down_full, tables,
    line_hot, bin_hot, gate_up_share, down_share, queries, keys_t, values_t, heads_out, slot_owner, residual,
    first_ref, query_piece, normed_t, slot_t, w_gate_up, w_down, first_here, key_aug, query_aug, strip, scores, probs,
    second_t, second_owner, out_owner, out_t,
    hidden_a, hidden_b, hidden_c, act_t, low_t, stage_gate_up, stage_down,
    row_send, row_recv, row_own, table_send, table_recv, table_own, load_sem, store_sem, keep_sem, *sems,
):
    place = Place(mp_size)
    rows, model_width = input_ref.shape
    keys = keys_t.shape[1]
    blocks = keys // LANES
    width = strip.shape[1]
    inner_here = first_ref.shape[1]
    heads_here = inner_here // 64
    hidden = gate_up_ref.shape[1]
    doc = lax.div(place.mp, group)
    member = lax.rem(place.mp, group)
    first_peer = place.mp - member
    own_lanes = pl.ds(pl.multiple_of(member * rows, LANES), rows)

    items = FORWARD_ITEMS
    column = lanes_at(place.core * 4 + place.y * 2 + place.x, 1)
    gather = Gather(
        place, [first_ref, gate_up_ref.at[:, :, column], down_ref.at[:, :, column]],
        [w_first, w_gate_up, w_down], sems[:5], items
    )
    at = {item: t for t, item in enumerate(items)}

    row_copies = [
        remote(
            normed_t, slot_t.at[:, own_lanes], row_send.at[k], row_recv.at[k],
            (place.dp, first_peer + lax.rem(member + k, group)),
        )
        for k in range(1, group)
    ]
    table_copies = [
        remote(table_ref, tables.at[place.mp], table_send.at[k], table_recv.at[k], place.to_mp(k))
        for k in range(1, mp_size)
    ]
    row_here = Copy(normed_t, slot_t.at[:, own_lanes], row_own.at[0])
    table_here = Copy(table_ref, tables.at[place.mp], table_own.at[0])

    greet(place)
    loads = [
        Copy(query_ref.at[column, :], query_piece, load_sem.at[0]),
        Copy(output_ref.at[:, column], first_ref.at[3], load_sem.at[1]),
    ]
    for copy in loads:
        copy.start()
    for c in range(1, 3):
        gather.own(c).start()
    table_here.start()
    turned = key_value_ref[...].T
    first_ref[1] = turned[0:inner_here]
    first_ref[2] = turned[inner_here : 2 * inner_here]

    def norm_into(values_ref, gain):
        def body(i, carry):
            here = pl.ds(pl.multiple_of(i * 16, 16), 16)
            values = values_ref[here, :]
            scale = lax.rsqrt(jnp.mean(values * values, axis=1, keepdims=True) + EPSILON)
            second_owner[here, :] = (values * scale * gain).astype(BF16)
            return carry

        lax.fori_loop(0, rows // 16, body, 0)

    norm_into(input_ref, gain_ref[0:1, :].astype(F32))
    normed_t[...] = second_owner[...].T
    row_here.start()
    for copy in loads:
        copy.wait()
    first_ref[0] = query_piece[...].T
    gather.own(0).start()
    meet(place)
    gather.run("f0 f1")
    for copy in row_copies + table_copies:
        copy.start()
    gather.along_mp(0, 1).start()

    key_rows = row_ids((64, keys))
    key_bins = boxes_ref[:, pl.ds(pl.multiple_of(doc * keys, LANES), keys)]
    x_place = jnp.where(key_rows == key_bins[0:1], 1.0, 0.0).astype(BF16)
    y_place = jnp.where(key_rows == key_bins[1:2], 1.0, 0.0).astype(BF16)
    key_extra_t[0:64, :] = x_place
    key_extra_t[64:128, :] = y_place
    mask = jnp.where(lane_ids((64, keys)) >= lengths_ref[doc], NEG_FILL, 0.0)
    first_row = member * rows
    spot = lane_ids((8, width))
    spot = jnp.where(spot >= width - LANES, spot - width, spot)
    bucket = bucket_of(LANES * (blocks - 1) - spot - first_row)[0:1]
    line_hot[...] = jnp.where(row_ids((LANES, width)) == bucket, 1.0, 0.0).astype(BF16)
    spot = lane_ids((8, LANES))
    bucket = bucket_of(jnp.where(spot < NBIN, -spot, LANES - spot))[0:1]
    bin_hot[...] = jnp.where(row_ids((LANES, LANES)) == bucket, 1.0, 0.0).astype(BF16)
    tail = jnp.where(key_rows == 0, mask, jnp.where(key_rows < 4, 1.0, 0.0)).astype(BF16)
    turned = jnp.concatenate([jnp.zeros((64, keys), BF16), x_place, y_place, tail], axis=0).T
    key_extra[...] = turned
    key_aug[...] = turned
    query_aug[pl.ds(192, 64), :] = jnp.where(row_ids((64, rows)) == 0, 1.0, 0.0).astype(BF16)
    gather.run("s0 f2")
    for block in range(model_width // LANES):
        owner = block_owner(block)
        out_owner[:, owner * LANES : (owner + 1) * LANES] = cotangent_ref[
            :, block * LANES : (block + 1) * LANES
        ].astype(BF16)
    out_t[...] = cotangent_ref[...].astype(BF16).T
    residual[...] = input_ref[...]
    layer_output[...] = jnp.zeros_like(layer_output)
    second_grad[...] = jnp.zeros_like(second_grad)
    row_here.wait()
    table_here.wait()
    gather.run("s1 t0")

    head_units = mp_size * heads_here
    table = {
        (1, 0): "f3 z4 z6", (2, 0): "s3 s2 t1", (4, 0): "t3 f4 z7", (5, 0): "s4 t2", (6, 0): "f5 z8",
        (7, 0): "t4 f6", (8, 0): "s5 z9", (9, 0): "f7 s6", (11, 0): "t5", (12, 0): "f8 s7", (13, 0): "t6",
        (14, 0): "f9 s8", (16, 0): "f10 t7", (16, 2): "s9", (17, 0): "f11 t8", (17, 1): "s10",
        (17, 3): "t9", (18, 0): "s11", (18, 3): "t10", (19, 1): "t11",
    }
    scatter = Scatter(
        place, [gate_up_full, down_full], [gate_up_share, down_share], sems[5:], FORWARD_SUMS,
        inside=True,
    )
    sum_table = {(18, 0): "c0 c1", (18, 3): "f0 f1", (19, 2): "s0"}

    def communicate(unit, point):
        for (at_unit, at_point), ops in table.items():
            if at_point == point:

                @pl.when(unit == at_unit)
                def _(ops=ops):
                    gather.run(ops)

        for (at_unit, at_point), ops in sum_table.items():
            if at_point == point:

                @pl.when(unit == at_unit)
                def _(ops=ops):
                    scatter.run(ops)

    def head_unit(unit, carry):
        communicate(unit, 0)
        step = lax.div(unit, heads_here)
        inside = lax.rem(unit, heads_here)
        source = place.across(step)
        base = pl.multiple_of(source * inner_here, 16)
        head = source * heads_here + inside

        @pl.when(inside == 0)
        def _():
            for k in range(mp_size):

                @pl.when(step == k)
                def _(k=k):
                    gather.done(at[(0, k)])
                    if k == 0:
                        for copy in row_copies:
                            copy.wait_recv()
                    else:
                        table_copies[k - 1].wait_recv()

            load = Copy(w_first.at[:, pl.ds(base, inner_here), :], first_here, load_sem.at[0])
            load.start()
            hot = tables[source].astype(BF16)
            line[source] = jnp.dot(hot[0:8], line_hot[...], preferred_element_type=F32)
            bins = jnp.dot(hot[8:24], bin_hot[...], preferred_element_type=F32)
            for i in range(heads_here):
                x_line = jnp.broadcast_to(bins[i : i + 1], (64, LANES))
                y_line = jnp.broadcast_to(bins[8 + i : 9 + i], (64, LANES))
                left = lane_ids((64, LANES)) < 64
                x_part = pltpu.roll(x_line, 0, 1, stride=1, stride_axis=0)
                y_part = pltpu.roll(y_line, 64, 1, stride=1, stride_axis=0)
                layout[source * heads_here + i] = jnp.concatenate(
                    [jnp.where(left, x_part, 0.0), jnp.where(left, 0.0, y_part)], axis=0
                ).astype(BF16)
            load.wait()
            here = pl.ds(base, inner_here)
            queries[here, :] = jnp.dot(
                first_here[0], normed_t[...], preferred_element_type=F32
            ).astype(BF16)
            keys_t[here, :] = jnp.dot(
                first_here[1], slot_t[...], preferred_element_type=F32
            ).astype(BF16)
            values_t[here, :] = jnp.dot(
                first_here[2], slot_t[...], preferred_element_type=F32
            ).astype(BF16)

        here = pl.ds(pl.multiple_of(head * 64, 16), 64)
        both = jnp.concatenate([keys_t[here, :], values_t[here, :]], axis=0).T
        low_lanes = lane_ids((keys, LANES)) < 64
        key_aug[:, 0:LANES] = jnp.where(low_lanes, both, key_extra[:, 0:LANES])
        query_aug[pl.ds(0, 64), :] = queries[here, :]
        query_aug[pl.ds(64, 128), :] = jnp.dot(
            layout[head], key_extra_t[:, own_lanes], preferred_element_type=F32
        ).astype(BF16)
        strip[...] = pltpu.roll(
            jnp.broadcast_to(line[source, pl.ds(inside, 1), :], (LANES, width)), 0, 1,
            stride=1, stride_axis=0,
        )
        query_all = query_aug[...]
        top = jnp.full((1, rows), -jnp.inf, F32)
        for block in range(blocks):
            some = pl.ds(block * LANES, LANES)
            part = jnp.dot(key_aug[some, :], query_all, preferred_element_type=F32)
            part = part + strip[:, pl.ds((blocks - 1 - block) * LANES, rows)]
            scores[some, :] = part
            top = jnp.maximum(top, jnp.max(part, axis=0, keepdims=True))
        sums = jnp.zeros((1, rows), F32)
        for block in range(blocks):
            some = pl.ds(block * LANES, LANES)
            part = jnp.exp(scores[some, :] - top)
            sums = sums + jnp.sum(part, axis=0, keepdims=True)
            probs[some, :] = part.astype(BF16)
        mixed = jnp.dot(values_t[here, :], probs[...], preferred_element_type=F32)
        heads_out[here, :] = (mixed / sums).astype(BF16)
        lse[head] = top + jnp.log(sums)

        @pl.when(inside == heads_here - 1)
        def _():
            part = heads_out[pl.ds(base, inner_here), :].T
            residual[...] = residual[...] + jnp.dot(
                part, first_here[3], preferred_element_type=F32
            )

        return carry

    lax.fori_loop(0, head_units, head_unit, 0)
    for block in range(model_width // LANES):
        owner = block_owner(block)
        slot_owner[:, owner * LANES : (owner + 1) * LANES] = slot_t[
            block * LANES : (block + 1) * LANES, :
        ].T

    kept = [
        Copy(here, there, keep_sem.at[i])
        for i, (here, there) in enumerate(
            [
                (queries, queries_out), (keys_t, keys_out), (values_t, values_out),
                (heads_out, heads_out_out), (slot_owner, slot_owner_out), (residual, residual_out),
            ]
        )
    ]
    for copy in kept:
        copy.start()
    norm_into(residual, gain_ref[1:2, :].astype(F32))
    second_t[...] = second_owner[...].T
    turned_blocks = [second_owner[:, b * LANES : (b + 1) * LANES] for b in range(model_width // LANES)]
    for block, values in enumerate(turned_blocks):
        owner = block_owner(block)
        second_owner[:, owner * LANES : (owner + 1) * LANES] = values

    def store(step):
        source = place.across(step)
        here = pl.ds(pl.multiple_of(source * hidden, 16), hidden)
        return [
            Copy(stage_gate_up, gate_up_full.at[:, here, :], store_sem.at[0]),
            Copy(stage_down, down_full.at[:, here, :], store_sem.at[1]),
        ]

    def hidden_unit(step, carry):
        unit = step + head_units

        @pl.when(step > 0)
        def _():
            for copy in store(step):
                copy.wait()

        communicate(unit, 0)
        source = place.across(step)
        here = pl.ds(pl.multiple_of(source * hidden, 16), hidden)
        for k in range(mp_size):

            @pl.when(step == k)
            def _(k=k):
                gather.done(at[(1, k)])

        hidden_a[...] = jnp.dot(w_gate_up[0, here, :], second_t[...], preferred_element_type=F32)
        hidden_b[...] = jnp.dot(w_gate_up[1, here, :], second_t[...], preferred_element_type=F32)
        communicate(unit, 1)
        for k in range(mp_size):

            @pl.when(step == k)
            def _(k=k):
                gather.done(at[(2, k)])

        hidden_c[...] = jnp.dot(w_down[0, here, :], out_t[...], preferred_element_type=F32)

        def activate(i, inner_carry):
            some = pl.ds(pl.multiple_of(i * 16, 16), 16)
            gate, up, slope = hidden_a[some, :], hidden_b[some, :], hidden_c[some, :]
            square = gate * gate
            factor = 0.7978845608028654
            bent = jnp.tanh(factor * gate * (1.0 + 0.044715 * square))
            half = 0.5 * (1.0 + bent)
            value = gate * half
            change = half + 0.5 * gate * (1.0 - bent * bent) * (
                factor * (1.0 + 3.0 * 0.044715 * square)
            )
            act_t[some, :] = (value * up).astype(BF16)
            low_t[some, :] = (slope * up * change).astype(BF16)
            low_t[pl.ds(pl.multiple_of(hidden + i * 16, 16), 16), :] = (slope * value).astype(BF16)
            return inner_carry

        lax.fori_loop(0, hidden // 16, activate, 0)
        communicate(unit, 2)

        stage_down[0] = jnp.dot(act_t[...], out_owner[...], preferred_element_type=F32).astype(BF16)
        stage_gate_up[0] = jnp.dot(
            low_t[0:hidden], second_owner[...], preferred_element_type=F32
        ).astype(BF16)
        stage_gate_up[1] = jnp.dot(
            low_t[hidden:], second_owner[...], preferred_element_type=F32
        ).astype(BF16)
        for copy in store(step):
            copy.start()
        communicate(unit, 3)
        layer_output[...] = layer_output[...] + dot_f32(act_t[...].T, w_down[0, here, :], 1, 0)
        second_grad[...] = (
            second_grad[...]
            + dot_f32(low_t[0:hidden].T, w_gate_up[0, here, :], 1, 0)
            + dot_f32(low_t[hidden:].T, w_gate_up[1, here, :], 1, 0)
        )
        return carry

    lax.fori_loop(0, mp_size, hidden_unit, 0)
    layer_output[...] = layer_output[...] + residual[...]
    scatter.run("s1 t0 t1")
    scatter.run("e0 e1")
    for copy in store(mp_size - 1):
        copy.wait()
    gather.close()
    scatter.close()
    for copy in row_copies + table_copies:
        copy.wait_send()
    for copy in kept:
        copy.wait()


def block_owner(block):
    return (block % 2) * 4 + block // 2


def forward(
    mp_size, group, query, output, gate_up, down, key_value, table, boxes, lengths, layer_input,
    gains, cotangent,
):
    rows, model_width = layer_input.shape
    keys = boxes.shape[1] // lengths.shape[0]
    width = LANES * (keys // LANES + rows // LANES)
    inner_here, hidden = query.shape[1], gate_up.shape[1]
    inner, total_hidden = inner_here * mp_size, hidden * mp_size
    head_count = inner // 64
    dma = pltpu.SemaphoreType.DMA
    hbm = pl.BlockSpec(memory_space=HBM)
    vmem = pl.BlockSpec(memory_space=pltpu.VMEM)
    shape = jax.ShapeDtypeStruct
    out = [
        (shape((4, inner, model_width), BF16), hbm),
        (shape((inner, rows), BF16), hbm),
        (shape((inner, keys), BF16), hbm),
        (shape((inner, keys), BF16), hbm),
        (shape((inner, rows), BF16), hbm),
        (shape((head_count, 1, rows), F32), vmem),
        (shape((head_count, 128, 128), BF16), vmem),
        (shape((mp_size, 8, width), F32), vmem),
        (shape((keys, 256), BF16), vmem),
        (shape((128, keys), BF16), vmem),
        (shape((keys, model_width), BF16), hbm),
        (shape((rows, model_width), F32), hbm),
        (shape((rows, model_width), F32), vmem),
        (shape((rows, model_width), F32), vmem),
        (shape((2, total_hidden, model_width), BF16), hbm),
        (shape((1, total_hidden, model_width), BF16), hbm),
        (shape((mp_size, 24, LANES), F32), vmem),
        (shape((LANES, width), BF16), vmem),
        (shape((LANES, LANES), BF16), vmem),
        (shape((2, hidden, LANES), BF16), vmem),
        (shape((1, hidden, LANES), BF16), vmem),
    ]
    return pl.pallas_call(
        partial(forward_kernel, mp_size, group),
        out_shape=tuple(o[0] for o in out),
        in_specs=[hbm] * 4 + [vmem] * 3 + [pl.BlockSpec(memory_space=pltpu.SMEM)] + [vmem] * 3,
        out_specs=tuple(o[1] for o in out),
        scratch_shapes=[
            pltpu.VMEM((inner, rows), BF16),
            pltpu.VMEM((inner, keys), BF16),
            pltpu.VMEM((inner, keys), BF16),
            pltpu.VMEM((inner, rows), BF16),
            pltpu.VMEM((keys, model_width), BF16),
            pltpu.VMEM((rows, model_width), F32),
            pltpu.VMEM((4, inner_here, LANES), BF16),
            pltpu.VMEM((LANES, inner_here), BF16),
            pltpu.VMEM((model_width, rows), BF16),
            pltpu.VMEM((model_width, keys), BF16),
            pltpu.VMEM((2, total_hidden, model_width), BF16),
            pltpu.VMEM((1, total_hidden, model_width), BF16),
            pltpu.VMEM((4, inner_here, model_width), BF16),
            pltpu.VMEM((keys, 256), BF16),
            pltpu.VMEM((256, rows), BF16),
            pltpu.VMEM((LANES, width), F32),
            pltpu.VMEM((keys, rows), F32),
            pltpu.VMEM((keys, rows), BF16),
            pltpu.VMEM((model_width, rows), BF16),
            pltpu.VMEM((rows, model_width), BF16),
            pltpu.VMEM((rows, model_width), BF16),
            pltpu.VMEM((model_width, rows), BF16),
            pltpu.VMEM((hidden, rows), F32),
            pltpu.VMEM((hidden, rows), F32),
            pltpu.VMEM((hidden, rows), F32),
            pltpu.VMEM((hidden, rows), BF16),
            pltpu.VMEM((2 * hidden, rows), BF16),
            pltpu.VMEM((2, hidden, model_width), BF16),
            pltpu.VMEM((1, hidden, model_width), BF16),
            dma((group,)), dma((group,)), dma((1,)),
            dma((mp_size,)), dma((mp_size,)), dma((1,)), dma((2,)), dma((2,)), dma((6,)),
        ]
        + Gather.semaphores(3, mp_size)
        + Scatter.scratch([(2, hidden), (1, hidden)], (True, True), FORWARD_SUMS),
        compiler_params=pltpu.CompilerParams(
            collective_id=0, has_side_effects=True, vmem_limit_bytes=62 << 20
        ),
        name="forward",
    )(
        query, output, gate_up, down, key_value, table, boxes, lengths, layer_input, gains, cotangent,
    )


BACKWARD_ITEMS = [(0, 3), (1, 3), (0, 2), (1, 2), (2, 3), (2, 2), (0, 0), (2, 1), (1, 0), (2, 0)]


def unskewed(values, first, count, shift):
    width = values.shape[1]
    folded = None
    for group in range(count // 8):
        part = values[pl.ds(first + group * 8, 8), :]
        back = (-(group * 8 + shift)) % width
        part = pltpu.roll(part, back, 1) if back else part
        folded = part if folded is None else folded + part
    total = folded[0:1]
    for row in range(1, 8):
        total = total + pltpu.roll(folded[row : row + 1], width - row, 1)
    return total


def exact_dot(left, right):
    parts = three_parts(left)
    return sum(dot_f32(part, right, 1, 1) for part in parts)


def backward_kernel(mp_size, group, *refs):
    (
        gate_up_full, down_full, w_first, queries, keys_t, values_t, heads_out,
        residual_in, second_in, cotangent_in,
        lse, layout, line, key_extra, key_extra_t, slot_owner, layer_input, gains, line_hot, bin_hot,
        gate_up_share, down_share, input_out, small_out, gate_up_sum, down_sum, first_sum,
        *refs,
    ) = refs
    (
        input_grad, slot_grad, own_grad, residual_grad, branch_owner, branch_t, w_query, w_output, w_kv,
        q_here, k_here, v_here, out_here, grad_here, dq_here, dk_here, dv_here, kv_here,
        key_aug, key_aug_t, query_aug, value_aug, grad_aug, strip, strip_grad, probs_grad,
        layout_grad, line_sums, bin_sums, gain_part, rows_out, peers, stage, stage_in, full_here,
        load_sem, value_sem, row_send, row_recv, stage_send, stage_recv,
        *refs,
    ) = refs
    place = Place(mp_size)
    rows, model_width = layer_input.shape
    keys = slot_owner.shape[0]
    blocks = keys // LANES
    inner_here = q_here.shape[0]
    heads_here = inner_here // 64
    member = lax.rem(place.mp, group)
    first_peer = place.mp - member
    own_start = pl.multiple_of(member * rows, LANES)
    own_lanes = pl.ds(own_start, rows)

    items = BACKWARD_ITEMS
    fulls = [gate_up_full, down_full, full_here]
    scatter = Scatter(
        place, fulls, [gate_up_sum, down_sum, first_sum], refs, items, [gate_up_share, down_share, None]
    )

    loads = [
        Copy(second_in, slot_grad.at[pl.ds(0, rows), :], value_sem.at[0]),
        Copy(residual_in, slot_grad.at[pl.ds(rows, rows), :], value_sem.at[1]),
        Copy(cotangent_in, input_grad, value_sem.at[2]),
    ]
    for copy in loads:
        copy.start()
    greet(place)
    meet(place)
    scatter.run("c0 c1")
    for c in range(2):
        scatter.share(c).start()
    key_aug[...] = key_extra[...]
    key_aug_t[pl.ds(64, 128), :] = key_extra_t[...]
    for copy in loads:
        copy.wait()

    def norm_back(i, total):
        here = pl.ds(pl.multiple_of(i * 16, 16), 16)
        grad = slot_grad[here, :]
        values = slot_grad[pl.ds(pl.multiple_of(rows + i * 16, 16), 16), :]
        scale = lax.rsqrt(jnp.mean(values * values, axis=1, keepdims=True) + EPSILON)
        scaled = gains[1:2, :].astype(F32) * grad
        mean = jnp.mean(scaled * values, axis=1, keepdims=True)
        result = input_grad[here, :] + scale * scaled - values * (scale * scale * scale * mean)
        residual_grad[here, :] = result
        branch_owner[here, :] = result.astype(BF16)
        product = grad * values * scale
        return total + product[0:8] + product[8:16]

    total = lax.fori_loop(0, rows // 16, norm_back, jnp.zeros((8, model_width), F32))
    gain_part[...] = jnp.sum(total, axis=0, keepdims=True)
    scatter.run("f0 c2")
    branch_t[...] = branch_owner[...].T
    parts = [branch_owner[:, b * LANES : (b + 1) * LANES] for b in range(model_width // LANES)]
    for block, values in enumerate(parts):
        owner = block_owner(block)
        branch_owner[:, owner * LANES : (owner + 1) * LANES] = values
    slot_grad[...] = jnp.zeros_like(slot_grad)
    own_grad[...] = jnp.zeros_like(own_grad)
    scatter.run("f1 c3")

    plan = {
        (0, 2): "s0 f2", (0, 3): "s1 f3", (0, 4): "t0 c4", (1, 1): "s2", (1, 2): "t1 f4", (1, 3): "s3 c6",
        (2, 0): "t2 c5", (2, 1): "s4 f5", (2, 2): "t3", (2, 3): "f6 c8", (2, 4): "t4 c7", (3, 1): "s5",
        (3, 2): "s6 f7", (3, 4): "t5 f8 c9",
    }

    def communicate(block, point):
        for (at_block, at_point), ops in plan.items():
            if at_point == point:

                @pl.when(block == at_block)
                def _(ops=ops):
                    scatter.run(ops)

    row_copies = [
        remote(
            rows_out.at[k - 1], peers.at[k - 1], row_send.at[k], row_recv.at[k],
            (place.dp, first_peer + lax.rem(member + k, group)),
        )
        for k in range(1, group)
    ]

    def block_unit(block, carry):
        communicate(block, 0)
        step = mp_size - 1 - block
        target = place.across(step)
        base = pl.multiple_of(target * inner_here, 16)
        here = pl.ds(base, inner_here)
        slot = lax.rem(block, 2)
        copies = [
            Copy(w_first.at[0, here, :], w_query, load_sem.at[0]),
            Copy(w_first.at[3, here, :], w_output, load_sem.at[1]),
            Copy(queries.at[here, :], q_here, load_sem.at[2]),
            Copy(keys_t.at[here, :], k_here, load_sem.at[3]),
            Copy(values_t.at[here, :], v_here, load_sem.at[4]),
            Copy(heads_out.at[here, :], out_here, load_sem.at[5]),
        ]
        for i in range(heads_here):
            for part in range(2):
                copies.append(
                    Copy(
                        w_first.at[1 + part, pl.ds(pl.multiple_of(base + i * 64, 16), 64), :],
                        w_kv.at[pl.ds(i * 128 + part * 64, 64), :],
                        load_sem.at[6 + 2 * i + part],
                    )
                )
        for copy in copies:
            copy.start()
        for copy in (copies[1], copies[5]):
            copy.wait()

        for b in range(2, mp_size):

            @pl.when(block == b)
            def _(b=b):
                scatter.left(items.index((2, mp_size + 1 - b)))

        grad_here[...] = jnp.dot(w_output[...], branch_t[...], preferred_element_type=F32).astype(BF16)
        full_here[slot, 3] = jnp.dot(
            out_here[...], branch_owner[...], preferred_element_type=F32
        ).astype(BF16)
        for copy in [copies[0]] + copies[2:5] + copies[6:]:
            copy.wait()

        def head_unit(inside, inner_carry):
            for point in range(1, heads_here):

                @pl.when(inside == point)
                def _(point=point):
                    communicate(block, point)

            head = target * heads_here + inside
            some = pl.ds(pl.multiple_of(inside * 64, 16), 64)
            q_head, k_head, v_head = q_here[some, :], k_here[some, :], v_here[some, :]
            grad_head = grad_here[some, :]
            both = jnp.concatenate([k_head, v_head], axis=0).T
            lanes = lane_ids((keys, LANES))
            key_aug[:, 0:LANES] = jnp.where(lanes < 64, both, key_extra[:, 0:LANES])
            ones = jnp.where(lanes < 3, 1.0, 0.0).astype(BF16)
            value_aug[...] = jnp.where(lanes < 64, ones, both)
            key_aug_t[pl.ds(0, 64), :] = k_head
            query_aug[pl.ds(0, 64), :] = q_head
            query_aug[pl.ds(64, 128), :] = jnp.dot(
                layout[head], key_extra_t[:, own_lanes], preferred_element_type=F32
            ).astype(BF16)
            high, middle, low = three_parts(-lse[head])
            tail = row_ids((64, rows))
            rows_of = lambda part: jnp.broadcast_to(part.astype(F32), (64, rows))
            query_aug[pl.ds(192, 64), :] = jnp.where(
                tail == 0, 1.0,
                jnp.where(
                    tail == 1, rows_of(high),
                    jnp.where(tail == 2, rows_of(middle), jnp.where(tail == 3, rows_of(low), 0.0)),
                ),
            ).astype(BF16)
            row_dot = jnp.sum(
                grad_head.astype(F32) * out_here[some, :].astype(F32), axis=0, keepdims=True
            )
            high, middle, low = three_parts(-row_dot)
            grad_aug[pl.ds(0, 64), :] = jnp.where(
                tail == 0, rows_of(high),
                jnp.where(tail == 1, rows_of(middle), jnp.where(tail == 2, rows_of(low), 0.0)),
            ).astype(BF16)
            grad_aug[pl.ds(64, 64), :] = grad_head
            width = strip.shape[1]
            strip[...] = pltpu.roll(
                jnp.broadcast_to(line[target, pl.ds(inside, 1), :], (LANES, width)), 0, 1,
                stride=1, stride_axis=0,
            )
            strip_grad[...] = jnp.zeros_like(strip_grad)
            query_and_grad = jnp.concatenate([q_head, grad_head], axis=0).T
            query_all = query_aug[...]
            grad_all = grad_aug[...]
            half = lane_ids((LANES, LANES)) < 64
            kv_lanes = pl.ds(pl.multiple_of(inside * LANES, LANES), LANES)
            for part_index in range(blocks):
                these = pl.ds(part_index * LANES, LANES)
                band = pl.ds((blocks - 1 - part_index) * LANES, rows)
                part = jnp.dot(key_aug[these, :], query_all, preferred_element_type=F32)
                part = jnp.exp(part + strip[:, band])
                slope = part * jnp.dot(value_aug[these, :], grad_all, preferred_element_type=F32)
                strip_grad[:, band] = strip_grad[:, band] + slope
                slope = slope.astype(BF16)
                probs_grad[these, :] = slope
                key_part = jnp.dot(slope, query_and_grad, preferred_element_type=F32)
                value_part = jnp.dot(part.astype(BF16), query_and_grad, preferred_element_type=F32)
                joined = jnp.where(half, key_part, value_part)
                kv_here[these, kv_lanes] = joined.astype(BF16)
                turned = joined.T.astype(BF16)
                dk_here[some, these] = turned[0:64]
                dv_here[some, these] = turned[64:128]
            query_part = jnp.dot(key_aug_t[...], probs_grad[...], preferred_element_type=F32)
            dq_here[some, :] = query_part[0:64].astype(BF16)
            bins = dot_f32(query_part[64:192].astype(BF16), key_extra_t[:, own_lanes], 1, 1)
            left = lane_ids((LANES, LANES)) < 64
            upper = row_ids((LANES, LANES)) < 64
            layout_grad[...] = jnp.where(left == upper, bins, 0.0)
            bin_sums[0, pl.ds(head, 1), :] = unskewed(layout_grad, 0, 64, 0)
            bin_sums[1, pl.ds(head, 1), :] = unskewed(layout_grad, 64, 64, 64)
            line_sums[pl.ds(head, 1), :] = unskewed(strip_grad, 0, LANES, 0)
            return inner_carry

        lax.fori_loop(0, heads_here, head_unit, 0)
        slot_grad[...] = slot_grad[...] + jnp.dot(
            kv_here[...], w_kv[...], preferred_element_type=F32
        )
        own_grad[...] = own_grad[...] + jnp.dot(
            dq_here[...].T, w_query[...], preferred_element_type=F32
        )

        @pl.when(block == mp_size - 1)
        def _():
            for k, copy in enumerate(row_copies):
                other = lax.rem(member + k + 1, group)
                rows_out[k] = slot_grad[pl.ds(pl.multiple_of(other * rows, 16), rows), :].astype(BF16)
                copy.start()

        full_here[slot, 0] = jnp.dot(
            dq_here[...], slot_owner[pl.ds(own_start, rows), :], preferred_element_type=F32
        ).astype(BF16)
        full_here[slot, 1] = jnp.dot(
            dk_here[...], slot_owner[...], preferred_element_type=F32
        ).astype(BF16)
        full_here[slot, 2] = jnp.dot(
            dv_here[...], slot_owner[...], preferred_element_type=F32
        ).astype(BF16)
        communicate(block, heads_here)
        return carry

    lax.fori_loop(0, mp_size, block_unit, 0)

    scatter.run("t6 f9")

    gain_rows = model_width // LANES
    head_count = bin_sums.shape[1]
    stage[0, 2 * gain_rows : 2 * gain_rows + head_count, :] = exact_dot(line_sums[...], line_hot[...])
    for i in range(2):
        start = 2 * gain_rows + (1 + i) * head_count
        stage[0, start : start + head_count, :] = exact_dot(bin_sums[i], bin_hot[...])
    for block in range(gain_rows):
        these = slice(block * LANES, (block + 1) * LANES)
        owner = block_owner(block)
        those = slice(owner * LANES, (owner + 1) * LANES)

        def gain_sum(i, total, these=these, those=those):
            here = pl.ds(pl.multiple_of(i * 64, 64), 64)
            product = slot_grad[here, these] * slot_owner[here, those].astype(F32)
            return total + jnp.sum(product.reshape(8, 8, LANES), axis=0)

        def own_sum(i, total, these=these, those=those):
            here = pl.ds(pl.multiple_of(i * 64, 64), 64)
            there = pl.ds(pl.multiple_of(own_start + i * 64, 64), 64)
            product = own_grad[here, these] * slot_owner[there, those].astype(F32)
            return total + jnp.sum(product.reshape(8, 8, LANES), axis=0)

        total = lax.fori_loop(0, keys // 64, gain_sum, jnp.zeros((8, LANES), F32))
        total = lax.fori_loop(0, rows // 64, own_sum, total)
        stage[0, block : block + 1, :] = (
            jnp.sum(total, axis=0, keepdims=True) / gains[0:1, these].astype(F32)
        )
        stage[0, gain_rows + block : gain_rows + block + 1, :] = gain_part[:, these]

    rounds = [[place.to_core], [place.to_x, place.to_y, place.to_corner]]
    rounds.append([place.to_mp(k) for k in range(1, mp_size)])
    at, sums = 0, []
    for i, partners in enumerate(rounds):
        sums.append(
            [
                remote(
                    stage.at[i], stage_in.at[at + j], stage_send.at[at + j], stage_recv.at[at + j], partner
                )
                for j, partner in enumerate(partners)
            ]
        )
        at += len(partners)
    def round_done(i):
        at = sum(len(partners) for partners in rounds[:i])
        value = stage[i]
        for j, copy in enumerate(sums[i]):
            copy.wait_recv()
            value = value + stage_in[at + j]
        return value

    for copy in sums[0]:
        copy.start()
    scatter.run("s7 s8 e0")
    stage[1] = round_done(0)
    for copy in sums[1]:
        copy.start()
    scatter.run("t7 s9")
    for copy in row_copies:
        copy.wait_recv()

    def input_back(i, carry):
        here = pl.ds(pl.multiple_of(i * 16, 16), 16)
        grad = own_grad[here, :] + slot_grad[pl.ds(pl.multiple_of(own_start + i * 16, 16), 16), :]
        for k in range(group - 1):
            grad = grad + peers[k, here, :].astype(F32)
        values = layer_input[here, :]
        scale = lax.rsqrt(jnp.mean(values * values, axis=1, keepdims=True) + EPSILON)
        scaled = gains[0:1, :].astype(F32) * grad
        mean = jnp.mean(scaled * values, axis=1, keepdims=True)
        input_grad[here, :] = (
            residual_grad[here, :] + scale * scaled - values * (scale * scale * scale * mean)
        )
        return carry

    lax.fori_loop(0, rows // 16, input_back, 0)
    leave = Copy(input_grad, input_out, value_sem.at[0])
    leave.start()
    stage[2] = round_done(1)
    for copy in sums[2]:
        copy.start()
    scatter.run("t8 t9")
    scatter.run("e1 e2")
    small_out[...] = round_done(2)
    sums = sum(sums, [])
    scatter.close()
    leave.wait()
    for copy in row_copies + sums:
        copy.wait_send()


def backward(
    mp_size, group, gate_up_full, down_full, w_first, queries, keys_t, values_t, heads_out,
    residual, second_grad, cotangent, lse, layout, line, key_extra, key_extra_t, slot_owner,
    layer_input, gains, line_hot, bin_hot, gate_up_share, down_share,
):
    rows, model_width = layer_input.shape
    keys = slot_owner.shape[0]
    width = line.shape[2]
    inner_here = queries.shape[0] // mp_size
    heads_here = inner_here // 64
    head_count = heads_here * mp_size
    hidden = down_full.shape[1] // mp_size
    sizes = [(2, hidden), (1, hidden), (4, inner_here)]
    count = 4 + mp_size - 1
    small_rows = 2 * model_width // LANES + 3 * head_count
    others = max(group - 1, 1)
    dma = pltpu.SemaphoreType.DMA
    hbm = pl.BlockSpec(memory_space=HBM)
    vmem = pl.BlockSpec(memory_space=pltpu.VMEM)
    shape = jax.ShapeDtypeStruct
    return pl.pallas_call(
        partial(backward_kernel, mp_size, group),
        out_shape=(
            shape((rows, model_width), F32),
            shape((small_rows, LANES), F32),
            *[shape((lead, n, LANES), F32) for lead, n in sizes],
        ),
        in_specs=[hbm] * 10 + [vmem] * 12,
        out_specs=(hbm,) + (vmem,) * 4,
        scratch_shapes=[
            pltpu.VMEM((rows, model_width), F32),
            pltpu.VMEM((keys, model_width), F32),
            pltpu.VMEM((rows, model_width), F32),
            pltpu.VMEM((rows, model_width), F32),
            pltpu.VMEM((rows, model_width), BF16),
            pltpu.VMEM((model_width, rows), BF16),
            pltpu.VMEM((inner_here, model_width), BF16),
            pltpu.VMEM((inner_here, model_width), BF16),
            pltpu.VMEM((2 * inner_here, model_width), BF16),
            pltpu.VMEM((inner_here, rows), BF16),
            pltpu.VMEM((inner_here, keys), BF16),
            pltpu.VMEM((inner_here, keys), BF16),
            pltpu.VMEM((inner_here, rows), BF16),
            pltpu.VMEM((inner_here, rows), BF16),
            pltpu.VMEM((inner_here, rows), BF16),
            pltpu.VMEM((inner_here, keys), BF16),
            pltpu.VMEM((inner_here, keys), BF16),
            pltpu.VMEM((keys, heads_here * LANES), BF16),
            pltpu.VMEM((keys, 256), BF16),
            pltpu.VMEM((192, keys), BF16),
            pltpu.VMEM((256, rows), BF16),
            pltpu.VMEM((keys, LANES), BF16),
            pltpu.VMEM((LANES, rows), BF16),
            pltpu.VMEM((LANES, width), F32),
            pltpu.VMEM((LANES, width), F32),
            pltpu.VMEM((keys, rows), BF16),
            pltpu.VMEM((LANES, LANES), F32),
            pltpu.VMEM((head_count, width), F32),
            pltpu.VMEM((2, head_count, LANES), F32),
            pltpu.VMEM((1, model_width), F32),
            pltpu.VMEM((others, rows, model_width), BF16),
            pltpu.VMEM((others, rows, model_width), BF16),
            pltpu.VMEM((3, small_rows, LANES), F32),
            pltpu.VMEM((count, small_rows, LANES), F32),
            pltpu.VMEM((2, 4, inner_here, model_width), BF16),
            dma((6 + 2 * heads_here,)), dma((3,)), dma((group,)), dma((group,)),
            dma((count,)), dma((count,)),
        ]
        + Scatter.scratch(sizes, (True, True, False), BACKWARD_ITEMS),
        compiler_params=pltpu.CompilerParams(
            collective_id=1, has_side_effects=True, vmem_limit_bytes=63 << 20
        ),
        name="backward",
    )(
        gate_up_full, down_full, w_first, queries, keys_t, values_t, heads_out, residual,
        second_grad, cotangent, lse, layout, line, key_extra, key_extra_t, slot_owner, layer_input,
        gains, line_hot, bin_hot, gate_up_share, down_share,
    )


def line_onehot(first_row, width, key_blocks):
    place = jnp.arange(width, dtype=jnp.int32)
    place = jnp.where(place >= width - LANES, place - width, place)
    offset = LANES * (key_blocks - 1) - place - first_row
    return (bucket_of(offset)[:, None] == jnp.arange(32, dtype=jnp.int32)[None, :]).astype(F32)


def bin_onehot():
    bins = np.arange(NBIN)
    offset = bins[:, None] - bins[None, :]
    distance = np.abs(offset)
    bucket = np.minimum(distance, 7) + sum((distance >= t).astype(np.int64) for t in THRESHOLDS)
    bucket = bucket + 16 * (offset > 0)
    return jnp.asarray(bucket[:, :, None] == np.arange(32), F32)


def gather_rows(local, axis_name):
    return lax.all_gather(local, axis_name, axis=0, tiled=True)


def scatter_grad(full):
    summed = lax.psum_scatter(full, "dp", scatter_dimension=1, tiled=True)
    return lax.psum_scatter(summed, "mp", scatter_dimension=0, tiled=True)


def per_device_plain(
    dp_size, mp_size,
    layer_input, norm_gains, query_weight, key_value_weight, output_weight,
    gate_up_weight, down_weight, bias_tables, doc_lengths, box_bins, cotangent,
):
    rows, model_width = layer_input.shape
    doc_count = doc_lengths.shape[0]
    slot_span = box_bins.shape[1] // doc_count
    group = mp_size // doc_count
    mp_index = lax.axis_index("mp")
    doc = mp_index // group
    first_row = (mp_index % group) * rows
    key_blocks = slot_span // LANES
    width = LANES * (key_blocks + (rows + LANES - 1) // LANES)
    groups = [[d * group + i for i in range(group)] for d in range(doc_count)]
    gain_first = norm_gains[0].astype(F32)
    gain_second = norm_gains[1].astype(F32)

    w_query = gather_rows(query_weight.T, "mp")
    inner_here = query_weight.shape[1]
    inner = inner_here * mp_size
    w_key = gather_rows(key_value_weight[:, 0].T, "mp")
    w_value = gather_rows(key_value_weight[:, 1].T, "mp")
    w_output = gather_rows(output_weight, "mp")
    w_gate = gather_rows(gate_up_weight[:, 0].T, "mp")
    w_up = gather_rows(gate_up_weight[:, 1].T, "mp")
    w_down = gather_rows(down_weight, "mp")
    tables = lax.all_gather(bias_tables, "mp", axis=2, tiled=True).astype(F32)
    head_count = tables.shape[2]

    onehot_line = line_onehot(first_row, width, key_blocks)
    line = jnp.dot(onehot_line, tables[0], precision=lax.Precision.HIGHEST)
    line = line.T.reshape(head_count, 1, width)
    onehot_bin = bin_onehot()
    x_part = jnp.einsum("ban,nh->hba", onehot_bin, tables[1], precision=lax.Precision.HIGHEST)
    y_part = jnp.einsum("ban,nh->hba", onehot_bin, tables[2], precision=lax.Precision.HIGHEST)
    empty = jnp.zeros_like(x_part)
    layout = jnp.concatenate(
        [jnp.concatenate([x_part, empty], axis=2), jnp.concatenate([empty, y_part], axis=2)], axis=1
    ).astype(BF16)
    key_bins = lax.dynamic_slice(box_bins, (0, doc * slot_span), (2, slot_span))
    own_bins = lax.dynamic_slice(key_bins, (0, first_row), (2, rows))
    bin_ids = jnp.arange(NBIN, dtype=jnp.int32)

    def placed_rows(bins):
        return jnp.concatenate(
            [bins[0][:, None] == bin_ids, bins[1][:, None] == bin_ids], axis=1
        ).astype(BF16)

    def placed_lanes(bins):
        return jnp.concatenate(
            [bin_ids[:, None] == bins[0][None], bin_ids[:, None] == bins[1][None]], axis=0
        ).astype(BF16)

    length = lax.dynamic_index_in_dim(doc_lengths, doc, keepdims=False)
    masked = jnp.arange(slot_span, dtype=jnp.int32)[:, None] >= length
    key_placed = placed_rows(key_bins)
    key_extra = jnp.concatenate(
        [
            jnp.zeros((slot_span, 64), BF16),
            key_placed,
            jnp.where(masked, NEG_FILL, 0.0).astype(BF16),
            jnp.ones((slot_span, 3), BF16),
            jnp.zeros((slot_span, 60), BF16),
        ],
        axis=1,
    )
    key_extra_t = placed_lanes(key_bins)
    query_bins_t = placed_rows(own_bins)
    query_bins = placed_lanes(own_bins)

    scale_first = inverse_rms(layer_input)
    normed = (layer_input * scale_first * gain_first).astype(BF16)
    slot_normed = lax.all_gather(normed, "mp", axis=0, tiled=True, axis_index_groups=groups)
    queries = dot_f32(w_query, normed, 1, 1).astype(BF16)
    keys_t = dot_f32(w_key, slot_normed, 1, 1).astype(BF16)
    values_t = dot_f32(w_value, slot_normed, 1, 1).astype(BF16)
    heads_out, lse = attend(queries, keys_t, values_t, layout, line, key_extra, query_bins)
    residual = layer_input + dot_f32(heads_out, w_output, 0, 0)
    scale_second = inverse_rms(residual)
    normed_second = (residual * scale_second * gain_second).astype(BF16)
    gate = dot_f32(normed_second, w_gate, 1, 1)
    up = dot_f32(normed_second, w_up, 1, 1)
    gelu_value, gelu_pull = jax.vjp(lambda v: jax.nn.gelu(v, approximate=True), gate)
    activated = (gelu_value * up).astype(BF16)
    layer_output = residual + dot_f32(activated, w_down, 1, 0)

    out_low = cotangent.astype(BF16)
    down_full = dot_f32(activated, out_low, 0, 0).astype(BF16)
    act_grad = dot_f32(out_low, w_down, 1, 1)
    gate_low = gelu_pull(act_grad * up)[0].astype(BF16)
    up_low = (act_grad * gelu_value).astype(BF16)
    gate_full = dot_f32(gate_low, normed_second, 0, 0).astype(BF16)
    up_full = dot_f32(up_low, normed_second, 0, 0).astype(BF16)
    second_grad = dot_f32(gate_low, w_gate, 1, 0) + dot_f32(up_low, w_up, 1, 0)
    gain_second_grad = jnp.sum(second_grad * residual * scale_second, axis=0)
    scaled = gain_second * second_grad
    residual_grad = (
        cotangent
        + scale_second * scaled
        - residual * scale_second**3 * jnp.mean(scaled * residual, axis=-1, keepdims=True)
    )

    branch_low = residual_grad.astype(BF16)
    output_full = dot_f32(heads_out, branch_low, 1, 0).astype(BF16)
    heads_grad = dot_f32(w_output, branch_low, 1, 1).astype(BF16)
    dq, dk, dv, line_grad, layout_grad = attend_back(
        queries, keys_t, values_t, heads_out, heads_grad, lse, layout, line,
        key_extra, key_extra_t, query_bins, query_bins_t,
    )
    query_full = dot_f32(dq, normed, 1, 0).astype(BF16)
    key_full = dot_f32(dk, slot_normed, 1, 0).astype(BF16)
    value_full = dot_f32(dv, slot_normed, 1, 0).astype(BF16)
    slot_grad = dot_f32(dk, w_key, 0, 0) + dot_f32(dv, w_value, 0, 0)
    first_grad = lax.psum_scatter(
        slot_grad.astype(BF16), "mp", scatter_dimension=0, tiled=True, axis_index_groups=groups
    ).astype(F32) + dot_f32(dq, w_query, 0, 0)
    gain_first_grad = jnp.sum(first_grad * layer_input * scale_first, axis=0)
    scaled = gain_first * first_grad
    input_grad = (
        residual_grad
        + scale_first * scaled
        - layer_input * scale_first**3 * jnp.mean(scaled * layer_input, axis=-1, keepdims=True)
    )

    gain_grad = lax.psum_scatter(
        jnp.stack([gain_first_grad, gain_second_grad]), ("dp", "mp"), scatter_dimension=1, tiled=True
    )
    line_part = jnp.dot(
        onehot_line.T, line_grad[:, 0].T, precision=lax.Precision.HIGHEST
    )
    x_part = jnp.einsum(
        "ban,hba->nh", onehot_bin, layout_grad[:, :64, :64], precision=lax.Precision.HIGHEST
    )
    y_part = jnp.einsum(
        "ban,hba->nh", onehot_bin, layout_grad[:, 64:, 64:], precision=lax.Precision.HIGHEST
    )
    table_full = jnp.stack([line_part, x_part, y_part])
    table_grad = lax.psum_scatter(
        lax.psum_scatter(table_full, "mp", scatter_dimension=2, tiled=True),
        "dp", scatter_dimension=1, tiled=True,
    )

    query_grad = scatter_grad(query_full).T.astype(F32)
    key_value_grad = jnp.stack(
        [scatter_grad(key_full).T, scatter_grad(value_full).T], axis=1
    ).astype(F32)
    output_grad = scatter_grad(output_full).astype(F32)
    gate_up_grad = jnp.stack(
        [scatter_grad(gate_full).T, scatter_grad(up_full).T], axis=1
    ).astype(F32)
    down_grad = scatter_grad(down_full).astype(F32)
    return (
        layer_output, input_grad, gain_grad, query_grad, key_value_grad,
        output_grad, gate_up_grad, down_grad, table_grad,
    )


def per_device_linked(
    dp_size, mp_size,
    layer_input, norm_gains, query_weight, key_value_weight, output_weight,
    gate_up_weight, down_weight, bias_tables, doc_lengths, box_bins, cotangent,
):
    rows, model_width = layer_input.shape
    doc_count = doc_lengths.shape[0]
    group = mp_size // doc_count
    dp_index, mp_index = lax.axis_index("dp"), lax.axis_index("mp")
    heads_here = bias_tables.shape[2]
    head_count = heads_here * mp_size
    inner_here = query_weight.shape[1]
    column = ((dp_index % 2) * 4 + dp_index // 2) * LANES
    key_value = lax.dynamic_slice_in_dim(key_value_weight, column, LANES, 0)
    table = jnp.swapaxes(bias_tables.astype(F32), 1, 2)
    table = jnp.pad(table, ((0, 0), (0, 8 - heads_here), (0, LANES - 32))).reshape(24, LANES)
    (
        w_first, queries, keys_t, values_t, heads_out, lse, layout, line, key_extra, key_extra_t,
        slot_owner, residual, layer_output, second_grad, gate_up_full, down_full, _, line_hot, bin_hot,
        gate_up_share, down_share,
    ) = forward(
        mp_size, group, query_weight, output_weight, jnp.transpose(gate_up_weight, (1, 2, 0)),
        down_weight[None], key_value.reshape(LANES, 2 * inner_here), table, box_bins, doc_lengths,
        layer_input, norm_gains, cotangent,
    )
    input_grad, small, gate_up_sum, down_sum, summed = backward(
        mp_size, group, gate_up_full, down_full, w_first, queries, keys_t, values_t, heads_out,
        residual, second_grad, cotangent, lse, layout, line, key_extra, key_extra_t, slot_owner,
        layer_input, norm_gains, line_hot, bin_hot, gate_up_share, down_share,
    )
    gain_rows = model_width // LANES
    gains = small[: 2 * gain_rows].reshape(2, model_width)
    share = model_width // (dp_size * mp_size)
    at = (dp_index * mp_size + mp_index) * share
    gain_grad = lax.dynamic_slice(gains, (0, at), (2, share))
    tables = small[2 * gain_rows :].reshape(3, head_count, LANES)
    table_grad = lax.dynamic_slice(
        tables,
        (0, mp_index * heads_here, dp_index * (32 // dp_size)),
        (3, heads_here, 32 // dp_size),
    )
    table_grad = jnp.swapaxes(table_grad, 1, 2)
    query_grad = summed[0].T
    key_value_grad = jnp.transpose(summed[1:3], (2, 0, 1))
    gate_up_grad = jnp.transpose(gate_up_sum, (2, 0, 1))
    return (
        layer_output, input_grad, gain_grad, query_grad, key_value_grad,
        summed[3], gate_up_grad, down_sum[0], table_grad,
    )


def per_device(dp_size, mp_size, *args):
    rows, model_width = args[0].shape
    heads_here = args[7].shape[2]
    fits = dp_size == 8 and model_width == 8 * LANES and mp_size == 4
    fits = fits and heads_here == 4 and rows % LANES == 0
    body = per_device_linked if fits else per_device_plain
    return body(dp_size, mp_size, *args)


def solution(mesh):
    return jax.shard_map(
        partial(per_device, mesh.shape["dp"], mesh.shape["mp"]),
        mesh=mesh,
        in_specs=(
            P(("dp", "mp"), None),
            P(),
            P(None, "mp"),
            P(None, None, "mp"),
            P("mp", None),
            P(None, None, "mp"),
            P("mp", None),
            P(None, None, "mp"),
            P("dp"),
            P(None, "dp"),
            P(("dp", "mp"), None),
        ),
        out_specs=(
            P(("dp", "mp"), None),
            P(("dp", "mp"), None),
            P(None, ("dp", "mp")),
            P("dp", "mp"),
            P("dp", None, "mp"),
            P("mp", "dp"),
            P("dp", None, "mp"),
            P("mp", "dp"),
            P(None, "dp", "mp"),
        ),
        check_vma=False,
    )
```
